32 devices in a mesh: ctx: 8 (over z, y), wshard: 4 (over x, core).
Axes of the slice: x: 2, y: 2, z: 4, core: 2. Of those that a mesh axis runs over, the one named last changes fastest.
Arguments:
- hidden: bfloat16 [2, 4, 2048, 768], P(None, 'wshard', 'ctx'), may hold values from -6 to 6
- out_grad: bfloat16 [2, 4, 2048, 768], P(None, 'wshard', 'ctx'), may hold values from -6 to 6
- doc_lengths: int32 [2, 4, 8], P(None, 'wshard'), may hold values from 1 to 24, 32 in all within a row
- rand_pick: int32 [2, 4, 32, 3], P(None, 'wshard', 'ctx'), may hold values from 0 to 65535
- w_query: bfloat16 [768, 768], P('wshard'), may hold values from -0.3125 to 0.3125
- w_key: bfloat16 [768, 768], P('wshard'), may hold values from -0.3125 to 0.3125
- w_value: bfloat16 [768, 768], P('wshard'), may hold values from -0.21875 to 0.21875
- w_out: bfloat16 [768, 768], P('wshard'), may hold values from -0.875 to 0.875
- w_up: bfloat16 [768, 3072], P('wshard'), may hold values from -0.21875 to 0.21875
- w_down: bfloat16 [3072, 768], P('wshard'), may hold values from -0.109375 to 0.109375
- b_query: bfloat16 [768], P('wshard'), may hold values from -3 to 3
- b_value: bfloat16 [768], P('wshard'), may hold values from -3 to 3
- b_out: bfloat16 [768], P('wshard'), may hold values from -3 to 3
- b_up: bfloat16 [3072], P('wshard'), may hold values from -3 to 3
- b_down: bfloat16 [768], P('wshard'), may hold values from -3 to 3
- ln1_gain: bfloat16 [768], P('wshard'), may hold values from 0.099609375 to 1.8984375
- ln1_shift: bfloat16 [768], P('wshard'), may hold values from -2 to 2
- ln2_gain: bfloat16 [768], P('wshard'), may hold values from 0.099609375 to 1.8984375
- ln2_shift: bfloat16 [768], P('wshard'), may hold values from -2 to 2
Outputs:
- block_out: bfloat16 [2, 4, 2048, 768], P(None, 'wshard', 'ctx')
- grad_hidden: float32 [2, 4, 2048, 768], P(None, 'wshard', 'ctx')
- grad_w_query: float32 [768, 768], P('wshard')
- grad_w_key: float32 [768, 768], P('wshard')
- grad_w_value: float32 [768, 768], P('wshard')
- grad_w_out: float32 [768, 768], P('wshard')
- grad_w_up: float32 [768, 3072], P('wshard')
- grad_w_down: float32 [3072, 768], P('wshard')
- grad_b_query: float32 [768], P('wshard')
- grad_b_value: float32 [768], P('wshard')
- grad_b_out: float32 [768], P('wshard')
- grad_b_up: float32 [3072], P('wshard')
- grad_b_down: float32 [768], P('wshard')
- grad_ln1_gain: float32 [768], P('wshard')
- grad_ln1_shift: float32 [768], P('wshard')
- grad_ln2_gain: float32 [768], P('wshard')
- grad_ln2_shift: float32 [768], P('wshard')
The draws below stay inside these ranges and needn't reach their ends.
Inputs may be any that keep to these rules, and one draw needn't show every extreme that they name: `doc_lengths`: each stream's lengths sum to 32.
All inputs are finite; a program needn't handle non-finite values.
Results may differ from the reference program's by a relative error of at most 0.02.
Values may be sent and summed in bfloat16 or wider, within the bound.
A program may use at most 256 MiB of HBM per device.

```python
import math
import jax
import jax.numpy as jnp
import numpy as np
from jax import lax

D = 768
HEADS = 12
HEAD_DIM = 64
FF = 3072
BLOCK = 64
RAND = 3
MICRO = 2
TOK_DEV = 256
STREAM_TOK = 2048
STREAM_BLK = 32
DOC_BLK = 24
DOCS = 8
STREAMS = 4


def set_ends(entries, stream_key, least, largest):
    longest = entries.shape.index(max(entries.shape))
    spots = []
    for shift in (0, 1):
        where = [jax.random.randint(jax.random.fold_in(stream_key, axis), (), 0, length) for axis, length in enumerate(entries.shape)]
        where[longest] = (where[longest] + shift) % entries.shape[longest]
        spots.append(tuple(where))
    return entries.at[spots[0]].set(least).at[spots[1]].set(largest)


def steps_of(key, shape, cuts, smallest, largest):
    def one(axis_at, blocks):
        steps = jax.random.uniform(jax.random.fold_in(jax.random.fold_in(key, 6), axis_at), (blocks,), jnp.float32, smallest / len(cuts), largest / len(cuts))
        return jnp.repeat(jnp.exp(steps), shape[axis_at] // blocks).reshape((-1,) + (1,) * (len(shape) - axis_at - 1))

    loudness = one(*cuts[0])
    for cut in cuts[1:]:
        loudness = loudness * one(*cut)
    return loudness


def length_profile(amount, total, limit, skew):
    portions = [(1 << 20) // math.isqrt(rank ** skew) + 1 for rank in range(2, amount + 1)]
    spare, given = total - limit - (amount - 1), [1] * (amount - 1)
    while spare > 0:
        free = [i for i in range(amount - 1) if given[i] < limit]
        whole, left = sum([portions[i] for i in free]), spare
        for i in free:
            extra = min(limit - given[i], max(1, left * portions[i] // whole), spare)
            given[i] = given[i] + extra
            spare = spare - extra
    return np.array([limit] + given)


def ragged(key, number_of, total, most, lean):
    if number_of == 2:
        one = jax.random.randint(key, (), max(1, total - most), min(most, total - 1) + 1)
        return jnp.stack([one, total - one])
    sizes = jnp.asarray(length_profile(number_of, total, most, lean), jnp.int32)
    couples = (number_of - 1) // 2
    source_of, receiver = sizes[1:1 + 2 * couples:2], sizes[2:2 + 2 * couples:2]
    room = jnp.minimum(source_of - 1, most - receiver)
    passed = jax.random.randint(jax.random.fold_in(key, 1), (couples,), 0, 1 << 20) % (room + 1)
    sizes = sizes.at[1:1 + 2 * couples:2].set(source_of - passed).at[2:2 + 2 * couples:2].set(receiver + passed)
    return sizes[jax.random.permutation(jax.random.fold_in(key, 2), number_of)]


def normal_values(key, shape, deviation, most, shards=(), held_as=jnp.bfloat16):
    gain = steps_of(key, shape, shards, -0.22, 0.18) if shards else 1.0
    entries = jax.random.normal(key, shape, jnp.float32) * deviation * gain
    return jnp.minimum(jnp.maximum(entries, -most), most).astype(held_as)


def setup_inputs(seed: int = 0) -> dict:
    key_list = jax.random.split(jax.random.key(seed), 20)
    return {
        "hidden": normal_values(key_list[0], (MICRO, STREAMS, STREAM_TOK, D), 1.0, 6.0, ((1, 4), (2, 8))),
        "out_grad": normal_values(key_list[1], (MICRO, STREAMS, STREAM_TOK, D), 1.0, 6.0, ((1, 4), (2, 8))),
        "doc_lengths": jax.vmap(lambda own: ragged(own, DOCS, STREAM_BLK, DOC_BLK, 2))(jax.random.split(key_list[2], MICRO * STREAMS)).reshape((MICRO, STREAMS, DOCS)).astype(jnp.int32),
        "rand_pick": set_ends(jax.random.randint(key_list[3], (MICRO, STREAMS, STREAM_BLK, RAND), 0, 65536), jax.random.fold_in(key_list[3], 1), 0, 65535).astype(jnp.int32),
        "w_query": normal_values(key_list[4], (D, D), (D // 2) ** -0.5, 0.3125, ((0, 4),)),
        "w_key": normal_values(key_list[5], (D, D), (D // 2) ** -0.5, 0.3125, ((0, 4),)),
        "w_value": normal_values(key_list[6], (D, D), D ** -0.5, 0.21875, ((0, 4),)),
        "w_out": normal_values(key_list[7], (D, D), (D // 16) ** -0.5, 0.875, ((0, 4),)),
        "w_up": normal_values(key_list[8], (D, FF), D ** -0.5, 0.21875, ((0, 4),)),
        "w_down": normal_values(key_list[9], (FF, D), FF ** -0.5, 0.109375, ((0, 4),)),
        "b_query": normal_values(key_list[10], (D,), 0.5, 3.0, ((0, 4),)),
        "b_value": normal_values(key_list[11], (D,), 0.5, 3.0, ((0, 4),)),
        "b_out": normal_values(key_list[12], (D,), 0.5, 3.0, ((0, 4),)),
        "b_up": normal_values(key_list[13], (FF,), 0.5, 3.0, ((0, 4),)),
        "b_down": normal_values(key_list[14], (D,), 0.5, 3.0, ((0, 4),)),
        "ln1_gain": jnp.clip(1.0 + 0.18 * jax.random.normal(key_list[15], (D,), jnp.float32), 0.099609375, 1.8984375).astype(jnp.bfloat16),
        "ln1_shift": normal_values(key_list[16], (D,), 0.3, 2.0, ((0, 4),)),
        "ln2_gain": jnp.clip(1.0 + 0.18 * jax.random.normal(key_list[17], (D,), jnp.float32), 0.099609375, 1.8984375).astype(jnp.bfloat16),
        "ln2_shift": normal_values(key_list[18], (D,), 0.3, 2.0, ((0, 4),)),
    }


@jax.custom_vjp
def low(v):
    return lax.optimization_barrier(v.astype(jnp.bfloat16)).astype(jnp.float32)

@jax.custom_vjp
def low_back(v):
    return v

def low_keep(v):
    return (low(v), None)

def low_pass(kept, grad):
    return (grad,)

def back_keep(v):
    return (v, None)

def back_low(kept, grad):
    return (low(grad),)
low.defvjp(low_keep, low_pass)
low_back.defvjp(back_keep, back_low)
masked_score = -1e+30
norm_eps = 1e-12

def matmul(left, right):
    return jnp.dot(left, right, precision=lax.Precision.HIGHEST, preferred_element_type=jnp.float32)

def layer_norm(values, ln_gain, ln_shift):
    center = values - lax.optimization_barrier(jnp.mean(values, axis=-1, keepdims=True))
    spread = lax.optimization_barrier(jnp.mean(center * center, axis=-1, keepdims=True))
    return center * lax.rsqrt(spread + norm_eps) * ln_gain + ln_shift

def candidates(blocks, lengths, chosen_raw):
    doc_ends = jnp.cumsum(lengths).astype(jnp.int32)
    doc_starts = (doc_ends - lengths).astype(jnp.int32)
    owner_doc = lax.optimization_barrier(jnp.sum((blocks[:, None] >= doc_ends[None, :]).astype(jnp.int32), axis=1)).astype(jnp.int32)
    doc_ids = jnp.arange(lengths.shape[0], dtype=jnp.int32)
    member = (owner_doc[:, None] == doc_ids[None, :]).astype(jnp.int32)
    doc_first = lax.optimization_barrier(jnp.sum(member * doc_starts[None, :], axis=1)).astype(jnp.int32)
    length = lax.optimization_barrier(jnp.sum(member * lengths[None, :], axis=1)).astype(jnp.int32)
    randoms = (doc_first[:, None] + chosen_raw % length[:, None]).astype(jnp.int32)
    columns = [blocks, blocks - 1, blocks + 1, doc_first, doc_first + 1]
    for column in range(chosen_raw.shape[1]):
        columns.append(randoms[:, column])
    chosen = jnp.stack(columns, axis=1).astype(jnp.int32)
    inside = (chosen >= doc_first[:, None]) & (chosen < (doc_first + length)[:, None])
    is_fresh = [jnp.ones(blocks.shape, dtype=jnp.bool_)]
    for column in range(1, chosen.shape[1]):
        is_fresh.append(jnp.all(chosen[:, :column] != chosen[:, column:column + 1], axis=1))
    allowed = inside & jnp.stack(is_fresh, axis=1)
    safe_blocks = jnp.where(allowed, chosen, blocks[:, None]).astype(jnp.int32)
    return (safe_blocks, allowed)

def attend(query_rows, key_all, value_all, safe_blocks, allowed):
    group_size = safe_blocks.shape[0]
    model_width = key_all.shape[1]
    key_blocks = key_all.reshape(-1, BLOCK, model_width)[safe_blocks].reshape(group_size, -1, HEADS, HEAD_DIM)
    value_blocks = value_all.reshape(-1, BLOCK, model_width)[safe_blocks].reshape(group_size, -1, HEADS, HEAD_DIM)
    query_heads = query_rows.reshape(group_size, BLOCK, HEADS, HEAD_DIM)
    scores = jnp.einsum('abhd,akhd->ahbk', query_heads, key_blocks, precision=lax.Precision.HIGHEST)
    scores = low_back(scores)
    key_mask = jnp.repeat(allowed, BLOCK, axis=1)
    scores = jnp.where(key_mask[:, None, None, :], scores, masked_score)
    attn_probs = jax.nn.softmax(scores, axis=-1)
    mixture = jnp.einsum('ahbk,akhd->abhd', low(attn_probs), value_blocks, precision=lax.Precision.HIGHEST)
    return mixture.reshape(group_size * BLOCK, model_width)

def stream_forward(hidden_row, params, safe_blocks, allowed):
    w_query, w_key, w_value, w_out, w_up, w_down, b_query, b_value, b_out, b_up, b_down, ln1_gain, ln1_shift, ln2_gain, ln2_shift = params
    score_scale = HEAD_DIM ** (-0.5)
    queries = low_back(low((matmul(hidden_row, w_query) + b_query) * score_scale))
    key_rows = low_back(low(matmul(hidden_row, w_key)))
    value_rows = low_back(low(matmul(hidden_row, w_value) + b_value))
    group_blocks = TOK_DEV // BLOCK
    groups = STREAM_BLK // group_blocks

    def one_group(pieces):
        return attend(pieces[0], key_rows, value_rows, pieces[1], pieces[2])
    context = lax.map(jax.checkpoint(one_group), (queries.reshape(groups, group_blocks * BLOCK, D), safe_blocks.reshape(groups, group_blocks, -1), allowed.reshape(groups, group_blocks, -1)))
    context = low_back(low(context.reshape(STREAM_TOK, D)))
    attn_out = low_back(matmul(context, w_out) + b_out)
    normed = layer_norm(hidden_row + attn_out, ln1_gain, ln1_shift)
    up_pre = low_back(matmul(low(normed), w_up) + b_up)
    activated = low(jax.nn.gelu(up_pre, approximate=True))
    branch = low_back(matmul(activated, w_down) + b_down)
    return layer_norm(normed + branch, ln2_gain, ln2_shift)

def reference(hidden, out_grad, doc_lengths, rand_pick, w_query, w_key, w_value, w_out, w_up, w_down, b_query, b_value, b_out, b_up, b_down, ln1_gain, ln1_shift, ln2_gain, ln2_shift):
    params = tuple((weight.astype(jnp.float32) for weight in (w_query, w_key, w_value, w_out, w_up, w_down, b_query, b_value, b_out, b_up, b_down, ln1_gain, ln1_shift, ln2_gain, ln2_shift)))
    streams = MICRO * STREAMS
    flat_hidden = hidden.reshape(streams, STREAM_TOK, D)
    flat_grad = out_grad.reshape(streams, STREAM_TOK, D)
    flat_lengths = doc_lengths.reshape(streams, DOCS)
    flat_pick = rand_pick.reshape(streams, STREAM_BLK, RAND)
    blocks = jnp.arange(STREAM_BLK, dtype=jnp.int32)

    def one_stream(totals, pieces):
        row_in, row_grad, lengths, chosen_raw = pieces
        safe_blocks, allowed = candidates(blocks, lengths, chosen_raw)

        def forward(inputs, weights):
            return stream_forward(inputs, weights, safe_blocks, allowed)
        output, pullback = jax.vjp(forward, row_in.astype(jnp.float32), params)
        grad_in, grad_params = pullback(row_grad.astype(jnp.float32))
        totals = tuple((total + term for total, term in zip(totals, grad_params)))
        return (totals, (output.astype(jnp.bfloat16), grad_in))
    initial = tuple((jnp.zeros_like(weight) for weight in params))
    totals, results = lax.scan(one_stream, initial, (flat_hidden, flat_grad, flat_lengths, flat_pick))
    block_out = results[0].reshape(hidden.shape)
    grad_hidden = results[1].reshape(hidden.shape)
    return (block_out, grad_hidden, totals[0], totals[1], totals[2], totals[3], totals[4], totals[5], totals[6], totals[7], totals[8], totals[9], totals[10], totals[11], totals[12], totals[13], totals[14])
```

```python
import functools
import math

import jax
import jax.numpy as jnp
from jax import lax
from jax.experimental import pallas as pl
from jax.experimental.pallas import tpu as pltpu
from jax.sharding import PartitionSpec as P

HEADS = 12
HEAD_DIM = 64
BLOCK = 64
MICRO = 2
GROUP = 4
LANES = GROUP * HEAD_DIM
CANDS = 8

masked_score = -1e30
norm_eps = 1e-12
score_scale = 1.0 / math.sqrt(HEAD_DIM)
bf16 = jnp.bfloat16
f32 = jnp.float32
MESH = pl.DeviceIdType.MESH


def layer_norm(values, ln_gain, ln_shift):
    center = values - jnp.mean(values, axis=-1, keepdims=True)
    spread = jnp.mean(center * center, axis=-1, keepdims=True)
    return center * lax.rsqrt(spread + norm_eps) * ln_gain + ln_shift


def candidates(blocks, lengths, chosen_raw):
    doc_ends = jnp.cumsum(lengths)
    doc_starts = doc_ends - lengths
    owner_doc = jnp.sum((blocks[:, None] >= doc_ends[None, :]).astype(jnp.int32), axis=1)
    doc_ids = jnp.arange(lengths.shape[0], dtype=jnp.int32)
    member = (owner_doc[:, None] == doc_ids[None, :]).astype(jnp.int32)
    doc_first = jnp.sum(member * doc_starts[None, :], axis=1)
    length = jnp.sum(member * lengths[None, :], axis=1)
    randoms = doc_first[:, None] + chosen_raw % length[:, None]
    columns = [blocks, blocks - 1, blocks + 1, doc_first, doc_first + 1]
    for column in range(chosen_raw.shape[1]):
        columns.append(randoms[:, column])
    chosen = jnp.stack(columns, axis=1)
    inside = (chosen >= doc_first[:, None]) & (chosen < (doc_first + length)[:, None])
    is_fresh = [jnp.ones(blocks.shape, dtype=jnp.bool_)]
    for column in range(1, chosen.shape[1]):
        is_fresh.append(jnp.all(chosen[:, :column] != chosen[:, column : column + 1], axis=1))
    allowed = inside & jnp.stack(is_fresh, axis=1)
    safe_blocks = jnp.where(allowed, chosen, blocks[:, None])
    return (safe_blocks, allowed)


def dot_nt(a, b):
    return lax.dot_general(a, b, (((1,), (1,)), ((), ())), preferred_element_type=f32)


def dot_nn(a, b):
    return lax.dot_general(a, b, (((1,), (0,)), ((), ())), preferred_element_type=f32)


def dot_tn(a, b):
    return lax.dot_general(a, b, (((0,), (0,)), ((), ())), preferred_element_type=f32)


def spread_heads(rows, head_of_lane):
    zero = jnp.zeros_like(rows)
    return jnp.concatenate([jnp.where(head_of_lane == h, rows, zero) for h in range(GROUP)], axis=0)


def pick_heads(rows, head_of_lane):
    total = jnp.zeros((BLOCK, LANES), f32)
    for h in range(GROUP):
        total = jnp.where(head_of_lane == h, rows[h * BLOCK : (h + 1) * BLOCK], total)
    return total


def attend_kernel(groups, width, pos_ref, q_ref, bias_ref, kv_ref, ctx_ref, probs_ref, cat):
    i = pl.program_id(0)
    for j in range(CANDS):
        start = pl.multiple_of(pos_ref[i * CANDS + j] * BLOCK, BLOCK)
        cat[j * BLOCK : (j + 1) * BLOCK, :] = kv_ref[pl.ds(start, BLOCK), :]
    head_of_lane = lax.broadcasted_iota(jnp.int32, (BLOCK, LANES), 1) // HEAD_DIM
    bias = bias_ref[0]
    for g in range(groups):
        lanes = slice(g * LANES, (g + 1) * LANES)
        v_lanes = slice(width + g * LANES, width + (g + 1) * LANES)
        q_all = spread_heads(q_ref[:, lanes], head_of_lane)
        scores = dot_nt(q_all, cat[:, lanes]) + bias
        row_max = jnp.max(scores, axis=-1, keepdims=True)
        shifted = jnp.exp(scores - row_max)
        row_total = jnp.sum(shifted, axis=-1, keepdims=True)
        probs = (shifted * (1.0 / row_total)).astype(bf16)
        probs_ref[0, g] = probs
        mixed = dot_nn(probs, cat[:, v_lanes])
        ctx_ref[:, lanes] = pick_heads(mixed, head_of_lane).astype(bf16)


def attend(pos, queries, bias, kv):
    rows, width = queries.shape
    blocks = rows // BLOCK
    groups = width // LANES
    keys = CANDS * BLOCK
    return pl.pallas_call(
        functools.partial(attend_kernel, groups, width),
        grid_spec=pltpu.PrefetchScalarGridSpec(
            num_scalar_prefetch=1,
            grid=(blocks,),
            in_specs=[
                pl.BlockSpec((BLOCK, width), lambda i, p: (i, 0)),
                pl.BlockSpec((1, 1, keys), lambda i, p: (i, 0, 0)),
                pl.BlockSpec(kv.shape, lambda i, p: (0, 0), pipeline_mode=pl.Buffered(1)),
            ],
            out_specs=[
                pl.BlockSpec((BLOCK, width), lambda i, p: (i, 0)),
                pl.BlockSpec((1, groups, GROUP * BLOCK, keys), lambda i, p: (i, 0, 0, 0)),
            ],
            scratch_shapes=[pltpu.VMEM((keys, 2 * width), bf16)],
        ),
        out_shape=[
            jax.ShapeDtypeStruct((rows, width), bf16),
            jax.ShapeDtypeStruct((blocks, groups, GROUP * BLOCK, keys), bf16),
        ],
        compiler_params=pltpu.CompilerParams(vmem_limit_bytes=48 << 20),
        cost_estimate=pl.CostEstimate(
            flops=blocks * groups * 4 * GROUP * BLOCK * keys * LANES,
            bytes_accessed=kv.size * 2 + rows * width * 4 + blocks * groups * GROUP * BLOCK * keys * 2,
            transcendentals=blocks * groups * GROUP * BLOCK * keys,
        ),
        name="attend",
    )(pos, queries, bias, kv)


def attend_back_kernel(
    groups, width, pos_ref, q_ref, dctx_ref, probs_ref, kv_ref, dq_ref, dkv_ref, cat, acc
):
    i = pl.program_id(0)

    @pl.when(i == 0)
    def _():
        acc[...] = jnp.zeros_like(acc)

    for j in range(CANDS):
        start = pl.multiple_of(pos_ref[i * CANDS + j] * BLOCK, BLOCK)
        cat[j * BLOCK : (j + 1) * BLOCK, :] = kv_ref[pl.ds(start, BLOCK), :]
    head_of_lane = lax.broadcasted_iota(jnp.int32, (BLOCK, LANES), 1) // HEAD_DIM
    for g in range(groups):
        lanes = slice(g * LANES, (g + 1) * LANES)
        v_lanes = slice(width + g * LANES, width + (g + 1) * LANES)
        q_all = spread_heads(q_ref[:, lanes], head_of_lane)
        d_all = spread_heads(dctx_ref[:, lanes], head_of_lane)
        probs_low = probs_ref[0, g]
        probs = probs_low.astype(f32)
        d_probs = dot_nt(d_all, cat[:, v_lanes])
        row_inner = jnp.sum(probs * d_probs, axis=-1, keepdims=True)
        d_scores = (probs * (d_probs - row_inner)).astype(bf16)
        dq_ref[:, lanes] = pick_heads(dot_nn(d_scores, cat[:, lanes]), head_of_lane).astype(bf16)
        d_key = dot_tn(d_scores, q_all)
        d_value = dot_tn(probs_low, d_all)
        for j in range(CANDS):
            start = pl.multiple_of(pos_ref[i * CANDS + j] * BLOCK, BLOCK)
            part = slice(j * BLOCK, (j + 1) * BLOCK)
            acc[pl.ds(start, BLOCK), lanes] += d_key[part]
            acc[pl.ds(start, BLOCK), v_lanes] += d_value[part]

    @pl.when(i == pl.num_programs(0) - 1)
    def _():
        dkv_ref[...] = acc[...].astype(bf16)


def attend_back(pos, queries, d_context, probs, kv):
    rows, width = queries.shape
    blocks = rows // BLOCK
    groups = width // LANES
    keys = CANDS * BLOCK
    return pl.pallas_call(
        functools.partial(attend_back_kernel, groups, width),
        grid_spec=pltpu.PrefetchScalarGridSpec(
            num_scalar_prefetch=1,
            grid=(blocks,),
            in_specs=[
                pl.BlockSpec((BLOCK, width), lambda i, p: (i, 0)),
                pl.BlockSpec((BLOCK, width), lambda i, p: (i, 0)),
                pl.BlockSpec((1, groups, GROUP * BLOCK, keys), lambda i, p: (i, 0, 0, 0)),
                pl.BlockSpec(kv.shape, lambda i, p: (0, 0), pipeline_mode=pl.Buffered(1)),
            ],
            out_specs=[
                pl.BlockSpec((BLOCK, width), lambda i, p: (i, 0)),
                pl.BlockSpec(kv.shape, lambda i, p: (0, 0), pipeline_mode=pl.Buffered(1)),
            ],
            scratch_shapes=[pltpu.VMEM((keys, 2 * width), bf16), pltpu.VMEM(kv.shape, f32)],
        ),
        out_shape=[
            jax.ShapeDtypeStruct((rows, width), bf16),
            jax.ShapeDtypeStruct(kv.shape, bf16),
        ],
        compiler_params=pltpu.CompilerParams(vmem_limit_bytes=60 << 20),
        cost_estimate=pl.CostEstimate(
            flops=blocks * groups * 8 * GROUP * BLOCK * keys * LANES,
            bytes_accessed=kv.size * 4 + rows * width * 6 + blocks * groups * GROUP * BLOCK * keys * 2,
            transcendentals=0,
        ),
        name="attend_back",
    )(pos, queries, d_context, probs, kv)


class Wires:
    def __init__(self, ctx_size, w_size):
        self.ctx_size, self.w_size = ctx_size, w_size
        self.lines = ctx_size // 4
        self.pairs = w_size // 2
        self.ctx = lax.axis_index("ctx")
        self.w = lax.axis_index("wshard")
        self.part = self.ctx // self.lines
        self.line = self.ctx % self.lines
        self.pair = self.w // 2
        self.core = self.w % 2

    def move(self, value, to):
        perm = []
        for ctx in range(self.ctx_size):
            for w in range(self.w_size):
                part, line, pair, core = to(ctx // self.lines, ctx % self.lines, w // 2, w % 2)
                target = (part * self.lines + line) * self.w_size + pair * 2 + core
                perm.append((ctx * self.w_size + w, target))
        return lax.ppermute(value, ("ctx", "wshard"), perm)

    def to_core(self, value):
        return self.move(value, lambda part, line, pair, core: (part, line, pair, 1 - core))

    def to_pair(self, value, flip):
        return self.move(value, lambda part, line, pair, core: (part, line, pair ^ flip, core))

    def to_line(self, value, flip):
        return self.move(value, lambda part, line, pair, core: (part, line ^ flip, pair, core))

    def to_part(self, value, flip):
        return self.move(value, lambda part, line, pair, core: (part ^ flip, line, pair, core))

    def deal(self, value, turn):
        return self.move(
            value,
            lambda part, line, pair, core: (2 * ((turn + part) % 2) + core, line, pair, part // 2),
        )

    def deal_back(self, value, turn):
        return self.move(
            value,
            lambda part, line, pair, core: (2 * core + (part // 2 + turn) % 2, line, pair, part % 2),
        )


def bits(count):
    flips = []
    flip = 1
    while flip < count:
        flips.append(flip)
        flip *= 2
    return flips


def gather_kernel(wires_of, refs, outs, own_shards, local_sem, send_sem, recv_sem):
    hidden, out_grad, ints, vectors, w_query, w_key, w_value, w_out, w_up, w_down = refs
    rows_out, grads_out, ints_out, vectors_out, query_out, kv_out, out_out, up_out, down_out = outs
    here = wires_of()
    lines, pairs = here.lines, here.pairs
    part, line, pair, core = here.part, here.line, here.pair, here.core
    width = w_query.shape[1]
    used = [0]
    sent = []
    local = []
    placed = []

    def at(part, line, pair, core):
        return (part * lines + line, pair * 2 + core)

    core_peer = at(part, line, pair, 1 - core)

    def line_peer(flip):
        return at(part, line ^ flip, pair, core)

    def pair_peer(flip):
        return at(part, line, pair ^ flip, core)

    def deal_target(turn):
        return at(2 * ((turn + part) % 2) + core, line, pair, part // 2)

    def deal_source(turn):
        return at(2 * core + (part // 2 + turn) % 2, line, pair, part % 2)

    stays = [
        jnp.logical_and(
            2 * ((turn + part) % 2) + core == part, part // 2 == core
        )
        for turn in range(2)
    ]

    barrier = pltpu.get_barrier_semaphore()

    def greet(device):
        pl.semaphore_signal(barrier, inc=1, device_id=device, device_id_type=MESH)

    peers = [core_peer]
    peers += [line_peer(flip) for flip in range(1, lines)]
    peers += [pair_peer(flip) for flip in range(1, pairs)]
    for device in peers:
        greet(device)
    for turn in range(2):

        @pl.when(jnp.logical_not(stays[turn]))
        def _(turn=turn):
            greet(deal_target(turn))
            greet(deal_source(turn))

    staying = sum(stay.astype(jnp.int32) for stay in stays)
    pl.semaphore_wait(barrier, len(peers) + 4 - 2 * staying)

    def send(src, dst, device, stay=None):
        n = used[0]
        used[0] += 1
        copy = pltpu.make_async_remote_copy(
            src_ref=src,
            dst_ref=dst,
            send_sem=send_sem.at[n],
            recv_sem=recv_sem.at[n],
            device_id=device,
            device_id_type=MESH,
        )
        if stay is None:
            copy.start()
        else:

            @pl.when(stay)
            def _():
                pltpu.make_async_copy(src, dst, recv_sem.at[n]).start()

            @pl.when(jnp.logical_not(stay))
            def _():
                copy.start()

        sent.append((copy, stay))
        return copy

    def stage(src, held):
        copy = pltpu.make_async_copy(src, held, local_sem.at[len(local)])
        copy.start()
        local.append(copy)

    def place_held(held, dst):
        local[len(placed)].wait()
        copy = pltpu.make_async_copy(held, dst, local_sem.at[len(local) + len(placed)])
        copy.start()
        placed.append(copy)

    me = pair * 2 + core

    dealt = [
        send(
            hidden.at[(turn + part) % 2, 0],
            rows_out.at[turn],
            deal_target(turn),
            stays[turn],
        )
        for turn in range(2)
    ]

    matrices = [
        (w_up, lambda shard: up_out.at[shard], True),
        (w_down, lambda shard: down_out.at[shard], True),
        (w_query, lambda shard: query_out.at[shard], False),
        (w_key, lambda shard: kv_out.at[shard, :, :width], False),
        (w_value, lambda shard: kv_out.at[shard, :, width:], False),
        (w_out, lambda shard: out_out.at[shard], False),
        (vectors, lambda shard: vectors_out.at[shard], False),
    ]
    side = line % 2
    for (src, _, _), held in zip(matrices, own_shards):
        stage(src, held)

    def half_cuts(src):
        half = src.shape[0] // 2
        first = pl.ds(pl.multiple_of(side * half, 8), half)
        return first, pl.ds(pl.multiple_of((1 - side) * half, 8), half)

    halves = [
        (
            flip,
            src,
            place,
            send(src.at[half_cuts(src)[0]], place(me).at[half_cuts(src)[0]], pair_peer(flip)),
        )
        for src, place, split in matrices
        if split
        for flip in range(1, pairs)
    ]
    late = [
        send(ints.at[(turn + part) % 2], ints_out.at[turn], deal_target(turn), stays[turn])
        for turn in range(2)
    ]
    for src, place, _ in matrices:
        late.append(send(src, place(me), core_peer))

    crossed = []
    for turn in range(2):
        dealt[turn].wait_recv()
        for flip in range(1, lines):
            crossed.append(
                (
                    flip * 2 + turn,
                    send(rows_out.at[turn], rows_out.at[flip * 2 + turn], line_peer(flip)),
                )
            )
        late.append(send(rows_out.at[turn], rows_out.at[lines * 2 + turn], core_peer))
    for (src, place, _), held in zip(matrices, own_shards):
        place_held(held, place(me))

    relayed = []
    whole = [
        (src, place, flip)
        for src, place, split in matrices
        if not split
        for flip in range(1, pairs)
    ]
    direct = []
    for step, (flip, src, place, copy) in enumerate(halves):
        copy.wait_recv()
        first, second = half_cuts(src)
        shard = (pair ^ flip) * 2 + core
        got = place(shard).at[first]
        relayed.append((place(shard).at[second], send(got, got, line_peer(1))))
        late.append(send(got, got, core_peer))
        share = -(-len(whole) // len(halves))
        for src, place, flip in whole[step * share : (step + 1) * share]:
            direct.append((flip, place, send(src, place(me), pair_peer(flip))))
    late += [
        send(
            out_grad.at[(turn + part) % 2, 0],
            grads_out.at[turn],
            deal_target(turn),
            stays[turn],
        )
        for turn in range(2)
    ]
    for index, copy in crossed:
        copy.wait_recv()
        late.append(send(rows_out.at[index], rows_out.at[lines * 2 + index], core_peer))
    for flip, place, copy in direct:
        copy.wait_recv()
        shard = (pair ^ flip) * 2 + core
        late.append(send(place(shard), place(shard), core_peer))
    for got, copy in relayed:
        copy.wait_recv()
        late.append(send(got, got, core_peer))
    for copy in late:
        copy.wait_recv()
    for copy in placed:
        copy.wait()
    for copy, stay in sent:
        if stay is None:
            copy.wait_send()
        else:

            @pl.when(jnp.logical_not(stay))
            def _(copy=copy):
                copy.wait_send()


def gather_all(ctx_size, w_size, hidden, out_grad, ints, vectors, weights):
    w_query, w_key, w_value, w_out, w_up, w_down = weights
    lines, pairs = ctx_size // 4, w_size // 2
    tok, width = hidden.shape[2], hidden.shape[3]
    rows = w_query.shape[0]
    shapes = [
        ((lines * 4, tok, width), bf16),
        ((2, tok, width), bf16),
        (ints.shape, ints.dtype),
        ((w_size,) + vectors.shape, bf16),
        ((w_size, rows, width), bf16),
        ((w_size, rows, 2 * width), bf16),
        ((w_size, rows, width), bf16),
        ((w_size,) + w_up.shape, bf16),
        ((w_size,) + w_down.shape, bf16),
    ]
    sems = 16 + 8 * lines + 20 * pairs

    def body(*refs):
        gather_kernel(
            lambda: Wires(ctx_size, w_size), refs[:10], refs[10:19], refs[19:26], *refs[26:]
        )

    return pl.pallas_call(
        body,
        in_specs=[pl.BlockSpec(memory_space=pl.ANY)] * 10,
        out_specs=[pl.BlockSpec(memory_space=pl.ANY)] * len(shapes),
        out_shape=[jax.ShapeDtypeStruct(shape, dtype) for shape, dtype in shapes],
        scratch_shapes=[
            *[
                pltpu.VMEM(shard.shape, bf16)
                for shard in (w_up, w_down, w_query, w_key, w_value, w_out, vectors)
            ],
            pltpu.SemaphoreType.DMA((14,)),
            pltpu.SemaphoreType.DMA((sems,)),
            pltpu.SemaphoreType.DMA((sems,)),
        ],
        compiler_params=pltpu.CompilerParams(collective_id=0, has_side_effects=True),
        name="gather_all",
    )(hidden, out_grad, ints, vectors, w_query, w_key, w_value, w_out, w_up, w_down)


def make_local(ctx_size, w_size):
    def local(
        hidden,
        out_grad,
        doc_lengths,
        rand_pick,
        w_query,
        w_key,
        w_value,
        w_out,
        w_up,
        w_down,
        b_query,
        b_value,
        b_out,
        b_up,
        b_down,
        ln1_gain,
        ln1_shift,
        ln2_gain,
        ln2_shift,
    ):
        wires = Wires(ctx_size, w_size)
        tok, width = hidden.shape[2], hidden.shape[3]
        ff = w_up.shape[1]
        tok_blocks = tok // BLOCK
        lines, pairs = wires.lines, wires.pairs
        micro = wires.part // 2
        odd_part = wires.part % 2

        small_ints = jnp.concatenate(
            [rand_pick.reshape(MICRO, -1), doc_lengths.reshape(MICRO, -1)], axis=1
        )
        int_count = small_ints.shape[1]
        small_ints = jnp.pad(small_ints, ((0, 0), (0, 1024 - int_count))).reshape(MICRO, 8, 128)
        vectors = [b_query, b_value, b_out, b_up, b_down, ln1_gain, ln1_shift, ln2_gain, ln2_shift]
        vector_sizes = [vector.shape[0] for vector in vectors]
        (
            all_rows,
            grads_dealt,
            ints_dealt,
            vector_table,
            full_query,
            full_kv,
            full_out,
            full_up,
            full_down,
        ) = gather_all(
            ctx_size,
            w_size,
            hidden,
            out_grad,
            small_ints,
            jnp.concatenate(vectors)[None],
            (w_query, w_key, w_value, w_out, w_up, w_down),
        )
        all_rows = all_rows.reshape(-1, width)
        own_rows = all_rows[: 2 * tok]
        grads_dealt = grads_dealt.reshape(-1, width)
        ints_dealt = ints_dealt.reshape(MICRO, -1)
        full_query, full_kv, full_out, full_up, full_down = [
            full.reshape(-1, full.shape[2]) for full in (full_query, full_kv, full_out, full_up, full_down)
        ]
        spread = []
        at = 0
        for size in vector_sizes:
            spread.append(vector_table[:, 0, at : at + size].reshape(-1).astype(f32))
            at += size
        (
            bias_query,
            bias_value,
            bias_out,
            bias_up,
            bias_down,
            gain_one,
            shift_one,
            gain_two,
            shift_two,
        ) = spread

        picks = jnp.stack(
            [ints_dealt[turn, : tok_blocks * 3].reshape(tok_blocks, 3) for turn in range(2)]
        ).reshape(-1, 3)
        lengths = ints_dealt[0, tok_blocks * 3 : int_count]
        in_chunk = jnp.arange(tok_blocks, dtype=jnp.int32)
        chunk_ids = [
            (2 * wires.core + (micro + turn) % 2) * lines + wires.line for turn in range(2)
        ]
        my_blocks = jnp.concatenate([chunk * tok_blocks + in_chunk for chunk in chunk_ids])
        safe_blocks, allowed = candidates(my_blocks, lengths, picks)
        chunk = safe_blocks // tok_blocks
        chunk_part, chunk_line = chunk // lines, chunk % lines
        place = (
            ((chunk_part // 2) ^ wires.core) * lines + (chunk_line ^ wires.line)
        ) * 2 + (chunk_part + micro) % 2
        pos = (place * tok_blocks + safe_blocks % tok_blocks).reshape(-1).astype(jnp.int32)
        bias = jnp.repeat(jnp.where(allowed, 0.0, masked_score).astype(f32), BLOCK, axis=1)[:, None]

        queries = ((dot_nn(own_rows, full_query) + bias_query) * score_scale).astype(bf16)
        kv_bias = jnp.concatenate([jnp.zeros_like(bias_value), bias_value])
        kv = (dot_nn(all_rows, full_kv) + kv_bias).astype(bf16)
        context, probs = attend(pos, queries, bias, kv)
        attn_out = dot_nn(context, full_out) + bias_out
        rows_f32 = own_rows.astype(f32)
        normed, ln1_back = jax.vjp(layer_norm, rows_f32 + attn_out, gain_one, shift_one)
        normed_low = normed.astype(bf16)
        up_pre = dot_nn(normed_low, full_up) + bias_up
        gelu_out, gelu_back = jax.vjp(lambda v: jax.nn.gelu(v, approximate=True), up_pre)
        activated = gelu_out.astype(bf16)
        branch = dot_nn(activated, full_down) + bias_down
        final, ln2_back = jax.vjp(layer_norm, normed + branch, gain_two, shift_two)
        final = final.astype(bf16)
        out_back = [wires.deal_back(final[turn * tok : (turn + 1) * tok], turn) for turn in range(2)]

        def by_shard(rows_a):
            shard = rows_a.shape[1] // w_size
            pieces = []
            for core_flip in range(2):
                for pair_flip in range(pairs):
                    index = (wires.pair ^ pair_flip) * 2 + (wires.core ^ core_flip)
                    pieces.append(
                        lax.dynamic_slice(
                            rows_a, (jnp.int32(0), index * shard), (rows_a.shape[0], shard)
                        )
                    )
            return jnp.concatenate(pieces, axis=1)

        def reduce_rows(rows_a, rows_b, scale=None):
            term = dot_tn(by_shard(rows_a), rows_b)
            if scale is not None:
                term = term * scale
            term = term.astype(bf16)
            half = term.shape[0] // 2

            def joined(kept, received):
                return (kept.astype(f32) + received.astype(f32)).astype(bf16)

            held = joined(term[:half], wires.to_core(term[half:]))
            for flip in reversed(bits(pairs)):
                half = held.shape[0] // 2
                held = joined(held[:half], wires.to_pair(held[half:], flip))
            steps = [(wires.to_line, wires.line, flip) for flip in bits(lines)]
            steps += [(wires.to_part, wires.part, flip) for flip in bits(4)]
            sides = []
            for send, index, flip in steps:
                side = (index // flip) % 2
                half = held.shape[0] // 2
                low, high = held[:half], held[half:]
                kept = jnp.where(side == 0, low, high)
                sent = jnp.where(side == 0, high, low)
                held = joined(kept, send(sent, flip))
                sides.append(side)
            for (send, _, flip), side in zip(reversed(steps), reversed(sides)):
                received = send(held, flip)
                first = jnp.where(side == 0, held, received)
                second = jnp.where(side == 0, received, held)
                held = jnp.concatenate([first, second], axis=0)
            return held.astype(f32)

        d_mid, grad_gain_two, grad_shift_two = ln2_back(grads_dealt.astype(f32))
        d_branch = d_mid.astype(bf16)
        grad_down = reduce_rows(activated, d_branch)
        d_act = dot_nt(d_branch, full_down)
        d_up = gelu_back(d_act)[0].astype(bf16)
        grad_up = reduce_rows(normed_low, d_up)
        d_normed = dot_nt(d_up, full_up) + d_mid
        d_sum, grad_gain_one, grad_shift_one = ln1_back(d_normed)
        d_attn = d_sum.astype(bf16)
        grad_out = reduce_rows(context, d_attn)
        d_context = dot_nt(d_attn, full_out).astype(bf16)
        d_query, d_kv = attend_back(pos, queries, d_context, probs, kv)

        through = dot_nt(d_kv, full_kv).astype(bf16)
        half = through.shape[0] // 2
        through = (
            through[:half].astype(f32) + wires.to_core(through[half:]).astype(f32)
        ).astype(bf16)
        mine = 2 * tok
        grad_in = d_sum + score_scale * dot_nt(d_query, full_query) + through[:mine].astype(f32)
        for step in range(1, lines):
            grad_in += wires.to_line(through[step * mine : (step + 1) * mine], step).astype(f32)
        grad_in = grad_in.astype(bf16)
        grad_back = [
            wires.deal_back(grad_in[turn * tok : (turn + 1) * tok], turn) for turn in range(2)
        ]

        grad_kv = reduce_rows(all_rows, d_kv)
        grad_query = reduce_rows(own_rows, d_query, score_scale)

        def column_sums(rows_a):
            return jnp.sum(rows_a.astype(f32), axis=0)

        sums = (
            score_scale * column_sums(d_query),
            column_sums(d_kv[:, width:]),
            column_sums(d_attn),
            column_sums(d_up),
            column_sums(d_branch),
            grad_gain_one,
            grad_shift_one,
            grad_gain_two,
            grad_shift_two,
        )
        table = jnp.concatenate([vector.reshape(w_size, -1) for vector in sums], axis=1)
        table = table + wires.to_core(table)
        for flip in bits(pairs):
            table = table + wires.to_pair(table, flip)
        for flip in bits(lines):
            table = table + wires.to_line(table, flip)
        for flip in bits(4):
            table = table + wires.to_part(table, flip)
        row = lax.dynamic_slice(table, (wires.w, jnp.int32(0)), (1, table.shape[1]))[0]
        small = []
        at = 0
        for size in vector_sizes:
            small.append(row[at : at + size])
            at += size

        def by_micro(received, dtype):
            first = jnp.where(odd_part == 0, received[0], received[1])
            second = jnp.where(odd_part == 0, received[1], received[0])
            return jnp.stack([first, second]).astype(dtype)[:, None]

        return (
            by_micro(out_back, bf16),
            by_micro(grad_back, f32),
            grad_query,
            grad_kv[:, :width],
            grad_kv[:, width:],
            grad_out,
            grad_up,
            grad_down,
            *small,
        )

    return local


def solution(mesh):
    tokens = P(None, "wshard", "ctx", None)
    in_specs = (
        tokens,
        tokens,
        P(None, "wshard", None),
        tokens,
        *[P("wshard", None)] * 6,
        *[P("wshard")] * 9,
    )
    out_specs = (tokens, tokens, *[P("wshard", None)] * 6, *[P("wshard")] * 9)
    return jax.shard_map(
        make_local(mesh.shape["ctx"], mesh.shape["wshard"]),
        mesh=mesh,
        in_specs=in_specs,
        out_specs=out_specs,
        check_vma=False,
    )
```

```python
import functools
import math

import jax
import jax.numpy as jnp
from jax import lax
from jax.experimental import pallas as pl
from jax.experimental.pallas import tpu as pltpu
from jax.sharding import PartitionSpec as P

HEADS = 12
HEAD_DIM = 64
BLOCK = 64
MICRO = 2
GROUP = 4
LANES = GROUP * HEAD_DIM
CANDS = 8

masked_score = -1e30
norm_eps = 1e-12
score_scale = 1.0 / math.sqrt(HEAD_DIM)
bf16 = jnp.bfloat16
f32 = jnp.float32
MESH = pl.DeviceIdType.MESH


def layer_norm(values, ln_gain, ln_shift):
    center = values - jnp.mean(values, axis=-1, keepdims=True)
    spread = jnp.mean(center * center, axis=-1, keepdims=True)
    return center * lax.rsqrt(spread + norm_eps) * ln_gain + ln_shift


def candidates(blocks, lengths, chosen_raw):
    doc_ends = jnp.cumsum(lengths)
    doc_starts = doc_ends - lengths
    owner_doc = jnp.sum((blocks[:, None] >= doc_ends[None, :]).astype(jnp.int32), axis=1)
    doc_ids = jnp.arange(lengths.shape[0], dtype=jnp.int32)
    member = (owner_doc[:, None] == doc_ids[None, :]).astype(jnp.int32)
    doc_first = jnp.sum(member * doc_starts[None, :], axis=1)
    length = jnp.sum(member * lengths[None, :], axis=1)
    randoms = doc_first[:, None] + chosen_raw % length[:, None]
    columns = [blocks, blocks - 1, blocks + 1, doc_first, doc_first + 1]
    for column in range(chosen_raw.shape[1]):
        columns.append(randoms[:, column])
    chosen = jnp.stack(columns, axis=1)
    inside = (chosen >= doc_first[:, None]) & (chosen < (doc_first + length)[:, None])
    is_fresh = [jnp.ones(blocks.shape, dtype=jnp.bool_)]
    for column in range(1, chosen.shape[1]):
        is_fresh.append(jnp.all(chosen[:, :column] != chosen[:, column : column + 1], axis=1))
    allowed = inside & jnp.stack(is_fresh, axis=1)
    safe_blocks = jnp.where(allowed, chosen, blocks[:, None])
    return (safe_blocks, allowed)


def dot_nt(a, b):
    return lax.dot_general(a, b, (((1,), (1,)), ((), ())), preferred_element_type=f32)


def dot_nn(a, b):
    return lax.dot_general(a, b, (((1,), (0,)), ((), ())), preferred_element_type=f32)


def dot_tn(a, b):
    return lax.dot_general(a, b, (((0,), (0,)), ((), ())), preferred_element_type=f32)


def spread_heads(rows, head_of_lane):
    zero = jnp.zeros_like(rows)
    return jnp.concatenate([jnp.where(head_of_lane == h, rows, zero) for h in range(GROUP)], axis=0)


def pick_heads(rows, head_of_lane):
    total = jnp.zeros((BLOCK, LANES), f32)
    for h in range(GROUP):
        total = jnp.where(head_of_lane == h, rows[h * BLOCK : (h + 1) * BLOCK], total)
    return total


def attend_kernel(groups, width, pos_ref, q_ref, bias_ref, kv_ref, ctx_ref, probs_ref, cat):
    i = pl.program_id(0)
    for j in range(CANDS):
        start = pl.multiple_of(pos_ref[i * CANDS + j] * BLOCK, BLOCK)
        cat[j * BLOCK : (j + 1) * BLOCK, :] = kv_ref[pl.ds(start, BLOCK), :]
    head_of_lane = lax.broadcasted_iota(jnp.int32, (BLOCK, LANES), 1) // HEAD_DIM
    bias = bias_ref[0]
    for g in range(groups):
        lanes = slice(g * LANES, (g + 1) * LANES)
        v_lanes = slice(width + g * LANES, width + (g + 1) * LANES)
        q_all = spread_heads(q_ref[:, lanes], head_of_lane)
        scores = dot_nt(q_all, cat[:, lanes]) + bias
        row_max = jnp.max(scores, axis=-1, keepdims=True)
        shifted = jnp.exp(scores - row_max)
        row_total = jnp.sum(shifted, axis=-1, keepdims=True)
        probs = (shifted * (1.0 / row_total)).astype(bf16)
        probs_ref[0, g] = probs
        mixed = dot_nn(probs, cat[:, v_lanes])
        ctx_ref[:, lanes] = pick_heads(mixed, head_of_lane).astype(bf16)


def attend(pos, queries, bias, kv):
    rows, width = queries.shape
    blocks = rows // BLOCK
    groups = width // LANES
    keys = CANDS * BLOCK
    return pl.pallas_call(
        functools.partial(attend_kernel, groups, width),
        grid_spec=pltpu.PrefetchScalarGridSpec(
            num_scalar_prefetch=1,
            grid=(blocks,),
            in_specs=[
                pl.BlockSpec((BLOCK, width), lambda i, p: (i, 0)),
                pl.BlockSpec((1, 1, keys), lambda i, p: (i, 0, 0)),
                pl.BlockSpec(kv.shape, lambda i, p: (0, 0), pipeline_mode=pl.Buffered(1)),
            ],
            out_specs=[
                pl.BlockSpec((BLOCK, width), lambda i, p: (i, 0)),
                pl.BlockSpec((1, groups, GROUP * BLOCK, keys), lambda i, p: (i, 0, 0, 0)),
            ],
            scratch_shapes=[pltpu.VMEM((keys, 2 * width), bf16)],
        ),
        out_shape=[
            jax.ShapeDtypeStruct((rows, width), bf16),
            jax.ShapeDtypeStruct((blocks, groups, GROUP * BLOCK, keys), bf16),
        ],
        compiler_params=pltpu.CompilerParams(vmem_limit_bytes=48 << 20),
        cost_estimate=pl.CostEstimate(
            flops=blocks * groups * 4 * GROUP * BLOCK * keys * LANES,
            bytes_accessed=kv.size * 2 + rows * width * 4 + blocks * groups * GROUP * BLOCK * keys * 2,
            transcendentals=blocks * groups * GROUP * BLOCK * keys,
        ),
        name="attend",
    )(pos, queries, bias, kv)


def attend_back_kernel(
    groups, width, pos_ref, q_ref, dctx_ref, probs_ref, kv_ref, dq_ref, dkv_ref, cat, acc
):
    i = pl.program_id(0)

    @pl.when(i == 0)
    def _():
        acc[...] = jnp.zeros_like(acc)

    for j in range(CANDS):
        start = pl.multiple_of(pos_ref[i * CANDS + j] * BLOCK, BLOCK)
        cat[j * BLOCK : (j + 1) * BLOCK, :] = kv_ref[pl.ds(start, BLOCK), :]
    head_of_lane = lax.broadcasted_iota(jnp.int32, (BLOCK, LANES), 1) // HEAD_DIM
    for g in range(groups):
        lanes = slice(g * LANES, (g + 1) * LANES)
        v_lanes = slice(width + g * LANES, width + (g + 1) * LANES)
        q_all = spread_heads(q_ref[:, lanes], head_of_lane)
        d_all = spread_heads(dctx_ref[:, lanes], head_of_lane)
        probs_low = probs_ref[0, g]
        probs = probs_low.astype(f32)
        d_probs = dot_nt(d_all, cat[:, v_lanes])
        row_inner = jnp.sum(probs * d_probs, axis=-1, keepdims=True)
        d_scores = (probs * (d_probs - row_inner)).astype(bf16)
        dq_ref[:, lanes] = pick_heads(dot_nn(d_scores, cat[:, lanes]), head_of_lane).astype(bf16)
        d_key = dot_tn(d_scores, q_all)
        d_value = dot_tn(probs_low, d_all)
        for j in range(CANDS):
            start = pl.multiple_of(pos_ref[i * CANDS + j] * BLOCK, BLOCK)
            part = slice(j * BLOCK, (j + 1) * BLOCK)
            acc[pl.ds(start, BLOCK), lanes] += d_key[part]
            acc[pl.ds(start, BLOCK), v_lanes] += d_value[part]

    @pl.when(i == pl.num_programs(0) - 1)
    def _():
        dkv_ref[...] = acc[...].astype(bf16)


def attend_back(pos, queries, d_context, probs, kv):
    rows, width = queries.shape
    blocks = rows // BLOCK
    groups = width // LANES
    keys = CANDS * BLOCK
    return pl.pallas_call(
        functools.partial(attend_back_kernel, groups, width),
        grid_spec=pltpu.PrefetchScalarGridSpec(
            num_scalar_prefetch=1,
            grid=(blocks,),
            in_specs=[
                pl.BlockSpec((BLOCK, width), lambda i, p: (i, 0)),
                pl.BlockSpec((BLOCK, width), lambda i, p: (i, 0)),
                pl.BlockSpec((1, groups, GROUP * BLOCK, keys), lambda i, p: (i, 0, 0, 0)),
                pl.BlockSpec(kv.shape, lambda i, p: (0, 0), pipeline_mode=pl.Buffered(1)),
            ],
            out_specs=[
                pl.BlockSpec((BLOCK, width), lambda i, p: (i, 0)),
                pl.BlockSpec(kv.shape, lambda i, p: (0, 0), pipeline_mode=pl.Buffered(1)),
            ],
            scratch_shapes=[pltpu.VMEM((keys, 2 * width), bf16), pltpu.VMEM(kv.shape, f32)],
        ),
        out_shape=[
            jax.ShapeDtypeStruct((rows, width), bf16),
            jax.ShapeDtypeStruct(kv.shape, bf16),
        ],
        compiler_params=pltpu.CompilerParams(vmem_limit_bytes=60 << 20),
        cost_estimate=pl.CostEstimate(
            flops=blocks * groups * 8 * GROUP * BLOCK * keys * LANES,
            bytes_accessed=kv.size * 4 + rows * width * 6 + blocks * groups * GROUP * BLOCK * keys * 2,
            transcendentals=0,
        ),
        name="attend_back",
    )(pos, queries, d_context, probs, kv)


class Wires:
    def __init__(self, ctx_size, w_size):
        self.ctx_size, self.w_size = ctx_size, w_size
        self.lines = ctx_size // 4
        self.pairs = w_size // 2
        self.ctx = lax.axis_index("ctx")
        self.w = lax.axis_index("wshard")
        self.part = self.ctx // self.lines
        self.line = self.ctx % self.lines
        self.pair = self.w // 2
        self.core = self.w % 2

    def at(self, part, line, pair, core):
        return (part * self.lines + line, pair * 2 + core)

    @property
    def core_peer(self):
        return self.at(self.part, self.line, self.pair, 1 - self.core)

    def pair_peer(self, flip):
        return self.at(self.part, self.line, self.pair ^ flip, self.core)

    def line_peer(self, flip):
        return self.at(self.part, self.line ^ flip, self.pair, self.core)

    def part_peer(self, flip):
        return self.at(self.part ^ flip, self.line, self.pair, self.core)

    def move(self, value, to):
        perm = []
        for ctx in range(self.ctx_size):
            for w in range(self.w_size):
                part, line, pair, core = to(ctx // self.lines, ctx % self.lines, w // 2, w % 2)
                target = (part * self.lines + line) * self.w_size + pair * 2 + core
                perm.append((ctx * self.w_size + w, target))
        return lax.ppermute(value, ("ctx", "wshard"), perm)

    def to_core(self, value):
        return self.move(value, lambda part, line, pair, core: (part, line, pair, 1 - core))

    def to_pair(self, value, flip):
        return self.move(value, lambda part, line, pair, core: (part, line, pair ^ flip, core))

    def to_line(self, value, flip):
        return self.move(value, lambda part, line, pair, core: (part, line ^ flip, pair, core))

    def to_part(self, value, flip):
        return self.move(value, lambda part, line, pair, core: (part ^ flip, line, pair, core))

    def deal(self, value, turn):
        return self.move(
            value,
            lambda part, line, pair, core: (2 * ((turn + part) % 2) + core, line, pair, part // 2),
        )

    def deal_back(self, value, turn):
        return self.move(
            value,
            lambda part, line, pair, core: (2 * core + (part // 2 + turn) % 2, line, pair, part % 2),
        )


def bits(count):
    flips = []
    flip = 1
    while flip < count:
        flips.append(flip)
        flip *= 2
    return flips


def gather_kernel(wires_of, refs, outs, own_shards, local_sem, send_sem, recv_sem):
    hidden, out_grad, ints, vectors, w_query, w_key, w_value, w_out, w_up, w_down = refs
    rows_out, grads_out, ints_out, vectors_out, query_out, kv_out, out_out, up_out, down_out = outs
    here = wires_of()
    lines, pairs = here.lines, here.pairs
    part, line, pair, core = here.part, here.line, here.pair, here.core
    width = w_query.shape[1]
    used = [0]
    sent = []
    local = []
    placed = []

    def at(part, line, pair, core):
        return (part * lines + line, pair * 2 + core)

    core_peer = at(part, line, pair, 1 - core)

    def line_peer(flip):
        return at(part, line ^ flip, pair, core)

    def pair_peer(flip):
        return at(part, line, pair ^ flip, core)

    def deal_target(turn):
        return at(2 * ((turn + part) % 2) + core, line, pair, part // 2)

    def deal_source(turn):
        return at(2 * core + (part // 2 + turn) % 2, line, pair, part % 2)

    stays = [
        jnp.logical_and(
            2 * ((turn + part) % 2) + core == part, part // 2 == core
        )
        for turn in range(2)
    ]

    barrier = pltpu.get_barrier_semaphore()

    def greet(device):
        pl.semaphore_signal(barrier, inc=1, device_id=device, device_id_type=MESH)

    peers = [core_peer]
    peers += [line_peer(flip) for flip in range(1, lines)]
    peers += [pair_peer(flip) for flip in range(1, pairs)]
    for device in peers:
        greet(device)
    for turn in range(2):

        @pl.when(jnp.logical_not(stays[turn]))
        def _(turn=turn):
            greet(deal_target(turn))
            greet(deal_source(turn))

    staying = sum(stay.astype(jnp.int32) for stay in stays)
    pl.semaphore_wait(barrier, len(peers) + 4 - 2 * staying)

    def send(src, dst, device, stay=None):
        n = used[0]
        used[0] += 1
        copy = pltpu.make_async_remote_copy(
            src_ref=src,
            dst_ref=dst,
            send_sem=send_sem.at[n],
            recv_sem=recv_sem.at[n],
            device_id=device,
            device_id_type=MESH,
        )
        if stay is None:
            copy.start()
        else:

            @pl.when(stay)
            def _():
                pltpu.make_async_copy(src, dst, recv_sem.at[n]).start()

            @pl.when(jnp.logical_not(stay))
            def _():
                copy.start()

        sent.append((copy, stay))
        return copy

    def stage(src, held):
        copy = pltpu.make_async_copy(src, held, local_sem.at[len(local)])
        copy.start()
        local.append(copy)

    def place_held(held, dst):
        local[len(placed)].wait()
        copy = pltpu.make_async_copy(held, dst, local_sem.at[len(local) + len(placed)])
        copy.start()
        placed.append(copy)

    me = pair * 2 + core

    dealt = [
        send(
            hidden.at[(turn + part) % 2, 0],
            rows_out.at[turn],
            deal_target(turn),
            stays[turn],
        )
        for turn in range(2)
    ]

    matrices = [
        (w_up, lambda shard: up_out.at[shard], True),
        (w_down, lambda shard: down_out.at[shard], True),
        (w_query, lambda shard: query_out.at[shard], False),
        (w_key, lambda shard: kv_out.at[shard, :, :width], False),
        (w_value, lambda shard: kv_out.at[shard, :, width:], False),
        (w_out, lambda shard: out_out.at[shard], False),
        (vectors, lambda shard: vectors_out.at[shard], False),
    ]
    side = line % 2
    for (src, _, _), held in zip(matrices, own_shards):
        stage(src, held)

    def half_cuts(src):
        half = src.shape[0] // 2
        first = pl.ds(pl.multiple_of(side * half, 8), half)
        return first, pl.ds(pl.multiple_of((1 - side) * half, 8), half)

    halves = [
        (
            flip,
            src,
            place,
            send(src.at[half_cuts(src)[0]], place(me).at[half_cuts(src)[0]], pair_peer(flip)),
        )
        for src, place, split in matrices
        if split
        for flip in range(1, pairs)
    ]
    late = [
        send(ints.at[(turn + part) % 2], ints_out.at[turn], deal_target(turn), stays[turn])
        for turn in range(2)
    ]
    for src, place, _ in matrices:
        late.append(send(src, place(me), core_peer))

    crossed = []
    for turn in range(2):
        dealt[turn].wait_recv()
        for flip in range(1, lines):
            crossed.append(
                (
                    flip * 2 + turn,
                    send(rows_out.at[turn], rows_out.at[flip * 2 + turn], line_peer(flip)),
                )
            )
        late.append(send(rows_out.at[turn], rows_out.at[lines * 2 + turn], core_peer))
    for (src, place, _), held in zip(matrices, own_shards):
        place_held(held, place(me))

    relayed = []
    whole = [
        (src, place, flip)
        for src, place, split in matrices
        if not split
        for flip in range(1, pairs)
    ]
    direct = []
    for step, (flip, src, place, copy) in enumerate(halves):
        copy.wait_recv()
        first, second = half_cuts(src)
        shard = (pair ^ flip) * 2 + core
        got = place(shard).at[first]
        relayed.append((place(shard).at[second], send(got, got, line_peer(1))))
        late.append(send(got, got, core_peer))
        share = -(-len(whole) // len(halves))
        for src, place, flip in whole[step * share : (step + 1) * share]:
            direct.append((flip, place, send(src, place(me), pair_peer(flip))))
    late += [
        send(
            out_grad.at[(turn + part) % 2, 0],
            grads_out.at[turn],
            deal_target(turn),
            stays[turn],
        )
        for turn in range(2)
    ]
    for index, copy in crossed:
        copy.wait_recv()
        late.append(send(rows_out.at[index], rows_out.at[lines * 2 + index], core_peer))
    for flip, place, copy in direct:
        copy.wait_recv()
        shard = (pair ^ flip) * 2 + core
        late.append(send(place(shard), place(shard), core_peer))
    for got, copy in relayed:
        copy.wait_recv()
        late.append(send(got, got, core_peer))
    for copy in late:
        copy.wait_recv()
    for copy in placed:
        copy.wait()
    for copy, stay in sent:
        if stay is None:
            copy.wait_send()
        else:

            @pl.when(jnp.logical_not(stay))
            def _(copy=copy):
                copy.wait_send()


def gather_all(ctx_size, w_size, hidden, out_grad, ints, vectors, weights):
    w_query, w_key, w_value, w_out, w_up, w_down = weights
    lines, pairs = ctx_size // 4, w_size // 2
    tok, width = hidden.shape[2], hidden.shape[3]
    rows = w_query.shape[0]
    shapes = [
        ((lines * 4, tok, width), bf16),
        ((2, tok, width), bf16),
        (ints.shape, ints.dtype),
        ((w_size,) + vectors.shape, bf16),
        ((w_size, rows, width), bf16),
        ((w_size, rows, 2 * width), bf16),
        ((w_size, rows, width), bf16),
        ((w_size,) + w_up.shape, bf16),
        ((w_size,) + w_down.shape, bf16),
    ]
    sems = 16 + 8 * lines + 20 * pairs

    def body(*refs):
        gather_kernel(
            lambda: Wires(ctx_size, w_size), refs[:10], refs[10:19], refs[19:26], *refs[26:]
        )

    return pl.pallas_call(
        body,
        in_specs=[pl.BlockSpec(memory_space=pl.ANY)] * 10,
        out_specs=[pl.BlockSpec(memory_space=pl.ANY)] * len(shapes),
        out_shape=[jax.ShapeDtypeStruct(shape, dtype) for shape, dtype in shapes],
        scratch_shapes=[
            *[
                pltpu.VMEM(shard.shape, bf16)
                for shard in (w_up, w_down, w_query, w_key, w_value, w_out, vectors)
            ],
            pltpu.SemaphoreType.DMA((14,)),
            pltpu.SemaphoreType.DMA((sems,)),
            pltpu.SemaphoreType.DMA((sems,)),
        ],
        compiler_params=pltpu.CompilerParams(collective_id=0, has_side_effects=True),
        name="gather_all",
    )(hidden, out_grad, ints, vectors, w_query, w_key, w_value, w_out, w_up, w_down)


class Copies:
    def __init__(self, local_sem, send_sem, recv_sem):
        self.local_sem, self.send_sem, self.recv_sem = local_sem, send_sem, recv_sem
        self.locals, self.sent = 0, []

    def load(self, src, dst):
        copy = pltpu.make_async_copy(src, dst, self.local_sem.at[self.locals])
        copy.start()
        self.locals += 1
        return copy

    def send(self, src, dst, device, stay=None):
        n = len(self.sent)
        copy = pltpu.make_async_remote_copy(
            src_ref=src,
            dst_ref=dst,
            send_sem=self.send_sem.at[n],
            recv_sem=self.recv_sem.at[n],
            device_id=device,
            device_id_type=MESH,
        )
        if stay is None:
            copy.start()
        else:

            @pl.when(stay)
            def _():
                pltpu.make_async_copy(src, dst, self.recv_sem.at[n]).start()

            @pl.when(jnp.logical_not(stay))
            def _():
                copy.start()

        self.sent.append((copy, stay))
        return copy

    def finish(self):
        for copy, stay in self.sent:
            if stay is None:
                copy.wait_send()
            else:

                @pl.when(jnp.logical_not(stay))
                def _(copy=copy):
                    copy.wait_send()


def add_blocks(dst, *srcs):
    rows = dst.shape[0]
    step = 48 if rows % 48 == 0 else 32

    def body(i, carry):
        cut = pl.ds(pl.multiple_of(i * step, step), step)
        total = srcs[0][cut, :].astype(f32)
        for src in srcs[1:]:
            total = total + src[cut, :].astype(f32)
        dst[cut, :] = total.astype(dst.dtype)
        return carry

    lax.fori_loop(0, rows // step, body, 0)


class Events:
    def __init__(self):
        self.items = []

    def add(self, time, action):
        self.items.append((time, len(self.items), action))

    def run(self):
        for _, _, action in sorted(self.items, key=lambda item: item[:2]):
            action()


def group_scratch(lines, pairs, rows, columns):
    block = (rows, columns)
    return [
        pltpu.VMEM((2 * lines, pairs) + block, bf16),
        pltpu.VMEM((2 * lines, pairs) + block, bf16),
        pltpu.VMEM((2 * lines, max(pairs - 1, 1)) + block, bf16),
        pltpu.VMEM((2 * lines,) + block, bf16),
        pltpu.VMEM((2, max(lines - 1, 1)) + block, bf16),
        pltpu.VMEM((2,) + block, bf16),
        pltpu.VMEM((2,) + block, bf16),
        pltpu.VMEM((2,) + block, bf16),
    ]


GROUP_SCRATCH = 8


def reduce_group(here, copies, events, links, chunks, scratch, out, base):
    from_core, own, from_pairs, paired, from_lines, lined, from_parts, parted = scratch
    lines, pairs = here.lines, here.pairs
    line, pair, core, part = here.line, here.pair, here.core, here.part
    low_part = part % 2
    state = {}

    def begin(i):
        state["core", i] = copies.send(chunks[i](1 - core), from_core.at[i], here.core_peer)
        state["own", i] = copies.load(chunks[i](core), own.at[i])

    def over_core(i):
        state["own", i].wait()
        state["core", i].wait_recv()
        for p in range(pairs):
            add_blocks(own.at[i, p], own.at[i, p], from_core.at[i, p])
        state["pair", i] = [
            copies.send(own.at[i, pair ^ flip], from_pairs.at[i, flip - 1], here.pair_peer(flip))
            for flip in range(1, pairs)
        ]

    def over_pairs(i):
        for copy in state["pair", i]:
            copy.wait_recv()
        add_blocks(
            paired.at[i], own.at[i, pair], *[from_pairs.at[i, flip - 1] for flip in range(1, pairs)]
        )

    def to_lines(h):
        state["line", h] = [
            copies.send(
                paired.at[h * lines + (line ^ flip)],
                from_lines.at[h, flip - 1],
                here.line_peer(flip),
            )
            for flip in range(1, lines)
        ]

    def over_lines(h):
        for copy in state["line", h]:
            copy.wait_recv()
        add_blocks(
            lined.at[h],
            paired.at[h * lines + line],
            *[from_lines.at[h, flip - 1] for flip in range(1, lines)],
        )

    def to_part_one():
        state["one"] = copies.send(lined.at[1 - low_part], from_parts.at[0], here.part_peer(1))

    def over_part_one():
        state["one"].wait_recv()
        add_blocks(parted.at[0], lined.at[low_part], from_parts.at[0])
        state["two"] = copies.send(parted.at[0], from_parts.at[1], here.part_peer(2))

    def over_part_two():
        state["two"].wait_recv()
        add_blocks(parted.at[1], parted.at[0], from_parts.at[1])
        place = out.at[base + low_part * lines + line]
        state["back"] = copies.send(parted.at[1], place, here.part_peer(1))
        state["place"] = copies.load(parted.at[1], place)
        state["spread"] = [
            copies.send(parted.at[1], place, here.line_peer(flip)) for flip in range(1, lines)
        ]

    def spread_other():
        state["back"].wait_recv()
        place = out.at[base + (1 - low_part) * lines + line]
        state["spread"] += [
            copies.send(place, place, here.line_peer(flip)) for flip in range(1, lines)
        ]

    def end():
        state["place"].wait()
        for copy in state["spread"]:
            copy.wait_recv()

    start = links["start"]
    core_at = start
    for i in range(2 * lines):
        events.add(-1000.0 + links["order"], functools.partial(begin, i))
        core_at += 0.2
        events.add(core_at, functools.partial(over_core, i))
        links["x"] = max(links["x"], core_at) + (pairs - 1)
        events.add(links["x"], functools.partial(over_pairs, i))
        if i % lines == lines - 1:
            h = i // lines
            events.add(links["x"] + 0.01, functools.partial(to_lines, h))
            links["y"] = max(links["y"], links["x"]) + (lines - 1) + 0.1
            lined_at = links["y"]
            events.add(lined_at, functools.partial(over_lines, h))
    links["start"] = core_at
    links["order"] += 1
    now = lined_at + 0.02
    events.add(now, to_part_one)
    links["z"] = max(links["z"], now) + 1.1
    events.add(links["z"], over_part_one)
    links["z"] += 2.1
    two_at = links["z"]
    events.add(two_at, over_part_two)
    links["z"] += 1.1
    events.add(links["z"], spread_other)
    events.add(links["z"] + 100.0, end)


def chunk_views(refs, kinds, lines):
    parts = lines // 2
    views = []
    for ref, kind in zip(refs, kinds):
        if kind == "wide":
            columns = ref.shape[3]
            width = ref.shape[2] * ref.shape[0] * 2 // parts
            for c in range(columns // width):
                views.append(
                    lambda core, ref=ref, cut=slice(c * width, (c + 1) * width): ref.at[
                        :, core, :, cut
                    ]
                )
        else:
            width = ref.shape[4] // parts
            for b in range(ref.shape[2]):
                for c in range(parts):
                    views.append(
                        lambda core, ref=ref, b=b, cut=slice(c * width, (c + 1) * width): ref.at[
                            :, core, b, :, cut
                        ]
                    )
    return views


def finish_kernel(ctx_size, w_size, kinds, tables, *refs):
    here = Wires(ctx_size, w_size)
    lines, pairs = here.lines, here.pairs
    part, line, pair, core = here.part, here.line, here.pair, here.core
    terms = refs[: len(kinds)]
    through, near, final, table = refs[len(kinds) : len(kinds) + 4]
    at = len(kinds) + 4
    out, final_out, grad_out, table_out = refs[at : at + 4]
    at += 4
    groups = (len(refs) - at - 8) // GROUP_SCRATCH
    scratches = [
        refs[at + g * GROUP_SCRATCH : at + (g + 1) * GROUP_SCRATCH] for g in range(groups)
    ]
    at += groups * GROUP_SCRATCH
    g_core, g_own, g_line, g_near, g_sum, table_in, table_sum = refs[at : at + 7]
    copies = Copies(*refs[at + 7])
    micro = part // 2

    def back_target(turn):
        return here.at(2 * core + (micro + turn) % 2, line, pair, part % 2)

    def back_source(turn):
        return here.at(2 * ((turn + part) % 2) + core, line, pair, part // 2)

    stays = [
        jnp.logical_and(2 * core + (micro + turn) % 2 == part, part % 2 == core)
        for turn in range(2)
    ]
    barrier = pltpu.get_barrier_semaphore()

    def greet(device):
        pl.semaphore_signal(barrier, inc=1, device_id=device, device_id_type=MESH)

    peers = [here.core_peer, here.part_peer(1), here.part_peer(2)]
    peers += [here.line_peer(flip) for flip in range(1, lines)]
    peers += [here.pair_peer(flip) for flip in range(1, pairs)]
    for device in peers:
        greet(device)
    for turn in range(2):

        @pl.when(jnp.logical_not(stays[turn]))
        def _(turn=turn):
            greet(back_target(turn))
            greet(back_source(turn))

    staying = sum(stay.astype(jnp.int32) for stay in stays)
    pl.semaphore_wait(barrier, len(peers) + 4 - 2 * staying)

    events = Events()
    state = {}
    count = 2 * lines

    def begin_rows():
        state["core"] = [
            copies.send(through.at[count + j], g_core.at[j], here.core_peer) for j in range(count)
        ]
        state["own"] = [copies.load(through.at[j], g_own.at[j]) for j in range(count)]
        state["near"] = copies.load(near, g_near)
        state["out"] = [
            copies.send(final.at[turn], final_out.at[micro], back_target(turn), stays[turn])
            for turn in range(2)
        ]

    def rows_over_core():
        for j in reversed(range(count)):
            state["own"][j].wait()
            state["core"][j].wait_recv()
            add_blocks(g_own.at[j], g_own.at[j], g_core.at[j])
            if j >= 2:
                state["line", j] = copies.send(
                    g_own.at[j], g_line.at[j - 2], here.line_peer(j // 2)
                )

    def rows_over_lines():
        state["near"].wait()
        state["back"] = []
        for turn in range(2):
            others = []
            for flip in range(1, lines):
                state["line", 2 * flip + turn].wait_recv()
                others.append(g_line.at[2 * flip + turn - 2])
            add_blocks(g_sum.at[turn], g_near.at[turn], g_own.at[turn], *others)
            state["back"].append(
                copies.send(g_sum.at[turn], grad_out.at[micro], back_target(turn), stays[turn])
            )

    def end_rows():
        for copy in state["out"] + state["back"]:
            copy.wait_recv()

    steps = [here.core_peer]
    steps += [here.pair_peer(flip) for flip in bits(pairs)]
    steps += [here.line_peer(flip) for flip in bits(lines)]
    steps += [here.part_peer(flip) for flip in bits(4)]

    def table_send(n):
        src = table if n == 0 else table_sum.at[n - 1]
        state["table", n] = copies.send(src, table_in.at[n], steps[n])

    def table_step(n):
        state["table", n].wait_recv()
        before = table[...] if n == 0 else table_sum[n - 1]
        total = before + table_in[n]
        if n + 1 < len(steps):
            table_sum[n] = total
            table_send(n + 1)
        else:
            table_out[...] = total

    links = {"start": 0.3, "x": 0.0, "y": 2.5, "z": 2.6, "order": 1}
    events.add(-1001.0, begin_rows)
    events.add(-1000.5, lambda: table_send(0))
    events.add(0.1, rows_over_core)
    events.add(2.5, rows_over_lines)
    events.add(900.0, end_rows)
    for n in range(len(steps)):
        events.add(0.35 + n * 1.0, functools.partial(table_step, n))
    views = chunk_views(terms, kinds, lines)
    size = 2 * lines
    for g in range(groups):
        reduce_group(
            here,
            copies,
            events,
            links,
            views[g * size : (g + 1) * size],
            scratches[g],
            out,
            g * size,
        )
    events.run()
    copies.finish()


def finish_all(ctx_size, w_size, terms, kinds, through, near, final, table):
    lines, pairs = ctx_size // 4, w_size // 2
    count = 2 * lines
    tok, width = through.shape[1:]
    rows = width // w_size
    columns = width // (lines // 2)
    chunks = sum(term.size for term in terms) // (w_size * rows * columns)
    groups = chunks // (2 * lines)
    table_steps = 1 + len(bits(pairs)) + len(bits(lines)) + len(bits(4))
    block = (tok, width)
    any_space = pl.BlockSpec(memory_space=pl.ANY)
    in_vmem = pl.BlockSpec(memory_space=pltpu.VMEM)
    sems = 40 + 10 * lines + groups * 2 * lines * (6 + pairs)
    scratch = []
    for _ in range(groups):
        scratch += group_scratch(lines, pairs, rows, columns)
    scratch += [
        pltpu.VMEM((count,) + block, bf16),
        pltpu.VMEM((count,) + block, bf16),
        pltpu.VMEM((max(count - 2, 1),) + block, bf16),
        pltpu.VMEM((2,) + block, f32),
        pltpu.VMEM((2,) + block, bf16),
        pltpu.VMEM((table_steps,) + table.shape, f32),
        pltpu.VMEM((table_steps,) + table.shape, f32),
        (
            pltpu.SemaphoreType.DMA((sems,)),
            pltpu.SemaphoreType.DMA((sems,)),
            pltpu.SemaphoreType.DMA((sems,)),
        ),
    ]
    return pl.pallas_call(
        functools.partial(finish_kernel, ctx_size, w_size, kinds, table_steps),
        in_specs=[any_space] * (len(terms) + 3) + [in_vmem],
        out_specs=[any_space, any_space, any_space, in_vmem],
        out_shape=[
            jax.ShapeDtypeStruct((chunks, rows, columns), bf16),
            jax.ShapeDtypeStruct((2,) + block, bf16),
            jax.ShapeDtypeStruct((2,) + block, bf16),
            jax.ShapeDtypeStruct(table.shape, f32),
        ],
        scratch_shapes=scratch,
        compiler_params=pltpu.CompilerParams(
            collective_id=1, has_side_effects=True, vmem_limit_bytes=60 << 20
        ),
        name="finish_all",
    )(*terms, through, near, final, table)


def make_local(ctx_size, w_size):
    def local(
        hidden,
        out_grad,
        doc_lengths,
        rand_pick,
        w_query,
        w_key,
        w_value,
        w_out,
        w_up,
        w_down,
        b_query,
        b_value,
        b_out,
        b_up,
        b_down,
        ln1_gain,
        ln1_shift,
        ln2_gain,
        ln2_shift,
    ):
        wires = Wires(ctx_size, w_size)
        tok, width = hidden.shape[2], hidden.shape[3]
        ff = w_up.shape[1]
        tok_blocks = tok // BLOCK
        lines, pairs = wires.lines, wires.pairs
        micro = wires.part // 2

        small_ints = jnp.concatenate(
            [rand_pick.reshape(MICRO, -1), doc_lengths.reshape(MICRO, -1)], axis=1
        )
        int_count = small_ints.shape[1]
        small_ints = jnp.pad(small_ints, ((0, 0), (0, 1024 - int_count))).reshape(MICRO, 8, 128)
        vectors = [b_query, b_value, b_out, b_up, b_down, ln1_gain, ln1_shift, ln2_gain, ln2_shift]
        vector_sizes = [vector.shape[0] for vector in vectors]
        (
            all_rows,
            grads_dealt,
            ints_dealt,
            vector_table,
            full_query,
            full_kv,
            full_out,
            full_up,
            full_down,
        ) = gather_all(
            ctx_size,
            w_size,
            hidden,
            out_grad,
            small_ints,
            jnp.concatenate(vectors)[None],
            (w_query, w_key, w_value, w_out, w_up, w_down),
        )
        all_rows = all_rows.reshape(-1, width)
        own_rows = all_rows[: 2 * tok]
        grads_dealt = grads_dealt.reshape(-1, width)
        ints_dealt = ints_dealt.reshape(MICRO, -1)
        full_query, full_kv, full_out, full_up, full_down = [
            full.reshape(-1, full.shape[2]) for full in (full_query, full_kv, full_out, full_up, full_down)
        ]
        spread = []
        at = 0
        for size in vector_sizes:
            spread.append(vector_table[:, 0, at : at + size].reshape(-1).astype(f32))
            at += size
        (
            bias_query,
            bias_value,
            bias_out,
            bias_up,
            bias_down,
            gain_one,
            shift_one,
            gain_two,
            shift_two,
        ) = spread

        picks = jnp.stack(
            [ints_dealt[turn, : tok_blocks * 3].reshape(tok_blocks, 3) for turn in range(2)]
        ).reshape(-1, 3)
        lengths = ints_dealt[0, tok_blocks * 3 : int_count]
        in_chunk = jnp.arange(tok_blocks, dtype=jnp.int32)
        chunk_ids = [
            (2 * wires.core + (micro + turn) % 2) * lines + wires.line for turn in range(2)
        ]
        my_blocks = jnp.concatenate([chunk * tok_blocks + in_chunk for chunk in chunk_ids])
        safe_blocks, allowed = candidates(my_blocks, lengths, picks)
        chunk = safe_blocks // tok_blocks
        chunk_part, chunk_line = chunk // lines, chunk % lines
        place = (
            ((chunk_part // 2) ^ wires.core) * lines + (chunk_line ^ wires.line)
        ) * 2 + (chunk_part + micro) % 2
        pos = (place * tok_blocks + safe_blocks % tok_blocks).reshape(-1).astype(jnp.int32)
        bias = jnp.repeat(jnp.where(allowed, 0.0, masked_score).astype(f32), BLOCK, axis=1)[:, None]

        queries = ((dot_nn(own_rows, full_query) + bias_query) * score_scale).astype(bf16)
        kv_bias = jnp.concatenate([jnp.zeros_like(bias_value), bias_value])
        kv = (dot_nn(all_rows, full_kv) + kv_bias).astype(bf16)
        context, probs = attend(pos, queries, bias, kv)
        attn_out = dot_nn(context, full_out) + bias_out
        rows_f32 = own_rows.astype(f32)
        normed, ln1_back = jax.vjp(layer_norm, rows_f32 + attn_out, gain_one, shift_one)
        normed_low = normed.astype(bf16)
        up_pre = dot_nn(normed_low, full_up) + bias_up
        gelu_out, gelu_back = jax.vjp(lambda v: jax.nn.gelu(v, approximate=True), up_pre)
        activated = gelu_out.astype(bf16)
        branch = dot_nn(activated, full_down) + bias_down
        final, ln2_back = jax.vjp(layer_norm, normed + branch, gain_two, shift_two)
        final = final.astype(bf16)

        def term_of(rows_a, rows_b, scale=None):
            term = dot_tn(rows_a, rows_b)
            if scale is not None:
                term = term * scale
            return term.astype(bf16).reshape(pairs, 2, -1, rows_b.shape[1])

        d_mid, grad_gain_two, grad_shift_two = ln2_back(grads_dealt.astype(f32))
        d_branch = d_mid.astype(bf16)
        term_down = term_of(activated, d_branch)
        d_act = dot_nt(d_branch, full_down)
        d_up = gelu_back(d_act)[0].astype(bf16)
        term_up = term_of(normed_low, d_up)
        d_normed = dot_nt(d_up, full_up) + d_mid
        d_sum, grad_gain_one, grad_shift_one = ln1_back(d_normed)
        d_attn = d_sum.astype(bf16)
        term_out = term_of(context, d_attn)
        d_context = dot_nt(d_attn, full_out).astype(bf16)
        d_query, d_kv = attend_back(pos, queries, d_context, probs, kv)

        through = dot_nt(d_kv, full_kv).astype(bf16)
        near = d_sum + score_scale * dot_nt(d_query, full_query)
        term_kv = term_of(all_rows, d_kv)
        term_query = term_of(own_rows, d_query, score_scale)

        def column_sums(rows_a):
            return jnp.sum(rows_a.astype(f32), axis=0)

        sums = (
            score_scale * column_sums(d_query),
            column_sums(d_kv[:, width:]),
            column_sums(d_attn),
            column_sums(d_up),
            column_sums(d_branch),
            grad_gain_one,
            grad_shift_one,
            grad_gain_two,
            grad_shift_two,
        )
        table = jnp.concatenate([vector.reshape(w_size, -1) for vector in sums], axis=1)[:, None]
        shard = width // w_size
        term_down = term_down.reshape(pairs, 2, -1, shard, width)
        summed, block_out, grad_hidden, table = finish_all(
            ctx_size,
            w_size,
            (term_up, term_down, term_query, term_kv, term_out),
            ("wide", "tall", "wide", "wide", "wide"),
            through.reshape(-1, tok, width),
            near.reshape(-1, tok, width),
            final.reshape(-1, tok, width),
            table,
        )
        row = lax.dynamic_slice(
            table, (wires.w, jnp.int32(0), jnp.int32(0)), (1, 1, table.shape[2])
        )[0, 0]
        small = []
        at = 0
        for size in vector_sizes:
            small.append(row[at : at + size])
            at += size

        parts = lines // 2
        at = 0

        def wide(columns):
            nonlocal at
            count = columns * parts // width
            pieces = summed[at : at + count].astype(f32)
            at += count
            return jnp.concatenate([pieces[c] for c in range(count)], axis=1)

        grad_up = wide(ff)
        count = ff * parts // width
        grad_down = summed[at : at + count].astype(f32).reshape(-1, parts, shard, width // parts)
        grad_down = jnp.swapaxes(grad_down, 1, 2).reshape(-1, width)
        at += count
        grad_query, grad_key, grad_value, grad_out = [wide(width) for _ in range(4)]
        return (
            block_out[:, None],
            grad_hidden.astype(f32)[:, None],
            grad_query,
            grad_key,
            grad_value,
            grad_out,
            grad_up,
            grad_down,
            *small,
        )

    return local


def solution(mesh):
    tokens = P(None, "wshard", "ctx", None)
    in_specs = (
        tokens,
        tokens,
        P(None, "wshard", None),
        tokens,
        *[P("wshard", None)] * 6,
        *[P("wshard")] * 9,
    )
    out_specs = (tokens, tokens, *[P("wshard", None)] * 6, *[P("wshard")] * 9)
    return jax.shard_map(
        make_local(mesh.shape["ctx"], mesh.shape["wshard"]),
        mesh=mesh,
        in_specs=in_specs,
        out_specs=out_specs,
        check_vma=False,
    )
```

```python
import functools
import heapq
import math

import jax
import jax.numpy as jnp
from jax import lax
from jax.experimental import pallas as pl
from jax.experimental.pallas import tpu as pltpu
from jax.sharding import PartitionSpec as P

HEADS = 12
HEAD_DIM = 64
BLOCK = 64
MICRO = 2
GROUP = 4
LANES = GROUP * HEAD_DIM
CANDS = 8

masked_score = -1e30
norm_eps = 1e-12
score_scale = 1.0 / math.sqrt(HEAD_DIM)
bf16 = jnp.bfloat16
f32 = jnp.float32
MESH = pl.DeviceIdType.MESH


def layer_norm(values, ln_gain, ln_shift):
    center = values - jnp.mean(values, axis=-1, keepdims=True)
    spread = jnp.mean(center * center, axis=-1, keepdims=True)
    return center * lax.rsqrt(spread + norm_eps) * ln_gain + ln_shift


def candidates(blocks, lengths, chosen_raw):
    doc_ends = jnp.cumsum(lengths)
    doc_starts = doc_ends - lengths
    owner_doc = jnp.sum((blocks[:, None] >= doc_ends[None, :]).astype(jnp.int32), axis=1)
    doc_ids = jnp.arange(lengths.shape[0], dtype=jnp.int32)
    member = (owner_doc[:, None] == doc_ids[None, :]).astype(jnp.int32)
    doc_first = jnp.sum(member * doc_starts[None, :], axis=1)
    length = jnp.sum(member * lengths[None, :], axis=1)
    randoms = doc_first[:, None] + chosen_raw % length[:, None]
    columns = [blocks, blocks - 1, blocks + 1, doc_first, doc_first + 1]
    for column in range(chosen_raw.shape[1]):
        columns.append(randoms[:, column])
    chosen = jnp.stack(columns, axis=1)
    inside = (chosen >= doc_first[:, None]) & (chosen < (doc_first + length)[:, None])
    is_fresh = [jnp.ones(blocks.shape, dtype=jnp.bool_)]
    for column in range(1, chosen.shape[1]):
        is_fresh.append(jnp.all(chosen[:, :column] != chosen[:, column : column + 1], axis=1))
    allowed = inside & jnp.stack(is_fresh, axis=1)
    safe_blocks = jnp.where(allowed, chosen, blocks[:, None])
    return (safe_blocks, allowed)


def dot_nt(a, b):
    return lax.dot_general(a, b, (((1,), (1,)), ((), ())), preferred_element_type=f32)


def dot_nn(a, b):
    return lax.dot_general(a, b, (((1,), (0,)), ((), ())), preferred_element_type=f32)


def dot_tn(a, b):
    return lax.dot_general(a, b, (((0,), (0,)), ((), ())), preferred_element_type=f32)


def spread_heads(rows, head_of_lane):
    zero = jnp.zeros_like(rows)
    return jnp.concatenate([jnp.where(head_of_lane == h, rows, zero) for h in range(GROUP)], axis=0)


def pick_heads(rows, head_of_lane):
    total = jnp.zeros((BLOCK, LANES), f32)
    for h in range(GROUP):
        total = jnp.where(head_of_lane == h, rows[h * BLOCK : (h + 1) * BLOCK], total)
    return total


def attend_kernel(groups, width, pos_ref, q_ref, bias_ref, kv_ref, ctx_ref, probs_ref, cat):
    i = pl.program_id(0)
    for j in range(CANDS):
        start = pl.multiple_of(pos_ref[i * CANDS + j] * BLOCK, BLOCK)
        cat[j * BLOCK : (j + 1) * BLOCK, :] = kv_ref[pl.ds(start, BLOCK), :]
    head_of_lane = lax.broadcasted_iota(jnp.int32, (BLOCK, LANES), 1) // HEAD_DIM
    bias = bias_ref[0]
    for g in range(groups):
        lanes = slice(g * LANES, (g + 1) * LANES)
        v_lanes = slice(width + g * LANES, width + (g + 1) * LANES)
        q_all = spread_heads(q_ref[:, lanes], head_of_lane)
        scores = dot_nt(q_all, cat[:, lanes]) + bias
        row_max = jnp.max(scores, axis=-1, keepdims=True)
        shifted = jnp.exp(scores - row_max)
        row_total = jnp.sum(shifted, axis=-1, keepdims=True)
        probs = (shifted * (1.0 / row_total)).astype(bf16)
        probs_ref[0, g] = probs
        mixed = dot_nn(probs, cat[:, v_lanes])
        ctx_ref[:, lanes] = pick_heads(mixed, head_of_lane).astype(bf16)


def attend(pos, queries, bias, kv):
    rows, width = queries.shape
    blocks = rows // BLOCK
    groups = width // LANES
    keys = CANDS * BLOCK
    return pl.pallas_call(
        functools.partial(attend_kernel, groups, width),
        grid_spec=pltpu.PrefetchScalarGridSpec(
            num_scalar_prefetch=1,
            grid=(blocks,),
            in_specs=[
                pl.BlockSpec((BLOCK, width), lambda i, p: (i, 0)),
                pl.BlockSpec((1, 1, keys), lambda i, p: (i, 0, 0)),
                pl.BlockSpec(kv.shape, lambda i, p: (0, 0), pipeline_mode=pl.Buffered(1)),
            ],
            out_specs=[
                pl.BlockSpec((BLOCK, width), lambda i, p: (i, 0)),
                pl.BlockSpec((1, groups, GROUP * BLOCK, keys), lambda i, p: (i, 0, 0, 0)),
            ],
            scratch_shapes=[pltpu.VMEM((keys, 2 * width), bf16)],
        ),
        out_shape=[
            jax.ShapeDtypeStruct((rows, width), bf16),
            jax.ShapeDtypeStruct((blocks, groups, GROUP * BLOCK, keys), bf16),
        ],
        compiler_params=pltpu.CompilerParams(vmem_limit_bytes=48 << 20),
        cost_estimate=pl.CostEstimate(
            flops=blocks * groups * 4 * GROUP * BLOCK * keys * LANES,
            bytes_accessed=kv.size * 2 + rows * width * 4 + blocks * groups * GROUP * BLOCK * keys * 2,
            transcendentals=blocks * groups * GROUP * BLOCK * keys,
        ),
        name="attend",
    )(pos, queries, bias, kv)


def attend_back_kernel(
    groups, width, pos_ref, q_ref, dctx_ref, probs_ref, kv_ref, dq_ref, dkv_ref, cat, acc
):
    i = pl.program_id(0)

    @pl.when(i == 0)
    def _():
        acc[...] = jnp.zeros_like(acc)

    for j in range(CANDS):
        start = pl.multiple_of(pos_ref[i * CANDS + j] * BLOCK, BLOCK)
        cat[j * BLOCK : (j + 1) * BLOCK, :] = kv_ref[pl.ds(start, BLOCK), :]
    head_of_lane = lax.broadcasted_iota(jnp.int32, (BLOCK, LANES), 1) // HEAD_DIM
    for g in range(groups):
        lanes = slice(g * LANES, (g + 1) * LANES)
        v_lanes = slice(width + g * LANES, width + (g + 1) * LANES)
        q_all = spread_heads(q_ref[:, lanes], head_of_lane)
        d_all = spread_heads(dctx_ref[:, lanes], head_of_lane)
        probs_low = probs_ref[0, g]
        probs = probs_low.astype(f32)
        d_probs = dot_nt(d_all, cat[:, v_lanes])
        row_inner = jnp.sum(probs * d_probs, axis=-1, keepdims=True)
        d_scores = (probs * (d_probs - row_inner)).astype(bf16)
        dq_ref[:, lanes] = pick_heads(dot_nn(d_scores, cat[:, lanes]), head_of_lane).astype(bf16)
        d_key = dot_tn(d_scores, q_all)
        d_value = dot_tn(probs_low, d_all)
        for j in range(CANDS):
            start = pl.multiple_of(pos_ref[i * CANDS + j] * BLOCK, BLOCK)
            part = slice(j * BLOCK, (j + 1) * BLOCK)
            acc[pl.ds(start, BLOCK), lanes] += d_key[part]
            acc[pl.ds(start, BLOCK), v_lanes] += d_value[part]

    @pl.when(i == pl.num_programs(0) - 1)
    def _():
        dkv_ref[...] = acc[...].astype(bf16)


def attend_back(pos, queries, d_context, probs, kv):
    rows, width = queries.shape
    blocks = rows // BLOCK
    groups = width // LANES
    keys = CANDS * BLOCK
    return pl.pallas_call(
        functools.partial(attend_back_kernel, groups, width),
        grid_spec=pltpu.PrefetchScalarGridSpec(
            num_scalar_prefetch=1,
            grid=(blocks,),
            in_specs=[
                pl.BlockSpec((BLOCK, width), lambda i, p: (i, 0)),
                pl.BlockSpec((BLOCK, width), lambda i, p: (i, 0)),
                pl.BlockSpec((1, groups, GROUP * BLOCK, keys), lambda i, p: (i, 0, 0, 0)),
                pl.BlockSpec(kv.shape, lambda i, p: (0, 0), pipeline_mode=pl.Buffered(1)),
            ],
            out_specs=[
                pl.BlockSpec((BLOCK, width), lambda i, p: (i, 0)),
                pl.BlockSpec(kv.shape, lambda i, p: (0, 0), pipeline_mode=pl.Buffered(1)),
            ],
            scratch_shapes=[pltpu.VMEM((keys, 2 * width), bf16), pltpu.VMEM(kv.shape, f32)],
        ),
        out_shape=[
            jax.ShapeDtypeStruct((rows, width), bf16),
            jax.ShapeDtypeStruct(kv.shape, bf16),
        ],
        compiler_params=pltpu.CompilerParams(vmem_limit_bytes=60 << 20),
        cost_estimate=pl.CostEstimate(
            flops=blocks * groups * 8 * GROUP * BLOCK * keys * LANES,
            bytes_accessed=kv.size * 4 + rows * width * 6 + blocks * groups * GROUP * BLOCK * keys * 2,
            transcendentals=0,
        ),
        name="attend_back",
    )(pos, queries, d_context, probs, kv)


class Wires:
    def __init__(self, ctx_size, w_size):
        self.ctx_size, self.w_size = ctx_size, w_size
        self.lines = ctx_size // 4
        self.pairs = w_size // 2
        self.ctx = lax.axis_index("ctx")
        self.w = lax.axis_index("wshard")
        self.part = self.ctx // self.lines
        self.line = self.ctx % self.lines
        self.pair = self.w // 2
        self.core = self.w % 2

    def at(self, part, line, pair, core):
        return (part * self.lines + line, pair * 2 + core)

    @property
    def core_peer(self):
        return self.at(self.part, self.line, self.pair, 1 - self.core)

    def pair_peer(self, flip):
        return self.at(self.part, self.line, self.pair ^ flip, self.core)

    def line_peer(self, flip):
        return self.at(self.part, self.line ^ flip, self.pair, self.core)

    def part_peer(self, flip):
        return self.at(self.part ^ flip, self.line, self.pair, self.core)

    def move(self, value, to):
        perm = []
        for ctx in range(self.ctx_size):
            for w in range(self.w_size):
                part, line, pair, core = to(ctx // self.lines, ctx % self.lines, w // 2, w % 2)
                target = (part * self.lines + line) * self.w_size + pair * 2 + core
                perm.append((ctx * self.w_size + w, target))
        return lax.ppermute(value, ("ctx", "wshard"), perm)

    def to_core(self, value):
        return self.move(value, lambda part, line, pair, core: (part, line, pair, 1 - core))

    def to_pair(self, value, flip):
        return self.move(value, lambda part, line, pair, core: (part, line, pair ^ flip, core))

    def to_line(self, value, flip):
        return self.move(value, lambda part, line, pair, core: (part, line ^ flip, pair, core))

    def to_part(self, value, flip):
        return self.move(value, lambda part, line, pair, core: (part ^ flip, line, pair, core))

    def deal(self, value, turn):
        return self.move(
            value,
            lambda part, line, pair, core: (2 * ((turn + part) % 2) + core, line, pair, part // 2),
        )

    def deal_back(self, value, turn):
        return self.move(
            value,
            lambda part, line, pair, core: (2 * core + (part // 2 + turn) % 2, line, pair, part % 2),
        )


def bits(count):
    flips = []
    flip = 1
    while flip < count:
        flips.append(flip)
        flip *= 2
    return flips


def gather_kernel(wires_of, refs, outs, own_shards, local_sem, send_sem, recv_sem):
    hidden, out_grad, ints, vectors, w_query, w_key, w_value, w_out, w_up, w_down = refs
    rows_out, grads_out, ints_out, vectors_out, query_out, kv_out, out_out, up_out, down_out = outs
    here = wires_of()
    lines, pairs = here.lines, here.pairs
    part, line, pair, core = here.part, here.line, here.pair, here.core
    width = w_query.shape[1]
    used = [0]
    sent = []
    local = []
    placed = []

    def at(part, line, pair, core):
        return (part * lines + line, pair * 2 + core)

    core_peer = at(part, line, pair, 1 - core)

    def line_peer(flip):
        return at(part, line ^ flip, pair, core)

    def pair_peer(flip):
        return at(part, line, pair ^ flip, core)

    def deal_target(turn):
        return at(2 * ((turn + part) % 2) + core, line, pair, part // 2)

    def deal_source(turn):
        return at(2 * core + (part // 2 + turn) % 2, line, pair, part % 2)

    stays = [
        jnp.logical_and(
            2 * ((turn + part) % 2) + core == part, part // 2 == core
        )
        for turn in range(2)
    ]

    barrier = pltpu.get_barrier_semaphore()

    def greet(device):
        pl.semaphore_signal(barrier, inc=1, device_id=device, device_id_type=MESH)

    peers = [core_peer]
    peers += [line_peer(flip) for flip in range(1, lines)]
    peers += [pair_peer(flip) for flip in range(1, pairs)]
    for device in peers:
        greet(device)
    for turn in range(2):

        @pl.when(jnp.logical_not(stays[turn]))
        def _(turn=turn):
            greet(deal_target(turn))
            greet(deal_source(turn))

    staying = sum(stay.astype(jnp.int32) for stay in stays)
    pl.semaphore_wait(barrier, len(peers) + 4 - 2 * staying)

    def send(src, dst, device, stay=None):
        n = used[0]
        used[0] += 1
        copy = pltpu.make_async_remote_copy(
            src_ref=src,
            dst_ref=dst,
            send_sem=send_sem.at[n],
            recv_sem=recv_sem.at[n],
            device_id=device,
            device_id_type=MESH,
        )
        if stay is None:
            copy.start()
        else:

            @pl.when(stay)
            def _():
                pltpu.make_async_copy(src, dst, recv_sem.at[n]).start()

            @pl.when(jnp.logical_not(stay))
            def _():
                copy.start()

        sent.append((copy, stay))
        return copy

    def stage(src, held):
        copy = pltpu.make_async_copy(src, held, local_sem.at[len(local)])
        copy.start()
        local.append(copy)

    def place_held(held, dst):
        local[len(placed)].wait()
        copy = pltpu.make_async_copy(held, dst, local_sem.at[len(local) + len(placed)])
        copy.start()
        placed.append(copy)

    me = pair * 2 + core

    dealt = [
        send(
            hidden.at[(turn + part) % 2, 0],
            rows_out.at[turn],
            deal_target(turn),
            stays[turn],
        )
        for turn in range(2)
    ]

    matrices = [
        (w_up, lambda shard: up_out.at[shard], True),
        (w_down, lambda shard: down_out.at[shard], True),
        (w_query, lambda shard: query_out.at[shard], False),
        (w_key, lambda shard: kv_out.at[shard, :, :width], False),
        (w_value, lambda shard: kv_out.at[shard, :, width:], False),
        (w_out, lambda shard: out_out.at[shard], False),
        (vectors, lambda shard: vectors_out.at[shard], False),
    ]
    side = line % 2
    for (src, _, _), held in zip(matrices, own_shards):
        stage(src, held)

    def half_cuts(src):
        half = src.shape[0] // 2
        first = pl.ds(pl.multiple_of(side * half, 8), half)
        return first, pl.ds(pl.multiple_of((1 - side) * half, 8), half)

    halves = [
        (
            flip,
            src,
            place,
            send(src.at[half_cuts(src)[0]], place(me).at[half_cuts(src)[0]], pair_peer(flip)),
        )
        for src, place, split in matrices
        if split
        for flip in range(1, pairs)
    ]
    late = [
        send(ints.at[(turn + part) % 2], ints_out.at[turn], deal_target(turn), stays[turn])
        for turn in range(2)
    ]
    for src, place, _ in matrices:
        late.append(send(src, place(me), core_peer))

    crossed = []
    for turn in range(2):
        dealt[turn].wait_recv()
        for flip in range(1, lines):
            crossed.append(
                (
                    flip * 2 + turn,
                    send(rows_out.at[turn], rows_out.at[flip * 2 + turn], line_peer(flip)),
                )
            )
        late.append(send(rows_out.at[turn], rows_out.at[lines * 2 + turn], core_peer))
    for (src, place, _), held in zip(matrices, own_shards):
        place_held(held, place(me))

    relayed = []
    whole = [
        (src, place, flip)
        for src, place, split in matrices
        if not split
        for flip in range(1, pairs)
    ]
    direct = []
    for step, (flip, src, place, copy) in enumerate(halves):
        copy.wait_recv()
        first, second = half_cuts(src)
        shard = (pair ^ flip) * 2 + core
        got = place(shard).at[first]
        relayed.append((place(shard).at[second], send(got, got, line_peer(1))))
        late.append(send(got, got, core_peer))
        share = -(-len(whole) // len(halves))
        for src, place, flip in whole[step * share : (step + 1) * share]:
            direct.append((flip, place, send(src, place(me), pair_peer(flip))))
    late += [
        send(
            out_grad.at[(turn + part) % 2, 0],
            grads_out.at[turn],
            deal_target(turn),
            stays[turn],
        )
        for turn in range(2)
    ]
    for index, copy in crossed:
        copy.wait_recv()
        late.append(send(rows_out.at[index], rows_out.at[lines * 2 + index], core_peer))
    for flip, place, copy in direct:
        copy.wait_recv()
        shard = (pair ^ flip) * 2 + core
        late.append(send(place(shard), place(shard), core_peer))
    for got, copy in relayed:
        copy.wait_recv()
        late.append(send(got, got, core_peer))
    for copy in late:
        copy.wait_recv()
    for copy in placed:
        copy.wait()
    for copy, stay in sent:
        if stay is None:
            copy.wait_send()
        else:

            @pl.when(jnp.logical_not(stay))
            def _(copy=copy):
                copy.wait_send()


def gather_all(ctx_size, w_size, hidden, out_grad, ints, vectors, weights):
    w_query, w_key, w_value, w_out, w_up, w_down = weights
    lines, pairs = ctx_size // 4, w_size // 2
    tok, width = hidden.shape[2], hidden.shape[3]
    rows = w_query.shape[0]
    shapes = [
        ((lines * 4, tok, width), bf16),
        ((2, tok, width), bf16),
        (ints.shape, ints.dtype),
        ((w_size,) + vectors.shape, bf16),
        ((w_size, rows, width), bf16),
        ((w_size, rows, 2 * width), bf16),
        ((w_size, rows, width), bf16),
        ((w_size,) + w_up.shape, bf16),
        ((w_size,) + w_down.shape, bf16),
    ]
    sems = 16 + 8 * lines + 20 * pairs

    def body(*refs):
        gather_kernel(
            lambda: Wires(ctx_size, w_size), refs[:10], refs[10:19], refs[19:26], *refs[26:]
        )

    return pl.pallas_call(
        body,
        in_specs=[pl.BlockSpec(memory_space=pl.ANY)] * 10,
        out_specs=[pl.BlockSpec(memory_space=pl.ANY)] * len(shapes),
        out_shape=[jax.ShapeDtypeStruct(shape, dtype) for shape, dtype in shapes],
        scratch_shapes=[
            *[
                pltpu.VMEM(shard.shape, bf16)
                for shard in (w_up, w_down, w_query, w_key, w_value, w_out, vectors)
            ],
            pltpu.SemaphoreType.DMA((14,)),
            pltpu.SemaphoreType.DMA((sems,)),
            pltpu.SemaphoreType.DMA((sems,)),
        ],
        compiler_params=pltpu.CompilerParams(collective_id=0, has_side_effects=True),
        name="gather_all",
    )(hidden, out_grad, ints, vectors, w_query, w_key, w_value, w_out, w_up, w_down)


class Sent:
    def __init__(self, make, stay=None):
        self.make, self.stay = make, stay

    def wait(self):
        self.make().wait()

    def wait_recv(self):
        self.make().wait_recv()


class Copies:
    def __init__(self, local_sem, send_sem, recv_sem):
        self.local_sem, self.send_sem, self.recv_sem = local_sem, send_sem, recv_sem
        self.locals, self.sent = 0, []

    def load(self, pair):
        n = self.locals
        self.locals += 1
        copy = Sent(lambda: pltpu.make_async_copy(*pair(), self.local_sem.at[n]))
        copy.make().start()
        return copy

    def send(self, triple, stay=None):
        n = len(self.sent)

        def make():
            src, dst, device = triple()
            return pltpu.make_async_remote_copy(
                src_ref=src,
                dst_ref=dst,
                send_sem=self.send_sem.at[n],
                recv_sem=self.recv_sem.at[n],
                device_id=device,
                device_id_type=MESH,
            )

        if stay is None:
            make().start()
        else:

            @pl.when(stay)
            def _():
                src, dst, _ = triple()
                pltpu.make_async_copy(src, dst, self.recv_sem.at[n]).start()

            @pl.when(jnp.logical_not(stay))
            def _():
                make().start()

        copy = Sent(make, stay)
        self.sent.append(copy)
        return copy

    def finish(self):
        for copy in self.sent:
            if copy.stay is None:
                copy.make().wait_send()
            else:

                @pl.when(jnp.logical_not(copy.stay))
                def _(copy=copy):
                    copy.make().wait_send()


def add_blocks(dst, *srcs):
    if len(dst.shape) == 3:

        def each(i, carry):
            total = srcs[0][i].astype(f32)
            for src in srcs[1:]:
                total = total + src[i].astype(f32)
            dst[i] = total.astype(dst.dtype)
            return carry

        lax.fori_loop(0, dst.shape[0], each, 0)
        return
    rows = dst.shape[0]
    step = 48 if rows % 48 == 0 else 32

    def body(i, carry):
        cut = pl.ds(pl.multiple_of(i * step, step), step)
        total = srcs[0][cut, :].astype(f32)
        for src in srcs[1:]:
            total = total + src[cut, :].astype(f32)
        dst[cut, :] = total.astype(dst.dtype)
        return carry

    lax.fori_loop(0, rows // step, body, 0)


class Events:
    def __init__(self):
        self.items = []

    def add(self, time, action):
        self.items.append((time, len(self.items), action))

    def take(self, until):
        due = sorted([item for item in self.items if item[0] <= until], key=lambda item: item[:2])
        self.items = [item for item in self.items if item[0] > until]
        return [action for _, _, action in due]

    def run(self, until=math.inf):
        for action in self.take(until):
            action()


class Plan:
    def __init__(self, events):
        self.events, self.heap, self.free, self.count = events, [], {}, 0

    def at(self, time, action):
        heapq.heappush(self.heap, (time, self.count, action))
        self.count += 1

    def do(self, time, action):
        self.events.add(time, action)

    def send(self, link, time, length, then):
        def start(now):
            begin = max(now, self.free.get(link, 0.0))
            self.free[link] = begin + length
            self.at(begin + length + 2.0, then)

        self.at(time, start)

    def run(self):
        while self.heap:
            time, _, action = heapq.heappop(self.heap)
            action(time)


def group_scratch(lines, pairs, rows, columns):
    block = (rows, columns)
    return [
        pltpu.VMEM((2 * lines, pairs) + block, bf16),
        pltpu.VMEM((2 * lines, pairs) + block, bf16),
        pltpu.VMEM((2 * lines, max(pairs - 1, 1)) + block, bf16),
        pltpu.VMEM((2 * lines,) + block, bf16),
        pltpu.VMEM((2, max(lines - 1, 1)) + block, bf16),
        pltpu.VMEM((2,) + block, bf16),
        pltpu.VMEM((2,) + block, bf16),
        pltpu.VMEM((2,) + block, bf16),
    ]


GROUP_SCRATCH = 8
BACK_GROUPS = 6


def reduce_group(here, copies, plan, chunks, scratch, out, base, unit, core_times):
    from_core, own, from_pairs, paired, from_lines, lined, from_parts, parted = scratch
    lines, pairs = here.lines, here.pairs
    line, pair, core, part = here.line, here.pair, here.core, here.part
    low_part = part % 2
    state = {}

    def to_core(i, view):
        state["core", i] = copies.send(lambda: (view(), from_core.at[i], here.core_peer))

    def begin(i):
        to_core(i, lambda: chunks[i](1 - core))
        state["own", i] = copies.load(lambda: (chunks[i](core), own.at[i]))

    def over_core(i):
        if ("own", i) in state:
            state["own", i].wait()
        state["core", i].wait_recv()
        for p in range(pairs):
            add_blocks(own.at[i, p], own.at[i, p], from_core.at[i, p])
        state["pair", i] = [
            copies.send(
                lambda flip=flip: (
                    own.at[i, pair ^ flip],
                    from_pairs.at[i, flip - 1],
                    here.pair_peer(flip),
                )
            )
            for flip in range(1, pairs)
        ]

    def over_pairs(i):
        for copy in state["pair", i]:
            copy.wait_recv()
        add_blocks(
            paired.at[i], own.at[i, pair], *[from_pairs.at[i, flip - 1] for flip in range(1, pairs)]
        )

    def to_lines(h):
        state["line", h] = [
            copies.send(
                lambda flip=flip: (
                    paired.at[h * lines + (line ^ flip)],
                    from_lines.at[h, flip - 1],
                    here.line_peer(flip),
                )
            )
            for flip in range(1, lines)
        ]

    def over_lines(h):
        for copy in state["line", h]:
            copy.wait_recv()
        add_blocks(
            lined.at[h],
            paired.at[h * lines + line],
            *[from_lines.at[h, flip - 1] for flip in range(1, lines)],
        )

    def to_part_one():
        state["one"] = copies.send(
            lambda: (lined.at[1 - low_part], from_parts.at[0], here.part_peer(1))
        )

    def over_part_one():
        state["one"].wait_recv()
        add_blocks(parted.at[0], lined.at[low_part], from_parts.at[0])
        state["two"] = copies.send(lambda: (parted.at[0], from_parts.at[1], here.part_peer(2)))

    def mine():
        return out.at[base + low_part * lines + line]

    def other():
        return out.at[base + (1 - low_part) * lines + line]

    def over_part_two():
        state["two"].wait_recv()
        add_blocks(parted.at[1], parted.at[0], from_parts.at[1])
        state["back"] = copies.send(lambda: (parted.at[1], mine(), here.part_peer(1)))
        state["place"] = copies.load(lambda: (parted.at[1], mine()))
        state["spread"] = [
            copies.send(lambda flip=flip: (parted.at[1], mine(), here.line_peer(flip)))
            for flip in range(1, lines)
        ]

    def spread_other():
        state["back"].wait_recv()
        state["spread"] += [
            copies.send(lambda flip=flip: (other(), other(), here.line_peer(flip)))
            for flip in range(1, lines)
        ]

    def end():
        state["place"].wait()
        for copy in state["spread"]:
            copy.wait_recv()

    lined_h = []

    def core_done(i, now):
        plan.do(now, functools.partial(over_core, i))
        plan.send("x", now + 0.7, (pairs - 1) * unit, functools.partial(pairs_done, i))

    def pairs_done(i, now):
        plan.do(now, functools.partial(over_pairs, i))
        if i % lines == lines - 1:
            h = i // lines
            plan.do(now + 0.01, functools.partial(to_lines, h))
            plan.send("y", now + 0.3, (lines - 1) * unit, functools.partial(lines_done, h))

    def lines_done(h, now):
        plan.do(now, functools.partial(over_lines, h))
        lined_h.append(h)
        if len(lined_h) == 2:
            plan.do(now + 0.01, to_part_one)
            plan.send("z", now + 0.3, unit, one_done)

    def one_done(now):
        plan.do(now, over_part_one)
        plan.send("z", now + 0.3, 2 * unit, two_done)

    def two_done(now):
        plan.do(now, over_part_two)
        plan.send("z", now + 0.3, unit, back_done)
        plan.send("y", now + 0.3, (lines - 1) * unit, lambda now: None)

    def back_done(now):
        plan.do(now, spread_other)
        plan.send("y", now + 0.1, (lines - 1) * unit, lambda now: None)

    for i in range(2 * lines):
        if chunks[i] is not None:
            plan.do(core_times[i - 2] + 0.01 if i >= 2 else -100.0, functools.partial(begin, i))
        plan.at(core_times[i], functools.partial(core_done, i))
    plan.do(10000.0, end)
    return to_core


def chunk_views(refs, kinds, width):
    views = []
    for ref, kind in zip(refs, kinds):
        if kind == "wide":
            for c in range(ref.shape[3] // width):
                views.append(
                    lambda core, ref=ref, cut=slice(c * width, (c + 1) * width): ref.at[
                        :, core, :, cut
                    ]
                )
        else:
            for b in range(ref.shape[2]):
                for c in range(ref.shape[4] // width):
                    views.append(
                        lambda core, ref=ref, b=b, cut=slice(c * width, (c + 1) * width): ref.at[
                            :, core, b, :, cut
                        ]
                    )
    return views


def finish_kernel(ctx_size, w_size, kinds, tables, *refs):
    here = Wires(ctx_size, w_size)
    lines, pairs = here.lines, here.pairs
    part, line, pair, core = here.part, here.line, here.pair, here.core
    terms = refs[: len(kinds)]
    through, near, final, table = refs[len(kinds) : len(kinds) + 4]
    at = len(kinds) + 4
    out, final_out, grad_out, table_out = refs[at : at + 4]
    at += 4
    groups = (len(refs) - at - 8) // GROUP_SCRATCH
    scratches = [
        refs[at + g * GROUP_SCRATCH : at + (g + 1) * GROUP_SCRATCH] for g in range(groups)
    ]
    at += groups * GROUP_SCRATCH
    g_core, g_own, g_line, g_near, g_sum, table_in, table_sum = refs[at : at + 7]
    copies = Copies(*refs[at + 7])
    micro = part // 2

    def back_target(turn):
        return here.at(2 * core + (micro + turn) % 2, line, pair, part % 2)

    def back_source(turn):
        return here.at(2 * ((turn + part) % 2) + core, line, pair, part // 2)

    stays = [
        jnp.logical_and(2 * core + (micro + turn) % 2 == part, part % 2 == core)
        for turn in range(2)
    ]
    barrier = pltpu.get_barrier_semaphore()

    def greet(device):
        pl.semaphore_signal(barrier, inc=1, device_id=device, device_id_type=MESH)

    peers = [here.core_peer, here.part_peer(1), here.part_peer(2)]
    peers += [here.line_peer(flip) for flip in range(1, lines)]
    peers += [here.pair_peer(flip) for flip in range(1, pairs)]
    for device in peers:
        greet(device)
    for turn in range(2):

        @pl.when(jnp.logical_not(stays[turn]))
        def _(turn=turn):
            greet(back_target(turn))
            greet(back_source(turn))

    staying = sum(stay.astype(jnp.int32) for stay in stays)
    pl.semaphore_wait(barrier, len(peers) + 4 - 2 * staying)

    events = Events()
    state = {}
    count = 2 * lines

    def begin_rows():
        state["core"] = [
            copies.send(lambda j=j: (through.at[count + j], g_core.at[j], here.core_peer))
            for j in range(count)
        ]
        state["own"] = [
            copies.load(lambda j=j: (through.at[j], g_own.at[j])) for j in range(count)
        ]
        state["near"] = copies.load(lambda: (near, g_near))
        state["out"] = [
            copies.send(
                lambda turn=turn: (final.at[turn], final_out.at[micro], back_target(turn)),
                stays[turn],
            )
            for turn in range(2)
        ]

    def rows_over_core():
        for j in reversed(range(count)):
            state["own"][j].wait()
            state["core"][j].wait_recv()
            add_blocks(g_own.at[j], g_own.at[j], g_core.at[j])
            if j >= 2:
                state["line", j] = copies.send(
                    lambda j=j: (g_own.at[j], g_line.at[j - 2], here.line_peer(j // 2))
                )

    def rows_over_lines():
        state["near"].wait()
        state["back"] = []
        for turn in range(2):
            others = []
            for flip in range(1, lines):
                state["line", 2 * flip + turn].wait_recv()
                others.append(g_line.at[2 * flip + turn - 2])
            add_blocks(g_sum.at[turn], g_near.at[turn], g_own.at[turn], *others)
            state["back"].append(
                copies.send(
                    lambda turn=turn: (g_sum.at[turn], grad_out.at[micro], back_target(turn)),
                    stays[turn],
                )
            )

    def end_rows():
        for copy in state["out"] + state["back"]:
            copy.wait_recv()

    steps = [here.core_peer]
    steps += [here.pair_peer(flip) for flip in bits(pairs)]
    steps += [here.line_peer(flip) for flip in bits(lines)]
    steps += [here.part_peer(flip) for flip in bits(4)]

    def table_send(n):
        src = table if n == 0 else table_sum.at[n - 1]
        state["table", n] = copies.send(lambda: (src, table_in.at[n], steps[n]))

    def table_step(n):
        state["table", n].wait_recv()
        before = table[...] if n == 0 else table_sum[n - 1]
        total = before + table_in[n]
        if n + 1 < len(steps):
            table_sum[n] = total
            table_send(n + 1)
        else:
            table_out[...] = total

    plan = Plan(events)
    events.add(-1001.0, begin_rows)
    events.add(-1000.5, lambda: table_send(0))
    events.add(0.5, rows_over_core)
    events.add(17.0, rows_over_lines)
    events.add(9000.0, end_rows)
    for n in range(len(steps)):
        events.add(2.5 + n * 6.0, functools.partial(table_step, n))
    views = chunk_views(terms, kinds, out.shape[2])
    size = 2 * lines
    for g in range(groups):
        reduce_group(
            here,
            copies,
            plan,
            views[g * size : (g + 1) * size],
            scratches[g],
            out,
            g * size,
            6.0,
            [2.0 + 1.5 * (g * size + i) for i in range(size)],
        )
    plan.run()
    events.run()
    copies.finish()


def finish_all(ctx_size, w_size, terms, kinds, through, near, final, table):
    lines, pairs = ctx_size // 4, w_size // 2
    count = 2 * lines
    tok, width = through.shape[1:]
    rows = width // w_size
    columns = width // (lines // 2)
    chunks = sum(term.size for term in terms) // (w_size * rows * columns)
    groups = chunks // (2 * lines)
    table_steps = 1 + len(bits(pairs)) + len(bits(lines)) + len(bits(4))
    block = (tok, width)
    any_space = pl.BlockSpec(memory_space=pl.ANY)
    in_vmem = pl.BlockSpec(memory_space=pltpu.VMEM)
    sems = 40 + 10 * lines + groups * 2 * lines * (6 + pairs)
    scratch = []
    for _ in range(groups):
        scratch += group_scratch(lines, pairs, rows, columns)
    scratch += [
        pltpu.VMEM((count,) + block, bf16),
        pltpu.VMEM((count,) + block, bf16),
        pltpu.VMEM((max(count - 2, 1),) + block, bf16),
        pltpu.VMEM((2,) + block, f32),
        pltpu.VMEM((2,) + block, bf16),
        pltpu.VMEM((table_steps,) + table.shape, f32),
        pltpu.VMEM((table_steps,) + table.shape, f32),
        (
            pltpu.SemaphoreType.DMA((sems,)),
            pltpu.SemaphoreType.DMA((sems,)),
            pltpu.SemaphoreType.DMA((sems,)),
        ),
    ]
    return pl.pallas_call(
        functools.partial(finish_kernel, ctx_size, w_size, kinds, table_steps),
        in_specs=[any_space] * (len(terms) + 3) + [in_vmem],
        out_specs=[any_space, any_space, any_space, in_vmem],
        out_shape=[
            jax.ShapeDtypeStruct((chunks, rows, columns), bf16),
            jax.ShapeDtypeStruct((2,) + block, bf16),
            jax.ShapeDtypeStruct((2,) + block, bf16),
            jax.ShapeDtypeStruct(table.shape, f32),
        ],
        scratch_shapes=scratch,
        compiler_params=pltpu.CompilerParams(
            collective_id=1, has_side_effects=True, vmem_limit_bytes=60 << 20
        ),
        name="finish_all",
    )(*terms, through, near, final, table)


def greet_all(here, back_target, back_source, stays):
    lines, pairs = here.lines, here.pairs
    barrier = pltpu.get_barrier_semaphore()

    def greet(device):
        pl.semaphore_signal(barrier, inc=1, device_id=device, device_id_type=MESH)

    peers = [here.core_peer, here.part_peer(1), here.part_peer(2)]
    peers += [here.line_peer(flip) for flip in range(1, lines)]
    peers += [here.pair_peer(flip) for flip in range(1, pairs)]
    for device in peers:
        greet(device)
    for turn in range(2):

        @pl.when(jnp.logical_not(stays[turn]))
        def _(turn=turn):
            greet(back_target(turn))
            greet(back_source(turn))

    staying = sum(stay.astype(jnp.int32) for stay in stays)
    pl.semaphore_wait(barrier, len(peers) + 4 - 2 * staying)


def back_kernel(ctx_size, w_size, *refs):
    here = Wires(ctx_size, w_size)
    lines, pairs = here.lines, here.pairs
    part, line, pair, core = here.part, here.line, here.pair, here.core
    micro = part // 2
    (
        pos,
        inv,
        table,
        queries,
        d_context,
        d_sum,
        probs,
        kv,
        rows_all,
        full_kv,
        full_query,
        final,
        term_up,
        term_down,
        term_out,
    ) = refs[:15]
    out, final_out, grad_out, table_out = refs[15:19]
    scratches = [
        refs[19 + g * GROUP_SCRATCH : 19 + (g + 1) * GROUP_SCRATCH] for g in range(BACK_GROUPS)
    ]
    (
        kv_buf,
        slots,
        cat,
        probs_buf,
        q_buf,
        dctx_buf,
        rows_buf,
        wq_buf,
        q_other,
        kv_other,
        g_near,
        g_core,
        g_line,
        g_sum,
        acc,
        value_sums,
        table_in,
        table_sum,
        probs_sem,
        sems,
    ) = refs[19 + BACK_GROUPS * GROUP_SCRATCH :]
    copies = Copies(*sems)
    own_tokens, width = q_buf.shape
    key_blocks = kv_buf.shape[0]
    tokens = key_blocks * BLOCK
    blocks = own_tokens // BLOCK
    piece = blocks // 2
    groups = width // LANES
    keys = CANDS * BLOCK
    shard = width // w_size
    half = width // 2

    def back_target(turn):
        return here.at(2 * core + (micro + turn) % 2, line, pair, part % 2)

    def back_source(turn):
        return here.at(2 * ((turn + part) % 2) + core, line, pair, part // 2)

    stays = [
        jnp.logical_and(2 * core + (micro + turn) % 2 == part, part % 2 == core)
        for turn in range(2)
    ]

    def fetch(i, slot):
        return pltpu.make_async_copy(probs.at[i], probs_buf.at[slot], probs_sem.at[slot])

    greet_all(here, back_target, back_source, stays)

    events = Events()
    state = {}
    count = 2 * lines

    w_kv = slots.at[pl.ds(0, width // BLOCK)]
    rows_from = 16
    all_rows = slots.at[pl.ds(rows_from, key_blocks), :, pl.ds(0, width)]
    through_from = rows_from + key_blocks

    def through_other(j):
        return slots.at[pl.ds(through_from + j * piece, piece), :, pl.ds(0, width)]

    def through_own(j):
        return slots.at[pl.ds(through_from + j * piece, piece), :, pl.ds(width, width)]

    def send_out():
        state["out"] = [
            copies.send(
                lambda turn=turn: (final.at[turn], final_out.at[micro], back_target(turn)),
                stays[turn],
            )
            for turn in range(2)
        ]

    def rows_over_core():
        for j in reversed(range(count)):
            state["through", j].wait_recv()
            add_blocks(through_own(j), through_own(j), g_core.at[j])
            if j >= 2:
                state["line", j] = copies.send(
                    lambda j=j: (through_own(j), g_line.at[j - 2], here.line_peer(j // 2))
                )

    def rows_over_lines():
        state["back"] = []
        for turn in range(2):
            others = []
            for flip in range(1, lines):
                state["line", 2 * flip + turn].wait_recv()
                others.append(g_line.at[2 * flip + turn - 2])
            add_blocks(
                g_sum.at[turn], g_near.at[pl.ds(turn * piece, piece)], through_own(turn), *others
            )
            state["back"].append(
                copies.send(
                    lambda turn=turn: (g_sum.at[turn], grad_out.at[micro], back_target(turn)),
                    stays[turn],
                )
            )

    def end_rows():
        for copy in state["out"] + state["back"]:
            copy.wait_recv()

    steps = [lambda: here.core_peer]
    steps += [lambda flip=flip: here.pair_peer(flip) for flip in bits(pairs)]
    steps += [lambda flip=flip: here.line_peer(flip) for flip in bits(lines)]
    steps += [lambda flip=flip: here.part_peer(flip) for flip in bits(4)]

    def table_send(n):
        state["table", n] = copies.send(lambda: (table_sum.at[n], table_in.at[n], steps[n]()))

    def table_step(n):
        state["table", n].wait_recv()
        total = table_sum[n] + table_in[n]
        if n + 1 < len(steps):
            table_sum[n + 1] = total
            table_send(n + 1)
        else:
            table_out[...] = total

    attend_at, attend_step = 9.0, 2.6
    gather_at = attend_at + blocks * attend_step + 3.0
    gather_step = 1.4
    through_at = gather_at + 8 * gather_step + 1.0
    through_step = 1.3
    terms_at = through_at + 8 * through_step
    terms_step = 2.6
    terms_end = terms_at + 4 * terms_step
    plan = Plan(events)
    plan.send("z", 0.0, 18.0, lambda now: None)

    views = chunk_views((term_up, term_down), ("wide", "tall"), half)
    size = 2 * lines
    ffn_groups = BACK_GROUPS - 2
    for g in range(ffn_groups):
        order = [g * size + i for i in range(size)]
        reduce_group(
            here,
            copies,
            plan,
            views[g * size : (g + 1) * size],
            scratches[g],
            out,
            g * size,
            3.0,
            [max(2.5 + 0.7 * n, 3.0 * n - 9.0) for n in order],
        )
    out_views = [
        lambda side, cut=slice(c * half, (c + 1) * half): term_out.at[:, side, :, cut]
        for c in range(2)
    ]
    q_own = scratches[ffn_groups][1]
    q_to_core = reduce_group(
        here,
        copies,
        plan,
        out_views + [None, None],
        scratches[ffn_groups],
        out,
        ffn_groups * size,
        3.0,
        [gather_at + 2.0 + 1.5 * i for i in range(4)],
    )
    kv_own = scratches[ffn_groups + 1][1]
    kv_to_core = reduce_group(
        here,
        copies,
        plan,
        [None] * 4,
        scratches[ffn_groups + 1],
        out,
        (ffn_groups + 1) * size,
        3.0,
        [terms_at + (i + 1) * terms_step + 1.5 for i in range(4)],
    )
    plan.do(-200.0, send_out)
    rows_at = through_at + 2 * count * through_step + 0.5

    def rows_done(now):
        plan.do(now, rows_over_lines)
        plan.send("z", now + 0.7, 18.0, lambda now: None)

    plan.do(rows_at, rows_over_core)
    plan.send("y", rows_at + 0.7, 18.0, rows_done)
    plan.do(9000.0, end_rows)
    for n in range(len(steps)):
        plan.do(through_at + 3.0 + n * 5.0, functools.partial(table_step, n))
    plan.run()

    def stepped(number, at, each, body):
        def loop(step, carry):
            body(step)
            for n in range(number):
                due = events.take(at + (n + 1) * each)
                if due:

                    @pl.when(step == n)
                    def _(due=due):
                        for action in due:
                            action()

            return carry

        lax.fori_loop(0, number, loop, 0)

    events.run(0.0)
    first = [
        copies.load(lambda: (kv, kv_buf)),
        copies.load(lambda: (queries, q_buf)),
        copies.load(lambda: (d_context, dctx_buf)),
    ]
    later = [
        copies.load(lambda: (rows_all.at[pl.ds(0, blocks)], rows_buf)),
        copies.load(lambda: (full_query, wq_buf)),
        copies.load(lambda: (d_sum, g_near)),
    ]

    fetch(0, 0).start()
    events.run(attend_at)
    for copy in first:
        copy.wait()
    slots[blocks * CANDS] = jnp.zeros((BLOCK, 2 * width), bf16)

    head_of_lane = lax.broadcasted_iota(jnp.int32, (BLOCK, LANES), 1) // HEAD_DIM

    def attend_block(i):
        slot = i % 2
        fetch(i, slot).wait()

        @pl.when(i + 1 < blocks)
        def _():
            fetch(i + 1, 1 - slot).start()

        for j in range(CANDS):
            cat[j * BLOCK : (j + 1) * BLOCK, :] = kv_buf[pos[i * CANDS + j]]
        mine = pl.ds(pl.multiple_of(i * BLOCK, BLOCK), BLOCK)
        rows = pl.ds(i * CANDS, CANDS)
        by_slot = (CANDS, BLOCK, LANES)
        for g in range(groups):
            lanes = slice(g * LANES, (g + 1) * LANES)
            v_lanes = slice(width + g * LANES, width + (g + 1) * LANES)
            q_all = spread_heads(q_buf[mine, lanes], head_of_lane)
            d_all = spread_heads(dctx_buf[mine, lanes], head_of_lane)
            probs_low = probs_buf[slot, g]
            shares = probs_low.astype(f32)
            d_probs = dot_nt(d_all, cat[:, v_lanes])
            row_inner = jnp.sum(shares * d_probs, axis=-1, keepdims=True)
            d_scores = (shares * (d_probs - row_inner)).astype(bf16)
            slots[rows, :, lanes] = dot_tn(d_scores, q_all).astype(bf16).reshape(by_slot)
            slots[rows, :, v_lanes] = dot_tn(probs_low, d_all).astype(bf16).reshape(by_slot)
            q_buf[mine, lanes] = pick_heads(dot_nn(d_scores, cat[:, lanes]), head_of_lane).astype(
                bf16
            )

    stepped(blocks, attend_at, attend_step, attend_block)

    for copy in later:
        copy.wait()
    for c in range(2):
        columns = slice(c * half, (c + 1) * half)
        own_rows = rows_buf[...].reshape(own_tokens, width)
        acc[...] = dot_tn(own_rows, q_buf[:, columns]) * score_scale
        for p in range(pairs):
            for side, place in ((core, q_own.at[2 + c, p]), (1 - core, q_other.at[c, p])):
                start = pl.multiple_of((2 * p + side) * shard, shard)
                place[...] = acc[pl.ds(start, shard), :].astype(bf16)
        q_to_core(2 + c, lambda c=c: q_other.at[c])

    def near_step(step, carry):
        cut = pl.ds(pl.multiple_of(step * BLOCK * 2, BLOCK * 2), BLOCK * 2)
        near = dot_nt(q_buf[cut, :], wq_buf[...]) * score_scale
        g_near[pl.ds(step * 2, 2)] += near.reshape(2, BLOCK, width)
        return carry

    lax.fori_loop(0, own_tokens // (BLOCK * 2), near_step, 0)
    value_sums[...] = jnp.zeros_like(value_sums)

    sub = value_sums.shape[0]

    def gather_some(step):
        def one(n, carry):
            block = step * (key_blocks // 8) + n

            named = [inv[block * blocks + i] for i in range(blocks)]
            for r in range(BLOCK // sub):
                cut = slice(r * sub, (r + 1) * sub)
                total = jnp.zeros((sub, 2 * width), f32)
                for i in range(blocks):
                    total = total + slots[named[i], cut, :].astype(f32)
                kv_buf[block, cut, :] = total.astype(bf16)
                value_sums[...] += total[:, width:]
            return carry

        lax.fori_loop(0, key_blocks // 8, one, 0)

    stepped(8, gather_at, gather_step, gather_some)
    weights = copies.load(lambda: (full_kv, w_kv))
    every = copies.load(lambda: (rows_all, all_rows))
    table_sum[0] = table[...]
    table_sum[0, pl.ds(w_size, 1), pl.ds(0, width)] = score_scale * jnp.sum(
        q_buf[...].astype(f32), axis=0, keepdims=True
    )
    table_sum[0, pl.ds(w_size + 1, 1), pl.ds(0, width)] = jnp.sum(
        value_sums[...], axis=0, keepdims=True
    )
    table_send(0)
    weights.wait()

    def through_tile(j, left, step):
        given = kv_buf[pl.ds(j * piece, piece)].reshape(piece * BLOCK, 2 * width)
        weight = slots[pl.ds(0, width // BLOCK)].reshape(width, 2 * width)
        tile = dot_nt(given, weight).astype(bf16).reshape(piece, BLOCK, width)
        slots[pl.ds(through_from + step * piece, piece), :, pl.ds(left, width)] = tile

    def other_tile(step):
        through_tile(count + step, 0, step)
        for n in range(count):

            @pl.when(step == n)
            def _(n=n):
                state["through", n] = copies.send(
                    lambda: (through_other(n), g_core.at[n], here.core_peer)
                )

    def own_tile(step):
        through_tile(step, width, step)

    stepped(count, through_at, through_step, other_tile)
    stepped(count, through_at + count * through_step, through_step, own_tile)
    every.wait()

    def kv_terms(c):
        columns = pl.ds(pl.multiple_of(c * half, 128), half)
        acc[...] = jnp.zeros_like(acc)

        def deep(t, carry):
            rows = slots[pl.ds(rows_from + t * blocks, blocks), :, 0:width]
            given = kv_buf[pl.ds(t * blocks, blocks), :, columns]
            acc[...] += dot_tn(
                rows.reshape(own_tokens, width), given.reshape(own_tokens, half)
            )
            return carry

        lax.fori_loop(0, tokens // own_tokens, deep, 0)
        for p in range(pairs):
            for side, place in ((core, kv_own.at[c, p]), (1 - core, kv_other.at[c, p])):
                start = pl.multiple_of((2 * p + side) * shard, shard)
                place[...] = acc[pl.ds(start, shard), :].astype(bf16)
        for n in range(4):

            @pl.when(c == n)
            def _(n=n):
                kv_to_core(n, lambda: kv_other.at[n])

    stepped(4, terms_at, terms_step, kv_terms)
    events.run()
    copies.finish()


def back_all(ctx_size, w_size, small, large, shapes):
    width, tok, tokens, table_shape = shapes
    lines, pairs = ctx_size // 4, w_size // 2
    rows = width // w_size
    own_tokens = 2 * tok
    blocks = own_tokens // BLOCK
    keys = CANDS * BLOCK
    half = width // 2
    table_steps = 1 + len(bits(pairs)) + len(bits(lines)) + len(bits(4))
    any_space = pl.BlockSpec(memory_space=pl.ANY)
    in_vmem = pl.BlockSpec(memory_space=pltpu.VMEM)
    in_smem = pl.BlockSpec(memory_space=pltpu.SMEM)
    scratch = []
    for _ in range(BACK_GROUPS):
        scratch += group_scratch(lines, pairs, rows, half)
    piece = (tok // BLOCK, BLOCK, width)
    scratch += [
        pltpu.VMEM((tokens // BLOCK, BLOCK, 2 * width), bf16),
        pltpu.VMEM((blocks * CANDS + 1, BLOCK, 2 * width), bf16),
        pltpu.VMEM((keys, 2 * width), bf16),
        pltpu.VMEM((2, width // LANES, GROUP * BLOCK, keys), bf16),
        pltpu.VMEM((own_tokens, width), bf16),
        pltpu.VMEM((own_tokens, width), bf16),
        pltpu.VMEM((blocks, BLOCK, width), bf16),
        pltpu.VMEM((width, width), bf16),
        pltpu.VMEM((2, pairs, rows, half), bf16),
        pltpu.VMEM((4, pairs, rows, half), bf16),
        pltpu.VMEM((blocks, BLOCK, width), f32),
        pltpu.VMEM((2 * lines,) + piece, bf16),
        pltpu.VMEM((2 * lines - 2,) + piece, bf16),
        pltpu.VMEM((2,) + piece, bf16),
        pltpu.VMEM((width, half), f32),
        pltpu.VMEM((16, width), f32),
        pltpu.VMEM((table_steps,) + table_shape, f32),
        pltpu.VMEM((table_steps,) + table_shape, f32),
        pltpu.SemaphoreType.DMA((2,)),
        (
            pltpu.SemaphoreType.DMA((60,)),
            pltpu.SemaphoreType.DMA((160,)),
            pltpu.SemaphoreType.DMA((160,)),
        ),
    ]
    return pl.pallas_call(
        functools.partial(back_kernel, ctx_size, w_size),
        in_specs=[in_smem, in_smem, in_vmem] + [any_space] * len(large),
        out_specs=[any_space] * 3 + [in_vmem],
        out_shape=[
            jax.ShapeDtypeStruct((2 * lines * BACK_GROUPS, rows, half), bf16),
            jax.ShapeDtypeStruct((2,) + piece, bf16),
            jax.ShapeDtypeStruct((2,) + piece, bf16),
            jax.ShapeDtypeStruct(table_shape, f32),
        ],
        scratch_shapes=scratch,
        compiler_params=pltpu.CompilerParams(
            collective_id=1, has_side_effects=True, vmem_limit_bytes=67043328
        ),
        name="back_all",
    )(*small, *large)


def make_local(ctx_size, w_size):
    def local(
        hidden,
        out_grad,
        doc_lengths,
        rand_pick,
        w_query,
        w_key,
        w_value,
        w_out,
        w_up,
        w_down,
        b_query,
        b_value,
        b_out,
        b_up,
        b_down,
        ln1_gain,
        ln1_shift,
        ln2_gain,
        ln2_shift,
    ):
        wires = Wires(ctx_size, w_size)
        tok, width = hidden.shape[2], hidden.shape[3]
        ff = w_up.shape[1]
        tok_blocks = tok // BLOCK
        lines, pairs = wires.lines, wires.pairs
        micro = wires.part // 2

        small_ints = jnp.concatenate(
            [rand_pick.reshape(MICRO, -1), doc_lengths.reshape(MICRO, -1)], axis=1
        )
        int_count = small_ints.shape[1]
        small_ints = jnp.pad(small_ints, ((0, 0), (0, 1024 - int_count))).reshape(MICRO, 8, 128)
        vectors = [b_query, b_value, b_out, b_up, b_down, ln1_gain, ln1_shift, ln2_gain, ln2_shift]
        vector_sizes = [vector.shape[0] for vector in vectors]
        (
            all_rows,
            grads_dealt,
            ints_dealt,
            vector_table,
            full_query,
            full_kv,
            full_out,
            full_up,
            full_down,
        ) = gather_all(
            ctx_size,
            w_size,
            hidden,
            out_grad,
            small_ints,
            jnp.concatenate(vectors)[None],
            (w_query, w_key, w_value, w_out, w_up, w_down),
        )
        all_rows = all_rows.reshape(-1, width)
        own_rows = all_rows[: 2 * tok]
        grads_dealt = grads_dealt.reshape(-1, width)
        ints_dealt = ints_dealt.reshape(MICRO, -1)
        full_query, full_kv, full_out, full_up, full_down = [
            full.reshape(-1, full.shape[2]) for full in (full_query, full_kv, full_out, full_up, full_down)
        ]
        spread = []
        at = 0
        for size in vector_sizes:
            spread.append(vector_table[:, 0, at : at + size].reshape(-1).astype(f32))
            at += size
        (
            bias_query,
            bias_value,
            bias_out,
            bias_up,
            bias_down,
            gain_one,
            shift_one,
            gain_two,
            shift_two,
        ) = spread

        picks = jnp.stack(
            [ints_dealt[turn, : tok_blocks * 3].reshape(tok_blocks, 3) for turn in range(2)]
        ).reshape(-1, 3)
        lengths = ints_dealt[0, tok_blocks * 3 : int_count]
        in_chunk = jnp.arange(tok_blocks, dtype=jnp.int32)
        chunk_ids = [
            (2 * wires.core + (micro + turn) % 2) * lines + wires.line for turn in range(2)
        ]
        my_blocks = jnp.concatenate([chunk * tok_blocks + in_chunk for chunk in chunk_ids])
        safe_blocks, allowed = candidates(my_blocks, lengths, picks)
        chunk = safe_blocks // tok_blocks
        chunk_part, chunk_line = chunk // lines, chunk % lines
        place = (
            ((chunk_part // 2) ^ wires.core) * lines + (chunk_line ^ wires.line)
        ) * 2 + (chunk_part + micro) % 2
        pos = (place * tok_blocks + safe_blocks % tok_blocks).reshape(-1).astype(jnp.int32)
        bias = jnp.repeat(jnp.where(allowed, 0.0, masked_score).astype(f32), BLOCK, axis=1)[:, None]

        queries = ((dot_nn(own_rows, full_query) + bias_query) * score_scale).astype(bf16)
        kv_bias = jnp.concatenate([jnp.zeros_like(bias_value), bias_value])
        kv = (dot_nn(all_rows, full_kv) + kv_bias).astype(bf16)
        context, probs = attend(pos, queries, bias, kv)
        attn_out = dot_nn(context, full_out) + bias_out
        rows_f32 = own_rows.astype(f32)
        normed, ln1_back = jax.vjp(layer_norm, rows_f32 + attn_out, gain_one, shift_one)
        normed_low = normed.astype(bf16)
        up_pre = dot_nn(normed_low, full_up) + bias_up
        gelu_out, gelu_back = jax.vjp(lambda v: jax.nn.gelu(v, approximate=True), up_pre)
        activated = gelu_out.astype(bf16)
        branch = dot_nn(activated, full_down) + bias_down
        final, ln2_back = jax.vjp(layer_norm, normed + branch, gain_two, shift_two)
        final = final.astype(bf16)

        def term_of(rows_a, rows_b, scale=None):
            term = dot_tn(rows_a, rows_b)
            if scale is not None:
                term = term * scale
            return term.astype(bf16).reshape(pairs, 2, -1, rows_b.shape[1])

        d_mid, grad_gain_two, grad_shift_two = ln2_back(grads_dealt.astype(f32))
        d_branch = d_mid.astype(bf16)
        term_down = term_of(activated, d_branch)
        d_act = dot_nt(d_branch, full_down)
        d_up = gelu_back(d_act)[0].astype(bf16)
        term_up = term_of(normed_low, d_up)
        d_normed = dot_nt(d_up, full_up) + d_mid
        d_sum, grad_gain_one, grad_shift_one = ln1_back(d_normed)
        d_attn = d_sum.astype(bf16)
        term_out = term_of(context, d_attn)
        d_context = dot_nt(d_attn, full_out).astype(bf16)

        def table_of(vectors):
            return jnp.concatenate([vector.reshape(w_size, -1) for vector in vectors], axis=1)

        def column_sums(rows_a):
            return jnp.sum(rows_a.astype(f32), axis=0)

        sums = (
            column_sums(d_attn),
            column_sums(d_up),
            column_sums(d_branch),
            grad_gain_one,
            grad_shift_one,
            grad_gain_two,
            grad_shift_two,
        )
        shard = width // w_size
        if lines == 2 and pairs == 2:
            named = pos.reshape(-1, CANDS)[None] == jnp.arange(
                all_rows.shape[0] // BLOCK, dtype=jnp.int32
            ).reshape(-1, 1, 1)
            named = jnp.logical_and(named, allowed[None])
            slot = jnp.arange(allowed.size, dtype=jnp.int32).reshape(allowed.shape)[None]
            inv = jnp.min(jnp.where(named, slot, allowed.size), axis=2).reshape(-1)
            table = table_of(sums)
            table = jnp.pad(table, ((0, 8 - w_size), (0, 0)))
            term_down = term_down.reshape(pairs, 2, -1, shard, width)
            by_block = (-1, BLOCK, width)
            summed, block_out, grad_hidden, table = back_all(
                ctx_size,
                w_size,
                (pos, inv, table),
                (
                    queries,
                    d_context,
                    d_sum.reshape(by_block),
                    probs,
                    kv.reshape(-1, BLOCK, 2 * width),
                    all_rows.reshape(by_block),
                    full_kv.reshape(-1, BLOCK, 2 * width),
                    full_query,
                    final.reshape(2, -1, BLOCK, width),
                    term_up,
                    term_down,
                    term_out,
                ),
                (width, tok, all_rows.shape[0], table.shape),
            )
            row = lax.dynamic_slice(table, (wires.w, jnp.int32(0)), (1, table.shape[1]))[0]
            both = lax.dynamic_slice(
                table, (jnp.int32(w_size), wires.w * shard), (2, shard)
            )
            small = [both[0], both[1]]
            at = 0
            for size in vector_sizes[2:]:
                small.append(row[at : at + size])
                at += size

            def beside(pieces):
                return jnp.concatenate([piece.astype(f32) for piece in pieces], axis=1)

            halves = width // 2
            count = ff // halves
            down = summed[count : 2 * count].astype(f32).reshape(-1, 2, shard, halves)
            down = jnp.swapaxes(down, 1, 2).reshape(-1, width)
            pairs_of = [beside([summed[c], summed[c + 1]]) for c in range(2 * count, 2 * count + 8, 2)]
            grad_out_w, grad_query, grad_key, grad_value = pairs_of
            return (
                block_out.reshape(2, 1, tok, width),
                grad_hidden.reshape(2, 1, tok, width).astype(f32),
                grad_query,
                grad_key,
                grad_value,
                grad_out_w,
                beside([summed[c] for c in range(count)]),
                down,
                *small,
            )

        d_query, d_kv = attend_back(pos, queries, d_context, probs, kv)

        through = dot_nt(d_kv, full_kv).astype(bf16)
        near = d_sum + score_scale * dot_nt(d_query, full_query)
        term_kv = term_of(all_rows, d_kv)
        term_query = term_of(own_rows, d_query, score_scale)

        sums = (score_scale * column_sums(d_query), column_sums(d_kv[:, width:])) + sums
        table = table_of(sums)[:, None]
        term_down = term_down.reshape(pairs, 2, -1, shard, width)
        summed, block_out, grad_hidden, table = finish_all(
            ctx_size,
            w_size,
            (term_up, term_down, term_query, term_kv, term_out),
            ("wide", "tall", "wide", "wide", "wide"),
            through.reshape(-1, tok, width),
            near.reshape(-1, tok, width),
            final.reshape(-1, tok, width),
            table,
        )
        row = lax.dynamic_slice(
            table, (wires.w, jnp.int32(0), jnp.int32(0)), (1, 1, table.shape[2])
        )[0, 0]
        small = []
        at = 0
        for size in vector_sizes:
            small.append(row[at : at + size])
            at += size

        parts = lines // 2
        at = 0

        def wide(columns):
            nonlocal at
            count = columns * parts // width
            pieces = summed[at : at + count].astype(f32)
            at += count
            return jnp.concatenate([pieces[c] for c in range(count)], axis=1)

        grad_up = wide(ff)
        count = ff * parts // width
        grad_down = summed[at : at + count].astype(f32).reshape(-1, parts, shard, width // parts)
        grad_down = jnp.swapaxes(grad_down, 1, 2).reshape(-1, width)
        at += count
        grad_query, grad_key, grad_value, grad_out = [wide(width) for _ in range(4)]
        return (
            block_out[:, None],
            grad_hidden.astype(f32)[:, None],
            grad_query,
            grad_key,
            grad_value,
            grad_out,
            grad_up,
            grad_down,
            *small,
        )

    return local


def solution(mesh):
    tokens = P(None, "wshard", "ctx", None)
    in_specs = (
        tokens,
        tokens,
        P(None, "wshard", None),
        tokens,
        *[P("wshard", None)] * 6,
        *[P("wshard")] * 9,
    )
    out_specs = (tokens, tokens, *[P("wshard", None)] * 6, *[P("wshard")] * 9)
    return jax.shard_map(
        make_local(mesh.shape["ctx"], mesh.shape["wshard"]),
        mesh=mesh,
        in_specs=in_specs,
        out_specs=out_specs,
        check_vma=False,
    )
```

```python
import functools
import heapq
import math

import jax
import jax.numpy as jnp
from jax import lax
from jax.experimental import pallas as pl
from jax.experimental.pallas import tpu as pltpu
from jax.sharding import PartitionSpec as P

HEADS = 12
HEAD_DIM = 64
BLOCK = 64
MICRO = 2
GROUP = 4
LANES = GROUP * HEAD_DIM
CANDS = 8

masked_score = -1e30
norm_eps = 1e-12
score_scale = 1.0 / math.sqrt(HEAD_DIM)
bf16 = jnp.bfloat16
f32 = jnp.float32
MESH = pl.DeviceIdType.MESH


def layer_norm(values, ln_gain, ln_shift):
    center = values - jnp.mean(values, axis=-1, keepdims=True)
    spread = jnp.mean(center * center, axis=-1, keepdims=True)
    return center * lax.rsqrt(spread + norm_eps) * ln_gain + ln_shift


def candidates(blocks, lengths, chosen_raw):
    doc_ends = jnp.cumsum(lengths)
    doc_starts = doc_ends - lengths
    owner_doc = jnp.sum((blocks[:, None] >= doc_ends[None, :]).astype(jnp.int32), axis=1)
    doc_ids = jnp.arange(lengths.shape[0], dtype=jnp.int32)
    member = (owner_doc[:, None] == doc_ids[None, :]).astype(jnp.int32)
    doc_first = jnp.sum(member * doc_starts[None, :], axis=1)
    length = jnp.sum(member * lengths[None, :], axis=1)
    randoms = doc_first[:, None] + chosen_raw % length[:, None]
    columns = [blocks, blocks - 1, blocks + 1, doc_first, doc_first + 1]
    for column in range(chosen_raw.shape[1]):
        columns.append(randoms[:, column])
    chosen = jnp.stack(columns, axis=1)
    inside = (chosen >= doc_first[:, None]) & (chosen < (doc_first + length)[:, None])
    is_fresh = [jnp.ones(blocks.shape, dtype=jnp.bool_)]
    for column in range(1, chosen.shape[1]):
        is_fresh.append(jnp.all(chosen[:, :column] != chosen[:, column : column + 1], axis=1))
    allowed = inside & jnp.stack(is_fresh, axis=1)
    safe_blocks = jnp.where(allowed, chosen, blocks[:, None])
    return (safe_blocks, allowed)


def dot_nt(a, b):
    return lax.dot_general(a, b, (((1,), (1,)), ((), ())), preferred_element_type=f32)


def dot_nn(a, b):
    return lax.dot_general(a, b, (((1,), (0,)), ((), ())), preferred_element_type=f32)


def dot_tn(a, b):
    return lax.dot_general(a, b, (((0,), (0,)), ((), ())), preferred_element_type=f32)


def spread_heads(rows, head_of_lane):
    zero = jnp.zeros_like(rows)
    return jnp.concatenate([jnp.where(head_of_lane == h, rows, zero) for h in range(GROUP)], axis=0)


def pick_heads(rows, head_of_lane):
    total = jnp.zeros((BLOCK, LANES), f32)
    for h in range(GROUP):
        total = jnp.where(head_of_lane == h, rows[h * BLOCK : (h + 1) * BLOCK], total)
    return total


def attend_kernel(groups, width, pos_ref, q_ref, bias_ref, kv_ref, ctx_ref, probs_ref, cat):
    i = pl.program_id(0)
    for j in range(CANDS):
        start = pl.multiple_of(pos_ref[i * CANDS + j] * BLOCK, BLOCK)
        cat[j * BLOCK : (j + 1) * BLOCK, :] = kv_ref[pl.ds(start, BLOCK), :]
    head_of_lane = lax.broadcasted_iota(jnp.int32, (BLOCK, LANES), 1) // HEAD_DIM
    bias = bias_ref[0]
    for g in range(groups):
        lanes = slice(g * LANES, (g + 1) * LANES)
        v_lanes = slice(width + g * LANES, width + (g + 1) * LANES)
        q_all = spread_heads(q_ref[:, lanes], head_of_lane)
        scores = dot_nt(q_all, cat[:, lanes]) + bias
        row_max = jnp.max(scores, axis=-1, keepdims=True)
        shifted = jnp.exp(scores - row_max)
        row_total = jnp.sum(shifted, axis=-1, keepdims=True)
        probs = (shifted * (1.0 / row_total)).astype(bf16)
        probs_ref[0, g] = probs
        mixed = dot_nn(probs, cat[:, v_lanes])
        ctx_ref[:, lanes] = pick_heads(mixed, head_of_lane).astype(bf16)


def attend(pos, queries, bias, kv):
    rows, width = queries.shape
    blocks = rows // BLOCK
    groups = width // LANES
    keys = CANDS * BLOCK
    return pl.pallas_call(
        functools.partial(attend_kernel, groups, width),
        grid_spec=pltpu.PrefetchScalarGridSpec(
            num_scalar_prefetch=1,
            grid=(blocks,),
            in_specs=[
                pl.BlockSpec((BLOCK, width), lambda i, p: (i, 0)),
                pl.BlockSpec((1, 1, keys), lambda i, p: (i, 0, 0)),
                pl.BlockSpec(kv.shape, lambda i, p: (0, 0), pipeline_mode=pl.Buffered(1)),
            ],
            out_specs=[
                pl.BlockSpec((BLOCK, width), lambda i, p: (i, 0)),
                pl.BlockSpec((1, groups, GROUP * BLOCK, keys), lambda i, p: (i, 0, 0, 0)),
            ],
            scratch_shapes=[pltpu.VMEM((keys, 2 * width), bf16)],
        ),
        out_shape=[
            jax.ShapeDtypeStruct((rows, width), bf16),
            jax.ShapeDtypeStruct((blocks, groups, GROUP * BLOCK, keys), bf16),
        ],
        compiler_params=pltpu.CompilerParams(vmem_limit_bytes=48 << 20),
        cost_estimate=pl.CostEstimate(
            flops=blocks * groups * 4 * GROUP * BLOCK * keys * LANES,
            bytes_accessed=kv.size * 2 + rows * width * 4 + blocks * groups * GROUP * BLOCK * keys * 2,
            transcendentals=blocks * groups * GROUP * BLOCK * keys,
        ),
        name="attend",
    )(pos, queries, bias, kv)


def attend_back_kernel(
    groups, width, pos_ref, q_ref, dctx_ref, probs_ref, kv_ref, dq_ref, dkv_ref, cat, acc
):
    i = pl.program_id(0)

    @pl.when(i == 0)
    def _():
        acc[...] = jnp.zeros_like(acc)

    for j in range(CANDS):
        start = pl.multiple_of(pos_ref[i * CANDS + j] * BLOCK, BLOCK)
        cat[j * BLOCK : (j + 1) * BLOCK, :] = kv_ref[pl.ds(start, BLOCK), :]
    head_of_lane = lax.broadcasted_iota(jnp.int32, (BLOCK, LANES), 1) // HEAD_DIM
    for g in range(groups):
        lanes = slice(g * LANES, (g + 1) * LANES)
        v_lanes = slice(width + g * LANES, width + (g + 1) * LANES)
        q_all = spread_heads(q_ref[:, lanes], head_of_lane)
        d_all = spread_heads(dctx_ref[:, lanes], head_of_lane)
        probs_low = probs_ref[0, g]
        probs = probs_low.astype(f32)
        d_probs = dot_nt(d_all, cat[:, v_lanes])
        row_inner = jnp.sum(probs * d_probs, axis=-1, keepdims=True)
        d_scores = (probs * (d_probs - row_inner)).astype(bf16)
        dq_ref[:, lanes] = pick_heads(dot_nn(d_scores, cat[:, lanes]), head_of_lane).astype(bf16)
        d_key = dot_tn(d_scores, q_all)
        d_value = dot_tn(probs_low, d_all)
        for j in range(CANDS):
            start = pl.multiple_of(pos_ref[i * CANDS + j] * BLOCK, BLOCK)
            part = slice(j * BLOCK, (j + 1) * BLOCK)
            acc[pl.ds(start, BLOCK), lanes] += d_key[part]
            acc[pl.ds(start, BLOCK), v_lanes] += d_value[part]

    @pl.when(i == pl.num_programs(0) - 1)
    def _():
        dkv_ref[...] = acc[...].astype(bf16)


def attend_back(pos, queries, d_context, probs, kv):
    rows, width = queries.shape
    blocks = rows // BLOCK
    groups = width // LANES
    keys = CANDS * BLOCK
    return pl.pallas_call(
        functools.partial(attend_back_kernel, groups, width),
        grid_spec=pltpu.PrefetchScalarGridSpec(
            num_scalar_prefetch=1,
            grid=(blocks,),
            in_specs=[
                pl.BlockSpec((BLOCK, width), lambda i, p: (i, 0)),
                pl.BlockSpec((BLOCK, width), lambda i, p: (i, 0)),
                pl.BlockSpec((1, groups, GROUP * BLOCK, keys), lambda i, p: (i, 0, 0, 0)),
                pl.BlockSpec(kv.shape, lambda i, p: (0, 0), pipeline_mode=pl.Buffered(1)),
            ],
            out_specs=[
                pl.BlockSpec((BLOCK, width), lambda i, p: (i, 0)),
                pl.BlockSpec(kv.shape, lambda i, p: (0, 0), pipeline_mode=pl.Buffered(1)),
            ],
            scratch_shapes=[pltpu.VMEM((keys, 2 * width), bf16), pltpu.VMEM(kv.shape, f32)],
        ),
        out_shape=[
            jax.ShapeDtypeStruct((rows, width), bf16),
            jax.ShapeDtypeStruct(kv.shape, bf16),
        ],
        compiler_params=pltpu.CompilerParams(vmem_limit_bytes=60 << 20),
        cost_estimate=pl.CostEstimate(
            flops=blocks * groups * 8 * GROUP * BLOCK * keys * LANES,
            bytes_accessed=kv.size * 4 + rows * width * 6 + blocks * groups * GROUP * BLOCK * keys * 2,
            transcendentals=0,
        ),
        name="attend_back",
    )(pos, queries, d_context, probs, kv)


class Wires:
    def __init__(self, ctx_size, w_size):
        self.ctx_size, self.w_size = ctx_size, w_size
        self.lines = ctx_size // 4
        self.pairs = w_size // 2
        self.ctx = lax.axis_index("ctx")
        self.w = lax.axis_index("wshard")
        self.part = self.ctx // self.lines
        self.line = self.ctx % self.lines
        self.pair = self.w // 2
        self.core = self.w % 2

    def at(self, part, line, pair, core):
        return (part * self.lines + line, pair * 2 + core)

    @property
    def core_peer(self):
        return self.at(self.part, self.line, self.pair, 1 - self.core)

    def pair_peer(self, flip):
        return self.at(self.part, self.line, self.pair ^ flip, self.core)

    def line_peer(self, flip):
        return self.at(self.part, self.line ^ flip, self.pair, self.core)

    def part_peer(self, flip):
        return self.at(self.part ^ flip, self.line, self.pair, self.core)

    def move(self, value, to):
        perm = []
        for ctx in range(self.ctx_size):
            for w in range(self.w_size):
                part, line, pair, core = to(ctx // self.lines, ctx % self.lines, w // 2, w % 2)
                target = (part * self.lines + line) * self.w_size + pair * 2 + core
                perm.append((ctx * self.w_size + w, target))
        return lax.ppermute(value, ("ctx", "wshard"), perm)

    def to_core(self, value):
        return self.move(value, lambda part, line, pair, core: (part, line, pair, 1 - core))

    def to_pair(self, value, flip):
        return self.move(value, lambda part, line, pair, core: (part, line, pair ^ flip, core))

    def to_line(self, value, flip):
        return self.move(value, lambda part, line, pair, core: (part, line ^ flip, pair, core))

    def to_part(self, value, flip):
        return self.move(value, lambda part, line, pair, core: (part ^ flip, line, pair, core))

    def deal(self, value, turn):
        return self.move(
            value,
            lambda part, line, pair, core: (2 * ((turn + part) % 2) + core, line, pair, part // 2),
        )

    def deal_back(self, value, turn):
        return self.move(
            value,
            lambda part, line, pair, core: (2 * core + (part // 2 + turn) % 2, line, pair, part % 2),
        )


def bits(count):
    flips = []
    flip = 1
    while flip < count:
        flips.append(flip)
        flip *= 2
    return flips


def gather_kernel(wires_of, refs, outs, own_shards, local_sem, send_sem, recv_sem):
    hidden, out_grad, ints, vectors, w_query, w_key, w_value, w_out, w_up, w_down = refs
    rows_out, grads_out, ints_out, vectors_out, query_out, kv_out, out_out, up_out, down_out = outs
    here = wires_of()
    lines, pairs = here.lines, here.pairs
    part, line, pair, core = here.part, here.line, here.pair, here.core
    width = w_query.shape[1]
    used = [0]
    sent = []
    local = []
    placed = []

    def at(part, line, pair, core):
        return (part * lines + line, pair * 2 + core)

    core_peer = at(part, line, pair, 1 - core)

    def line_peer(flip):
        return at(part, line ^ flip, pair, core)

    def pair_peer(flip):
        return at(part, line, pair ^ flip, core)

    def deal_target(turn):
        return at(2 * ((turn + part) % 2) + core, line, pair, part // 2)

    def deal_source(turn):
        return at(2 * core + (part // 2 + turn) % 2, line, pair, part % 2)

    stays = [
        jnp.logical_and(
            2 * ((turn + part) % 2) + core == part, part // 2 == core
        )
        for turn in range(2)
    ]

    barrier = pltpu.get_barrier_semaphore()

    def greet(device):
        pl.semaphore_signal(barrier, inc=1, device_id=device, device_id_type=MESH)

    peers = [core_peer]
    peers += [line_peer(flip) for flip in range(1, lines)]
    peers += [pair_peer(flip) for flip in range(1, pairs)]
    for device in peers:
        greet(device)
    for turn in range(2):

        @pl.when(jnp.logical_not(stays[turn]))
        def _(turn=turn):
            greet(deal_target(turn))
            greet(deal_source(turn))

    staying = sum(stay.astype(jnp.int32) for stay in stays)
    pl.semaphore_wait(barrier, len(peers) + 4 - 2 * staying)

    def send(src, dst, device, stay=None):
        n = used[0]
        used[0] += 1
        copy = pltpu.make_async_remote_copy(
            src_ref=src,
            dst_ref=dst,
            send_sem=send_sem.at[n],
            recv_sem=recv_sem.at[n],
            device_id=device,
            device_id_type=MESH,
        )
        if stay is None:
            copy.start()
        else:

            @pl.when(stay)
            def _():
                pltpu.make_async_copy(src, dst, recv_sem.at[n]).start()

            @pl.when(jnp.logical_not(stay))
            def _():
                copy.start()

        sent.append((copy, stay))
        return copy

    def stage(src, held):
        copy = pltpu.make_async_copy(src, held, local_sem.at[len(local)])
        copy.start()
        local.append(copy)

    def place_held(held, dst):
        local[len(placed)].wait()
        copy = pltpu.make_async_copy(held, dst, local_sem.at[len(local) + len(placed)])
        copy.start()
        placed.append(copy)

    me = pair * 2 + core

    dealt = [
        send(
            hidden.at[(turn + part) % 2, 0],
            rows_out.at[turn],
            deal_target(turn),
            stays[turn],
        )
        for turn in range(2)
    ]

    matrices = [
        (w_up, lambda shard: up_out.at[shard], True),
        (w_down, lambda shard: down_out.at[shard], True),
        (w_query, lambda shard: query_out.at[shard], False),
        (w_key, lambda shard: kv_out.at[shard, :, :width], False),
        (w_value, lambda shard: kv_out.at[shard, :, width:], False),
        (w_out, lambda shard: out_out.at[shard], False),
        (vectors, lambda shard: vectors_out.at[shard], False),
    ]
    side = line % 2
    for (src, _, _), held in zip(matrices, own_shards):
        stage(src, held)

    def half_cuts(src):
        half = src.shape[0] // 2
        first = pl.ds(pl.multiple_of(side * half, 8), half)
        return first, pl.ds(pl.multiple_of((1 - side) * half, 8), half)

    halves = [
        (
            flip,
            src,
            place,
            send(src.at[half_cuts(src)[0]], place(me).at[half_cuts(src)[0]], pair_peer(flip)),
        )
        for src, place, split in matrices
        if split
        for flip in range(1, pairs)
    ]
    late = [
        send(ints.at[(turn + part) % 2], ints_out.at[turn], deal_target(turn), stays[turn])
        for turn in range(2)
    ]
    for src, place, _ in matrices:
        late.append(send(src, place(me), core_peer))

    crossed = []
    for turn in range(2):
        dealt[turn].wait_recv()
        for flip in range(1, lines):
            crossed.append(
                (
                    flip * 2 + turn,
                    send(rows_out.at[turn], rows_out.at[flip * 2 + turn], line_peer(flip)),
                )
            )
        late.append(send(rows_out.at[turn], rows_out.at[lines * 2 + turn], core_peer))
    for (src, place, _), held in zip(matrices, own_shards):
        place_held(held, place(me))

    relayed = []
    whole = [
        (src, place, flip)
        for src, place, split in matrices
        if not split
        for flip in range(1, pairs)
    ]
    direct = []
    for step, (flip, src, place, copy) in enumerate(halves):
        copy.wait_recv()
        first, second = half_cuts(src)
        shard = (pair ^ flip) * 2 + core
        got = place(shard).at[first]
        relayed.append((place(shard).at[second], send(got, got, line_peer(1))))
        late.append(send(got, got, core_peer))
        share = -(-len(whole) // len(halves))
        for src, place, flip in whole[step * share : (step + 1) * share]:
            direct.append((flip, place, send(src, place(me), pair_peer(flip))))
    late += [
        send(
            out_grad.at[(turn + part) % 2, 0],
            grads_out.at[turn],
            deal_target(turn),
            stays[turn],
        )
        for turn in range(2)
    ]
    for index, copy in crossed:
        copy.wait_recv()
        late.append(send(rows_out.at[index], rows_out.at[lines * 2 + index], core_peer))
    for flip, place, copy in direct:
        copy.wait_recv()
        shard = (pair ^ flip) * 2 + core
        late.append(send(place(shard), place(shard), core_peer))
    for got, copy in relayed:
        copy.wait_recv()
        late.append(send(got, got, core_peer))
    for copy in late:
        copy.wait_recv()
    for copy in placed:
        copy.wait()
    for copy, stay in sent:
        if stay is None:
            copy.wait_send()
        else:

            @pl.when(jnp.logical_not(stay))
            def _(copy=copy):
                copy.wait_send()


def gather_all(ctx_size, w_size, hidden, out_grad, ints, vectors, weights):
    w_query, w_key, w_value, w_out, w_up, w_down = weights
    lines, pairs = ctx_size // 4, w_size // 2
    tok, width = hidden.shape[2], hidden.shape[3]
    rows = w_query.shape[0]
    shapes = [
        ((lines * 4, tok, width), bf16),
        ((2, tok, width), bf16),
        (ints.shape, ints.dtype),
        ((w_size,) + vectors.shape, f32),
        ((w_size, rows, width), bf16),
        ((w_size, rows, 2 * width), bf16),
        ((w_size, rows, width), bf16),
        ((w_size,) + w_up.shape, bf16),
        ((w_size,) + w_down.shape, bf16),
    ]
    sems = 16 + 8 * lines + 20 * pairs

    def body(*refs):
        gather_kernel(
            lambda: Wires(ctx_size, w_size), refs[:10], refs[10:19], refs[19:26], *refs[26:]
        )

    return pl.pallas_call(
        body,
        in_specs=[pl.BlockSpec(memory_space=pl.ANY)] * 10,
        out_specs=[pl.BlockSpec(memory_space=pl.ANY)] * len(shapes),
        out_shape=[jax.ShapeDtypeStruct(shape, dtype) for shape, dtype in shapes],
        scratch_shapes=[
            *[
                pltpu.VMEM(shard.shape, shard.dtype)
                for shard in (w_up, w_down, w_query, w_key, w_value, w_out, vectors)
            ],
            pltpu.SemaphoreType.DMA((14,)),
            pltpu.SemaphoreType.DMA((sems,)),
            pltpu.SemaphoreType.DMA((sems,)),
        ],
        compiler_params=pltpu.CompilerParams(collective_id=0, has_side_effects=True),
        name="gather_all",
    )(hidden, out_grad, ints, vectors, w_query, w_key, w_value, w_out, w_up, w_down)


class Sent:
    def __init__(self, make, stay=None):
        self.make, self.stay = make, stay

    def wait(self):
        self.make().wait()

    def wait_recv(self):
        self.make().wait_recv()


class Copies:
    def __init__(self, local_sem, send_sem, recv_sem):
        self.local_sem, self.send_sem, self.recv_sem = local_sem, send_sem, recv_sem
        self.locals, self.sent = 0, []

    def load(self, pair):
        n = self.locals
        self.locals += 1
        copy = Sent(lambda: pltpu.make_async_copy(*pair(), self.local_sem.at[n]))
        copy.make().start()
        return copy

    def send(self, triple, stay=None):
        n = len(self.sent)

        def make():
            src, dst, device = triple()
            return pltpu.make_async_remote_copy(
                src_ref=src,
                dst_ref=dst,
                send_sem=self.send_sem.at[n],
                recv_sem=self.recv_sem.at[n],
                device_id=device,
                device_id_type=MESH,
            )

        if stay is None:
            make().start()
        else:

            @pl.when(stay)
            def _():
                src, dst, _ = triple()
                pltpu.make_async_copy(src, dst, self.recv_sem.at[n]).start()

            @pl.when(jnp.logical_not(stay))
            def _():
                make().start()

        copy = Sent(make, stay)
        self.sent.append(copy)
        return copy

    def finish(self):
        for copy in self.sent:
            if copy.stay is None:
                copy.make().wait_send()
            else:

                @pl.when(jnp.logical_not(copy.stay))
                def _(copy=copy):
                    copy.make().wait_send()


def add_blocks(dst, *srcs):
    if len(dst.shape) == 3:

        def each(i, carry):
            total = srcs[0][i].astype(f32)
            for src in srcs[1:]:
                total = total + src[i].astype(f32)
            dst[i] = total.astype(dst.dtype)
            return carry

        lax.fori_loop(0, dst.shape[0], each, 0)
        return
    rows = dst.shape[0]
    step = 48 if rows % 48 == 0 else 32

    def body(i, carry):
        cut = pl.ds(pl.multiple_of(i * step, step), step)
        total = srcs[0][cut, :].astype(f32)
        for src in srcs[1:]:
            total = total + src[cut, :].astype(f32)
        dst[cut, :] = total.astype(dst.dtype)
        return carry

    lax.fori_loop(0, rows // step, body, 0)


class Events:
    def __init__(self):
        self.items = []

    def add(self, time, action):
        self.items.append((time, len(self.items), action))

    def take(self, until):
        due = sorted([item for item in self.items if item[0] <= until], key=lambda item: item[:2])
        self.items = [item for item in self.items if item[0] > until]
        return [action for _, _, action in due]

    def run(self, until=math.inf):
        for action in self.take(until):
            action()


class Plan:
    def __init__(self, events):
        self.events, self.heap, self.free, self.count = events, [], {}, 0

    def at(self, time, action):
        heapq.heappush(self.heap, (time, self.count, action))
        self.count += 1

    def do(self, time, action):
        self.events.add(time, action)

    def send(self, link, time, length, then):
        def start(now):
            begin = max(now, self.free.get(link, 0.0))
            self.free[link] = begin + length
            self.at(begin + length + 2.0, then)

        self.at(time, start)

    def run(self):
        while self.heap:
            time, _, action = heapq.heappop(self.heap)
            action(time)


def group_scratch(lines, pairs, rows, columns):
    block = (rows, columns)
    return [
        pltpu.VMEM((2 * lines, pairs) + block, bf16),
        pltpu.VMEM((2 * lines, pairs) + block, bf16),
        pltpu.VMEM((2 * lines, max(pairs - 1, 1)) + block, bf16),
        pltpu.VMEM((2 * lines,) + block, bf16),
        pltpu.VMEM((2, max(lines - 1, 1)) + block, bf16),
        pltpu.VMEM((2,) + block, bf16),
        pltpu.VMEM((2,) + block, bf16),
        pltpu.VMEM((2,) + block, bf16),
    ]


GROUP_SCRATCH = 8
BACK_GROUPS = 6


def reduce_group(here, copies, plan, chunks, scratch, place, unit, core_times):
    from_core, own, from_pairs, paired, from_lines, lined, from_parts, parted = scratch
    lines, pairs = here.lines, here.pairs
    line, pair, core, part = here.line, here.pair, here.core, here.part
    low_part = part % 2
    state = {}

    def to_core(i, view):
        state["core", i] = copies.send(lambda: (view(), from_core.at[i], here.core_peer))

    def begin(i):
        to_core(i, lambda: chunks[i](1 - core))
        state["own", i] = copies.load(lambda: (chunks[i](core), own.at[i]))

    def over_core(i):
        if ("own", i) in state:
            state["own", i].wait()
        state["core", i].wait_recv()
        for p in range(pairs):
            add_blocks(own.at[i, p], own.at[i, p], from_core.at[i, p])
        state["pair", i] = [
            copies.send(
                lambda flip=flip: (
                    own.at[i, pair ^ flip],
                    from_pairs.at[i, flip - 1],
                    here.pair_peer(flip),
                )
            )
            for flip in range(1, pairs)
        ]

    def over_pairs(i):
        for copy in state["pair", i]:
            copy.wait_recv()
        add_blocks(
            paired.at[i], own.at[i, pair], *[from_pairs.at[i, flip - 1] for flip in range(1, pairs)]
        )

    def to_lines(h):
        state["line", h] = [
            copies.send(
                lambda flip=flip: (
                    paired.at[h * lines + (line ^ flip)],
                    from_lines.at[h, flip - 1],
                    here.line_peer(flip),
                )
            )
            for flip in range(1, lines)
        ]

    def over_lines(h):
        for copy in state["line", h]:
            copy.wait_recv()
        add_blocks(
            lined.at[h],
            paired.at[h * lines + line],
            *[from_lines.at[h, flip - 1] for flip in range(1, lines)],
        )

    def to_part_one():
        state["one"] = copies.send(
            lambda: (lined.at[1 - low_part], from_parts.at[0], here.part_peer(1))
        )

    def over_part_one():
        state["one"].wait_recv()
        add_blocks(parted.at[0], lined.at[low_part], from_parts.at[0])
        state["two"] = copies.send(lambda: (parted.at[0], from_parts.at[1], here.part_peer(2)))

    def mine():
        return place(low_part, line)

    def other():
        return place(1 - low_part, line)

    def over_part_two():
        state["two"].wait_recv()
        add_blocks(parted.at[1], parted.at[0], from_parts.at[1])
        state["back"] = copies.send(lambda: (parted.at[1], mine(), here.part_peer(1)))
        state["place"] = copies.load(lambda: (parted.at[1], mine()))
        state["spread"] = [
            copies.send(lambda flip=flip: (parted.at[1], mine(), here.line_peer(flip)))
            for flip in range(1, lines)
        ]

    def spread_other():
        state["back"].wait_recv()
        state["spread"] += [
            copies.send(lambda flip=flip: (other(), other(), here.line_peer(flip)))
            for flip in range(1, lines)
        ]

    def end():
        state["place"].wait()
        for copy in state["spread"]:
            copy.wait_recv()

    lined_h = []

    def core_done(i, now):
        plan.do(now, functools.partial(over_core, i))
        plan.send("x", now + 0.7, (pairs - 1) * unit, functools.partial(pairs_done, i))

    def pairs_done(i, now):
        plan.do(now, functools.partial(over_pairs, i))
        if i % lines == lines - 1:
            h = i // lines
            plan.do(now + 0.01, functools.partial(to_lines, h))
            plan.send("y", now + 0.3, (lines - 1) * unit, functools.partial(lines_done, h))

    def lines_done(h, now):
        plan.do(now, functools.partial(over_lines, h))
        lined_h.append(h)
        if len(lined_h) == 2:
            plan.do(now + 0.01, to_part_one)
            plan.send("z", now + 0.3, unit, one_done)

    def one_done(now):
        plan.do(now, over_part_one)
        plan.send("z", now + 0.3, 2 * unit, two_done)

    def two_done(now):
        plan.do(now, over_part_two)
        plan.send("z", now + 0.3, unit, back_done)
        plan.send("y", now + 0.3, (lines - 1) * unit, lambda now: None)

    def back_done(now):
        plan.do(now, spread_other)
        plan.send("y", now + 0.1, (lines - 1) * unit, lambda now: None)

    for i in range(2 * lines):
        if chunks[i] is not None:
            plan.do(core_times[i - 2] + 0.01 if i >= 2 else -100.0, functools.partial(begin, i))
        plan.at(core_times[i], functools.partial(core_done, i))
    plan.do(10000.0, end)
    return to_core


def chunk_views(refs, kinds, width):
    views = []
    for ref, kind in zip(refs, kinds):
        if kind == "wide":
            for c in range(ref.shape[3] // width):
                views.append(
                    lambda core, ref=ref, cut=slice(c * width, (c + 1) * width): ref.at[
                        :, core, :, cut
                    ]
                )
        else:
            for b in range(ref.shape[2]):
                for c in range(ref.shape[4] // width):
                    views.append(
                        lambda core, ref=ref, b=b, cut=slice(c * width, (c + 1) * width): ref.at[
                            :, core, b, :, cut
                        ]
                    )
    return views


def finish_kernel(ctx_size, w_size, kinds, tables, *refs):
    here = Wires(ctx_size, w_size)
    lines, pairs = here.lines, here.pairs
    part, line, pair, core = here.part, here.line, here.pair, here.core
    terms = refs[: len(kinds)]
    through, near, final, table = refs[len(kinds) : len(kinds) + 4]
    at = len(kinds) + 4
    out, final_out, grad_out, table_out = refs[at : at + 4]
    at += 4
    groups = (len(refs) - at - 8) // GROUP_SCRATCH
    scratches = [
        refs[at + g * GROUP_SCRATCH : at + (g + 1) * GROUP_SCRATCH] for g in range(groups)
    ]
    at += groups * GROUP_SCRATCH
    g_core, g_own, g_line, g_near, g_sum, table_in, table_sum = refs[at : at + 7]
    copies = Copies(*refs[at + 7])
    micro = part // 2

    def back_target(turn):
        return here.at(2 * core + (micro + turn) % 2, line, pair, part % 2)

    def back_source(turn):
        return here.at(2 * ((turn + part) % 2) + core, line, pair, part // 2)

    stays = [
        jnp.logical_and(2 * core + (micro + turn) % 2 == part, part % 2 == core)
        for turn in range(2)
    ]
    barrier = pltpu.get_barrier_semaphore()

    def greet(device):
        pl.semaphore_signal(barrier, inc=1, device_id=device, device_id_type=MESH)

    peers = [here.core_peer, here.part_peer(1), here.part_peer(2)]
    peers += [here.line_peer(flip) for flip in range(1, lines)]
    peers += [here.pair_peer(flip) for flip in range(1, pairs)]
    for device in peers:
        greet(device)
    for turn in range(2):

        @pl.when(jnp.logical_not(stays[turn]))
        def _(turn=turn):
            greet(back_target(turn))
            greet(back_source(turn))

    staying = sum(stay.astype(jnp.int32) for stay in stays)
    pl.semaphore_wait(barrier, len(peers) + 4 - 2 * staying)

    events = Events()
    state = {}
    count = 2 * lines

    def begin_rows():
        state["core"] = [
            copies.send(lambda j=j: (through.at[count + j], g_core.at[j], here.core_peer))
            for j in range(count)
        ]
        state["own"] = [
            copies.load(lambda j=j: (through.at[j], g_own.at[j])) for j in range(count)
        ]
        state["near"] = copies.load(lambda: (near, g_near))
        state["out"] = [
            copies.send(
                lambda turn=turn: (final.at[turn], final_out.at[micro], back_target(turn)),
                stays[turn],
            )
            for turn in range(2)
        ]

    def rows_over_core():
        for j in reversed(range(count)):
            state["own"][j].wait()
            state["core"][j].wait_recv()
            add_blocks(g_own.at[j], g_own.at[j], g_core.at[j])
            if j >= 2:
                state["line", j] = copies.send(
                    lambda j=j: (g_own.at[j], g_line.at[j - 2], here.line_peer(j // 2))
                )

    def rows_over_lines():
        state["near"].wait()
        state["back"] = []
        for turn in range(2):
            others = []
            for flip in range(1, lines):
                state["line", 2 * flip + turn].wait_recv()
                others.append(g_line.at[2 * flip + turn - 2])
            add_blocks(g_sum.at[turn], g_near.at[turn], g_own.at[turn], *others)
            state["back"].append(
                copies.send(
                    lambda turn=turn: (g_sum.at[turn], grad_out.at[micro], back_target(turn)),
                    stays[turn],
                )
            )

    def end_rows():
        for copy in state["out"] + state["back"]:
            copy.wait_recv()

    steps = [here.core_peer]
    steps += [here.pair_peer(flip) for flip in bits(pairs)]
    steps += [here.line_peer(flip) for flip in bits(lines)]
    steps += [here.part_peer(flip) for flip in bits(4)]

    def table_send(n):
        src = table if n == 0 else table_sum.at[n - 1]
        state["table", n] = copies.send(lambda: (src, table_in.at[n], steps[n]))

    def table_step(n):
        state["table", n].wait_recv()
        before = table[...] if n == 0 else table_sum[n - 1]
        total = before + table_in[n]
        if n + 1 < len(steps):
            table_sum[n] = total
            table_send(n + 1)
        else:
            table_out[...] = total

    plan = Plan(events)
    events.add(-1001.0, begin_rows)
    events.add(-1000.5, lambda: table_send(0))
    events.add(0.5, rows_over_core)
    events.add(17.0, rows_over_lines)
    events.add(9000.0, end_rows)
    for n in range(len(steps)):
        events.add(2.5 + n * 6.0, functools.partial(table_step, n))
    views = chunk_views(terms, kinds, out.shape[2])
    size = 2 * lines
    for g in range(groups):
        reduce_group(
            here,
            copies,
            plan,
            views[g * size : (g + 1) * size],
            scratches[g],
            lambda h, line, g=g: out.at[g * size + h * lines + line],
            6.0,
            [2.0 + 1.5 * (g * size + i) for i in range(size)],
        )
    plan.run()
    events.run()
    copies.finish()


def finish_all(ctx_size, w_size, terms, kinds, through, near, final, table):
    lines, pairs = ctx_size // 4, w_size // 2
    count = 2 * lines
    tok, width = through.shape[1:]
    rows = width // w_size
    columns = width // (lines // 2)
    chunks = sum(term.size for term in terms) // (w_size * rows * columns)
    groups = chunks // (2 * lines)
    table_steps = 1 + len(bits(pairs)) + len(bits(lines)) + len(bits(4))
    block = (tok, width)
    any_space = pl.BlockSpec(memory_space=pl.ANY)
    in_vmem = pl.BlockSpec(memory_space=pltpu.VMEM)
    sems = 40 + 10 * lines + groups * 2 * lines * (6 + pairs)
    scratch = []
    for _ in range(groups):
        scratch += group_scratch(lines, pairs, rows, columns)
    scratch += [
        pltpu.VMEM((count,) + block, bf16),
        pltpu.VMEM((count,) + block, bf16),
        pltpu.VMEM((max(count - 2, 1),) + block, bf16),
        pltpu.VMEM((2,) + block, f32),
        pltpu.VMEM((2,) + block, bf16),
        pltpu.VMEM((table_steps,) + table.shape, f32),
        pltpu.VMEM((table_steps,) + table.shape, f32),
        (
            pltpu.SemaphoreType.DMA((sems,)),
            pltpu.SemaphoreType.DMA((sems,)),
            pltpu.SemaphoreType.DMA((sems,)),
        ),
    ]
    return pl.pallas_call(
        functools.partial(finish_kernel, ctx_size, w_size, kinds, table_steps),
        in_specs=[any_space] * (len(terms) + 3) + [in_vmem],
        out_specs=[any_space, any_space, any_space, in_vmem],
        out_shape=[
            jax.ShapeDtypeStruct((chunks, rows, columns), bf16),
            jax.ShapeDtypeStruct((2,) + block, bf16),
            jax.ShapeDtypeStruct((2,) + block, bf16),
            jax.ShapeDtypeStruct(table.shape, f32),
        ],
        scratch_shapes=scratch,
        compiler_params=pltpu.CompilerParams(
            collective_id=1, has_side_effects=True, vmem_limit_bytes=60 << 20
        ),
        name="finish_all",
    )(*terms, through, near, final, table)


def greet_all(here, back_target, back_source, stays):
    lines, pairs = here.lines, here.pairs
    barrier = pltpu.get_barrier_semaphore()

    def greet(device):
        pl.semaphore_signal(barrier, inc=1, device_id=device, device_id_type=MESH)

    peers = [here.core_peer, here.part_peer(1), here.part_peer(2)]
    peers += [here.line_peer(flip) for flip in range(1, lines)]
    peers += [here.pair_peer(flip) for flip in range(1, pairs)]
    for device in peers:
        greet(device)
    for turn in range(2):

        @pl.when(jnp.logical_not(stays[turn]))
        def _(turn=turn):
            greet(back_target(turn))
            greet(back_source(turn))

    staying = sum(stay.astype(jnp.int32) for stay in stays)
    pl.semaphore_wait(barrier, len(peers) + 4 - 2 * staying)


def back_kernel(ctx_size, w_size, *refs):
    here = Wires(ctx_size, w_size)
    lines, pairs = here.lines, here.pairs
    part, line, pair, core = here.part, here.line, here.pair, here.core
    micro = part // 2
    (
        pos,
        inv,
        table,
        queries,
        d_context,
        d_sum,
        probs,
        kv,
        rows_all,
        full_kv,
        full_query,
        final,
        term_up,
        term_down,
        term_out,
    ) = refs[:15]
    up_out, down_out, oq_out, kv_out, final_out, grad_out, table_out = refs[15:22]
    scratches = [
        refs[22 + g * GROUP_SCRATCH : 22 + (g + 1) * GROUP_SCRATCH] for g in range(BACK_GROUPS)
    ]
    (
        kv_buf,
        slots,
        cat,
        probs_buf,
        q_buf,
        dctx_buf,
        rows_buf,
        wq_buf,
        q_other,
        kv_other,
        g_near,
        g_core,
        g_line,
        g_sum,
        acc,
        value_sums,
        table_in,
        table_sum,
        probs_sem,
        sems,
    ) = refs[22 + BACK_GROUPS * GROUP_SCRATCH :]
    copies = Copies(*sems)
    own_tokens, width = q_buf.shape
    key_blocks = kv_buf.shape[0]
    tokens = key_blocks * BLOCK
    blocks = own_tokens // BLOCK
    piece = blocks // 2
    groups = width // LANES
    keys = CANDS * BLOCK
    shard = width // w_size
    half = width // 2

    def back_target(turn):
        return here.at(2 * core + (micro + turn) % 2, line, pair, part % 2)

    def back_source(turn):
        return here.at(2 * ((turn + part) % 2) + core, line, pair, part // 2)

    stays = [
        jnp.logical_and(2 * core + (micro + turn) % 2 == part, part % 2 == core)
        for turn in range(2)
    ]

    def fetch(i, slot):
        return pltpu.make_async_copy(probs.at[i], probs_buf.at[slot], probs_sem.at[slot])

    greet_all(here, back_target, back_source, stays)

    events = Events()
    state = {}
    count = 2 * lines

    w_kv = slots.at[pl.ds(0, width // BLOCK)]
    rows_from = 16
    all_rows = slots.at[pl.ds(rows_from, key_blocks), :, pl.ds(0, width)]
    through_from = rows_from + key_blocks

    def through_other(j):
        return slots.at[pl.ds(through_from + j * piece, piece), :, pl.ds(0, width)]

    def through_own(j):
        return slots.at[pl.ds(through_from + j * piece, piece), :, pl.ds(width, width)]

    def send_out():
        state["out"] = [
            copies.send(
                lambda turn=turn: (final.at[turn], final_out.at[micro], back_target(turn)),
                stays[turn],
            )
            for turn in range(2)
        ]

    def rows_over_core():
        for j in reversed(range(count)):
            state["through", j].wait_recv()
            add_blocks(through_own(j), through_own(j), g_core.at[j])
            if j >= 2:
                state["line", j] = copies.send(
                    lambda j=j: (through_own(j), g_line.at[j - 2], here.line_peer(j // 2))
                )

    def rows_over_lines():
        state["back"] = []
        for turn in range(2):
            others = []
            for flip in range(1, lines):
                state["line", 2 * flip + turn].wait_recv()
                others.append(g_line.at[2 * flip + turn - 2])
            add_blocks(
                g_sum.at[turn], g_near.at[pl.ds(turn * piece, piece)], through_own(turn), *others
            )
            state["back"].append(
                copies.send(
                    lambda turn=turn: (g_sum.at[turn], grad_out.at[micro], back_target(turn)),
                    stays[turn],
                )
            )

    def end_rows():
        for copy in state["out"] + state["back"]:
            copy.wait_recv()

    steps = [lambda: here.core_peer]
    steps += [lambda flip=flip: here.pair_peer(flip) for flip in bits(pairs)]
    steps += [lambda flip=flip: here.line_peer(flip) for flip in bits(lines)]
    steps += [lambda flip=flip: here.part_peer(flip) for flip in bits(4)]

    def table_send(n):
        state["table", n] = copies.send(lambda: (table_sum.at[n], table_in.at[n], steps[n]()))

    def table_step(n):
        state["table", n].wait_recv()
        total = table_sum[n] + table_in[n]
        if n + 1 < len(steps):
            table_sum[n + 1] = total
            table_send(n + 1)
        else:
            table_out[...] = total

    attend_at, attend_step = 9.0, 2.6
    gather_at = attend_at + blocks * attend_step + 3.0
    gather_step = 1.4
    through_at = gather_at + 8 * gather_step + 1.0
    through_step = 1.3
    terms_at = through_at + 8 * through_step
    terms_step = 2.6
    terms_end = terms_at + 4 * terms_step
    plan = Plan(events)
    plan.send("z", 0.0, 18.0, lambda now: None)

    views = chunk_views((term_up, term_down), ("wide", "tall"), half)
    size = 2 * lines
    ffn_groups = BACK_GROUPS - 2

    def half_columns(number):
        return pl.ds(pl.multiple_of(number * half, 128), half)

    def up_place(g):
        return lambda h, line: up_out.at[:, half_columns(g * size + h * lines + line)]

    def down_place(g):
        return lambda h, line: down_out.at[
            pl.ds(pl.multiple_of((2 * g + h) * shard, 16), shard), half_columns(line)
        ]

    places = [up_place(g) for g in range(ffn_groups // 2)]
    places += [down_place(g) for g in range(ffn_groups // 2)]
    for g in range(ffn_groups):
        order = [g * size + i for i in range(size)]
        reduce_group(
            here,
            copies,
            plan,
            views[g * size : (g + 1) * size],
            scratches[g],
            places[g],
            3.0,
            [max(2.5 + 0.7 * n, 3.0 * n - 9.0) for n in order],
        )
    out_views = [
        lambda side, cut=slice(c * half, (c + 1) * half): term_out.at[:, side, :, cut]
        for c in range(2)
    ]
    q_own = scratches[ffn_groups][1]
    q_to_core = reduce_group(
        here,
        copies,
        plan,
        out_views + [None, None],
        scratches[ffn_groups],
        lambda h, line: oq_out.at[h, :, half_columns(line)],
        3.0,
        [gather_at + 2.0 + 1.5 * i for i in range(4)],
    )
    kv_own = scratches[ffn_groups + 1][1]
    kv_to_core = reduce_group(
        here,
        copies,
        plan,
        [None] * 4,
        scratches[ffn_groups + 1],
        lambda h, line: kv_out.at[h, :, half_columns(line)],
        3.0,
        [terms_at + (i + 1) * terms_step + 1.5 for i in range(4)],
    )
    plan.do(-200.0, send_out)
    rows_at = through_at + 2 * count * through_step + 0.5

    def rows_done(now):
        plan.do(now, rows_over_lines)
        plan.send("z", now + 0.7, 18.0, lambda now: None)

    plan.do(rows_at, rows_over_core)
    plan.send("y", rows_at + 0.7, 18.0, rows_done)
    plan.do(9000.0, end_rows)
    for n in range(len(steps)):
        plan.do(through_at + 3.0 + n * 5.0, functools.partial(table_step, n))
    plan.run()

    def stepped(number, at, each, body):
        def loop(step, carry):
            body(step)
            for n in range(number):
                due = events.take(at + (n + 1) * each)
                if due:

                    @pl.when(step == n)
                    def _(due=due):
                        for action in due:
                            action()

            return carry

        lax.fori_loop(0, number, loop, 0)

    events.run(0.0)
    first = [
        copies.load(lambda: (kv, kv_buf)),
        copies.load(lambda: (queries, q_buf)),
        copies.load(lambda: (d_context, dctx_buf)),
    ]
    later = [
        copies.load(lambda: (rows_all.at[pl.ds(0, blocks)], rows_buf)),
        copies.load(lambda: (full_query, wq_buf)),
        copies.load(lambda: (d_sum, g_near)),
    ]

    fetch(0, 0).start()
    events.run(attend_at)
    for copy in first:
        copy.wait()
    slots[blocks * CANDS] = jnp.zeros((BLOCK, 2 * width), bf16)

    head_of_lane = lax.broadcasted_iota(jnp.int32, (BLOCK, LANES), 1) // HEAD_DIM

    def attend_block(i):
        slot = i % 2
        fetch(i, slot).wait()

        @pl.when(i + 1 < blocks)
        def _():
            fetch(i + 1, 1 - slot).start()

        for j in range(CANDS):
            cat[j * BLOCK : (j + 1) * BLOCK, :] = kv_buf[pos[i * CANDS + j]]
        mine = pl.ds(pl.multiple_of(i * BLOCK, BLOCK), BLOCK)
        rows = pl.ds(i * CANDS, CANDS)
        by_slot = (CANDS, BLOCK, LANES)
        for g in range(groups):
            lanes = slice(g * LANES, (g + 1) * LANES)
            v_lanes = slice(width + g * LANES, width + (g + 1) * LANES)
            q_all = spread_heads(q_buf[mine, lanes], head_of_lane)
            d_all = spread_heads(dctx_buf[mine, lanes], head_of_lane)
            probs_low = probs_buf[slot, g]
            shares = probs_low.astype(f32)
            d_probs = dot_nt(d_all, cat[:, v_lanes])
            row_inner = jnp.sum(shares * d_probs, axis=-1, keepdims=True)
            d_scores = (shares * (d_probs - row_inner)).astype(bf16)
            slots[rows, :, lanes] = dot_tn(d_scores, q_all).astype(bf16).reshape(by_slot)
            slots[rows, :, v_lanes] = dot_tn(probs_low, d_all).astype(bf16).reshape(by_slot)
            q_buf[mine, lanes] = pick_heads(dot_nn(d_scores, cat[:, lanes]), head_of_lane).astype(
                bf16
            )

    stepped(blocks, attend_at, attend_step, attend_block)

    for copy in later:
        copy.wait()
    for c in range(2):
        columns = slice(c * half, (c + 1) * half)
        own_rows = rows_buf[...].reshape(own_tokens, width)
        acc[...] = dot_tn(own_rows, q_buf[:, columns]) * score_scale
        for p in range(pairs):
            for side, place in ((core, q_own.at[2 + c, p]), (1 - core, q_other.at[c, p])):
                start = pl.multiple_of((2 * p + side) * shard, shard)
                place[...] = acc[pl.ds(start, shard), :].astype(bf16)
        q_to_core(2 + c, lambda c=c: q_other.at[c])

    def near_step(step, carry):
        cut = pl.ds(pl.multiple_of(step * BLOCK * 2, BLOCK * 2), BLOCK * 2)
        near = dot_nt(q_buf[cut, :], wq_buf[...]) * score_scale
        g_near[pl.ds(step * 2, 2)] += near.reshape(2, BLOCK, width)
        return carry

    lax.fori_loop(0, own_tokens // (BLOCK * 2), near_step, 0)
    value_sums[...] = jnp.zeros_like(value_sums)

    sub = value_sums.shape[0]

    def gather_some(step):
        def one(n, carry):
            block = step * (key_blocks // 8) + n

            named = [inv[block * blocks + i] for i in range(blocks)]
            for r in range(BLOCK // sub):
                cut = slice(r * sub, (r + 1) * sub)
                total = jnp.zeros((sub, 2 * width), f32)
                for i in range(blocks):
                    total = total + slots[named[i], cut, :].astype(f32)
                kv_buf[block, cut, :] = total.astype(bf16)
                value_sums[...] += total[:, width:]
            return carry

        lax.fori_loop(0, key_blocks // 8, one, 0)

    stepped(8, gather_at, gather_step, gather_some)
    weights = copies.load(lambda: (full_kv, w_kv))
    every = copies.load(lambda: (rows_all, all_rows))
    table_sum[0] = table[...]
    table_sum[0, pl.ds(w_size, 1), pl.ds(0, width)] = score_scale * jnp.sum(
        q_buf[...].astype(f32), axis=0, keepdims=True
    )
    table_sum[0, pl.ds(w_size + 1, 1), pl.ds(0, width)] = jnp.sum(
        value_sums[...], axis=0, keepdims=True
    )
    table_send(0)
    weights.wait()

    def through_tile(j, left, step):
        given = kv_buf[pl.ds(j * piece, piece)].reshape(piece * BLOCK, 2 * width)
        weight = slots[pl.ds(0, width // BLOCK)].reshape(width, 2 * width)
        tile = dot_nt(given, weight).astype(bf16).reshape(piece, BLOCK, width)
        slots[pl.ds(through_from + step * piece, piece), :, pl.ds(left, width)] = tile

    def other_tile(step):
        through_tile(count + step, 0, step)
        for n in range(count):

            @pl.when(step == n)
            def _(n=n):
                state["through", n] = copies.send(
                    lambda: (through_other(n), g_core.at[n], here.core_peer)
                )

    def own_tile(step):
        through_tile(step, width, step)

    stepped(count, through_at, through_step, other_tile)
    stepped(count, through_at + count * through_step, through_step, own_tile)
    every.wait()

    def kv_terms(c):
        columns = pl.ds(pl.multiple_of(c * half, 128), half)
        acc[...] = jnp.zeros_like(acc)

        def deep(t, carry):
            rows = slots[pl.ds(rows_from + t * blocks, blocks), :, 0:width]
            given = kv_buf[pl.ds(t * blocks, blocks), :, columns]
            acc[...] += dot_tn(
                rows.reshape(own_tokens, width), given.reshape(own_tokens, half)
            )
            return carry

        lax.fori_loop(0, tokens // own_tokens, deep, 0)
        for p in range(pairs):
            for side, place in ((core, kv_own.at[c, p]), (1 - core, kv_other.at[c, p])):
                start = pl.multiple_of((2 * p + side) * shard, shard)
                place[...] = acc[pl.ds(start, shard), :].astype(bf16)
        for n in range(4):

            @pl.when(c == n)
            def _(n=n):
                kv_to_core(n, lambda: kv_other.at[n])

    stepped(4, terms_at, terms_step, kv_terms)
    events.run()
    copies.finish()


def back_all(ctx_size, w_size, small, large, shapes):
    width, tok, tokens, table_shape = shapes
    lines, pairs = ctx_size // 4, w_size // 2
    rows = width // w_size
    own_tokens = 2 * tok
    blocks = own_tokens // BLOCK
    keys = CANDS * BLOCK
    half = width // 2
    table_steps = 1 + len(bits(pairs)) + len(bits(lines)) + len(bits(4))
    any_space = pl.BlockSpec(memory_space=pl.ANY)
    in_vmem = pl.BlockSpec(memory_space=pltpu.VMEM)
    in_smem = pl.BlockSpec(memory_space=pltpu.SMEM)
    scratch = []
    for _ in range(BACK_GROUPS):
        scratch += group_scratch(lines, pairs, rows, half)
    piece = (tok // BLOCK, BLOCK, width)
    scratch += [
        pltpu.VMEM((tokens // BLOCK, BLOCK, 2 * width), bf16),
        pltpu.VMEM((blocks * CANDS + 1, BLOCK, 2 * width), bf16),
        pltpu.VMEM((keys, 2 * width), bf16),
        pltpu.VMEM((2, width // LANES, GROUP * BLOCK, keys), bf16),
        pltpu.VMEM((own_tokens, width), bf16),
        pltpu.VMEM((own_tokens, width), bf16),
        pltpu.VMEM((blocks, BLOCK, width), bf16),
        pltpu.VMEM((width, width), bf16),
        pltpu.VMEM((2, pairs, rows, half), bf16),
        pltpu.VMEM((4, pairs, rows, half), bf16),
        pltpu.VMEM((blocks, BLOCK, width), f32),
        pltpu.VMEM((2 * lines,) + piece, bf16),
        pltpu.VMEM((2 * lines - 2,) + piece, bf16),
        pltpu.VMEM((2,) + piece, bf16),
        pltpu.VMEM((width, half), f32),
        pltpu.VMEM((16, width), f32),
        pltpu.VMEM((table_steps,) + table_shape, f32),
        pltpu.VMEM((table_steps,) + table_shape, f32),
        pltpu.SemaphoreType.DMA((2,)),
        (
            pltpu.SemaphoreType.DMA((60,)),
            pltpu.SemaphoreType.DMA((160,)),
            pltpu.SemaphoreType.DMA((160,)),
        ),
    ]
    return pl.pallas_call(
        functools.partial(back_kernel, ctx_size, w_size),
        in_specs=[in_smem, in_smem, in_vmem] + [any_space] * len(large),
        out_specs=[any_space] * 6 + [in_vmem],
        out_shape=[
            jax.ShapeDtypeStruct((rows, 4 * width), bf16),
            jax.ShapeDtypeStruct((4 * rows, width), bf16),
            jax.ShapeDtypeStruct((2, rows, width), bf16),
            jax.ShapeDtypeStruct((2, rows, width), bf16),
            jax.ShapeDtypeStruct((2,) + piece, bf16),
            jax.ShapeDtypeStruct((2,) + piece, bf16),
            jax.ShapeDtypeStruct(table_shape, f32),
        ],
        scratch_shapes=scratch,
        compiler_params=pltpu.CompilerParams(
            collective_id=1, has_side_effects=True, vmem_limit_bytes=67043328
        ),
        name="back_all",
    )(*small, *large)


def front_kernel(ctx_size, w_size, *refs):
    here = Wires(ctx_size, w_size)
    lines, pairs = here.lines, here.pairs
    part, line, pair, core = here.part, here.line, here.pair, here.core
    (
        hidden,
        out_grad,
        ints,
        bias,
        vectors,
        w_query,
        w_key,
        w_value,
        w_out,
        w_up,
        w_down,
    ) = refs[:11]
    (
        rows_out,
        grads_out,
        ints_out,
        vectors_out,
        query_out,
        kv_weight_out,
        out_out,
        up_out,
        down_out,
        queries_out,
        kv_out,
        context_out,
        probs_out,
    ) = refs[11:24]
    (
        held_up,
        held_down,
        held_out,
        rows_buf,
        wq_buf,
        wkv_buf,
        vectors_buf,
        bias_buf,
        q_buf,
        ctx_buf,
        kv_buf,
        cat,
        probs_buf,
        pos,
        probs_sem,
        sems,
    ) = refs[24:]
    copies = Copies(*sems)
    width = w_query.shape[1]
    tok = rows_buf.shape[1]
    chunk_blocks = tok // BLOCK
    blocks = 2 * chunk_blocks
    groups = width // LANES
    chunks = rows_buf.shape[0]
    me = pair * 2 + core
    side = line % 2

    def target(turn):
        return here.at(2 * ((turn + part) % 2) + core, line, pair, part // 2)

    def source(turn):
        return here.at(2 * core + (part // 2 + turn) % 2, line, pair, part % 2)

    stays = [
        jnp.logical_and(2 * ((turn + part) % 2) + core == part, part // 2 == core)
        for turn in range(2)
    ]
    greet_all(here, target, source, stays)

    def deal(src, dst, turn):
        return copies.send(
            lambda: (src((turn + part) % 2), dst(turn), target(turn)), stays[turn]
        )

    dealt = [deal(lambda m: hidden.at[m, 0], lambda t: rows_buf.at[t], turn) for turn in range(2)]
    dealt_ints = [deal(lambda m: ints.at[m], lambda t: ints_out.at[t], turn) for turn in range(2)]
    dealt_bias = [deal(lambda m: bias.at[m], lambda t: bias_buf.at[t], turn) for turn in range(2)]

    early = [
        (w_key, lambda shard: wkv_buf.at[shard, :, pl.ds(0, width)]),
        (w_value, lambda shard: wkv_buf.at[shard, :, pl.ds(width, width)]),
        (vectors, lambda shard: vectors_buf.at[shard]),
        (w_query, lambda shard: wq_buf.at[shard]),
    ]
    late = [
        (w_up, held_up, lambda shard: up_out.at[shard]),
        (w_down, held_down, lambda shard: down_out.at[shard]),
        (w_out, held_out, lambda shard: out_out.at[shard]),
    ]
    across = [
        copies.send(lambda src=src, place=place: (src, place(me), here.pair_peer(1)))
        for src, place in early
    ]
    ready = [copies.load(lambda src=src, place=place: (src, place(me))) for src, place in early]
    arrive = [
        copies.send(lambda src=src, place=place: (src, place(me), here.core_peer))
        for src, place in early
    ]

    def half_cut(src, which):
        half = src.shape[0] // 2
        return pl.ds(pl.multiple_of(which * half, 16), half)

    halves = [
        copies.send(
            lambda src=src, place=place: (
                src.at[half_cut(src, side)],
                place(me).at[half_cut(src, side)],
                here.pair_peer(1),
            )
        )
        for src, _, place in late[:2]
    ]
    out_across = copies.send(lambda: (w_out, out_out.at[me], here.pair_peer(1)))
    staged = [copies.load(lambda src=src, held=held: (src, held)) for src, held, _ in late]
    ends = [
        copies.send(lambda src=src, place=place: (src, place(me), here.core_peer))
        for src, _, place in late
    ]
    placed = []

    crossed = []
    from_core = {}
    for turn in range(2):
        dealt[turn].wait_recv()
        for flip in range(1, lines):
            crossed.append(
                copies.send(
                    lambda turn=turn, flip=flip: (
                        rows_buf.at[turn],
                        rows_buf.at[flip * 2 + turn],
                        here.line_peer(flip),
                    )
                )
            )
        from_core[turn] = copies.send(
            lambda turn=turn: (rows_buf.at[turn], rows_buf.at[lines * 2 + turn], here.core_peer)
        )
    for turn in range(2):
        dealt_ints[turn].wait_recv()
    pos_ready = copies.load(lambda: (ints_out, pos))
    for copy, (src, held, place) in zip(staged, late):
        copy.wait()
        placed.append(copies.load(lambda held=held, place=place: (held, place(me))))
    theirs = (pair ^ 1) * 2 + core
    for copy, (src, place) in zip(across, early):
        copy.wait_recv()
        arrive.append(
            copies.send(lambda place=place: (place(theirs), place(theirs), here.core_peer))
        )
    for n, copy in enumerate(crossed):
        copy.wait_recv()
        from_core[2 + n] = copies.send(
            lambda n=n: (rows_buf.at[2 + n], rows_buf.at[lines * 2 + 2 + n], here.core_peer)
        )
    gradients = [
        deal(lambda m: out_grad.at[m, 0], lambda t: grads_out.at[t], turn) for turn in range(2)
    ]
    for copy in ready + arrive:
        copy.wait() if copy in ready else copy.wait_recv()
    keep = [
        copies.load(lambda: (wq_buf, query_out)),
        copies.load(lambda: (wkv_buf, kv_weight_out)),
    ]
    relayed = []

    def relay(n):
        halves[n].wait_recv()
        src, _, place = late[n]
        relayed.append(
            copies.send(
                lambda: (
                    place(theirs).at[half_cut(src, side)],
                    place(theirs).at[half_cut(src, side)],
                    here.line_peer(1),
                )
            )
        )
        ends.append(
            copies.send(
                lambda: (
                    place(theirs).at[half_cut(src, side)],
                    place(theirs).at[half_cut(src, side)],
                    here.core_peer,
                )
            )
        )

    def relay_last(n):
        relayed[n].wait_recv()
        src, _, place = late[n]
        ends.append(
            copies.send(
                lambda: (
                    place(theirs).at[half_cut(src, 1 - side)],
                    place(theirs).at[half_cut(src, 1 - side)],
                    here.core_peer,
                )
            )
        )

    def relay_out():
        out_across.wait_recv()
        ends.append(
            copies.send(lambda: (out_out.at[theirs], out_out.at[theirs], here.core_peer))
        )

    vectors_total = vectors_buf[0]
    for w in range(1, w_size):
        vectors_total = vectors_total + vectors_buf[w]
    vectors_out[...] = vectors_total
    kv_bias = jnp.concatenate(
        [jnp.zeros((1, width), f32), vectors_out[pl.ds(1, 1), :]], axis=1
    )
    query_bias = vectors_out[pl.ds(0, 1), :]

    weight = wq_buf[...].reshape(width, width)
    for turn in range(2):
        rows = pl.ds(turn * tok, tok)
        q_buf[rows, :] = (
            (dot_nn(rows_buf[turn], weight) + query_bias) * score_scale
        ).astype(bf16)

    def keys_and_values(step):
        for n in range(lines * 2, chunks):

            @pl.when(step == n)
            def _(n=n):
                from_core[n - lines * 2].wait_recv()

        both = dot_nn(rows_buf[step], wkv_buf[...].reshape(width, 2 * width))
        both = both + kv_bias
        kv_buf[pl.ds(step * chunk_blocks, chunk_blocks)] = both.astype(bf16).reshape(
            chunk_blocks, BLOCK, 2 * width
        )

        return step

    lax.fori_loop(0, chunks, lambda step, carry: (keys_and_values(step), carry)[1], 0)
    keep += [
        copies.load(lambda: (q_buf, queries_out)),
        copies.load(lambda: (kv_buf, kv_out)),
        copies.load(lambda: (rows_buf, rows_out)),
    ]
    relay(0)
    pos_ready.wait()
    for turn in range(2):
        dealt_bias[turn].wait_recv()
    head_of_lane = lax.broadcasted_iota(jnp.int32, (BLOCK, LANES), 1) // HEAD_DIM

    def put(i, slot):
        return pltpu.make_async_copy(probs_buf.at[slot], probs_out.at[i], probs_sem.at[slot])

    def attend_block(i, carry):
        turn, row, slot = i // chunk_blocks, i % chunk_blocks, i % 2
        for j in range(CANDS):
            cat[j * BLOCK : (j + 1) * BLOCK, :] = kv_buf[pos[turn, 0, row * CANDS + j]]

        @pl.when(i >= 2)
        def _():
            put(i - 2, slot).wait()

        mine = pl.ds(pl.multiple_of(i * BLOCK, BLOCK), BLOCK)
        masked = bias_buf[turn, row]
        for g in range(groups):
            lanes = slice(g * LANES, (g + 1) * LANES)
            v_lanes = slice(width + g * LANES, width + (g + 1) * LANES)
            q_all = spread_heads(q_buf[mine, lanes], head_of_lane)
            scores = dot_nt(q_all, cat[:, lanes]) + masked
            row_max = jnp.max(scores, axis=-1, keepdims=True)
            shifted = jnp.exp(scores - row_max)
            row_total = jnp.sum(shifted, axis=-1, keepdims=True)
            shares = (shifted * (1.0 / row_total)).astype(bf16)
            probs_buf[slot, g] = shares
            mixed = dot_nn(shares, cat[:, v_lanes])
            ctx_buf[mine, lanes] = pick_heads(mixed, head_of_lane).astype(bf16)
        put(i, slot).start()

        @pl.when(i == blocks - 3)
        def _():
            relay(1)

        return carry

    lax.fori_loop(0, blocks, attend_block, 0)
    keep.append(copies.load(lambda: (ctx_buf, context_out)))
    for n in range(2):
        relay_last(n)
        if n == 0:
            relay_out()
    for copy in gradients + ends:
        copy.wait_recv()
    for copy in placed + keep:
        copy.wait()
    for n in range(2):
        put(blocks - 2 + n, n).wait()
    copies.finish()


def front_all(ctx_size, w_size, hidden, out_grad, ints, bias, vectors, weights):
    w_query, w_key, w_value, w_out, w_up, w_down = weights
    lines = ctx_size // 4
    tok, width = hidden.shape[2], hidden.shape[3]
    rows = w_query.shape[0]
    chunks = lines * 4
    blocks = 2 * tok // BLOCK
    keys = CANDS * BLOCK
    groups = width // LANES
    probs_shape = (groups, GROUP * BLOCK, keys)
    key_blocks = chunks * tok // BLOCK
    shapes = [
        ((chunks, tok, width), bf16),
        ((2, tok, width), bf16),
        (ints.shape, ints.dtype),
        (vectors.shape, f32),
        ((w_size, rows, width), bf16),
        ((w_size, rows, 2 * width), bf16),
        ((w_size, rows, width), bf16),
        ((w_size,) + w_up.shape, bf16),
        ((w_size,) + w_down.shape, bf16),
        ((2 * tok, width), bf16),
        ((key_blocks, BLOCK, 2 * width), bf16),
        ((2 * tok, width), bf16),
        ((blocks,) + probs_shape, bf16),
    ]
    any_space = pl.BlockSpec(memory_space=pl.ANY)
    out_specs = [any_space] * len(shapes)
    out_specs[3] = pl.BlockSpec(memory_space=pltpu.VMEM)
    return pl.pallas_call(
        functools.partial(front_kernel, ctx_size, w_size),
        in_specs=[any_space] * 11,
        out_specs=out_specs,
        out_shape=[jax.ShapeDtypeStruct(shape, dtype) for shape, dtype in shapes],
        scratch_shapes=[
            pltpu.VMEM(w_up.shape, bf16),
            pltpu.VMEM(w_down.shape, bf16),
            pltpu.VMEM(w_out.shape, bf16),
            pltpu.VMEM((chunks, tok, width), bf16),
            pltpu.VMEM((w_size, rows, width), bf16),
            pltpu.VMEM((w_size, rows, 2 * width), bf16),
            pltpu.VMEM((w_size,) + vectors.shape, f32),
            pltpu.VMEM(bias.shape, f32),
            pltpu.VMEM((2 * tok, width), bf16),
            pltpu.VMEM((2 * tok, width), bf16),
            pltpu.VMEM((key_blocks, BLOCK, 2 * width), bf16),
            pltpu.VMEM((keys, 2 * width), bf16),
            pltpu.VMEM((2,) + probs_shape, bf16),
            pltpu.SMEM(ints.shape, ints.dtype),
            pltpu.SemaphoreType.DMA((2,)),
            (
                pltpu.SemaphoreType.DMA((24,)),
                pltpu.SemaphoreType.DMA((64,)),
                pltpu.SemaphoreType.DMA((64,)),
            ),
        ],
        compiler_params=pltpu.CompilerParams(
            collective_id=0, has_side_effects=True, vmem_limit_bytes=56 << 20
        ),
        name="front_all",
    )(hidden, out_grad, ints, bias, vectors, w_query, w_key, w_value, w_out, w_up, w_down)


def make_local(ctx_size, w_size):
    def local(
        hidden,
        out_grad,
        doc_lengths,
        rand_pick,
        w_query,
        w_key,
        w_value,
        w_out,
        w_up,
        w_down,
        b_query,
        b_value,
        b_out,
        b_up,
        b_down,
        ln1_gain,
        ln1_shift,
        ln2_gain,
        ln2_shift,
    ):
        wires = Wires(ctx_size, w_size)
        tok, width = hidden.shape[2], hidden.shape[3]
        ff = w_up.shape[1]
        tok_blocks = tok // BLOCK
        lines, pairs = wires.lines, wires.pairs
        micro = wires.part // 2

        vectors = [b_query, b_value, b_out, b_up, b_down, ln1_gain, ln1_shift, ln2_gain, ln2_shift]
        vector_sizes = [vector.shape[0] for vector in vectors]
        merged = lines == 2 and pairs == 2
        in_chunk = jnp.arange(tok_blocks, dtype=jnp.int32)
        if merged:
            raw_ids = wires.ctx * tok_blocks + in_chunk
            packed, masks = [], []
            for m in range(MICRO):
                safe_blocks, allowed = candidates(raw_ids, doc_lengths[m, 0], rand_pick[m, 0])
                chunk = safe_blocks // tok_blocks
                chunk_part, chunk_line = chunk // lines, chunk % lines
                place = (
                    ((chunk_part // 2) ^ (wires.part // 2)) * lines + (chunk_line ^ wires.line)
                ) * 2 + (chunk_part + m) % 2
                place = (place * tok_blocks + safe_blocks % tok_blocks).astype(jnp.int32)
                packed.append(
                    jnp.concatenate([place.reshape(-1), allowed.astype(jnp.int32).reshape(-1)])
                )
                masks.append(jnp.where(allowed, 0.0, masked_score).astype(f32))
            ints = jnp.pad(jnp.stack(packed), ((0, 0), (0, 1024 - 2 * tok_blocks * CANDS)))
            bias = jnp.repeat(jnp.stack(masks), BLOCK, axis=2)[:, :, None]
            flat = jnp.zeros((8 * b_query.shape[0],), f32)
            narrow = [vector for vector in vectors if vector is not b_up]
            for n, vector in enumerate(narrow):
                size = vector.shape[0]
                flat = flat + jnp.pad(vector.astype(f32), (n * size, (7 - n) * size))
            table = lax.dynamic_update_slice(
                jnp.zeros((16, width), f32),
                flat.reshape(8, -1),
                (jnp.int32(0), wires.w * b_query.shape[0]),
            )
            table = lax.dynamic_update_slice(
                table, b_up.astype(f32)[None], (8 + wires.w, jnp.int32(0))
            )
            (
                all_rows,
                grads_dealt,
                ints_dealt,
                vector_table,
                full_query,
                full_kv,
                full_out,
                full_up,
                full_down,
                queries,
                kv,
                context,
                probs,
            ) = front_all(
                ctx_size,
                w_size,
                hidden,
                out_grad,
                ints.reshape(MICRO, 8, 128),
                bias,
                table,
                (w_query, w_key, w_value, w_out, w_up, w_down),
            )
            bias_out, bias_down, gain_one, shift_one, gain_two, shift_two = [
                vector_table[n] for n in range(2, 8)
            ]
            bias_up = vector_table[8:12].reshape(-1)
            ints_dealt = ints_dealt[:, 0, : 2 * tok_blocks * CANDS].reshape(2, 2, -1, CANDS)
            pos = ints_dealt[:, 0].reshape(-1)
            allowed = ints_dealt[:, 1].reshape(-1, CANDS) != 0
        else:
            small_ints = jnp.concatenate(
                [rand_pick.reshape(MICRO, -1), doc_lengths.reshape(MICRO, -1)], axis=1
            )
            int_count = small_ints.shape[1]
            small_ints = jnp.pad(small_ints, ((0, 0), (0, 1024 - int_count))).reshape(MICRO, 8, 128)
            vector_row = vector_sizes[0]
            (
                all_rows,
                grads_dealt,
                ints_dealt,
                vector_table,
                full_query,
                full_kv,
                full_out,
                full_up,
                full_down,
            ) = gather_all(
                ctx_size,
                w_size,
                hidden,
                out_grad,
                small_ints,
                jnp.concatenate(
                    [vector.astype(f32).reshape(-1, vector_row) for vector in vectors], axis=0
                ),
                (w_query, w_key, w_value, w_out, w_up, w_down),
            )
            ints_dealt = ints_dealt.reshape(MICRO, -1)
            spread = []
            at = 0
            for size in vector_sizes:
                count = size // vector_row
                spread.append(vector_table[:, at : at + count].reshape(-1))
                at += count
            (
                bias_query,
                bias_value,
                bias_out,
                bias_up,
                bias_down,
                gain_one,
                shift_one,
                gain_two,
                shift_two,
            ) = spread

            picks = jnp.stack(
                [ints_dealt[turn, : tok_blocks * 3].reshape(tok_blocks, 3) for turn in range(2)]
            ).reshape(-1, 3)
            lengths = ints_dealt[0, tok_blocks * 3 : int_count]
            chunk_ids = [
                (2 * wires.core + (micro + turn) % 2) * lines + wires.line for turn in range(2)
            ]
            my_blocks = jnp.concatenate([chunk * tok_blocks + in_chunk for chunk in chunk_ids])
            safe_blocks, allowed = candidates(my_blocks, lengths, picks)
            chunk = safe_blocks // tok_blocks
            chunk_part, chunk_line = chunk // lines, chunk % lines
            place = (
                ((chunk_part // 2) ^ wires.core) * lines + (chunk_line ^ wires.line)
            ) * 2 + (chunk_part + micro) % 2
            pos = (place * tok_blocks + safe_blocks % tok_blocks).reshape(-1).astype(jnp.int32)
            bias = jnp.repeat(jnp.where(allowed, 0.0, masked_score).astype(f32), BLOCK, axis=1)[:, None]

            queries = ((dot_nn(all_rows.reshape(-1, width)[: 2 * tok], full_query.reshape(-1, width)) + bias_query) * score_scale).astype(bf16)
            kv_bias = jnp.concatenate([jnp.zeros_like(bias_value), bias_value])
            kv = (dot_nn(all_rows.reshape(-1, width), full_kv.reshape(-1, 2 * width)) + kv_bias).astype(bf16)
            context, probs = attend(pos, queries, bias, kv)
        all_rows = all_rows.reshape(-1, width)
        own_rows = all_rows[: 2 * tok]
        grads_dealt = grads_dealt.reshape(-1, width)
        full_query, full_kv, full_out, full_up, full_down = [
            full.reshape(-1, full.shape[2]) for full in (full_query, full_kv, full_out, full_up, full_down)
        ]
        rows_f32 = own_rows.astype(f32)

        attn_out = dot_nn(context, full_out) + bias_out
        normed, ln1_back = jax.vjp(layer_norm, rows_f32 + attn_out, gain_one, shift_one)
        normed_low = normed.astype(bf16)
        up_pre = dot_nn(normed_low, full_up) + bias_up
        gelu_out, gelu_back = jax.vjp(lambda v: jax.nn.gelu(v, approximate=True), up_pre)
        activated = gelu_out.astype(bf16)
        branch = dot_nn(activated, full_down) + bias_down
        final, ln2_back = jax.vjp(layer_norm, normed + branch, gain_two, shift_two)
        final = final.astype(bf16)

        def term_of(rows_a, rows_b, scale=None):
            term = dot_tn(rows_a, rows_b)
            if scale is not None:
                term = term * scale
            return term.astype(bf16).reshape(pairs, 2, -1, rows_b.shape[1])

        d_mid, grad_gain_two, grad_shift_two = ln2_back(grads_dealt.astype(f32))
        d_branch = d_mid.astype(bf16)
        term_down = term_of(activated, d_branch)
        d_act = dot_nt(d_branch, full_down)
        d_up = gelu_back(d_act)[0].astype(bf16)
        term_up = term_of(normed_low, d_up)
        d_normed = dot_nt(d_up, full_up) + d_mid
        d_sum, grad_gain_one, grad_shift_one = ln1_back(d_normed)
        d_attn = d_sum.astype(bf16)
        term_out = term_of(context, d_attn)
        d_context = dot_nt(d_attn, full_out).astype(bf16)

        def table_of(vectors):
            return jnp.concatenate([vector.reshape(w_size, -1) for vector in vectors], axis=1)

        def column_sums(rows_a):
            return jnp.sum(rows_a.astype(f32), axis=0)

        sums = (
            column_sums(d_attn),
            column_sums(d_up),
            column_sums(d_branch),
            grad_gain_one,
            grad_shift_one,
            grad_gain_two,
            grad_shift_two,
        )
        shard = width // w_size
        if merged:
            named = pos.reshape(-1, CANDS)[None] == jnp.arange(
                all_rows.shape[0] // BLOCK, dtype=jnp.int32
            ).reshape(-1, 1, 1)
            named = jnp.logical_and(named, allowed[None])
            slot = jnp.arange(allowed.size, dtype=jnp.int32).reshape(allowed.shape)[None]
            inv = jnp.min(jnp.where(named, slot, allowed.size), axis=2).reshape(-1)
            table = table_of(sums)
            table = jnp.pad(table, ((0, 8 - w_size), (0, 0)))
            term_down = term_down.reshape(pairs, 2, -1, shard, width)
            by_block = (-1, BLOCK, width)
            up, down, out_query, key_value, block_out, grad_hidden, table = back_all(
                ctx_size,
                w_size,
                (pos, inv, table),
                (
                    queries,
                    d_context,
                    d_sum.reshape(by_block),
                    probs,
                    kv,
                    all_rows.reshape(by_block),
                    full_kv.reshape(-1, BLOCK, 2 * width),
                    full_query,
                    final.reshape(2, -1, BLOCK, width),
                    term_up,
                    term_down,
                    term_out,
                ),
                (width, tok, all_rows.shape[0], table.shape),
            )
            row = lax.dynamic_slice(table, (wires.w, jnp.int32(0)), (1, table.shape[1]))[0]
            both = lax.dynamic_slice(
                table, (jnp.int32(w_size), wires.w * shard), (2, shard)
            )
            small = [both[0], both[1]]
            at = 0
            for size in vector_sizes[2:]:
                small.append(row[at : at + size])
                at += size

            return (
                block_out.reshape(2, 1, tok, width),
                grad_hidden.reshape(2, 1, tok, width).astype(f32),
                out_query[1].astype(f32),
                key_value[0].astype(f32),
                key_value[1].astype(f32),
                out_query[0].astype(f32),
                up.astype(f32),
                down.astype(f32),
                *small,
            )

        d_query, d_kv = attend_back(pos, queries, d_context, probs, kv)

        through = dot_nt(d_kv, full_kv).astype(bf16)
        near = d_sum + score_scale * dot_nt(d_query, full_query)
        term_kv = term_of(all_rows, d_kv)
        term_query = term_of(own_rows, d_query, score_scale)

        sums = (score_scale * column_sums(d_query), column_sums(d_kv[:, width:])) + sums
        table = table_of(sums)[:, None]
        term_down = term_down.reshape(pairs, 2, -1, shard, width)
        summed, block_out, grad_hidden, table = finish_all(
            ctx_size,
            w_size,
            (term_up, term_down, term_query, term_kv, term_out),
            ("wide", "tall", "wide", "wide", "wide"),
            through.reshape(-1, tok, width),
            near.reshape(-1, tok, width),
            final.reshape(-1, tok, width),
            table,
        )
        row = lax.dynamic_slice(
            table, (wires.w, jnp.int32(0), jnp.int32(0)), (1, 1, table.shape[2])
        )[0, 0]
        small = []
        at = 0
        for size in vector_sizes:
            small.append(row[at : at + size])
            at += size

        parts = lines // 2
        at = 0

        def wide(columns):
            nonlocal at
            count = columns * parts // width
            pieces = summed[at : at + count].astype(f32)
            at += count
            return jnp.concatenate([pieces[c] for c in range(count)], axis=1)

        grad_up = wide(ff)
        count = ff * parts // width
        grad_down = summed[at : at + count].astype(f32).reshape(-1, parts, shard, width // parts)
        grad_down = jnp.swapaxes(grad_down, 1, 2).reshape(-1, width)
        at += count
        grad_query, grad_key, grad_value, grad_out = [wide(width) for _ in range(4)]
        return (
            block_out[:, None],
            grad_hidden.astype(f32)[:, None],
            grad_query,
            grad_key,
            grad_value,
            grad_out,
            grad_up,
            grad_down,
            *small,
        )

    return local


def solution(mesh):
    tokens = P(None, "wshard", "ctx", None)
    in_specs = (
        tokens,
        tokens,
        P(None, "wshard", None),
        tokens,
        *[P("wshard", None)] * 6,
        *[P("wshard")] * 9,
    )
    out_specs = (tokens, tokens, *[P("wshard", None)] * 6, *[P("wshard")] * 9)
    return jax.shard_map(
        make_local(mesh.shape["ctx"], mesh.shape["wshard"]),
        mesh=mesh,
        in_specs=in_specs,
        out_specs=out_specs,
        check_vma=False,
    )
```

```python
import functools
import heapq
import math

import jax
import jax.numpy as jnp
from jax import lax
from jax.experimental import pallas as pl
from jax.experimental.pallas import tpu as pltpu
from jax.sharding import PartitionSpec as P

HEADS = 12
HEAD_DIM = 64
BLOCK = 64
MICRO = 2
GROUP = 4
LANES = GROUP * HEAD_DIM
CANDS = 8

masked_score = -1e30
norm_eps = 1e-12
score_scale = 1.0 / math.sqrt(HEAD_DIM)
bf16 = jnp.bfloat16
f32 = jnp.float32
MESH = pl.DeviceIdType.MESH


def layer_norm(values, ln_gain, ln_shift):
    center = values - jnp.mean(values, axis=-1, keepdims=True)
    spread = jnp.mean(center * center, axis=-1, keepdims=True)
    return center * lax.rsqrt(spread + norm_eps) * ln_gain + ln_shift


def candidates(blocks, lengths, chosen_raw):
    doc_ends = jnp.cumsum(lengths)
    doc_starts = doc_ends - lengths
    owner_doc = jnp.sum((blocks[:, None] >= doc_ends[None, :]).astype(jnp.int32), axis=1)
    doc_ids = jnp.arange(lengths.shape[0], dtype=jnp.int32)
    member = (owner_doc[:, None] == doc_ids[None, :]).astype(jnp.int32)
    doc_first = jnp.sum(member * doc_starts[None, :], axis=1)
    length = jnp.sum(member * lengths[None, :], axis=1)
    randoms = doc_first[:, None] + chosen_raw % length[:, None]
    columns = [blocks, blocks - 1, blocks + 1, doc_first, doc_first + 1]
    for column in range(chosen_raw.shape[1]):
        columns.append(randoms[:, column])
    chosen = jnp.stack(columns, axis=1)
    inside = (chosen >= doc_first[:, None]) & (chosen < (doc_first + length)[:, None])
    is_fresh = [jnp.ones(blocks.shape, dtype=jnp.bool_)]
    for column in range(1, chosen.shape[1]):
        is_fresh.append(jnp.all(chosen[:, :column] != chosen[:, column : column + 1], axis=1))
    allowed = inside & jnp.stack(is_fresh, axis=1)
    safe_blocks = jnp.where(allowed, chosen, blocks[:, None])
    return (safe_blocks, allowed)


def dot_nt(a, b):
    return lax.dot_general(a, b, (((1,), (1,)), ((), ())), preferred_element_type=f32)


def dot_nn(a, b):
    return lax.dot_general(a, b, (((1,), (0,)), ((), ())), preferred_element_type=f32)


def dot_tn(a, b):
    return lax.dot_general(a, b, (((0,), (0,)), ((), ())), preferred_element_type=f32)


def spread_heads(rows, head_of_lane):
    zero = jnp.zeros_like(rows)
    return jnp.concatenate([jnp.where(head_of_lane == h, rows, zero) for h in range(GROUP)], axis=0)


def pick_heads(rows, head_of_lane):
    total = jnp.zeros((BLOCK, LANES), f32)
    for h in range(GROUP):
        total = jnp.where(head_of_lane == h, rows[h * BLOCK : (h + 1) * BLOCK], total)
    return total


def attend_kernel(groups, width, pos_ref, q_ref, bias_ref, kv_ref, ctx_ref, probs_ref, cat):
    i = pl.program_id(0)
    for j in range(CANDS):
        start = pl.multiple_of(pos_ref[i * CANDS + j] * BLOCK, BLOCK)
        cat[j * BLOCK : (j + 1) * BLOCK, :] = kv_ref[pl.ds(start, BLOCK), :]
    head_of_lane = lax.broadcasted_iota(jnp.int32, (BLOCK, LANES), 1) // HEAD_DIM
    bias = bias_ref[0]
    for g in range(groups):
        lanes = slice(g * LANES, (g + 1) * LANES)
        v_lanes = slice(width + g * LANES, width + (g + 1) * LANES)
        q_all = spread_heads(q_ref[:, lanes], head_of_lane)
        scores = dot_nt(q_all, cat[:, lanes]) + bias
        row_max = jnp.max(scores, axis=-1, keepdims=True)
        shifted = jnp.exp(scores - row_max)
        row_total = jnp.sum(shifted, axis=-1, keepdims=True)
        probs = (shifted * (1.0 / row_total)).astype(bf16)
        probs_ref[0, g] = probs
        mixed = dot_nn(probs, cat[:, v_lanes])
        ctx_ref[:, lanes] = pick_heads(mixed, head_of_lane).astype(bf16)


def attend(pos, queries, bias, kv):
    rows, width = queries.shape
    blocks = rows // BLOCK
    groups = width // LANES
    keys = CANDS * BLOCK
    return pl.pallas_call(
        functools.partial(attend_kernel, groups, width),
        grid_spec=pltpu.PrefetchScalarGridSpec(
            num_scalar_prefetch=1,
            grid=(blocks,),
            in_specs=[
                pl.BlockSpec((BLOCK, width), lambda i, p: (i, 0)),
                pl.BlockSpec((1, 1, keys), lambda i, p: (i, 0, 0)),
                pl.BlockSpec(kv.shape, lambda i, p: (0, 0), pipeline_mode=pl.Buffered(1)),
            ],
            out_specs=[
                pl.BlockSpec((BLOCK, width), lambda i, p: (i, 0)),
                pl.BlockSpec((1, groups, GROUP * BLOCK, keys), lambda i, p: (i, 0, 0, 0)),
            ],
            scratch_shapes=[pltpu.VMEM((keys, 2 * width), bf16)],
        ),
        out_shape=[
            jax.ShapeDtypeStruct((rows, width), bf16),
            jax.ShapeDtypeStruct((blocks, groups, GROUP * BLOCK, keys), bf16),
        ],
        compiler_params=pltpu.CompilerParams(vmem_limit_bytes=48 << 20),
        cost_estimate=pl.CostEstimate(
            flops=blocks * groups * 4 * GROUP * BLOCK * keys * LANES,
            bytes_accessed=kv.size * 2 + rows * width * 4 + blocks * groups * GROUP * BLOCK * keys * 2,
            transcendentals=blocks * groups * GROUP * BLOCK * keys,
        ),
        name="attend",
    )(pos, queries, bias, kv)


def attend_back_kernel(
    groups, width, pos_ref, q_ref, dctx_ref, probs_ref, kv_ref, dq_ref, dkv_ref, cat, acc
):
    i = pl.program_id(0)

    @pl.when(i == 0)
    def _():
        acc[...] = jnp.zeros_like(acc)

    for j in range(CANDS):
        start = pl.multiple_of(pos_ref[i * CANDS + j] * BLOCK, BLOCK)
        cat[j * BLOCK : (j + 1) * BLOCK, :] = kv_ref[pl.ds(start, BLOCK), :]
    head_of_lane = lax.broadcasted_iota(jnp.int32, (BLOCK, LANES), 1) // HEAD_DIM
    for g in range(groups):
        lanes = slice(g * LANES, (g + 1) * LANES)
        v_lanes = slice(width + g * LANES, width + (g + 1) * LANES)
        q_all = spread_heads(q_ref[:, lanes], head_of_lane)
        d_all = spread_heads(dctx_ref[:, lanes], head_of_lane)
        probs_low = probs_ref[0, g]
        probs = probs_low.astype(f32)
        d_probs = dot_nt(d_all, cat[:, v_lanes])
        row_inner = jnp.sum(probs * d_probs, axis=-1, keepdims=True)
        d_scores = (probs * (d_probs - row_inner)).astype(bf16)
        dq_ref[:, lanes] = pick_heads(dot_nn(d_scores, cat[:, lanes]), head_of_lane).astype(bf16)
        d_key = dot_tn(d_scores, q_all)
        d_value = dot_tn(probs_low, d_all)
        for j in range(CANDS):
            start = pl.multiple_of(pos_ref[i * CANDS + j] * BLOCK, BLOCK)
            part = slice(j * BLOCK, (j + 1) * BLOCK)
            acc[pl.ds(start, BLOCK), lanes] += d_key[part]
            acc[pl.ds(start, BLOCK), v_lanes] += d_value[part]

    @pl.when(i == pl.num_programs(0) - 1)
    def _():
        dkv_ref[...] = acc[...].astype(bf16)


def attend_back(pos, queries, d_context, probs, kv):
    rows, width = queries.shape
    blocks = rows // BLOCK
    groups = width // LANES
    keys = CANDS * BLOCK
    return pl.pallas_call(
        functools.partial(attend_back_kernel, groups, width),
        grid_spec=pltpu.PrefetchScalarGridSpec(
            num_scalar_prefetch=1,
            grid=(blocks,),
            in_specs=[
                pl.BlockSpec((BLOCK, width), lambda i, p: (i, 0)),
                pl.BlockSpec((BLOCK, width), lambda i, p: (i, 0)),
                pl.BlockSpec((1, groups, GROUP * BLOCK, keys), lambda i, p: (i, 0, 0, 0)),
                pl.BlockSpec(kv.shape, lambda i, p: (0, 0), pipeline_mode=pl.Buffered(1)),
            ],
            out_specs=[
                pl.BlockSpec((BLOCK, width), lambda i, p: (i, 0)),
                pl.BlockSpec(kv.shape, lambda i, p: (0, 0), pipeline_mode=pl.Buffered(1)),
            ],
            scratch_shapes=[pltpu.VMEM((keys, 2 * width), bf16), pltpu.VMEM(kv.shape, f32)],
        ),
        out_shape=[
            jax.ShapeDtypeStruct((rows, width), bf16),
            jax.ShapeDtypeStruct(kv.shape, bf16),
        ],
        compiler_params=pltpu.CompilerParams(vmem_limit_bytes=60 << 20),
        cost_estimate=pl.CostEstimate(
            flops=blocks * groups * 8 * GROUP * BLOCK * keys * LANES,
            bytes_accessed=kv.size * 4 + rows * width * 6 + blocks * groups * GROUP * BLOCK * keys * 2,
            transcendentals=0,
        ),
        name="attend_back",
    )(pos, queries, d_context, probs, kv)


class Wires:
    def __init__(self, ctx_size, w_size):
        self.ctx_size, self.w_size = ctx_size, w_size
        self.lines = ctx_size // 4
        self.pairs = w_size // 2
        self.ctx = lax.axis_index("ctx")
        self.w = lax.axis_index("wshard")
        self.part = self.ctx // self.lines
        self.line = self.ctx % self.lines
        self.pair = self.w // 2
        self.core = self.w % 2

    def at(self, part, line, pair, core):
        return (part * self.lines + line, pair * 2 + core)

    @property
    def core_peer(self):
        return self.at(self.part, self.line, self.pair, 1 - self.core)

    def pair_peer(self, flip):
        return self.at(self.part, self.line, self.pair ^ flip, self.core)

    def line_peer(self, flip):
        return self.at(self.part, self.line ^ flip, self.pair, self.core)

    def part_peer(self, flip):
        return self.at(self.part ^ flip, self.line, self.pair, self.core)

    def move(self, value, to):
        perm = []
        for ctx in range(self.ctx_size):
            for w in range(self.w_size):
                part, line, pair, core = to(ctx // self.lines, ctx % self.lines, w // 2, w % 2)
                target = (part * self.lines + line) * self.w_size + pair * 2 + core
                perm.append((ctx * self.w_size + w, target))
        return lax.ppermute(value, ("ctx", "wshard"), perm)

    def to_core(self, value):
        return self.move(value, lambda part, line, pair, core: (part, line, pair, 1 - core))

    def to_pair(self, value, flip):
        return self.move(value, lambda part, line, pair, core: (part, line, pair ^ flip, core))

    def to_line(self, value, flip):
        return self.move(value, lambda part, line, pair, core: (part, line ^ flip, pair, core))

    def to_part(self, value, flip):
        return self.move(value, lambda part, line, pair, core: (part ^ flip, line, pair, core))

    def deal(self, value, turn):
        return self.move(
            value,
            lambda part, line, pair, core: (2 * ((turn + part) % 2) + core, line, pair, part // 2),
        )

    def deal_back(self, value, turn):
        return self.move(
            value,
            lambda part, line, pair, core: (2 * core + (part // 2 + turn) % 2, line, pair, part % 2),
        )


def bits(count):
    flips = []
    flip = 1
    while flip < count:
        flips.append(flip)
        flip *= 2
    return flips


def gather_kernel(wires_of, refs, outs, own_shards, local_sem, send_sem, recv_sem):
    hidden, out_grad, ints, vectors, w_query, w_key, w_value, w_out, w_up, w_down = refs
    rows_out, grads_out, ints_out, vectors_out, query_out, kv_out, out_out, up_out, down_out = outs
    here = wires_of()
    lines, pairs = here.lines, here.pairs
    part, line, pair, core = here.part, here.line, here.pair, here.core
    width = w_query.shape[1]
    used = [0]
    sent = []
    local = []
    placed = []

    def at(part, line, pair, core):
        return (part * lines + line, pair * 2 + core)

    core_peer = at(part, line, pair, 1 - core)

    def line_peer(flip):
        return at(part, line ^ flip, pair, core)

    def pair_peer(flip):
        return at(part, line, pair ^ flip, core)

    def deal_target(turn):
        return at(2 * ((turn + part) % 2) + core, line, pair, part // 2)

    def deal_source(turn):
        return at(2 * core + (part // 2 + turn) % 2, line, pair, part % 2)

    stays = [
        jnp.logical_and(
            2 * ((turn + part) % 2) + core == part, part // 2 == core
        )
        for turn in range(2)
    ]

    barrier = pltpu.get_barrier_semaphore()

    def greet(device):
        pl.semaphore_signal(barrier, inc=1, device_id=device, device_id_type=MESH)

    peers = [core_peer]
    peers += [line_peer(flip) for flip in range(1, lines)]
    peers += [pair_peer(flip) for flip in range(1, pairs)]
    for device in peers:
        greet(device)
    for turn in range(2):

        @pl.when(jnp.logical_not(stays[turn]))
        def _(turn=turn):
            greet(deal_target(turn))
            greet(deal_source(turn))

    staying = sum(stay.astype(jnp.int32) for stay in stays)
    pl.semaphore_wait(barrier, len(peers) + 4 - 2 * staying)

    def send(src, dst, device, stay=None):
        n = used[0]
        used[0] += 1
        copy = pltpu.make_async_remote_copy(
            src_ref=src,
            dst_ref=dst,
            send_sem=send_sem.at[n],
            recv_sem=recv_sem.at[n],
            device_id=device,
            device_id_type=MESH,
        )
        if stay is None:
            copy.start()
        else:

            @pl.when(stay)
            def _():
                pltpu.make_async_copy(src, dst, recv_sem.at[n]).start()

            @pl.when(jnp.logical_not(stay))
            def _():
                copy.start()

        sent.append((copy, stay))
        return copy

    def stage(src, held):
        copy = pltpu.make_async_copy(src, held, local_sem.at[len(local)])
        copy.start()
        local.append(copy)

    def place_held(held, dst):
        local[len(placed)].wait()
        copy = pltpu.make_async_copy(held, dst, local_sem.at[len(local) + len(placed)])
        copy.start()
        placed.append(copy)

    me = pair * 2 + core

    dealt = [
        send(
            hidden.at[(turn + part) % 2, 0],
            rows_out.at[turn],
            deal_target(turn),
            stays[turn],
        )
        for turn in range(2)
    ]

    matrices = [
        (w_up, lambda shard: up_out.at[shard], True),
        (w_down, lambda shard: down_out.at[shard], True),
        (w_query, lambda shard: query_out.at[shard], False),
        (w_key, lambda shard: kv_out.at[shard, :, :width], False),
        (w_value, lambda shard: kv_out.at[shard, :, width:], False),
        (w_out, lambda shard: out_out.at[shard], False),
        (vectors, lambda shard: vectors_out.at[shard], False),
    ]
    side = line % 2
    for (src, _, _), held in zip(matrices, own_shards):
        stage(src, held)

    def half_cuts(src):
        half = src.shape[0] // 2
        first = pl.ds(pl.multiple_of(side * half, 8), half)
        return first, pl.ds(pl.multiple_of((1 - side) * half, 8), half)

    halves = [
        (
            flip,
            src,
            place,
            send(src.at[half_cuts(src)[0]], place(me).at[half_cuts(src)[0]], pair_peer(flip)),
        )
        for src, place, split in matrices
        if split
        for flip in range(1, pairs)
    ]
    late = [
        send(ints.at[(turn + part) % 2], ints_out.at[turn], deal_target(turn), stays[turn])
        for turn in range(2)
    ]
    for src, place, _ in matrices:
        late.append(send(src, place(me), core_peer))

    crossed = []
    for turn in range(2):
        dealt[turn].wait_recv()
        for flip in range(1, lines):
            crossed.append(
                (
                    flip * 2 + turn,
                    send(rows_out.at[turn], rows_out.at[flip * 2 + turn], line_peer(flip)),
                )
            )
        late.append(send(rows_out.at[turn], rows_out.at[lines * 2 + turn], core_peer))
    for (src, place, _), held in zip(matrices, own_shards):
        place_held(held, place(me))

    relayed = []
    whole = [
        (src, place, flip)
        for src, place, split in matrices
        if not split
        for flip in range(1, pairs)
    ]
    direct = []
    for step, (flip, src, place, copy) in enumerate(halves):
        copy.wait_recv()
        first, second = half_cuts(src)
        shard = (pair ^ flip) * 2 + core
        got = place(shard).at[first]
        relayed.append((place(shard).at[second], send(got, got, line_peer(1))))
        late.append(send(got, got, core_peer))
        share = -(-len(whole) // len(halves))
        for src, place, flip in whole[step * share : (step + 1) * share]:
            direct.append((flip, place, send(src, place(me), pair_peer(flip))))
    late += [
        send(
            out_grad.at[(turn + part) % 2, 0],
            grads_out.at[turn],
            deal_target(turn),
            stays[turn],
        )
        for turn in range(2)
    ]
    for index, copy in crossed:
        copy.wait_recv()
        late.append(send(rows_out.at[index], rows_out.at[lines * 2 + index], core_peer))
    for flip, place, copy in direct:
        copy.wait_recv()
        shard = (pair ^ flip) * 2 + core
        late.append(send(place(shard), place(shard), core_peer))
    for got, copy in relayed:
        copy.wait_recv()
        late.append(send(got, got, core_peer))
    for copy in late:
        copy.wait_recv()
    for copy in placed:
        copy.wait()
    for copy, stay in sent:
        if stay is None:
            copy.wait_send()
        else:

            @pl.when(jnp.logical_not(stay))
            def _(copy=copy):
                copy.wait_send()


def gather_all(ctx_size, w_size, hidden, out_grad, ints, vectors, weights):
    w_query, w_key, w_value, w_out, w_up, w_down = weights
    lines, pairs = ctx_size // 4, w_size // 2
    tok, width = hidden.shape[2], hidden.shape[3]
    rows = w_query.shape[0]
    shapes = [
        ((lines * 4, tok, width), bf16),
        ((2, tok, width), bf16),
        (ints.shape, ints.dtype),
        ((w_size,) + vectors.shape, f32),
        ((w_size, rows, width), bf16),
        ((w_size, rows, 2 * width), bf16),
        ((w_size, rows, width), bf16),
        ((w_size,) + w_up.shape, bf16),
        ((w_size,) + w_down.shape, bf16),
    ]
    sems = 16 + 8 * lines + 20 * pairs

    def body(*refs):
        gather_kernel(
            lambda: Wires(ctx_size, w_size), refs[:10], refs[10:19], refs[19:26], *refs[26:]
        )

    return pl.pallas_call(
        body,
        in_specs=[pl.BlockSpec(memory_space=pl.ANY)] * 10,
        out_specs=[pl.BlockSpec(memory_space=pl.ANY)] * len(shapes),
        out_shape=[jax.ShapeDtypeStruct(shape, dtype) for shape, dtype in shapes],
        scratch_shapes=[
            *[
                pltpu.VMEM(shard.shape, shard.dtype)
                for shard in (w_up, w_down, w_query, w_key, w_value, w_out, vectors)
            ],
            pltpu.SemaphoreType.DMA((14,)),
            pltpu.SemaphoreType.DMA((sems,)),
            pltpu.SemaphoreType.DMA((sems,)),
        ],
        compiler_params=pltpu.CompilerParams(collective_id=0, has_side_effects=True),
        name="gather_all",
    )(hidden, out_grad, ints, vectors, w_query, w_key, w_value, w_out, w_up, w_down)


class Sent:
    def __init__(self, make, stay=None):
        self.make, self.stay = make, stay

    def wait(self):
        self.make().wait()

    def wait_recv(self):
        self.make().wait_recv()


class Copies:
    def __init__(self, local_sem, send_sem, recv_sem):
        self.local_sem, self.send_sem, self.recv_sem = local_sem, send_sem, recv_sem
        self.locals, self.sent = 0, []

    def load(self, pair):
        n = self.locals
        self.locals += 1
        copy = Sent(lambda: pltpu.make_async_copy(*pair(), self.local_sem.at[n]))
        copy.make().start()
        return copy

    def send(self, triple, stay=None):
        n = len(self.sent)

        def make():
            src, dst, device = triple()
            return pltpu.make_async_remote_copy(
                src_ref=src,
                dst_ref=dst,
                send_sem=self.send_sem.at[n],
                recv_sem=self.recv_sem.at[n],
                device_id=device,
                device_id_type=MESH,
            )

        if stay is None:
            make().start()
        else:

            @pl.when(stay)
            def _():
                src, dst, _ = triple()
                pltpu.make_async_copy(src, dst, self.recv_sem.at[n]).start()

            @pl.when(jnp.logical_not(stay))
            def _():
                make().start()

        copy = Sent(make, stay)
        self.sent.append(copy)
        return copy

    def finish(self):
        for copy in self.sent:
            if copy.stay is None:
                copy.make().wait_send()
            else:

                @pl.when(jnp.logical_not(copy.stay))
                def _(copy=copy):
                    copy.make().wait_send()


def add_blocks(dst, *srcs):
    if len(dst.shape) == 3:

        def each(i, carry):
            total = srcs[0][i].astype(f32)
            for src in srcs[1:]:
                total = total + src[i].astype(f32)
            dst[i] = total.astype(dst.dtype)
            return carry

        lax.fori_loop(0, dst.shape[0], each, 0)
        return
    rows = dst.shape[0]
    step = 48 if rows % 48 == 0 else 32

    def body(i, carry):
        cut = pl.ds(pl.multiple_of(i * step, step), step)
        total = srcs[0][cut, :].astype(f32)
        for src in srcs[1:]:
            total = total + src[cut, :].astype(f32)
        dst[cut, :] = total.astype(dst.dtype)
        return carry

    lax.fori_loop(0, rows // step, body, 0)


class Events:
    def __init__(self):
        self.items = []

    def add(self, time, action):
        self.items.append((time, len(self.items), action))

    def take(self, until):
        due = sorted([item for item in self.items if item[0] <= until], key=lambda item: item[:2])
        self.items = [item for item in self.items if item[0] > until]
        return [action for _, _, action in due]

    def run(self, until=math.inf):
        for action in self.take(until):
            action()


class Plan:
    def __init__(self, events):
        self.events, self.heap, self.free, self.count = events, [], {}, 0

    def at(self, time, action):
        heapq.heappush(self.heap, (time, self.count, action))
        self.count += 1

    def do(self, time, action):
        self.events.add(time, action)

    def send(self, link, time, length, then):
        def start(now):
            begin = max(now, self.free.get(link, 0.0))
            self.free[link] = begin + length
            self.at(begin + length + 2.0, then)

        self.at(time, start)

    def run(self):
        while self.heap:
            time, _, action = heapq.heappop(self.heap)
            action(time)


def group_scratch(lines, pairs, rows, columns):
    block = (rows, columns)
    return [
        pltpu.VMEM((2 * lines, pairs) + block, bf16),
        pltpu.VMEM((2 * lines, pairs) + block, bf16),
        pltpu.VMEM((2 * lines, max(pairs - 1, 1)) + block, bf16),
        pltpu.VMEM((2 * lines,) + block, bf16),
        pltpu.VMEM((2, max(lines - 1, 1)) + block, bf16),
        pltpu.VMEM((2,) + block, bf16),
        pltpu.VMEM((2,) + block, bf16),
        pltpu.VMEM((2,) + block, bf16),
    ]


GROUP_SCRATCH = 8
BACK_GROUPS = 6
ROWS_DELAY = (20.0, 30.0)


def reduce_group(here, copies, plan, chunks, scratch, place, unit, core_times):
    from_core, own, from_pairs, paired, from_lines, lined, from_parts, parted = scratch
    lines, pairs = here.lines, here.pairs
    line, pair, core, part = here.line, here.pair, here.core, here.part
    low_part = part % 2
    state = {}

    def to_core(i, view):
        state["core", i] = copies.send(lambda: (view(), from_core.at[i], here.core_peer))

    def begin(i):
        to_core(i, lambda: chunks[i](1 - core))
        state["own", i] = copies.load(lambda: (chunks[i](core), own.at[i]))

    def over_core(i):
        if ("own", i) in state:
            state["own", i].wait()
        state["core", i].wait_recv()
        for p in range(pairs):
            add_blocks(own.at[i, p], own.at[i, p], from_core.at[i, p])
        state["pair", i] = [
            copies.send(
                lambda flip=flip: (
                    own.at[i, pair ^ flip],
                    from_pairs.at[i, flip - 1],
                    here.pair_peer(flip),
                )
            )
            for flip in range(1, pairs)
        ]

    def over_pairs(i):
        for copy in state["pair", i]:
            copy.wait_recv()
        add_blocks(
            paired.at[i], own.at[i, pair], *[from_pairs.at[i, flip - 1] for flip in range(1, pairs)]
        )

    def to_lines(h):
        state["line", h] = [
            copies.send(
                lambda flip=flip: (
                    paired.at[h * lines + (line ^ flip)],
                    from_lines.at[h, flip - 1],
                    here.line_peer(flip),
                )
            )
            for flip in range(1, lines)
        ]

    def over_lines(h):
        for copy in state["line", h]:
            copy.wait_recv()
        add_blocks(
            lined.at[h],
            paired.at[h * lines + line],
            *[from_lines.at[h, flip - 1] for flip in range(1, lines)],
        )

    def to_part_one():
        state["one"] = copies.send(
            lambda: (lined.at[1 - low_part], from_parts.at[0], here.part_peer(1))
        )

    def over_part_one():
        state["one"].wait_recv()
        add_blocks(parted.at[0], lined.at[low_part], from_parts.at[0])
        state["two"] = copies.send(lambda: (parted.at[0], from_parts.at[1], here.part_peer(2)))

    def mine():
        return place(low_part, line)

    def other():
        return place(1 - low_part, line)

    def over_part_two():
        state["two"].wait_recv()
        add_blocks(parted.at[1], parted.at[0], from_parts.at[1])
        state["back"] = copies.send(lambda: (parted.at[1], mine(), here.part_peer(1)))
        state["place"] = copies.load(lambda: (parted.at[1], mine()))
        state["spread"] = [
            copies.send(lambda flip=flip: (parted.at[1], mine(), here.line_peer(flip)))
            for flip in range(1, lines)
        ]

    def spread_other():
        state["back"].wait_recv()
        state["spread"] += [
            copies.send(lambda flip=flip: (other(), other(), here.line_peer(flip)))
            for flip in range(1, lines)
        ]

    def end():
        state["place"].wait()
        for copy in state["spread"]:
            copy.wait_recv()

    lined_h = []

    def core_done(i, now):
        plan.do(now, functools.partial(over_core, i))
        plan.send("x", now + 0.7, (pairs - 1) * unit, functools.partial(pairs_done, i))

    def pairs_done(i, now):
        plan.do(now, functools.partial(over_pairs, i))
        if i % lines == lines - 1:
            h = i // lines
            plan.do(now + 0.01, functools.partial(to_lines, h))
            plan.send("y", now + 0.3, (lines - 1) * unit, functools.partial(lines_done, h))

    def lines_done(h, now):
        plan.do(now, functools.partial(over_lines, h))
        lined_h.append(h)
        if len(lined_h) == 2:
            plan.do(now + 0.01, to_part_one)
            plan.send("z", now + 0.3, unit, one_done)

    def one_done(now):
        plan.do(now, over_part_one)
        plan.send("z", now + 0.3, 2 * unit, two_done)

    def two_done(now):
        plan.do(now, over_part_two)
        plan.send("z", now + 0.3, unit, back_done)
        plan.send("y", now + 0.3, (lines - 1) * unit, lambda now: None)

    def back_done(now):
        plan.do(now, spread_other)
        plan.send("y", now + 0.1, (lines - 1) * unit, lambda now: None)

    for i in range(2 * lines):
        if chunks[i] is not None:
            plan.do(core_times[i - 2] + 0.01 if i >= 2 else -100.0, functools.partial(begin, i))
        plan.at(core_times[i], functools.partial(core_done, i))
    plan.do(10000.0, end)
    return to_core


def chunk_views(refs, kinds, width):
    views = []
    for ref, kind in zip(refs, kinds):
        if kind == "wide":
            for c in range(ref.shape[3] // width):
                views.append(
                    lambda core, ref=ref, cut=slice(c * width, (c + 1) * width): ref.at[
                        :, core, :, cut
                    ]
                )
        else:
            for b in range(ref.shape[2]):
                for c in range(ref.shape[4] // width):
                    views.append(
                        lambda core, ref=ref, b=b, cut=slice(c * width, (c + 1) * width): ref.at[
                            :, core, b, :, cut
                        ]
                    )
    return views


def finish_kernel(ctx_size, w_size, kinds, tables, *refs):
    here = Wires(ctx_size, w_size)
    lines, pairs = here.lines, here.pairs
    part, line, pair, core = here.part, here.line, here.pair, here.core
    terms = refs[: len(kinds)]
    through, near, final, table = refs[len(kinds) : len(kinds) + 4]
    at = len(kinds) + 4
    out, final_out, grad_out, table_out = refs[at : at + 4]
    at += 4
    groups = (len(refs) - at - 8) // GROUP_SCRATCH
    scratches = [
        refs[at + g * GROUP_SCRATCH : at + (g + 1) * GROUP_SCRATCH] for g in range(groups)
    ]
    at += groups * GROUP_SCRATCH
    g_core, g_own, g_line, g_near, g_sum, table_in, table_sum = refs[at : at + 7]
    copies = Copies(*refs[at + 7])
    micro = part // 2

    def back_target(turn):
        return here.at(2 * core + (micro + turn) % 2, line, pair, part % 2)

    def back_source(turn):
        return here.at(2 * ((turn + part) % 2) + core, line, pair, part // 2)

    stays = [
        jnp.logical_and(2 * core + (micro + turn) % 2 == part, part % 2 == core)
        for turn in range(2)
    ]
    barrier = pltpu.get_barrier_semaphore()

    def greet(device):
        pl.semaphore_signal(barrier, inc=1, device_id=device, device_id_type=MESH)

    peers = [here.core_peer, here.part_peer(1), here.part_peer(2)]
    peers += [here.line_peer(flip) for flip in range(1, lines)]
    peers += [here.pair_peer(flip) for flip in range(1, pairs)]
    for device in peers:
        greet(device)
    for turn in range(2):

        @pl.when(jnp.logical_not(stays[turn]))
        def _(turn=turn):
            greet(back_target(turn))
            greet(back_source(turn))

    staying = sum(stay.astype(jnp.int32) for stay in stays)
    pl.semaphore_wait(barrier, len(peers) + 4 - 2 * staying)

    events = Events()
    state = {}
    count = 2 * lines

    def begin_rows():
        state["core"] = [
            copies.send(lambda j=j: (through.at[count + j], g_core.at[j], here.core_peer))
            for j in range(count)
        ]
        state["own"] = [
            copies.load(lambda j=j: (through.at[j], g_own.at[j])) for j in range(count)
        ]
        state["near"] = copies.load(lambda: (near, g_near))
        state["out"] = [
            copies.send(
                lambda turn=turn: (final.at[turn], final_out.at[micro], back_target(turn)),
                stays[turn],
            )
            for turn in range(2)
        ]

    def rows_over_core():
        for j in reversed(range(count)):
            state["own"][j].wait()
            state["core"][j].wait_recv()
            add_blocks(g_own.at[j], g_own.at[j], g_core.at[j])
            if j >= 2:
                state["line", j] = copies.send(
                    lambda j=j: (g_own.at[j], g_line.at[j - 2], here.line_peer(j // 2))
                )

    def rows_over_lines():
        state["near"].wait()
        state["back"] = []
        for turn in range(2):
            others = []
            for flip in range(1, lines):
                state["line", 2 * flip + turn].wait_recv()
                others.append(g_line.at[2 * flip + turn - 2])
            add_blocks(g_sum.at[turn], g_near.at[turn], g_own.at[turn], *others)
            state["back"].append(
                copies.send(
                    lambda turn=turn: (g_sum.at[turn], grad_out.at[micro], back_target(turn)),
                    stays[turn],
                )
            )

    def end_rows():
        for copy in state["out"] + state["back"]:
            copy.wait_recv()

    steps = [here.core_peer]
    steps += [here.pair_peer(flip) for flip in bits(pairs)]
    steps += [here.line_peer(flip) for flip in bits(lines)]
    steps += [here.part_peer(flip) for flip in bits(4)]

    def table_send(n):
        src = table if n == 0 else table_sum.at[n - 1]
        state["table", n] = copies.send(lambda: (src, table_in.at[n], steps[n]))

    def table_step(n):
        state["table", n].wait_recv()
        before = table[...] if n == 0 else table_sum[n - 1]
        total = before + table_in[n]
        if n + 1 < len(steps):
            table_sum[n] = total
            table_send(n + 1)
        else:
            table_out[...] = total

    plan = Plan(events)
    events.add(-1001.0, begin_rows)
    events.add(-1000.5, lambda: table_send(0))
    events.add(0.5, rows_over_core)
    events.add(17.0, rows_over_lines)
    events.add(9000.0, end_rows)
    for n in range(len(steps)):
        events.add(2.5 + n * 6.0, functools.partial(table_step, n))
    views = chunk_views(terms, kinds, out.shape[2])
    size = 2 * lines
    for g in range(groups):
        reduce_group(
            here,
            copies,
            plan,
            views[g * size : (g + 1) * size],
            scratches[g],
            lambda h, line, g=g: out.at[g * size + h * lines + line],
            6.0,
            [2.0 + 1.5 * (g * size + i) for i in range(size)],
        )
    plan.run()
    events.run()
    copies.finish()


def finish_all(ctx_size, w_size, terms, kinds, through, near, final, table):
    lines, pairs = ctx_size // 4, w_size // 2
    count = 2 * lines
    tok, width = through.shape[1:]
    rows = width // w_size
    columns = width // (lines // 2)
    chunks = sum(term.size for term in terms) // (w_size * rows * columns)
    groups = chunks // (2 * lines)
    table_steps = 1 + len(bits(pairs)) + len(bits(lines)) + len(bits(4))
    block = (tok, width)
    any_space = pl.BlockSpec(memory_space=pl.ANY)
    in_vmem = pl.BlockSpec(memory_space=pltpu.VMEM)
    sems = 40 + 10 * lines + groups * 2 * lines * (6 + pairs)
    scratch = []
    for _ in range(groups):
        scratch += group_scratch(lines, pairs, rows, columns)
    scratch += [
        pltpu.VMEM((count,) + block, bf16),
        pltpu.VMEM((count,) + block, bf16),
        pltpu.VMEM((max(count - 2, 1),) + block, bf16),
        pltpu.VMEM((2,) + block, f32),
        pltpu.VMEM((2,) + block, bf16),
        pltpu.VMEM((table_steps,) + table.shape, f32),
        pltpu.VMEM((table_steps,) + table.shape, f32),
        (
            pltpu.SemaphoreType.DMA((sems,)),
            pltpu.SemaphoreType.DMA((sems,)),
            pltpu.SemaphoreType.DMA((sems,)),
        ),
    ]
    return pl.pallas_call(
        functools.partial(finish_kernel, ctx_size, w_size, kinds, table_steps),
        in_specs=[any_space] * (len(terms) + 3) + [in_vmem],
        out_specs=[any_space, any_space, any_space, in_vmem],
        out_shape=[
            jax.ShapeDtypeStruct((chunks, rows, columns), bf16),
            jax.ShapeDtypeStruct((2,) + block, bf16),
            jax.ShapeDtypeStruct((2,) + block, bf16),
            jax.ShapeDtypeStruct(table.shape, f32),
        ],
        scratch_shapes=scratch,
        compiler_params=pltpu.CompilerParams(
            collective_id=1, has_side_effects=True, vmem_limit_bytes=60 << 20
        ),
        name="finish_all",
    )(*terms, through, near, final, table)


def greet_all(here, back_target, back_source, stays):
    lines, pairs = here.lines, here.pairs
    barrier = pltpu.get_barrier_semaphore()

    def greet(device):
        pl.semaphore_signal(barrier, inc=1, device_id=device, device_id_type=MESH)

    peers = [here.core_peer, here.part_peer(1), here.part_peer(2)]
    peers += [here.line_peer(flip) for flip in range(1, lines)]
    peers += [here.pair_peer(flip) for flip in range(1, pairs)]
    for device in peers:
        greet(device)
    for turn in range(2):

        @pl.when(jnp.logical_not(stays[turn]))
        def _(turn=turn):
            greet(back_target(turn))
            greet(back_source(turn))

    staying = sum(stay.astype(jnp.int32) for stay in stays)
    pl.semaphore_wait(barrier, len(peers) + 4 - 2 * staying)


def back_kernel(ctx_size, w_size, *refs):
    here = Wires(ctx_size, w_size)
    lines, pairs = here.lines, here.pairs
    part, line, pair, core = here.part, here.line, here.pair, here.core
    micro = part // 2
    (
        pos,
        inv,
        table,
        queries,
        d_context,
        d_sum,
        probs,
        kv,
        rows_all,
        full_kv,
        full_query,
        final,
        term_up,
        term_down,
        term_out,
    ) = refs[:15]
    up_out, down_out, oq_out, kv_out, final_out, grad_out, table_out = refs[15:22]
    scratches = [
        refs[22 + g * GROUP_SCRATCH : 22 + (g + 1) * GROUP_SCRATCH] for g in range(BACK_GROUPS)
    ]
    (
        kv_buf,
        slots,
        cat,
        probs_buf,
        q_buf,
        dctx_buf,
        rows_buf,
        wq_buf,
        q_other,
        kv_other,
        g_near,
        g_core,
        g_line,
        g_sum,
        acc,
        value_sums,
        table_in,
        table_sum,
        probs_sem,
        sems,
    ) = refs[22 + BACK_GROUPS * GROUP_SCRATCH :]
    copies = Copies(*sems)
    own_tokens, width = q_buf.shape
    key_blocks = kv_buf.shape[0]
    tokens = key_blocks * BLOCK
    blocks = own_tokens // BLOCK
    piece = blocks // 2
    groups = width // LANES
    keys = CANDS * BLOCK
    shard = width // w_size
    half = width // 2

    def back_target(turn):
        return here.at(2 * core + (micro + turn) % 2, line, pair, part % 2)

    def back_source(turn):
        return here.at(2 * ((turn + part) % 2) + core, line, pair, part // 2)

    stays = [
        jnp.logical_and(2 * core + (micro + turn) % 2 == part, part % 2 == core)
        for turn in range(2)
    ]

    def fetch(i, slot):
        return pltpu.make_async_copy(probs.at[i], probs_buf.at[slot], probs_sem.at[slot])

    greet_all(here, back_target, back_source, stays)

    events = Events()
    state = {}
    count = 2 * lines

    w_kv = slots.at[pl.ds(0, width // BLOCK)]
    rows_from = 16
    all_rows = slots.at[pl.ds(rows_from, key_blocks), :, pl.ds(0, width)]
    through_from = rows_from + key_blocks

    def through_other(j):
        return slots.at[pl.ds(through_from + j * piece, piece), :, pl.ds(0, width)]

    def through_own(j):
        return slots.at[pl.ds(through_from + j * piece, piece), :, pl.ds(width, width)]

    def send_out():
        state["out"] = [
            copies.send(
                lambda turn=turn: (final.at[turn], final_out.at[micro], back_target(turn)),
                stays[turn],
            )
            for turn in range(2)
        ]

    def rows_over_core(turn):
        for j in reversed(range(turn, count, 2)):
            state["through", j].wait_recv()
            add_blocks(through_own(j), through_own(j), g_core.at[j])
            if j >= 2:
                state["line", j] = copies.send(
                    lambda j=j: (through_own(j), g_line.at[j - 2], here.line_peer(j // 2))
                )

    def rows_over_lines(turn):
        others = []
        for flip in range(1, lines):
            state["line", 2 * flip + turn].wait_recv()
            others.append(g_line.at[2 * flip + turn - 2])
        add_blocks(
            g_sum.at[turn], g_near.at[pl.ds(turn * piece, piece)], through_own(turn), *others
        )
        state["back", turn] = copies.send(
            lambda: (g_sum.at[turn], grad_out.at[micro], back_target(turn)), stays[turn]
        )

    def end_rows():
        for copy in state["out"] + [state["back", turn] for turn in range(2)]:
            copy.wait_recv()

    steps = [lambda: here.core_peer]
    steps += [lambda flip=flip: here.pair_peer(flip) for flip in bits(pairs)]
    steps += [lambda flip=flip: here.line_peer(flip) for flip in bits(lines)]
    steps += [lambda flip=flip: here.part_peer(flip) for flip in bits(4)]

    def table_send(n):
        state["table", n] = copies.send(lambda: (table_sum.at[n], table_in.at[n], steps[n]()))

    def table_step(n):
        state["table", n].wait_recv()
        total = table_sum[n] + table_in[n]
        if n + 1 < len(steps):
            table_sum[n + 1] = total
            table_send(n + 1)
        else:
            table_out[...] = total

    attend_at, attend_step = 9.0, 2.6
    gather_at = attend_at + blocks * attend_step + 3.0
    gather_step = 1.4
    through_at = gather_at + 8 * gather_step + 1.0
    through_step = 1.3
    terms_at = through_at + 8 * through_step
    terms_step = 2.6
    terms_end = terms_at + 4 * terms_step
    plan = Plan(events)
    plan.send("z", 0.0, 18.0, lambda now: None)

    views = chunk_views((term_up, term_down), ("wide", "tall"), half)
    size = 2 * lines
    ffn_groups = BACK_GROUPS - 2

    def half_columns(number):
        return pl.ds(pl.multiple_of(number * half, 128), half)

    def up_place(g):
        return lambda h, line: up_out.at[:, half_columns(g * size + h * lines + line)]

    def down_place(g):
        return lambda h, line: down_out.at[
            pl.ds(pl.multiple_of((2 * g + h) * shard, 16), shard), half_columns(line)
        ]

    places = [up_place(g) for g in range(ffn_groups // 2)]
    places += [down_place(g) for g in range(ffn_groups // 2)]
    for g in range(ffn_groups):
        order = [g * size + i for i in range(size)]
        reduce_group(
            here,
            copies,
            plan,
            views[g * size : (g + 1) * size],
            scratches[g],
            places[g],
            3.0,
            [max(2.5 + 0.7 * n, 3.0 * n - 9.0) for n in order],
        )
    out_views = [
        lambda side, cut=slice(c * half, (c + 1) * half): term_out.at[:, side, :, cut]
        for c in range(2)
    ]
    q_own = scratches[ffn_groups][1]
    q_to_core = reduce_group(
        here,
        copies,
        plan,
        out_views + [None, None],
        scratches[ffn_groups],
        lambda h, line: oq_out.at[h, :, half_columns(line)],
        3.0,
        [gather_at + 2.0 + 1.5 * i for i in range(4)],
    )
    kv_own = scratches[ffn_groups + 1][1]
    kv_to_core = reduce_group(
        here,
        copies,
        plan,
        [None] * 4,
        scratches[ffn_groups + 1],
        lambda h, line: kv_out.at[h, :, half_columns(line)],
        3.0,
        [terms_at + (i + 1) * terms_step + 1.5 for i in range(4)],
    )
    plan.do(-200.0, send_out)
    rows_at = through_at + 2 * count * through_step + 0.5

    def rows_done(turn, now):
        plan.do(now, functools.partial(rows_over_lines, turn))
        plan.send("z", now + 0.7, 9.0, lambda now: None)

    for turn in range(2):
        rows_time = rows_at + ROWS_DELAY[turn]
        plan.do(rows_time, functools.partial(rows_over_core, turn))
        plan.send("y", rows_time + 0.7, 9.0, functools.partial(rows_done, turn))
    plan.do(9000.0, end_rows)
    for n in range(len(steps)):
        plan.do(through_at + 3.0 + n * 5.0, functools.partial(table_step, n))
    plan.run()

    def stepped(number, at, each, body):
        def loop(step, carry):
            body(step)
            for n in range(number):
                due = events.take(at + (n + 1) * each)
                if due:

                    @pl.when(step == n)
                    def _(due=due):
                        for action in due:
                            action()

            return carry

        lax.fori_loop(0, number, loop, 0)

    events.run(0.0)
    first = [
        copies.load(lambda: (kv, kv_buf)),
        copies.load(lambda: (queries, q_buf)),
        copies.load(lambda: (d_context, dctx_buf)),
    ]
    later = [
        copies.load(lambda: (rows_all.at[pl.ds(0, blocks)], rows_buf)),
        copies.load(lambda: (full_query, wq_buf)),
        copies.load(lambda: (d_sum, g_near)),
    ]

    fetch(0, 0).start()
    events.run(attend_at)
    for copy in first:
        copy.wait()
    slots[blocks * CANDS] = jnp.zeros((BLOCK, 2 * width), bf16)

    head_of_lane = lax.broadcasted_iota(jnp.int32, (BLOCK, LANES), 1) // HEAD_DIM

    def attend_block(i):
        slot = i % 2
        fetch(i, slot).wait()

        @pl.when(i + 1 < blocks)
        def _():
            fetch(i + 1, 1 - slot).start()

        for j in range(CANDS):
            cat[j * BLOCK : (j + 1) * BLOCK, :] = kv_buf[pos[i * CANDS + j]]
        mine = pl.ds(pl.multiple_of(i * BLOCK, BLOCK), BLOCK)
        rows = pl.ds(i * CANDS, CANDS)
        by_slot = (CANDS, BLOCK, LANES)
        for g in range(groups):
            lanes = slice(g * LANES, (g + 1) * LANES)
            v_lanes = slice(width + g * LANES, width + (g + 1) * LANES)
            q_all = spread_heads(q_buf[mine, lanes], head_of_lane)
            d_all = spread_heads(dctx_buf[mine, lanes], head_of_lane)
            probs_low = probs_buf[slot, g]
            shares = probs_low.astype(f32)
            d_probs = dot_nt(d_all, cat[:, v_lanes])
            row_inner = jnp.sum(shares * d_probs, axis=-1, keepdims=True)
            d_scores = (shares * (d_probs - row_inner)).astype(bf16)
            slots[rows, :, lanes] = dot_tn(d_scores, q_all).astype(bf16).reshape(by_slot)
            slots[rows, :, v_lanes] = dot_tn(probs_low, d_all).astype(bf16).reshape(by_slot)
            q_buf[mine, lanes] = pick_heads(dot_nn(d_scores, cat[:, lanes]), head_of_lane).astype(
                bf16
            )

    stepped(blocks, attend_at, attend_step, attend_block)

    for copy in later:
        copy.wait()
    for c in range(2):
        columns = slice(c * half, (c + 1) * half)
        own_rows = rows_buf[...].reshape(own_tokens, width)
        acc[...] = dot_tn(own_rows, q_buf[:, columns]) * score_scale
        for p in range(pairs):
            for side, place in ((core, q_own.at[2 + c, p]), (1 - core, q_other.at[c, p])):
                start = pl.multiple_of((2 * p + side) * shard, shard)
                place[...] = acc[pl.ds(start, shard), :].astype(bf16)
        q_to_core(2 + c, lambda c=c: q_other.at[c])

    def near_step(step, carry):
        cut = pl.ds(pl.multiple_of(step * BLOCK * 2, BLOCK * 2), BLOCK * 2)
        near = dot_nt(q_buf[cut, :], wq_buf[...]) * score_scale
        g_near[pl.ds(step * 2, 2)] += near.reshape(2, BLOCK, width)
        return carry

    lax.fori_loop(0, own_tokens // (BLOCK * 2), near_step, 0)
    value_sums[...] = jnp.zeros_like(value_sums)

    sub = value_sums.shape[0]

    def gather_some(step):
        def one(n, carry):
            block = step * (key_blocks // 8) + n

            named = [inv[block * blocks + i] for i in range(blocks)]
            for r in range(BLOCK // sub):
                cut = slice(r * sub, (r + 1) * sub)
                total = jnp.zeros((sub, 2 * width), f32)
                for i in range(blocks):
                    total = total + slots[named[i], cut, :].astype(f32)
                kv_buf[block, cut, :] = total.astype(bf16)
                value_sums[...] += total[:, width:]
            return carry

        lax.fori_loop(0, key_blocks // 8, one, 0)

    stepped(8, gather_at, gather_step, gather_some)
    weights = copies.load(lambda: (full_kv, w_kv))
    every = copies.load(lambda: (rows_all, all_rows))
    table_sum[0] = table[...]
    table_sum[0, pl.ds(w_size, 1), pl.ds(0, width)] = score_scale * jnp.sum(
        q_buf[...].astype(f32), axis=0, keepdims=True
    )
    table_sum[0, pl.ds(w_size + 1, 1), pl.ds(0, width)] = jnp.sum(
        value_sums[...], axis=0, keepdims=True
    )
    table_send(0)
    weights.wait()

    def through_tile(j, left, step):
        given = kv_buf[pl.ds(j * piece, piece)].reshape(piece * BLOCK, 2 * width)
        weight = slots[pl.ds(0, width // BLOCK)].reshape(width, 2 * width)
        tile = dot_nt(given, weight).astype(bf16).reshape(piece, BLOCK, width)
        slots[pl.ds(through_from + step * piece, piece), :, pl.ds(left, width)] = tile

    def other_tile(step):
        through_tile(count + step, 0, step)
        for n in range(count):

            @pl.when(step == n)
            def _(n=n):
                state["through", n] = copies.send(
                    lambda: (through_other(n), g_core.at[n], here.core_peer)
                )

    def own_tile(step):
        through_tile(step, width, step)

    stepped(count, through_at, through_step, other_tile)
    stepped(count, through_at + count * through_step, through_step, own_tile)
    every.wait()

    def kv_terms(c):
        columns = pl.ds(pl.multiple_of(c * half, 128), half)
        acc[...] = jnp.zeros_like(acc)

        def deep(t, carry):
            rows = slots[pl.ds(rows_from + t * blocks, blocks), :, 0:width]
            given = kv_buf[pl.ds(t * blocks, blocks), :, columns]
            acc[...] += dot_tn(
                rows.reshape(own_tokens, width), given.reshape(own_tokens, half)
            )
            return carry

        lax.fori_loop(0, tokens // own_tokens, deep, 0)
        for p in range(pairs):
            for side, place in ((core, kv_own.at[c, p]), (1 - core, kv_other.at[c, p])):
                start = pl.multiple_of((2 * p + side) * shard, shard)
                place[...] = acc[pl.ds(start, shard), :].astype(bf16)
        for n in range(4):

            @pl.when(c == n)
            def _(n=n):
                kv_to_core(n, lambda: kv_other.at[n])

    stepped(4, terms_at, terms_step, kv_terms)
    events.run()
    copies.finish()


def back_all(ctx_size, w_size, small, large, shapes):
    width, tok, tokens, table_shape = shapes
    lines, pairs = ctx_size // 4, w_size // 2
    rows = width // w_size
    own_tokens = 2 * tok
    blocks = own_tokens // BLOCK
    keys = CANDS * BLOCK
    half = width // 2
    table_steps = 1 + len(bits(pairs)) + len(bits(lines)) + len(bits(4))
    any_space = pl.BlockSpec(memory_space=pl.ANY)
    in_vmem = pl.BlockSpec(memory_space=pltpu.VMEM)
    in_smem = pl.BlockSpec(memory_space=pltpu.SMEM)
    scratch = []
    for _ in range(BACK_GROUPS):
        scratch += group_scratch(lines, pairs, rows, half)
    piece = (tok // BLOCK, BLOCK, width)
    scratch += [
        pltpu.VMEM((tokens // BLOCK, BLOCK, 2 * width), bf16),
        pltpu.VMEM((blocks * CANDS + 1, BLOCK, 2 * width), bf16),
        pltpu.VMEM((keys, 2 * width), bf16),
        pltpu.VMEM((2, width // LANES, GROUP * BLOCK, keys), bf16),
        pltpu.VMEM((own_tokens, width), bf16),
        pltpu.VMEM((own_tokens, width), bf16),
        pltpu.VMEM((blocks, BLOCK, width), bf16),
        pltpu.VMEM((width, width), bf16),
        pltpu.VMEM((2, pairs, rows, half), bf16),
        pltpu.VMEM((4, pairs, rows, half), bf16),
        pltpu.VMEM((blocks, BLOCK, width), f32),
        pltpu.VMEM((2 * lines,) + piece, bf16),
        pltpu.VMEM((2 * lines - 2,) + piece, bf16),
        pltpu.VMEM((2,) + piece, bf16),
        pltpu.VMEM((width, half), f32),
        pltpu.VMEM((16, width), f32),
        pltpu.VMEM((table_steps,) + table_shape, f32),
        pltpu.VMEM((table_steps,) + table_shape, f32),
        pltpu.SemaphoreType.DMA((2,)),
        (
            pltpu.SemaphoreType.DMA((60,)),
            pltpu.SemaphoreType.DMA((160,)),
            pltpu.SemaphoreType.DMA((160,)),
        ),
    ]
    return pl.pallas_call(
        functools.partial(back_kernel, ctx_size, w_size),
        in_specs=[in_smem, in_smem, in_vmem] + [any_space] * len(large),
        out_specs=[any_space] * 6 + [in_vmem],
        out_shape=[
            jax.ShapeDtypeStruct((rows, 4 * width), bf16),
            jax.ShapeDtypeStruct((4 * rows, width), bf16),
            jax.ShapeDtypeStruct((2, rows, width), bf16),
            jax.ShapeDtypeStruct((2, rows, width), bf16),
            jax.ShapeDtypeStruct((2,) + piece, bf16),
            jax.ShapeDtypeStruct((2,) + piece, bf16),
            jax.ShapeDtypeStruct(table_shape, f32),
        ],
        scratch_shapes=scratch,
        compiler_params=pltpu.CompilerParams(
            collective_id=1, has_side_effects=True, vmem_limit_bytes=67043328
        ),
        name="back_all",
    )(*small, *large)


def front_kernel(ctx_size, w_size, *refs):
    here = Wires(ctx_size, w_size)
    lines, pairs = here.lines, here.pairs
    part, line, pair, core = here.part, here.line, here.pair, here.core
    (
        hidden,
        out_grad,
        ints,
        bias,
        vectors,
        w_query,
        w_key,
        w_value,
        w_out,
        w_up,
        w_down,
    ) = refs[:11]
    (
        rows_out,
        grads_out,
        ints_out,
        vectors_out,
        query_out,
        kv_weight_out,
        out_out,
        up_out,
        down_out,
        queries_out,
        kv_out,
        context_out,
        probs_out,
    ) = refs[11:24]
    (
        held_up,
        held_down,
        held_out,
        rows_buf,
        wq_buf,
        wkv_buf,
        vectors_buf,
        bias_buf,
        q_buf,
        ctx_buf,
        kv_buf,
        cat,
        probs_buf,
        pos,
        probs_sem,
        sems,
    ) = refs[24:]
    copies = Copies(*sems)
    width = w_query.shape[1]
    tok = rows_buf.shape[1]
    chunk_blocks = tok // BLOCK
    blocks = 2 * chunk_blocks
    groups = width // LANES
    chunks = rows_buf.shape[0]
    me = pair * 2 + core
    side = line % 2

    def target(turn):
        return here.at(2 * ((turn + part) % 2) + core, line, pair, part // 2)

    def source(turn):
        return here.at(2 * core + (part // 2 + turn) % 2, line, pair, part % 2)

    stays = [
        jnp.logical_and(2 * ((turn + part) % 2) + core == part, part // 2 == core)
        for turn in range(2)
    ]
    greet_all(here, target, source, stays)

    def deal(src, dst, turn):
        return copies.send(
            lambda: (src((turn + part) % 2), dst(turn), target(turn)), stays[turn]
        )

    dealt = [deal(lambda m: hidden.at[m, 0], lambda t: rows_buf.at[t], turn) for turn in range(2)]
    dealt_ints = [deal(lambda m: ints.at[m], lambda t: ints_out.at[t], turn) for turn in range(2)]
    dealt_bias = [deal(lambda m: bias.at[m], lambda t: bias_buf.at[t], turn) for turn in range(2)]

    early = [
        (w_key, lambda shard: wkv_buf.at[shard, :, pl.ds(0, width)]),
        (w_value, lambda shard: wkv_buf.at[shard, :, pl.ds(width, width)]),
        (vectors, lambda shard: vectors_buf.at[shard]),
        (w_query, lambda shard: wq_buf.at[shard]),
    ]
    late = [
        (w_up, held_up, lambda shard: up_out.at[shard]),
        (w_down, held_down, lambda shard: down_out.at[shard]),
        (w_out, held_out, lambda shard: out_out.at[shard]),
    ]
    across = [
        copies.send(lambda src=src, place=place: (src, place(me), here.pair_peer(1)))
        for src, place in early
    ]
    ready = [copies.load(lambda src=src, place=place: (src, place(me))) for src, place in early]
    arrive = [
        copies.send(lambda src=src, place=place: (src, place(me), here.core_peer))
        for src, place in early
    ]

    def half_cut(src, which):
        half = src.shape[0] // 2
        return pl.ds(pl.multiple_of(which * half, 16), half)

    halves = [
        copies.send(
            lambda src=src, place=place: (
                src.at[half_cut(src, side)],
                place(me).at[half_cut(src, side)],
                here.pair_peer(1),
            )
        )
        for src, _, place in late[:2]
    ]
    out_across = copies.send(lambda: (w_out, out_out.at[me], here.pair_peer(1)))
    staged = [copies.load(lambda src=src, held=held: (src, held)) for src, held, _ in late]
    ends = [
        copies.send(lambda src=src, place=place: (src, place(me), here.core_peer))
        for src, _, place in late
    ]
    placed = []

    crossed = []
    from_core = {}
    for turn in range(2):
        dealt[turn].wait_recv()
        for flip in range(1, lines):
            crossed.append(
                copies.send(
                    lambda turn=turn, flip=flip: (
                        rows_buf.at[turn],
                        rows_buf.at[flip * 2 + turn],
                        here.line_peer(flip),
                    )
                )
            )
        from_core[turn] = copies.send(
            lambda turn=turn: (rows_buf.at[turn], rows_buf.at[lines * 2 + turn], here.core_peer)
        )
    for turn in range(2):
        dealt_ints[turn].wait_recv()
    pos_ready = copies.load(lambda: (ints_out, pos))
    for copy, (src, held, place) in zip(staged, late):
        copy.wait()
        placed.append(copies.load(lambda held=held, place=place: (held, place(me))))
    theirs = (pair ^ 1) * 2 + core
    for copy, (src, place) in zip(across, early):
        copy.wait_recv()
        arrive.append(
            copies.send(lambda place=place: (place(theirs), place(theirs), here.core_peer))
        )
    for n, copy in enumerate(crossed):
        copy.wait_recv()
        from_core[2 + n] = copies.send(
            lambda n=n: (rows_buf.at[2 + n], rows_buf.at[lines * 2 + 2 + n], here.core_peer)
        )
    gradients = [
        deal(lambda m: out_grad.at[m, 0], lambda t: grads_out.at[t], turn) for turn in range(2)
    ]
    for copy in ready + arrive:
        copy.wait() if copy in ready else copy.wait_recv()
    keep = [
        copies.load(lambda: (wq_buf, query_out)),
        copies.load(lambda: (wkv_buf, kv_weight_out)),
    ]
    relayed = []

    def relay(n):
        halves[n].wait_recv()
        src, _, place = late[n]
        relayed.append(
            copies.send(
                lambda: (
                    place(theirs).at[half_cut(src, side)],
                    place(theirs).at[half_cut(src, side)],
                    here.line_peer(1),
                )
            )
        )
        ends.append(
            copies.send(
                lambda: (
                    place(theirs).at[half_cut(src, side)],
                    place(theirs).at[half_cut(src, side)],
                    here.core_peer,
                )
            )
        )

    def relay_last(n):
        relayed[n].wait_recv()
        src, _, place = late[n]
        ends.append(
            copies.send(
                lambda: (
                    place(theirs).at[half_cut(src, 1 - side)],
                    place(theirs).at[half_cut(src, 1 - side)],
                    here.core_peer,
                )
            )
        )

    def relay_out():
        out_across.wait_recv()
        ends.append(
            copies.send(lambda: (out_out.at[theirs], out_out.at[theirs], here.core_peer))
        )

    vectors_total = vectors_buf[0]
    for w in range(1, w_size):
        vectors_total = vectors_total + vectors_buf[w]
    vectors_out[...] = vectors_total
    kv_bias = jnp.concatenate(
        [jnp.zeros((1, width), f32), vectors_out[pl.ds(1, 1), :]], axis=1
    )
    query_bias = vectors_out[pl.ds(0, 1), :]

    weight = wq_buf[...].reshape(width, width)
    for turn in range(2):
        rows = pl.ds(turn * tok, tok)
        q_buf[rows, :] = (
            (dot_nn(rows_buf[turn], weight) + query_bias) * score_scale
        ).astype(bf16)

    def keys_and_values(step):
        for n in range(lines * 2, chunks):

            @pl.when(step == n)
            def _(n=n):
                from_core[n - lines * 2].wait_recv()

        both = dot_nn(rows_buf[step], wkv_buf[...].reshape(width, 2 * width))
        both = both + kv_bias
        kv_buf[pl.ds(step * chunk_blocks, chunk_blocks)] = both.astype(bf16).reshape(
            chunk_blocks, BLOCK, 2 * width
        )

        return step

    lax.fori_loop(0, chunks, lambda step, carry: (keys_and_values(step), carry)[1], 0)
    keep += [
        copies.load(lambda: (q_buf, queries_out)),
        copies.load(lambda: (kv_buf, kv_out)),
        copies.load(lambda: (rows_buf, rows_out)),
    ]
    relay(0)
    pos_ready.wait()
    for turn in range(2):
        dealt_bias[turn].wait_recv()
    head_of_lane = lax.broadcasted_iota(jnp.int32, (BLOCK, LANES), 1) // HEAD_DIM

    def put(i, slot):
        return pltpu.make_async_copy(probs_buf.at[slot], probs_out.at[i], probs_sem.at[slot])

    def attend_block(i, carry):
        turn, row, slot = i // chunk_blocks, i % chunk_blocks, i % 2
        for j in range(CANDS):
            cat[j * BLOCK : (j + 1) * BLOCK, :] = kv_buf[pos[turn, 0, row * CANDS + j]]

        @pl.when(i >= 2)
        def _():
            put(i - 2, slot).wait()

        mine = pl.ds(pl.multiple_of(i * BLOCK, BLOCK), BLOCK)
        masked = bias_buf[turn, row]
        for g in range(groups):
            lanes = slice(g * LANES, (g + 1) * LANES)
            v_lanes = slice(width + g * LANES, width + (g + 1) * LANES)
            q_all = spread_heads(q_buf[mine, lanes], head_of_lane)
            scores = dot_nt(q_all, cat[:, lanes]) + masked
            row_max = jnp.max(scores, axis=-1, keepdims=True)
            shifted = jnp.exp(scores - row_max)
            row_total = jnp.sum(shifted, axis=-1, keepdims=True)
            shares = (shifted * (1.0 / row_total)).astype(bf16)
            probs_buf[slot, g] = shares
            mixed = dot_nn(shares, cat[:, v_lanes])
            ctx_buf[mine, lanes] = pick_heads(mixed, head_of_lane).astype(bf16)
        put(i, slot).start()

        @pl.when(i == blocks - 3)
        def _():
            relay(1)

        return carry

    lax.fori_loop(0, blocks, attend_block, 0)
    keep.append(copies.load(lambda: (ctx_buf, context_out)))
    for n in range(2):
        relay_last(n)
        if n == 0:
            relay_out()
    for copy in gradients + ends:
        copy.wait_recv()
    for copy in placed + keep:
        copy.wait()
    for n in range(2):
        put(blocks - 2 + n, n).wait()
    copies.finish()


def front_all(ctx_size, w_size, hidden, out_grad, ints, bias, vectors, weights):
    w_query, w_key, w_value, w_out, w_up, w_down = weights
    lines = ctx_size // 4
    tok, width = hidden.shape[2], hidden.shape[3]
    rows = w_query.shape[0]
    chunks = lines * 4
    blocks = 2 * tok // BLOCK
    keys = CANDS * BLOCK
    groups = width // LANES
    probs_shape = (groups, GROUP * BLOCK, keys)
    key_blocks = chunks * tok // BLOCK
    shapes = [
        ((chunks, tok, width), bf16),
        ((2, tok, width), bf16),
        (ints.shape, ints.dtype),
        (vectors.shape, f32),
        ((w_size, rows, width), bf16),
        ((w_size, rows, 2 * width), bf16),
        ((w_size, rows, width), bf16),
        ((w_size,) + w_up.shape, bf16),
        ((w_size,) + w_down.shape, bf16),
        ((2 * tok, width), bf16),
        ((key_blocks, BLOCK, 2 * width), bf16),
        ((2 * tok, width), bf16),
        ((blocks,) + probs_shape, bf16),
    ]
    any_space = pl.BlockSpec(memory_space=pl.ANY)
    out_specs = [any_space] * len(shapes)
    out_specs[3] = pl.BlockSpec(memory_space=pltpu.VMEM)
    return pl.pallas_call(
        functools.partial(front_kernel, ctx_size, w_size),
        in_specs=[any_space] * 11,
        out_specs=out_specs,
        out_shape=[jax.ShapeDtypeStruct(shape, dtype) for shape, dtype in shapes],
        scratch_shapes=[
            pltpu.VMEM(w_up.shape, bf16),
            pltpu.VMEM(w_down.shape, bf16),
            pltpu.VMEM(w_out.shape, bf16),
            pltpu.VMEM((chunks, tok, width), bf16),
            pltpu.VMEM((w_size, rows, width), bf16),
            pltpu.VMEM((w_size, rows, 2 * width), bf16),
            pltpu.VMEM((w_size,) + vectors.shape, f32),
            pltpu.VMEM(bias.shape, f32),
            pltpu.VMEM((2 * tok, width), bf16),
            pltpu.VMEM((2 * tok, width), bf16),
            pltpu.VMEM((key_blocks, BLOCK, 2 * width), bf16),
            pltpu.VMEM((keys, 2 * width), bf16),
            pltpu.VMEM((2,) + probs_shape, bf16),
            pltpu.SMEM(ints.shape, ints.dtype),
            pltpu.SemaphoreType.DMA((2,)),
            (
                pltpu.SemaphoreType.DMA((24,)),
                pltpu.SemaphoreType.DMA((64,)),
                pltpu.SemaphoreType.DMA((64,)),
            ),
        ],
        compiler_params=pltpu.CompilerParams(
            collective_id=0, has_side_effects=True, vmem_limit_bytes=56 << 20
        ),
        name="front_all",
    )(hidden, out_grad, ints, bias, vectors, w_query, w_key, w_value, w_out, w_up, w_down)


def make_local(ctx_size, w_size):
    def local(
        hidden,
        out_grad,
        doc_lengths,
        rand_pick,
        w_query,
        w_key,
        w_value,
        w_out,
        w_up,
        w_down,
        b_query,
        b_value,
        b_out,
        b_up,
        b_down,
        ln1_gain,
        ln1_shift,
        ln2_gain,
        ln2_shift,
    ):
        wires = Wires(ctx_size, w_size)
        tok, width = hidden.shape[2], hidden.shape[3]
        ff = w_up.shape[1]
        tok_blocks = tok // BLOCK
        lines, pairs = wires.lines, wires.pairs
        micro = wires.part // 2

        vectors = [b_query, b_value, b_out, b_up, b_down, ln1_gain, ln1_shift, ln2_gain, ln2_shift]
        vector_sizes = [vector.shape[0] for vector in vectors]
        merged = lines == 2 and pairs == 2
        in_chunk = jnp.arange(tok_blocks, dtype=jnp.int32)
        if merged:
            raw_ids = wires.ctx * tok_blocks + in_chunk
            packed, masks = [], []
            for m in range(MICRO):
                safe_blocks, allowed = candidates(raw_ids, doc_lengths[m, 0], rand_pick[m, 0])
                chunk = safe_blocks // tok_blocks
                chunk_part, chunk_line = chunk // lines, chunk % lines
                place = (
                    ((chunk_part // 2) ^ (wires.part // 2)) * lines + (chunk_line ^ wires.line)
                ) * 2 + (chunk_part + m) % 2
                place = (place * tok_blocks + safe_blocks % tok_blocks).astype(jnp.int32)
                packed.append(
                    jnp.concatenate([place.reshape(-1), allowed.astype(jnp.int32).reshape(-1)])
                )
                masks.append(jnp.where(allowed, 0.0, masked_score).astype(f32))
            ints = jnp.pad(jnp.stack(packed), ((0, 0), (0, 1024 - 2 * tok_blocks * CANDS)))
            bias = jnp.repeat(jnp.stack(masks), BLOCK, axis=2)[:, :, None]
            flat = jnp.zeros((8 * b_query.shape[0],), f32)
            narrow = [vector for vector in vectors if vector is not b_up]
            for n, vector in enumerate(narrow):
                size = vector.shape[0]
                flat = flat + jnp.pad(vector.astype(f32), (n * size, (7 - n) * size))
            table = lax.dynamic_update_slice(
                jnp.zeros((16, width), f32),
                flat.reshape(8, -1),
                (jnp.int32(0), wires.w * b_query.shape[0]),
            )
            table = lax.dynamic_update_slice(
                table, b_up.astype(f32)[None], (8 + wires.w, jnp.int32(0))
            )
            (
                all_rows,
                grads_dealt,
                ints_dealt,
                vector_table,
                full_query,
                full_kv,
                full_out,
                full_up,
                full_down,
                queries,
                kv,
                context,
                probs,
            ) = front_all(
                ctx_size,
                w_size,
                hidden,
                out_grad,
                ints.reshape(MICRO, 8, 128),
                bias,
                table,
                (w_query, w_key, w_value, w_out, w_up, w_down),
            )
            bias_out, bias_down, gain_one, shift_one, gain_two, shift_two = [
                vector_table[n] for n in range(2, 8)
            ]
            bias_up = vector_table[8:12].reshape(-1)
            ints_dealt = ints_dealt[:, 0, : 2 * tok_blocks * CANDS].reshape(2, 2, -1, CANDS)
            pos = ints_dealt[:, 0].reshape(-1)
            allowed = ints_dealt[:, 1].reshape(-1, CANDS) != 0
        else:
            small_ints = jnp.concatenate(
                [rand_pick.reshape(MICRO, -1), doc_lengths.reshape(MICRO, -1)], axis=1
            )
            int_count = small_ints.shape[1]
            small_ints = jnp.pad(small_ints, ((0, 0), (0, 1024 - int_count))).reshape(MICRO, 8, 128)
            vector_row = vector_sizes[0]
            (
                all_rows,
                grads_dealt,
                ints_dealt,
                vector_table,
                full_query,
                full_kv,
                full_out,
                full_up,
                full_down,
            ) = gather_all(
                ctx_size,
                w_size,
                hidden,
                out_grad,
                small_ints,
                jnp.concatenate(
                    [vector.astype(f32).reshape(-1, vector_row) for vector in vectors], axis=0
                ),
                (w_query, w_key, w_value, w_out, w_up, w_down),
            )
            ints_dealt = ints_dealt.reshape(MICRO, -1)
            spread = []
            at = 0
            for size in vector_sizes:
                count = size // vector_row
                spread.append(vector_table[:, at : at + count].reshape(-1))
                at += count
            (
                bias_query,
                bias_value,
                bias_out,
                bias_up,
                bias_down,
                gain_one,
                shift_one,
                gain_two,
                shift_two,
            ) = spread

            picks = jnp.stack(
                [ints_dealt[turn, : tok_blocks * 3].reshape(tok_blocks, 3) for turn in range(2)]
            ).reshape(-1, 3)
            lengths = ints_dealt[0, tok_blocks * 3 : int_count]
            chunk_ids = [
                (2 * wires.core + (micro + turn) % 2) * lines + wires.line for turn in range(2)
            ]
            my_blocks = jnp.concatenate([chunk * tok_blocks + in_chunk for chunk in chunk_ids])
            safe_blocks, allowed = candidates(my_blocks, lengths, picks)
            chunk = safe_blocks // tok_blocks
            chunk_part, chunk_line = chunk // lines, chunk % lines
            place = (
                ((chunk_part // 2) ^ wires.core) * lines + (chunk_line ^ wires.line)
            ) * 2 + (chunk_part + micro) % 2
            pos = (place * tok_blocks + safe_blocks % tok_blocks).reshape(-1).astype(jnp.int32)
            bias = jnp.repeat(jnp.where(allowed, 0.0, masked_score).astype(f32), BLOCK, axis=1)[:, None]

            queries = ((dot_nn(all_rows.reshape(-1, width)[: 2 * tok], full_query.reshape(-1, width)) + bias_query) * score_scale).astype(bf16)
            kv_bias = jnp.concatenate([jnp.zeros_like(bias_value), bias_value])
            kv = (dot_nn(all_rows.reshape(-1, width), full_kv.reshape(-1, 2 * width)) + kv_bias).astype(bf16)
            context, probs = attend(pos, queries, bias, kv)
        all_rows = all_rows.reshape(-1, width)
        own_rows = all_rows[: 2 * tok]
        grads_dealt = grads_dealt.reshape(-1, width)
        full_query, full_kv, full_out, full_up, full_down = [
            full.reshape(-1, full.shape[2]) for full in (full_query, full_kv, full_out, full_up, full_down)
        ]
        rows_f32 = own_rows.astype(f32)

        attn_out = dot_nn(context, full_out) + bias_out
        normed, ln1_back = jax.vjp(layer_norm, rows_f32 + attn_out, gain_one, shift_one)
        normed_low = normed.astype(bf16)
        up_pre = dot_nn(normed_low, full_up) + bias_up
        gelu_out, gelu_back = jax.vjp(lambda v: jax.nn.gelu(v, approximate=True), up_pre)
        activated = gelu_out.astype(bf16)
        branch = dot_nn(activated, full_down) + bias_down
        final, ln2_back = jax.vjp(layer_norm, normed + branch, gain_two, shift_two)
        final = final.astype(bf16)

        def term_of(rows_a, rows_b, scale=None):
            term = dot_tn(rows_a, rows_b)
            if scale is not None:
                term = term * scale
            return term.astype(bf16).reshape(pairs, 2, -1, rows_b.shape[1])

        d_mid, grad_gain_two, grad_shift_two = ln2_back(grads_dealt.astype(f32))
        d_branch = d_mid.astype(bf16)
        term_down = term_of(activated, d_branch)
        d_act = dot_nt(d_branch, full_down)
        d_up = gelu_back(d_act)[0].astype(bf16)
        term_up = term_of(normed_low, d_up)
        d_normed = dot_nt(d_up, full_up) + d_mid
        d_sum, grad_gain_one, grad_shift_one = ln1_back(d_normed)
        d_attn = d_sum.astype(bf16)
        term_out = term_of(context, d_attn)
        d_context = dot_nt(d_attn, full_out).astype(bf16)

        def table_of(vectors):
            return jnp.concatenate([vector.reshape(w_size, -1) for vector in vectors], axis=1)

        def column_sums(rows_a):
            return jnp.sum(rows_a.astype(f32), axis=0)

        sums = (
            column_sums(d_attn),
            column_sums(d_up),
            column_sums(d_branch),
            grad_gain_one,
            grad_shift_one,
            grad_gain_two,
            grad_shift_two,
        )
        shard = width // w_size
        if merged:
            named = pos.reshape(-1, CANDS)[None] == jnp.arange(
                all_rows.shape[0] // BLOCK, dtype=jnp.int32
            ).reshape(-1, 1, 1)
            named = jnp.logical_and(named, allowed[None])
            slot = jnp.arange(allowed.size, dtype=jnp.int32).reshape(allowed.shape)[None]
            inv = jnp.min(jnp.where(named, slot, allowed.size), axis=2).reshape(-1)
            table = table_of(sums)
            table = jnp.pad(table, ((0, 8 - w_size), (0, 0)))
            term_down = term_down.reshape(pairs, 2, -1, shard, width)
            by_block = (-1, BLOCK, width)
            up, down, out_query, key_value, block_out, grad_hidden, table = back_all(
                ctx_size,
                w_size,
                (pos, inv, table),
                (
                    queries,
                    d_context,
                    d_sum.reshape(by_block),
                    probs,
                    kv,
                    all_rows.reshape(by_block),
                    full_kv.reshape(-1, BLOCK, 2 * width),
                    full_query,
                    final.reshape(2, -1, BLOCK, width),
                    term_up,
                    term_down,
                    term_out,
                ),
                (width, tok, all_rows.shape[0], table.shape),
            )
            row = lax.dynamic_slice(table, (wires.w, jnp.int32(0)), (1, table.shape[1]))[0]
            both = lax.dynamic_slice(
                table, (jnp.int32(w_size), wires.w * shard), (2, shard)
            )
            small = [both[0], both[1]]
            at = 0
            for size in vector_sizes[2:]:
                small.append(row[at : at + size])
                at += size

            return (
                block_out.reshape(2, 1, tok, width),
                grad_hidden.reshape(2, 1, tok, width).astype(f32),
                out_query[1].astype(f32),
                key_value[0].astype(f32),
                key_value[1].astype(f32),
                out_query[0].astype(f32),
                up.astype(f32),
                down.astype(f32),
                *small,
            )

        d_query, d_kv = attend_back(pos, queries, d_context, probs, kv)

        through = dot_nt(d_kv, full_kv).astype(bf16)
        near = d_sum + score_scale * dot_nt(d_query, full_query)
        term_kv = term_of(all_rows, d_kv)
        term_query = term_of(own_rows, d_query, score_scale)

        sums = (score_scale * column_sums(d_query), column_sums(d_kv[:, width:])) + sums
        table = table_of(sums)[:, None]
        term_down = term_down.reshape(pairs, 2, -1, shard, width)
        summed, block_out, grad_hidden, table = finish_all(
            ctx_size,
            w_size,
            (term_up, term_down, term_query, term_kv, term_out),
            ("wide", "tall", "wide", "wide", "wide"),
            through.reshape(-1, tok, width),
            near.reshape(-1, tok, width),
            final.reshape(-1, tok, width),
            table,
        )
        row = lax.dynamic_slice(
            table, (wires.w, jnp.int32(0), jnp.int32(0)), (1, 1, table.shape[2])
        )[0, 0]
        small = []
        at = 0
        for size in vector_sizes:
            small.append(row[at : at + size])
            at += size

        parts = lines // 2
        at = 0

        def wide(columns):
            nonlocal at
            count = columns * parts // width
            pieces = summed[at : at + count].astype(f32)
            at += count
            return jnp.concatenate([pieces[c] for c in range(count)], axis=1)

        grad_up = wide(ff)
        count = ff * parts // width
        grad_down = summed[at : at + count].astype(f32).reshape(-1, parts, shard, width // parts)
        grad_down = jnp.swapaxes(grad_down, 1, 2).reshape(-1, width)
        at += count
        grad_query, grad_key, grad_value, grad_out = [wide(width) for _ in range(4)]
        return (
            block_out[:, None],
            grad_hidden.astype(f32)[:, None],
            grad_query,
            grad_key,
            grad_value,
            grad_out,
            grad_up,
            grad_down,
            *small,
        )

    return local


def solution(mesh):
    tokens = P(None, "wshard", "ctx", None)
    in_specs = (
        tokens,
        tokens,
        P(None, "wshard", None),
        tokens,
        *[P("wshard", None)] * 6,
        *[P("wshard")] * 9,
    )
    out_specs = (tokens, tokens, *[P("wshard", None)] * 6, *[P("wshard")] * 9)
    return jax.shard_map(
        make_local(mesh.shape["ctx"], mesh.shape["wshard"]),
        mesh=mesh,
        in_specs=in_specs,
        out_specs=out_specs,
        check_vma=False,
    )
```

```python
import functools
import heapq
import math

import jax
import jax.numpy as jnp
from jax import lax
from jax.experimental import pallas as pl
from jax.experimental.pallas import tpu as pltpu
from jax.sharding import PartitionSpec as P

HEADS = 12
HEAD_DIM = 64
BLOCK = 64
MICRO = 2
GROUP = 4
LANES = GROUP * HEAD_DIM
CANDS = 8

masked_score = -1e30
norm_eps = 1e-12
score_scale = 1.0 / math.sqrt(HEAD_DIM)
bf16 = jnp.bfloat16
f32 = jnp.float32
MESH = pl.DeviceIdType.MESH


def layer_norm(values, ln_gain, ln_shift):
    center = values - jnp.mean(values, axis=-1, keepdims=True)
    spread = jnp.mean(center * center, axis=-1, keepdims=True)
    return center * lax.rsqrt(spread + norm_eps) * ln_gain + ln_shift


def candidates(blocks, lengths, chosen_raw):
    doc_ends = jnp.cumsum(lengths)
    doc_starts = doc_ends - lengths
    owner_doc = jnp.sum((blocks[:, None] >= doc_ends[None, :]).astype(jnp.int32), axis=1)
    doc_ids = jnp.arange(lengths.shape[0], dtype=jnp.int32)
    member = (owner_doc[:, None] == doc_ids[None, :]).astype(jnp.int32)
    doc_first = jnp.sum(member * doc_starts[None, :], axis=1)
    length = jnp.sum(member * lengths[None, :], axis=1)
    randoms = doc_first[:, None] + chosen_raw % length[:, None]
    columns = [blocks, blocks - 1, blocks + 1, doc_first, doc_first + 1]
    for column in range(chosen_raw.shape[1]):
        columns.append(randoms[:, column])
    chosen = jnp.stack(columns, axis=1)
    inside = (chosen >= doc_first[:, None]) & (chosen < (doc_first + length)[:, None])
    is_fresh = [jnp.ones(blocks.shape, dtype=jnp.bool_)]
    for column in range(1, chosen.shape[1]):
        is_fresh.append(jnp.all(chosen[:, :column] != chosen[:, column : column + 1], axis=1))
    allowed = inside & jnp.stack(is_fresh, axis=1)
    safe_blocks = jnp.where(allowed, chosen, blocks[:, None])
    return (safe_blocks, allowed)


def dot_nt(a, b):
    return lax.dot_general(a, b, (((1,), (1,)), ((), ())), preferred_element_type=f32)


def dot_nn(a, b):
    return lax.dot_general(a, b, (((1,), (0,)), ((), ())), preferred_element_type=f32)


def dot_tn(a, b):
    return lax.dot_general(a, b, (((0,), (0,)), ((), ())), preferred_element_type=f32)


def spread_heads(rows, head_of_lane):
    zero = jnp.zeros_like(rows)
    return jnp.concatenate([jnp.where(head_of_lane == h, rows, zero) for h in range(GROUP)], axis=0)


def pick_heads(rows, head_of_lane):
    total = jnp.zeros((BLOCK, LANES), f32)
    for h in range(GROUP):
        total = jnp.where(head_of_lane == h, rows[h * BLOCK : (h + 1) * BLOCK], total)
    return total


def attend_kernel(groups, width, pos_ref, q_ref, bias_ref, kv_ref, ctx_ref, probs_ref, cat):
    i = pl.program_id(0)
    for j in range(CANDS):
        start = pl.multiple_of(pos_ref[i * CANDS + j] * BLOCK, BLOCK)
        cat[j * BLOCK : (j + 1) * BLOCK, :] = kv_ref[pl.ds(start, BLOCK), :]
    head_of_lane = lax.broadcasted_iota(jnp.int32, (BLOCK, LANES), 1) // HEAD_DIM
    bias = bias_ref[0]
    for g in range(groups):
        lanes = slice(g * LANES, (g + 1) * LANES)
        v_lanes = slice(width + g * LANES, width + (g + 1) * LANES)
        q_all = spread_heads(q_ref[:, lanes], head_of_lane)
        scores = dot_nt(q_all, cat[:, lanes]) + bias
        row_max = jnp.max(scores, axis=-1, keepdims=True)
        shifted = jnp.exp(scores - row_max)
        row_total = jnp.sum(shifted, axis=-1, keepdims=True)
        probs = (shifted * (1.0 / row_total)).astype(bf16)
        probs_ref[0, g] = probs
        mixed = dot_nn(probs, cat[:, v_lanes])
        ctx_ref[:, lanes] = pick_heads(mixed, head_of_lane).astype(bf16)


def attend(pos, queries, bias, kv):
    rows, width = queries.shape
    blocks = rows // BLOCK
    groups = width // LANES
    keys = CANDS * BLOCK
    return pl.pallas_call(
        functools.partial(attend_kernel, groups, width),
        grid_spec=pltpu.PrefetchScalarGridSpec(
            num_scalar_prefetch=1,
            grid=(blocks,),
            in_specs=[
                pl.BlockSpec((BLOCK, width), lambda i, p: (i, 0)),
                pl.BlockSpec((1, 1, keys), lambda i, p: (i, 0, 0)),
                pl.BlockSpec(kv.shape, lambda i, p: (0, 0), pipeline_mode=pl.Buffered(1)),
            ],
            out_specs=[
                pl.BlockSpec((BLOCK, width), lambda i, p: (i, 0)),
                pl.BlockSpec((1, groups, GROUP * BLOCK, keys), lambda i, p: (i, 0, 0, 0)),
            ],
            scratch_shapes=[pltpu.VMEM((keys, 2 * width), bf16)],
        ),
        out_shape=[
            jax.ShapeDtypeStruct((rows, width), bf16),
            jax.ShapeDtypeStruct((blocks, groups, GROUP * BLOCK, keys), bf16),
        ],
        compiler_params=pltpu.CompilerParams(vmem_limit_bytes=48 << 20),
        cost_estimate=pl.CostEstimate(
            flops=blocks * groups * 4 * GROUP * BLOCK * keys * LANES,
            bytes_accessed=kv.size * 2 + rows * width * 4 + blocks * groups * GROUP * BLOCK * keys * 2,
            transcendentals=blocks * groups * GROUP * BLOCK * keys,
        ),
        name="attend",
    )(pos, queries, bias, kv)


def attend_back_kernel(
    groups, width, pos_ref, q_ref, dctx_ref, probs_ref, kv_ref, dq_ref, dkv_ref, cat, acc
):
    i = pl.program_id(0)

    @pl.when(i == 0)
    def _():
        acc[...] = jnp.zeros_like(acc)

    for j in range(CANDS):
        start = pl.multiple_of(pos_ref[i * CANDS + j] * BLOCK, BLOCK)
        cat[j * BLOCK : (j + 1) * BLOCK, :] = kv_ref[pl.ds(start, BLOCK), :]
    head_of_lane = lax.broadcasted_iota(jnp.int32, (BLOCK, LANES), 1) // HEAD_DIM
    for g in range(groups):
        lanes = slice(g * LANES, (g + 1) * LANES)
        v_lanes = slice(width + g * LANES, width + (g + 1) * LANES)
        q_all = spread_heads(q_ref[:, lanes], head_of_lane)
        d_all = spread_heads(dctx_ref[:, lanes], head_of_lane)
        probs_low = probs_ref[0, g]
        probs = probs_low.astype(f32)
        d_probs = dot_nt(d_all, cat[:, v_lanes])
        row_inner = jnp.sum(probs * d_probs, axis=-1, keepdims=True)
        d_scores = (probs * (d_probs - row_inner)).astype(bf16)
        dq_ref[:, lanes] = pick_heads(dot_nn(d_scores, cat[:, lanes]), head_of_lane).astype(bf16)
        d_key = dot_tn(d_scores, q_all)
        d_value = dot_tn(probs_low, d_all)
        for j in range(CANDS):
            start = pl.multiple_of(pos_ref[i * CANDS + j] * BLOCK, BLOCK)
            part = slice(j * BLOCK, (j + 1) * BLOCK)
            acc[pl.ds(start, BLOCK), lanes] += d_key[part]
            acc[pl.ds(start, BLOCK), v_lanes] += d_value[part]

    @pl.when(i == pl.num_programs(0) - 1)
    def _():
        dkv_ref[...] = acc[...].astype(bf16)


def attend_back(pos, queries, d_context, probs, kv):
    rows, width = queries.shape
    blocks = rows // BLOCK
    groups = width // LANES
    keys = CANDS * BLOCK
    return pl.pallas_call(
        functools.partial(attend_back_kernel, groups, width),
        grid_spec=pltpu.PrefetchScalarGridSpec(
            num_scalar_prefetch=1,
            grid=(blocks,),
            in_specs=[
                pl.BlockSpec((BLOCK, width), lambda i, p: (i, 0)),
                pl.BlockSpec((BLOCK, width), lambda i, p: (i, 0)),
                pl.BlockSpec((1, groups, GROUP * BLOCK, keys), lambda i, p: (i, 0, 0, 0)),
                pl.BlockSpec(kv.shape, lambda i, p: (0, 0), pipeline_mode=pl.Buffered(1)),
            ],
            out_specs=[
                pl.BlockSpec((BLOCK, width), lambda i, p: (i, 0)),
                pl.BlockSpec(kv.shape, lambda i, p: (0, 0), pipeline_mode=pl.Buffered(1)),
            ],
            scratch_shapes=[pltpu.VMEM((keys, 2 * width), bf16), pltpu.VMEM(kv.shape, f32)],
        ),
        out_shape=[
            jax.ShapeDtypeStruct((rows, width), bf16),
            jax.ShapeDtypeStruct(kv.shape, bf16),
        ],
        compiler_params=pltpu.CompilerParams(vmem_limit_bytes=60 << 20),
        cost_estimate=pl.CostEstimate(
            flops=blocks * groups * 8 * GROUP * BLOCK * keys * LANES,
            bytes_accessed=kv.size * 4 + rows * width * 6 + blocks * groups * GROUP * BLOCK * keys * 2,
            transcendentals=0,
        ),
        name="attend_back",
    )(pos, queries, d_context, probs, kv)


class Wires:
    def __init__(self, ctx_size, w_size):
        self.ctx_size, self.w_size = ctx_size, w_size
        self.lines = ctx_size // 4
        self.pairs = w_size // 2
        self.ctx = lax.axis_index("ctx")
        self.w = lax.axis_index("wshard")
        self.part = self.ctx // self.lines
        self.line = self.ctx % self.lines
        self.pair = self.w // 2
        self.core = self.w % 2

    def at(self, part, line, pair, core):
        return (part * self.lines + line, pair * 2 + core)

    @property
    def core_peer(self):
        return self.at(self.part, self.line, self.pair, 1 - self.core)

    def pair_peer(self, flip):
        return self.at(self.part, self.line, self.pair ^ flip, self.core)

    def line_peer(self, flip):
        return self.at(self.part, self.line ^ flip, self.pair, self.core)

    def part_peer(self, flip):
        return self.at(self.part ^ flip, self.line, self.pair, self.core)

    def move(self, value, to):
        perm = []
        for ctx in range(self.ctx_size):
            for w in range(self.w_size):
                part, line, pair, core = to(ctx // self.lines, ctx % self.lines, w // 2, w % 2)
                target = (part * self.lines + line) * self.w_size + pair * 2 + core
                perm.append((ctx * self.w_size + w, target))
        return lax.ppermute(value, ("ctx", "wshard"), perm)

    def to_core(self, value):
        return self.move(value, lambda part, line, pair, core: (part, line, pair, 1 - core))

    def to_pair(self, value, flip):
        return self.move(value, lambda part, line, pair, core: (part, line, pair ^ flip, core))

    def to_line(self, value, flip):
        return self.move(value, lambda part, line, pair, core: (part, line ^ flip, pair, core))

    def to_part(self, value, flip):
        return self.move(value, lambda part, line, pair, core: (part ^ flip, line, pair, core))

    def deal(self, value, turn):
        return self.move(
            value,
            lambda part, line, pair, core: (2 * ((turn + part) % 2) + core, line, pair, part // 2),
        )

    def deal_back(self, value, turn):
        return self.move(
            value,
            lambda part, line, pair, core: (2 * core + (part // 2 + turn) % 2, line, pair, part % 2),
        )


def bits(count):
    flips = []
    flip = 1
    while flip < count:
        flips.append(flip)
        flip *= 2
    return flips


def gather_kernel(wires_of, refs, outs, own_shards, local_sem, send_sem, recv_sem):
    hidden, out_grad, ints, vectors, w_query, w_key, w_value, w_out, w_up, w_down = refs
    rows_out, grads_out, ints_out, vectors_out, query_out, kv_out, out_out, up_out, down_out = outs
    here = wires_of()
    lines, pairs = here.lines, here.pairs
    part, line, pair, core = here.part, here.line, here.pair, here.core
    width = w_query.shape[1]
    used = [0]
    sent = []
    local = []
    placed = []

    def at(part, line, pair, core):
        return (part * lines + line, pair * 2 + core)

    core_peer = at(part, line, pair, 1 - core)

    def line_peer(flip):
        return at(part, line ^ flip, pair, core)

    def pair_peer(flip):
        return at(part, line, pair ^ flip, core)

    def deal_target(turn):
        return at(2 * ((turn + part) % 2) + core, line, pair, part // 2)

    def deal_source(turn):
        return at(2 * core + (part // 2 + turn) % 2, line, pair, part % 2)

    stays = [
        jnp.logical_and(
            2 * ((turn + part) % 2) + core == part, part // 2 == core
        )
        for turn in range(2)
    ]

    barrier = pltpu.get_barrier_semaphore()

    def greet(device):
        pl.semaphore_signal(barrier, inc=1, device_id=device, device_id_type=MESH)

    peers = [core_peer]
    peers += [line_peer(flip) for flip in range(1, lines)]
    peers += [pair_peer(flip) for flip in range(1, pairs)]
    for device in peers:
        greet(device)
    for turn in range(2):

        @pl.when(jnp.logical_not(stays[turn]))
        def _(turn=turn):
            greet(deal_target(turn))
            greet(deal_source(turn))

    staying = sum(stay.astype(jnp.int32) for stay in stays)
    pl.semaphore_wait(barrier, len(peers) + 4 - 2 * staying)

    def send(src, dst, device, stay=None):
        n = used[0]
        used[0] += 1
        copy = pltpu.make_async_remote_copy(
            src_ref=src,
            dst_ref=dst,
            send_sem=send_sem.at[n],
            recv_sem=recv_sem.at[n],
            device_id=device,
            device_id_type=MESH,
        )
        if stay is None:
            copy.start()
        else:

            @pl.when(stay)
            def _():
                pltpu.make_async_copy(src, dst, recv_sem.at[n]).start()

            @pl.when(jnp.logical_not(stay))
            def _():
                copy.start()

        sent.append((copy, stay))
        return copy

    def stage(src, held):
        copy = pltpu.make_async_copy(src, held, local_sem.at[len(local)])
        copy.start()
        local.append(copy)

    def place_held(held, dst):
        local[len(placed)].wait()
        copy = pltpu.make_async_copy(held, dst, local_sem.at[len(local) + len(placed)])
        copy.start()
        placed.append(copy)

    me = pair * 2 + core

    dealt = [
        send(
            hidden.at[(turn + part) % 2, 0],
            rows_out.at[turn],
            deal_target(turn),
            stays[turn],
        )
        for turn in range(2)
    ]

    matrices = [
        (w_up, lambda shard: up_out.at[shard], True),
        (w_down, lambda shard: down_out.at[shard], True),
        (w_query, lambda shard: query_out.at[shard], False),
        (w_key, lambda shard: kv_out.at[shard, :, :width], False),
        (w_value, lambda shard: kv_out.at[shard, :, width:], False),
        (w_out, lambda shard: out_out.at[shard], False),
        (vectors, lambda shard: vectors_out.at[shard], False),
    ]
    side = line % 2
    for (src, _, _), held in zip(matrices, own_shards):
        stage(src, held)

    def half_cuts(src):
        half = src.shape[0] // 2
        first = pl.ds(pl.multiple_of(side * half, 8), half)
        return first, pl.ds(pl.multiple_of((1 - side) * half, 8), half)

    halves = [
        (
            flip,
            src,
            place,
            send(src.at[half_cuts(src)[0]], place(me).at[half_cuts(src)[0]], pair_peer(flip)),
        )
        for src, place, split in matrices
        if split
        for flip in range(1, pairs)
    ]
    late = [
        send(ints.at[(turn + part) % 2], ints_out.at[turn], deal_target(turn), stays[turn])
        for turn in range(2)
    ]
    for src, place, _ in matrices:
        late.append(send(src, place(me), core_peer))

    crossed = []
    for turn in range(2):
        dealt[turn].wait_recv()
        for flip in range(1, lines):
            crossed.append(
                (
                    flip * 2 + turn,
                    send(rows_out.at[turn], rows_out.at[flip * 2 + turn], line_peer(flip)),
                )
            )
        late.append(send(rows_out.at[turn], rows_out.at[lines * 2 + turn], core_peer))
    for (src, place, _), held in zip(matrices, own_shards):
        place_held(held, place(me))

    relayed = []
    whole = [
        (src, place, flip)
        for src, place, split in matrices
        if not split
        for flip in range(1, pairs)
    ]
    direct = []
    for step, (flip, src, place, copy) in enumerate(halves):
        copy.wait_recv()
        first, second = half_cuts(src)
        shard = (pair ^ flip) * 2 + core
        got = place(shard).at[first]
        relayed.append((place(shard).at[second], send(got, got, line_peer(1))))
        late.append(send(got, got, core_peer))
        share = -(-len(whole) // len(halves))
        for src, place, flip in whole[step * share : (step + 1) * share]:
            direct.append((flip, place, send(src, place(me), pair_peer(flip))))
    late += [
        send(
            out_grad.at[(turn + part) % 2, 0],
            grads_out.at[turn],
            deal_target(turn),
            stays[turn],
        )
        for turn in range(2)
    ]
    for index, copy in crossed:
        copy.wait_recv()
        late.append(send(rows_out.at[index], rows_out.at[lines * 2 + index], core_peer))
    for flip, place, copy in direct:
        copy.wait_recv()
        shard = (pair ^ flip) * 2 + core
        late.append(send(place(shard), place(shard), core_peer))
    for got, copy in relayed:
        copy.wait_recv()
        late.append(send(got, got, core_peer))
    for copy in late:
        copy.wait_recv()
    for copy in placed:
        copy.wait()
    for copy, stay in sent:
        if stay is None:
            copy.wait_send()
        else:

            @pl.when(jnp.logical_not(stay))
            def _(copy=copy):
                copy.wait_send()


def gather_all(ctx_size, w_size, hidden, out_grad, ints, vectors, weights):
    w_query, w_key, w_value, w_out, w_up, w_down = weights
    lines, pairs = ctx_size // 4, w_size // 2
    tok, width = hidden.shape[2], hidden.shape[3]
    rows = w_query.shape[0]
    shapes = [
        ((lines * 4, tok, width), bf16),
        ((2, tok, width), bf16),
        (ints.shape, ints.dtype),
        ((w_size,) + vectors.shape, f32),
        ((w_size, rows, width), bf16),
        ((w_size, rows, 2 * width), bf16),
        ((w_size, rows, width), bf16),
        ((w_size,) + w_up.shape, bf16),
        ((w_size,) + w_down.shape, bf16),
    ]
    sems = 16 + 8 * lines + 20 * pairs

    def body(*refs):
        gather_kernel(
            lambda: Wires(ctx_size, w_size), refs[:10], refs[10:19], refs[19:26], *refs[26:]
        )

    return pl.pallas_call(
        body,
        in_specs=[pl.BlockSpec(memory_space=pl.ANY)] * 10,
        out_specs=[pl.BlockSpec(memory_space=pl.ANY)] * len(shapes),
        out_shape=[jax.ShapeDtypeStruct(shape, dtype) for shape, dtype in shapes],
        scratch_shapes=[
            *[
                pltpu.VMEM(shard.shape, shard.dtype)
                for shard in (w_up, w_down, w_query, w_key, w_value, w_out, vectors)
            ],
            pltpu.SemaphoreType.DMA((14,)),
            pltpu.SemaphoreType.DMA((sems,)),
            pltpu.SemaphoreType.DMA((sems,)),
        ],
        compiler_params=pltpu.CompilerParams(collective_id=0, has_side_effects=True),
        name="gather_all",
    )(hidden, out_grad, ints, vectors, w_query, w_key, w_value, w_out, w_up, w_down)


class Sent:
    def __init__(self, make, stay=None):
        self.make, self.stay = make, stay

    def wait(self):
        self.make().wait()

    def wait_recv(self):
        self.make().wait_recv()


class Copies:
    def __init__(self, local_sem, send_sem, recv_sem):
        self.local_sem, self.send_sem, self.recv_sem = local_sem, send_sem, recv_sem
        self.locals, self.sent = 0, []

    def load(self, pair):
        n = self.locals
        self.locals += 1
        copy = Sent(lambda: pltpu.make_async_copy(*pair(), self.local_sem.at[n]))
        copy.make().start()
        return copy

    def send(self, triple, stay=None):
        n = len(self.sent)

        def make():
            src, dst, device = triple()
            return pltpu.make_async_remote_copy(
                src_ref=src,
                dst_ref=dst,
                send_sem=self.send_sem.at[n],
                recv_sem=self.recv_sem.at[n],
                device_id=device,
                device_id_type=MESH,
            )

        if stay is None:
            make().start()
        else:

            @pl.when(stay)
            def _():
                src, dst, _ = triple()
                pltpu.make_async_copy(src, dst, self.recv_sem.at[n]).start()

            @pl.when(jnp.logical_not(stay))
            def _():
                make().start()

        copy = Sent(make, stay)
        self.sent.append(copy)
        return copy

    def finish(self):
        for copy in self.sent:
            if copy.stay is None:
                copy.make().wait_send()
            else:

                @pl.when(jnp.logical_not(copy.stay))
                def _(copy=copy):
                    copy.make().wait_send()


def add_blocks(dst, *srcs):
    if len(dst.shape) == 3:

        def each(i, carry):
            total = srcs[0][i].astype(f32)
            for src in srcs[1:]:
                total = total + src[i].astype(f32)
            dst[i] = total.astype(dst.dtype)
            return carry

        lax.fori_loop(0, dst.shape[0], each, 0)
        return
    rows = dst.shape[0]
    step = 48 if rows % 48 == 0 else 32

    def body(i, carry):
        cut = pl.ds(pl.multiple_of(i * step, step), step)
        total = srcs[0][cut, :].astype(f32)
        for src in srcs[1:]:
            total = total + src[cut, :].astype(f32)
        dst[cut, :] = total.astype(dst.dtype)
        return carry

    lax.fori_loop(0, rows // step, body, 0)


class Events:
    def __init__(self):
        self.items = []

    def add(self, time, action):
        self.items.append((time, len(self.items), action))

    def take(self, until):
        due = sorted([item for item in self.items if item[0] <= until], key=lambda item: item[:2])
        self.items = [item for item in self.items if item[0] > until]
        return [action for _, _, action in due]

    def run(self, until=math.inf):
        for action in self.take(until):
            action()


class Plan:
    def __init__(self, events):
        self.events, self.heap, self.free, self.count = events, [], {}, 0

    def at(self, time, action):
        heapq.heappush(self.heap, (time, self.count, action))
        self.count += 1

    def do(self, time, action):
        self.events.add(time, action)

    def send(self, link, time, length, then):
        def start(now):
            begin = max(now, self.free.get(link, 0.0))
            self.free[link] = begin + length
            self.at(begin + length + 2.0, then)

        self.at(time, start)

    def run(self):
        while self.heap:
            time, _, action = heapq.heappop(self.heap)
            action(time)


def group_scratch(lines, pairs, rows, columns):
    block = (rows, columns)
    return [
        pltpu.VMEM((2 * lines, pairs) + block, bf16),
        pltpu.VMEM((2 * lines, pairs) + block, bf16),
        pltpu.VMEM((2 * lines, max(pairs - 1, 1)) + block, bf16),
        pltpu.VMEM((2 * lines,) + block, bf16),
        pltpu.VMEM((2, max(lines - 1, 1)) + block, bf16),
        pltpu.VMEM((2,) + block, bf16),
        pltpu.VMEM((2,) + block, bf16),
        pltpu.VMEM((2,) + block, bf16),
    ]


GROUP_SCRATCH = 8
BACK_GROUPS = 6
ROWS_DELAY = (20.0, 30.0)


def reduce_group(here, copies, plan, chunks, scratch, place, unit, core_times):
    from_core, own, from_pairs, paired, from_lines, lined, from_parts, parted = scratch
    lines, pairs = here.lines, here.pairs
    line, pair, core, part = here.line, here.pair, here.core, here.part
    low_part = part % 2
    state = {}

    def to_core(i, view):
        state["core", i] = copies.send(lambda: (view(), from_core.at[i], here.core_peer))

    def begin(i):
        to_core(i, lambda: chunks[i](1 - core))
        state["own", i] = copies.load(lambda: (chunks[i](core), own.at[i]))

    def over_core(i):
        if ("own", i) in state:
            state["own", i].wait()
        state["core", i].wait_recv()
        for p in range(pairs):
            add_blocks(own.at[i, p], own.at[i, p], from_core.at[i, p])
        state["pair", i] = [
            copies.send(
                lambda flip=flip: (
                    own.at[i, pair ^ flip],
                    from_pairs.at[i, flip - 1],
                    here.pair_peer(flip),
                )
            )
            for flip in range(1, pairs)
        ]

    def over_pairs(i):
        for copy in state["pair", i]:
            copy.wait_recv()
        add_blocks(
            paired.at[i], own.at[i, pair], *[from_pairs.at[i, flip - 1] for flip in range(1, pairs)]
        )

    def to_lines(h):
        state["line", h] = [
            copies.send(
                lambda flip=flip: (
                    paired.at[h * lines + (line ^ flip)],
                    from_lines.at[h, flip - 1],
                    here.line_peer(flip),
                )
            )
            for flip in range(1, lines)
        ]

    def over_lines(h):
        for copy in state["line", h]:
            copy.wait_recv()
        add_blocks(
            lined.at[h],
            paired.at[h * lines + line],
            *[from_lines.at[h, flip - 1] for flip in range(1, lines)],
        )

    def to_part_one():
        state["one"] = copies.send(
            lambda: (lined.at[1 - low_part], from_parts.at[0], here.part_peer(1))
        )

    def over_part_one():
        state["one"].wait_recv()
        add_blocks(parted.at[0], lined.at[low_part], from_parts.at[0])
        state["two"] = copies.send(lambda: (parted.at[0], from_parts.at[1], here.part_peer(2)))

    def mine():
        return place(low_part, line)

    def other():
        return place(1 - low_part, line)

    def over_part_two():
        state["two"].wait_recv()
        add_blocks(parted.at[1], parted.at[0], from_parts.at[1])
        state["back"] = copies.send(lambda: (parted.at[1], mine(), here.part_peer(1)))
        state["place"] = copies.load(lambda: (parted.at[1], mine()))
        state["spread"] = [
            copies.send(lambda flip=flip: (parted.at[1], mine(), here.line_peer(flip)))
            for flip in range(1, lines)
        ]

    def spread_other():
        state["back"].wait_recv()
        state["spread"] += [
            copies.send(lambda flip=flip: (other(), other(), here.line_peer(flip)))
            for flip in range(1, lines)
        ]

    def end():
        state["place"].wait()
        for copy in state["spread"]:
            copy.wait_recv()

    lined_h = []

    def core_done(i, now):
        plan.do(now, functools.partial(over_core, i))
        plan.send("x", now + 0.7, (pairs - 1) * unit, functools.partial(pairs_done, i))

    def pairs_done(i, now):
        plan.do(now, functools.partial(over_pairs, i))
        if i % lines == lines - 1:
            h = i // lines
            plan.do(now + 0.01, functools.partial(to_lines, h))
            plan.send("y", now + 0.3, (lines - 1) * unit, functools.partial(lines_done, h))

    def lines_done(h, now):
        plan.do(now, functools.partial(over_lines, h))
        lined_h.append(h)
        if len(lined_h) == 2:
            plan.do(now + 0.01, to_part_one)
            plan.send("z", now + 0.3, unit, one_done)

    def one_done(now):
        plan.do(now, over_part_one)
        plan.send("z", now + 0.3, 2 * unit, two_done)

    def two_done(now):
        plan.do(now, over_part_two)
        plan.send("z", now + 0.3, unit, back_done)
        plan.send("y", now + 0.3, (lines - 1) * unit, lambda now: None)

    def back_done(now):
        plan.do(now, spread_other)
        plan.send("y", now + 0.1, (lines - 1) * unit, lambda now: None)

    for i in range(2 * lines):
        if chunks[i] is not None:
            plan.do(core_times[i - 2] + 0.01 if i >= 2 else -100.0, functools.partial(begin, i))
        plan.at(core_times[i], functools.partial(core_done, i))
    plan.do(10000.0, end)
    return to_core


def chunk_views(refs, kinds, width):
    views = []
    for ref, kind in zip(refs, kinds):
        if kind == "wide":
            for c in range(ref.shape[3] // width):
                views.append(
                    lambda core, ref=ref, cut=slice(c * width, (c + 1) * width): ref.at[
                        :, core, :, cut
                    ]
                )
        else:
            for b in range(ref.shape[2]):
                for c in range(ref.shape[4] // width):
                    views.append(
                        lambda core, ref=ref, b=b, cut=slice(c * width, (c + 1) * width): ref.at[
                            :, core, b, :, cut
                        ]
                    )
    return views


def finish_kernel(ctx_size, w_size, kinds, tables, *refs):
    here = Wires(ctx_size, w_size)
    lines, pairs = here.lines, here.pairs
    part, line, pair, core = here.part, here.line, here.pair, here.core
    terms = refs[: len(kinds)]
    through, near, final, table = refs[len(kinds) : len(kinds) + 4]
    at = len(kinds) + 4
    out, final_out, grad_out, table_out = refs[at : at + 4]
    at += 4
    groups = (len(refs) - at - 8) // GROUP_SCRATCH
    scratches = [
        refs[at + g * GROUP_SCRATCH : at + (g + 1) * GROUP_SCRATCH] for g in range(groups)
    ]
    at += groups * GROUP_SCRATCH
    g_core, g_own, g_line, g_near, g_sum, table_in, table_sum = refs[at : at + 7]
    copies = Copies(*refs[at + 7])
    micro = part // 2

    def back_target(turn):
        return here.at(2 * core + (micro + turn) % 2, line, pair, part % 2)

    def back_source(turn):
        return here.at(2 * ((turn + part) % 2) + core, line, pair, part // 2)

    stays = [
        jnp.logical_and(2 * core + (micro + turn) % 2 == part, part % 2 == core)
        for turn in range(2)
    ]
    barrier = pltpu.get_barrier_semaphore()

    def greet(device):
        pl.semaphore_signal(barrier, inc=1, device_id=device, device_id_type=MESH)

    peers = [here.core_peer, here.part_peer(1), here.part_peer(2)]
    peers += [here.line_peer(flip) for flip in range(1, lines)]
    peers += [here.pair_peer(flip) for flip in range(1, pairs)]
    for device in peers:
        greet(device)
    for turn in range(2):

        @pl.when(jnp.logical_not(stays[turn]))
        def _(turn=turn):
            greet(back_target(turn))
            greet(back_source(turn))

    staying = sum(stay.astype(jnp.int32) for stay in stays)
    pl.semaphore_wait(barrier, len(peers) + 4 - 2 * staying)

    events = Events()
    state = {}
    count = 2 * lines

    def begin_rows():
        state["core"] = [
            copies.send(lambda j=j: (through.at[count + j], g_core.at[j], here.core_peer))
            for j in range(count)
        ]
        state["own"] = [
            copies.load(lambda j=j: (through.at[j], g_own.at[j])) for j in range(count)
        ]
        state["near"] = copies.load(lambda: (near, g_near))
        state["out"] = [
            copies.send(
                lambda turn=turn: (final.at[turn], final_out.at[micro], back_target(turn)),
                stays[turn],
            )
            for turn in range(2)
        ]

    def rows_over_core():
        for j in reversed(range(count)):
            state["own"][j].wait()
            state["core"][j].wait_recv()
            add_blocks(g_own.at[j], g_own.at[j], g_core.at[j])
            if j >= 2:
                state["line", j] = copies.send(
                    lambda j=j: (g_own.at[j], g_line.at[j - 2], here.line_peer(j // 2))
                )

    def rows_over_lines():
        state["near"].wait()
        state["back"] = []
        for turn in range(2):
            others = []
            for flip in range(1, lines):
                state["line", 2 * flip + turn].wait_recv()
                others.append(g_line.at[2 * flip + turn - 2])
            add_blocks(g_sum.at[turn], g_near.at[turn], g_own.at[turn], *others)
            state["back"].append(
                copies.send(
                    lambda turn=turn: (g_sum.at[turn], grad_out.at[micro], back_target(turn)),
                    stays[turn],
                )
            )

    def end_rows():
        for copy in state["out"] + state["back"]:
            copy.wait_recv()

    steps = [here.core_peer]
    steps += [here.pair_peer(flip) for flip in bits(pairs)]
    steps += [here.line_peer(flip) for flip in bits(lines)]
    steps += [here.part_peer(flip) for flip in bits(4)]

    def table_send(n):
        src = table if n == 0 else table_sum.at[n - 1]
        state["table", n] = copies.send(lambda: (src, table_in.at[n], steps[n]))

    def table_step(n):
        state["table", n].wait_recv()
        before = table[...] if n == 0 else table_sum[n - 1]
        total = before + table_in[n]
        if n + 1 < len(steps):
            table_sum[n] = total
            table_send(n + 1)
        else:
            table_out[...] = total

    plan = Plan(events)
    events.add(-1001.0, begin_rows)
    events.add(-1000.5, lambda: table_send(0))
    events.add(0.5, rows_over_core)
    events.add(17.0, rows_over_lines)
    events.add(9000.0, end_rows)
    for n in range(len(steps)):
        events.add(2.5 + n * 6.0, functools.partial(table_step, n))
    views = chunk_views(terms, kinds, out.shape[2])
    size = 2 * lines
    for g in range(groups):
        reduce_group(
            here,
            copies,
            plan,
            views[g * size : (g + 1) * size],
            scratches[g],
            lambda h, line, g=g: out.at[g * size + h * lines + line],
            6.0,
            [2.0 + 1.5 * (g * size + i) for i in range(size)],
        )
    plan.run()
    events.run()
    copies.finish()


def finish_all(ctx_size, w_size, terms, kinds, through, near, final, table):
    lines, pairs = ctx_size // 4, w_size // 2
    count = 2 * lines
    tok, width = through.shape[1:]
    rows = width // w_size
    columns = width // (lines // 2)
    chunks = sum(term.size for term in terms) // (w_size * rows * columns)
    groups = chunks // (2 * lines)
    table_steps = 1 + len(bits(pairs)) + len(bits(lines)) + len(bits(4))
    block = (tok, width)
    any_space = pl.BlockSpec(memory_space=pl.ANY)
    in_vmem = pl.BlockSpec(memory_space=pltpu.VMEM)
    sems = 40 + 10 * lines + groups * 2 * lines * (6 + pairs)
    scratch = []
    for _ in range(groups):
        scratch += group_scratch(lines, pairs, rows, columns)
    scratch += [
        pltpu.VMEM((count,) + block, bf16),
        pltpu.VMEM((count,) + block, bf16),
        pltpu.VMEM((max(count - 2, 1),) + block, bf16),
        pltpu.VMEM((2,) + block, f32),
        pltpu.VMEM((2,) + block, bf16),
        pltpu.VMEM((table_steps,) + table.shape, f32),
        pltpu.VMEM((table_steps,) + table.shape, f32),
        (
            pltpu.SemaphoreType.DMA((sems,)),
            pltpu.SemaphoreType.DMA((sems,)),
            pltpu.SemaphoreType.DMA((sems,)),
        ),
    ]
    return pl.pallas_call(
        functools.partial(finish_kernel, ctx_size, w_size, kinds, table_steps),
        in_specs=[any_space] * (len(terms) + 3) + [in_vmem],
        out_specs=[any_space, any_space, any_space, in_vmem],
        out_shape=[
            jax.ShapeDtypeStruct((chunks, rows, columns), bf16),
            jax.ShapeDtypeStruct((2,) + block, bf16),
            jax.ShapeDtypeStruct((2,) + block, bf16),
            jax.ShapeDtypeStruct(table.shape, f32),
        ],
        scratch_shapes=scratch,
        compiler_params=pltpu.CompilerParams(
            collective_id=1, has_side_effects=True, vmem_limit_bytes=60 << 20
        ),
        name="finish_all",
    )(*terms, through, near, final, table)


def greet_all(here, back_target, back_source, stays):
    lines, pairs = here.lines, here.pairs
    barrier = pltpu.get_barrier_semaphore()

    def greet(device):
        pl.semaphore_signal(barrier, inc=1, device_id=device, device_id_type=MESH)

    peers = [here.core_peer, here.part_peer(1), here.part_peer(2)]
    peers += [here.line_peer(flip) for flip in range(1, lines)]
    peers += [here.pair_peer(flip) for flip in range(1, pairs)]
    for device in peers:
        greet(device)
    for turn in range(2):

        @pl.when(jnp.logical_not(stays[turn]))
        def _(turn=turn):
            greet(back_target(turn))
            greet(back_source(turn))

    staying = sum(stay.astype(jnp.int32) for stay in stays)
    pl.semaphore_wait(barrier, len(peers) + 4 - 2 * staying)


def back_kernel(ctx_size, w_size, *refs):
    here = Wires(ctx_size, w_size)
    lines, pairs = here.lines, here.pairs
    part, line, pair, core = here.part, here.line, here.pair, here.core
    micro = part // 2
    (
        named,
        table,
        queries,
        d_context,
        d_sum,
        probs,
        kv,
        rows_all,
        full_kv,
        full_query,
        final,
        term_up,
        term_down,
        term_out,
    ) = refs[:14]
    up_out, down_out, oq_out, kv_out, final_out, grad_out, table_out = refs[14:21]
    scratches = [
        refs[21 + g * GROUP_SCRATCH : 21 + (g + 1) * GROUP_SCRATCH] for g in range(BACK_GROUPS)
    ]
    (
        kv_buf,
        slots,
        cat,
        probs_buf,
        q_buf,
        dctx_buf,
        rows_buf,
        wq_buf,
        q_other,
        kv_other,
        g_near,
        g_core,
        g_line,
        g_sum,
        acc,
        value_sums,
        table_in,
        table_sum,
        probs_sem,
        sems,
    ) = refs[21 + BACK_GROUPS * GROUP_SCRATCH :]
    copies = Copies(*sems)
    own_tokens, width = q_buf.shape
    key_blocks = kv_buf.shape[0]
    tokens = key_blocks * BLOCK
    blocks = own_tokens // BLOCK
    piece = blocks // 2
    groups = width // LANES
    keys = CANDS * BLOCK
    shard = width // w_size
    half = width // 2

    def back_target(turn):
        return here.at(2 * core + (micro + turn) % 2, line, pair, part % 2)

    def back_source(turn):
        return here.at(2 * ((turn + part) % 2) + core, line, pair, part // 2)

    stays = [
        jnp.logical_and(2 * core + (micro + turn) % 2 == part, part % 2 == core)
        for turn in range(2)
    ]

    def fetch(i, slot):
        return pltpu.make_async_copy(probs.at[i], probs_buf.at[slot], probs_sem.at[slot])

    greet_all(here, back_target, back_source, stays)

    events = Events()
    state = {}
    count = 2 * lines

    w_kv = slots.at[pl.ds(0, width // BLOCK)]
    rows_from = 16
    all_rows = slots.at[pl.ds(rows_from, key_blocks), :, pl.ds(0, width)]
    through_from = rows_from + key_blocks

    def through_other(j):
        return slots.at[pl.ds(through_from + j * piece, piece), :, pl.ds(0, width)]

    def through_own(j):
        return slots.at[pl.ds(through_from + j * piece, piece), :, pl.ds(width, width)]

    def send_out():
        state["out"] = [
            copies.send(
                lambda turn=turn: (final.at[turn], final_out.at[micro], back_target(turn)),
                stays[turn],
            )
            for turn in range(2)
        ]

    def rows_over_core(turn):
        for j in reversed(range(turn, count, 2)):
            state["through", j].wait_recv()
            add_blocks(through_own(j), through_own(j), g_core.at[j])
            if j >= 2:
                state["line", j] = copies.send(
                    lambda j=j: (through_own(j), g_line.at[j - 2], here.line_peer(j // 2))
                )

    def rows_over_lines(turn):
        others = []
        for flip in range(1, lines):
            state["line", 2 * flip + turn].wait_recv()
            others.append(g_line.at[2 * flip + turn - 2])
        add_blocks(
            g_sum.at[turn], g_near.at[pl.ds(turn * piece, piece)], through_own(turn), *others
        )
        state["back", turn] = copies.send(
            lambda: (g_sum.at[turn], grad_out.at[micro], back_target(turn)), stays[turn]
        )

    def end_rows():
        for copy in state["out"] + [state["back", turn] for turn in range(2)]:
            copy.wait_recv()

    steps = [lambda: here.core_peer]
    steps += [lambda flip=flip: here.pair_peer(flip) for flip in bits(pairs)]
    steps += [lambda flip=flip: here.line_peer(flip) for flip in bits(lines)]
    steps += [lambda flip=flip: here.part_peer(flip) for flip in bits(4)]

    def table_send(n):
        state["table", n] = copies.send(lambda: (table_sum.at[n], table_in.at[n], steps[n]()))

    def table_step(n):
        state["table", n].wait_recv()
        total = table_sum[n] + table_in[n]
        if n + 1 < len(steps):
            table_sum[n + 1] = total
            table_send(n + 1)
        else:
            table_out[...] = total

    attend_at, attend_step = 9.0, 2.6
    gather_at = attend_at + blocks * attend_step + 3.0
    gather_step = 1.4
    through_at = gather_at + 8 * gather_step + 1.0
    through_step = 1.3
    terms_at = through_at + 8 * through_step
    terms_step = 2.6
    terms_end = terms_at + 4 * terms_step
    plan = Plan(events)
    plan.send("z", 0.0, 18.0, lambda now: None)

    views = chunk_views((term_up, term_down), ("wide", "tall"), half)
    size = 2 * lines
    ffn_groups = BACK_GROUPS - 2

    def half_columns(number):
        return pl.ds(pl.multiple_of(number * half, 128), half)

    def up_place(g):
        return lambda h, line: up_out.at[:, half_columns(g * size + h * lines + line)]

    def down_place(g):
        return lambda h, line: down_out.at[
            pl.ds(pl.multiple_of((2 * g + h) * shard, 16), shard), half_columns(line)
        ]

    places = [up_place(g) for g in range(ffn_groups // 2)]
    places += [down_place(g) for g in range(ffn_groups // 2)]
    for g in range(ffn_groups):
        order = [g * size + i for i in range(size)]
        reduce_group(
            here,
            copies,
            plan,
            views[g * size : (g + 1) * size],
            scratches[g],
            places[g],
            3.0,
            [max(2.5 + 0.7 * n, 3.0 * n - 9.0) for n in order],
        )
    out_views = [
        lambda side, cut=slice(c * half, (c + 1) * half): term_out.at[:, side, :, cut]
        for c in range(2)
    ]
    q_own = scratches[ffn_groups][1]
    q_to_core = reduce_group(
        here,
        copies,
        plan,
        out_views + [None, None],
        scratches[ffn_groups],
        lambda h, line: oq_out.at[h, :, half_columns(line)],
        3.0,
        [gather_at + 2.0 + 1.5 * i for i in range(4)],
    )
    kv_own = scratches[ffn_groups + 1][1]
    kv_to_core = reduce_group(
        here,
        copies,
        plan,
        [None] * 4,
        scratches[ffn_groups + 1],
        lambda h, line: kv_out.at[h, :, half_columns(line)],
        3.0,
        [terms_at + (i + 1) * terms_step + 1.5 for i in range(4)],
    )
    plan.do(-200.0, send_out)
    rows_at = through_at + 2 * count * through_step + 0.5

    def rows_done(turn, now):
        plan.do(now, functools.partial(rows_over_lines, turn))
        plan.send("z", now + 0.7, 9.0, lambda now: None)

    for turn in range(2):
        rows_time = rows_at + ROWS_DELAY[turn]
        plan.do(rows_time, functools.partial(rows_over_core, turn))
        plan.send("y", rows_time + 0.7, 9.0, functools.partial(rows_done, turn))
    plan.do(9000.0, end_rows)
    for n in range(len(steps)):
        plan.do(through_at + 3.0 + n * 5.0, functools.partial(table_step, n))
    plan.run()

    def stepped(number, at, each, body):
        def loop(step, carry):
            body(step)
            for n in range(number):
                due = events.take(at + (n + 1) * each)
                if due:

                    @pl.when(step == n)
                    def _(due=due):
                        for action in due:
                            action()

            return carry

        lax.fori_loop(0, number, loop, 0)

    events.run(0.0)
    first = [
        copies.load(lambda: (kv, kv_buf)),
        copies.load(lambda: (queries, q_buf)),
        copies.load(lambda: (d_context, dctx_buf)),
    ]
    later = [
        copies.load(lambda: (rows_all.at[pl.ds(0, blocks)], rows_buf)),
        copies.load(lambda: (full_query, wq_buf)),
        copies.load(lambda: (d_sum, g_near)),
    ]

    fetch(0, 0).start()
    events.run(attend_at)
    for copy in first:
        copy.wait()
    slots[blocks * CANDS] = jnp.zeros((BLOCK, 2 * width), bf16)

    head_of_lane = lax.broadcasted_iota(jnp.int32, (BLOCK, LANES), 1) // HEAD_DIM

    def attend_block(i):
        slot = i % 2
        fetch(i, slot).wait()

        @pl.when(i + 1 < blocks)
        def _():
            fetch(i + 1, 1 - slot).start()

        for j in range(CANDS):
            place = named[i // piece, 0, (i % piece) * CANDS + j]
            cat[j * BLOCK : (j + 1) * BLOCK, :] = kv_buf[place]
        mine = pl.ds(pl.multiple_of(i * BLOCK, BLOCK), BLOCK)
        rows = pl.ds(i * CANDS, CANDS)
        by_slot = (CANDS, BLOCK, LANES)
        for g in range(groups):
            lanes = slice(g * LANES, (g + 1) * LANES)
            v_lanes = slice(width + g * LANES, width + (g + 1) * LANES)
            q_all = spread_heads(q_buf[mine, lanes], head_of_lane)
            d_all = spread_heads(dctx_buf[mine, lanes], head_of_lane)
            probs_low = probs_buf[slot, g]
            shares = probs_low.astype(f32)
            d_probs = dot_nt(d_all, cat[:, v_lanes])
            row_inner = jnp.sum(shares * d_probs, axis=-1, keepdims=True)
            d_scores = (shares * (d_probs - row_inner)).astype(bf16)
            slots[rows, :, lanes] = dot_tn(d_scores, q_all).astype(bf16).reshape(by_slot)
            slots[rows, :, v_lanes] = dot_tn(probs_low, d_all).astype(bf16).reshape(by_slot)
            q_buf[mine, lanes] = pick_heads(dot_nn(d_scores, cat[:, lanes]), head_of_lane).astype(
                bf16
            )

    stepped(blocks, attend_at, attend_step, attend_block)

    for copy in later:
        copy.wait()
    for c in range(2):
        columns = slice(c * half, (c + 1) * half)
        own_rows = rows_buf[...].reshape(own_tokens, width)
        acc[...] = dot_tn(own_rows, q_buf[:, columns]) * score_scale
        for p in range(pairs):
            for side, place in ((core, q_own.at[2 + c, p]), (1 - core, q_other.at[c, p])):
                start = pl.multiple_of((2 * p + side) * shard, shard)
                place[...] = acc[pl.ds(start, shard), :].astype(bf16)
        q_to_core(2 + c, lambda c=c: q_other.at[c])

    def near_step(step, carry):
        cut = pl.ds(pl.multiple_of(step * BLOCK * 2, BLOCK * 2), BLOCK * 2)
        near = dot_nt(q_buf[cut, :], wq_buf[...]) * score_scale
        g_near[pl.ds(step * 2, 2)] += near.reshape(2, BLOCK, width)
        return carry

    lax.fori_loop(0, own_tokens // (BLOCK * 2), near_step, 0)
    value_sums[...] = jnp.zeros_like(value_sums)

    sub = value_sums.shape[0]

    def gather_some(step):
        def one(n, carry):
            block = step * (key_blocks // 8) + n

            users = [named[i // piece, 1, block * piece + i % piece] for i in range(blocks)]
            for r in range(BLOCK // sub):
                cut = slice(r * sub, (r + 1) * sub)
                total = jnp.zeros((sub, 2 * width), f32)
                for i in range(blocks):
                    total = total + slots[users[i], cut, :].astype(f32)
                kv_buf[block, cut, :] = total.astype(bf16)
                value_sums[...] += total[:, width:]
            return carry

        lax.fori_loop(0, key_blocks // 8, one, 0)

    stepped(8, gather_at, gather_step, gather_some)
    weights = copies.load(lambda: (full_kv, w_kv))
    every = copies.load(lambda: (rows_all, all_rows))
    table_sum[0] = table[...]
    table_sum[0, pl.ds(w_size, 1), pl.ds(0, width)] = score_scale * jnp.sum(
        q_buf[...].astype(f32), axis=0, keepdims=True
    )
    table_sum[0, pl.ds(w_size + 1, 1), pl.ds(0, width)] = jnp.sum(
        value_sums[...], axis=0, keepdims=True
    )
    table_send(0)
    weights.wait()

    def through_tile(j, left, step):
        given = kv_buf[pl.ds(j * piece, piece)].reshape(piece * BLOCK, 2 * width)
        weight = slots[pl.ds(0, width // BLOCK)].reshape(width, 2 * width)
        tile = dot_nt(given, weight).astype(bf16).reshape(piece, BLOCK, width)
        slots[pl.ds(through_from + step * piece, piece), :, pl.ds(left, width)] = tile

    def other_tile(step):
        through_tile(count + step, 0, step)
        for n in range(count):

            @pl.when(step == n)
            def _(n=n):
                state["through", n] = copies.send(
                    lambda: (through_other(n), g_core.at[n], here.core_peer)
                )

    def own_tile(step):
        through_tile(step, width, step)

    stepped(count, through_at, through_step, other_tile)
    stepped(count, through_at + count * through_step, through_step, own_tile)
    every.wait()

    def kv_terms(c):
        columns = pl.ds(pl.multiple_of(c * half, 128), half)
        acc[...] = jnp.zeros_like(acc)

        def deep(t, carry):
            rows = slots[pl.ds(rows_from + t * blocks, blocks), :, 0:width]
            given = kv_buf[pl.ds(t * blocks, blocks), :, columns]
            acc[...] += dot_tn(
                rows.reshape(own_tokens, width), given.reshape(own_tokens, half)
            )
            return carry

        lax.fori_loop(0, tokens // own_tokens, deep, 0)
        for p in range(pairs):
            for side, place in ((core, kv_own.at[c, p]), (1 - core, kv_other.at[c, p])):
                start = pl.multiple_of((2 * p + side) * shard, shard)
                place[...] = acc[pl.ds(start, shard), :].astype(bf16)
        for n in range(4):

            @pl.when(c == n)
            def _(n=n):
                kv_to_core(n, lambda: kv_other.at[n])

    stepped(4, terms_at, terms_step, kv_terms)
    events.run()
    copies.finish()


def back_all(ctx_size, w_size, small, large, shapes):
    width, tok, tokens, table_shape = shapes
    lines, pairs = ctx_size // 4, w_size // 2
    rows = width // w_size
    own_tokens = 2 * tok
    blocks = own_tokens // BLOCK
    keys = CANDS * BLOCK
    half = width // 2
    table_steps = 1 + len(bits(pairs)) + len(bits(lines)) + len(bits(4))
    any_space = pl.BlockSpec(memory_space=pl.ANY)
    in_vmem = pl.BlockSpec(memory_space=pltpu.VMEM)
    in_smem = pl.BlockSpec(memory_space=pltpu.SMEM)
    scratch = []
    for _ in range(BACK_GROUPS):
        scratch += group_scratch(lines, pairs, rows, half)
    piece = (tok // BLOCK, BLOCK, width)
    scratch += [
        pltpu.VMEM((tokens // BLOCK, BLOCK, 2 * width), bf16),
        pltpu.VMEM((blocks * CANDS + 1, BLOCK, 2 * width), bf16),
        pltpu.VMEM((keys, 2 * width), bf16),
        pltpu.VMEM((2, width // LANES, GROUP * BLOCK, keys), bf16),
        pltpu.VMEM((own_tokens, width), bf16),
        pltpu.VMEM((own_tokens, width), bf16),
        pltpu.VMEM((blocks, BLOCK, width), bf16),
        pltpu.VMEM((width, width), bf16),
        pltpu.VMEM((2, pairs, rows, half), bf16),
        pltpu.VMEM((4, pairs, rows, half), bf16),
        pltpu.VMEM((blocks, BLOCK, width), f32),
        pltpu.VMEM((2 * lines,) + piece, bf16),
        pltpu.VMEM((2 * lines - 2,) + piece, bf16),
        pltpu.VMEM((2,) + piece, bf16),
        pltpu.VMEM((width, half), f32),
        pltpu.VMEM((16, width), f32),
        pltpu.VMEM((table_steps,) + table_shape, f32),
        pltpu.VMEM((table_steps,) + table_shape, f32),
        pltpu.SemaphoreType.DMA((2,)),
        (
            pltpu.SemaphoreType.DMA((60,)),
            pltpu.SemaphoreType.DMA((160,)),
            pltpu.SemaphoreType.DMA((160,)),
        ),
    ]
    return pl.pallas_call(
        functools.partial(back_kernel, ctx_size, w_size),
        in_specs=[in_smem, in_vmem] + [any_space] * len(large),
        out_specs=[any_space] * 6 + [in_vmem],
        out_shape=[
            jax.ShapeDtypeStruct((rows, 4 * width), bf16),
            jax.ShapeDtypeStruct((4 * rows, width), bf16),
            jax.ShapeDtypeStruct((2, rows, width), bf16),
            jax.ShapeDtypeStruct((2, rows, width), bf16),
            jax.ShapeDtypeStruct((2,) + piece, bf16),
            jax.ShapeDtypeStruct((2,) + piece, bf16),
            jax.ShapeDtypeStruct(table_shape, f32),
        ],
        scratch_shapes=scratch,
        compiler_params=pltpu.CompilerParams(
            collective_id=1, has_side_effects=True, vmem_limit_bytes=67043328
        ),
        name="back_all",
    )(*small, *large)


def prepare_kernel(ctx_size, w_size, lengths, picks, ints, bias):
    here = Wires(ctx_size, w_size)
    lines = here.lines
    micros, _, chunk_blocks, randoms = picks.shape
    slots = 2 * chunk_blocks * CANDS
    head = lax.broadcasted_iota(jnp.int32, (1, CANDS * BLOCK), 1) // BLOCK
    key_blocks = ctx_size * chunk_blocks
    one, nothing = jnp.int32(1), jnp.int32(0)

    for m in range(micros):

        def clear(n, carry):
            ints[m, 1, n] = jnp.int32(slots)
            return carry

        lax.fori_loop(0, key_blocks * chunk_blocks, clear, 0)
        turn = lax.rem(m + here.part, 2)
        for b in range(chunk_blocks):
            block = here.ctx * chunk_blocks + b
            begin, first, length = nothing, nothing, one
            for d in range(lengths.shape[2]):
                size = lengths[m, 0, d]
                end = begin + size
                inside = jnp.logical_and(block >= begin, block < end)
                first = jnp.where(inside, begin, first)
                length = jnp.where(inside, size, length)
                begin = end
            chosen = [block, block - 1, block + 1, first, first + 1]
            for r in range(randoms):
                chosen.append(first + lax.rem(picks[m, 0, b, r], length))
            row = jnp.zeros(head.shape, f32)
            for j, candidate in enumerate(chosen):
                allowed = jnp.logical_and(candidate >= first, candidate < first + length)
                for earlier in chosen[:j]:
                    allowed = jnp.logical_and(allowed, candidate != earlier)
                safe = jnp.where(allowed, candidate, block)
                chunk = lax.div(safe, chunk_blocks)
                chunk_part, chunk_line = lax.div(chunk, lines), lax.rem(chunk, lines)
                low, high = lax.rem(chunk_part, 2), lax.div(chunk_part, 2)
                place = (high ^ lax.div(here.part, 2)) * lines + (chunk_line ^ here.line)
                place = (place * 2 + lax.rem(low + m, 2)) * chunk_blocks
                place = place + lax.rem(safe, chunk_blocks)
                ints[m, 0, b * CANDS + j] = place

                @pl.when(allowed)
                def _(place=place, b=b, j=j):
                    ints[m, 1, place * chunk_blocks + b] = (turn * chunk_blocks + b) * CANDS + j

                score = jnp.where(allowed, 0.0, masked_score).astype(f32)
                row = jnp.where(head == j, score, row)
            bias[m, b] = row


def prepare(ctx_size, w_size, lengths, picks):
    micros, _, chunk_blocks, _ = picks.shape
    return pl.pallas_call(
        functools.partial(prepare_kernel, ctx_size, w_size),
        in_specs=[pl.BlockSpec(memory_space=pltpu.SMEM)] * 2,
        out_specs=[pl.BlockSpec(memory_space=pltpu.SMEM), pl.BlockSpec(memory_space=pltpu.VMEM)],
        out_shape=[
            jax.ShapeDtypeStruct((micros, 8, 128), jnp.int32),
            jax.ShapeDtypeStruct((micros, chunk_blocks, 1, CANDS * BLOCK), f32),
        ],
        name="prepare",
    )(lengths, picks)


def front_kernel(ctx_size, w_size, *refs):
    here = Wires(ctx_size, w_size)
    lines, pairs = here.lines, here.pairs
    part, line, pair, core = here.part, here.line, here.pair, here.core
    (
        hidden,
        out_grad,
        ints,
        bias,
        vectors,
        w_query,
        w_key,
        w_value,
        w_out,
        w_up,
        w_down,
    ) = refs[:11]
    (
        rows_out,
        grads_out,
        ints_out,
        vectors_out,
        query_out,
        kv_weight_out,
        out_out,
        up_out,
        down_out,
        queries_out,
        kv_out,
        context_out,
        probs_out,
        own_out,
    ) = refs[11:25]
    (
        held_up,
        held_down,
        held_out,
        rows_buf,
        wq_buf,
        wkv_buf,
        vectors_buf,
        bias_buf,
        q_buf,
        ctx_buf,
        kv_buf,
        cat,
        probs_buf,
        pos,
        probs_sem,
        sems,
    ) = refs[25:]
    copies = Copies(*sems)
    width = w_query.shape[1]
    tok = rows_buf.shape[1]
    chunk_blocks = tok // BLOCK
    blocks = 2 * chunk_blocks
    groups = width // LANES
    chunks = rows_buf.shape[0]
    me = pair * 2 + core
    side = line % 2

    def target(turn):
        return here.at(2 * ((turn + part) % 2) + core, line, pair, part // 2)

    def source(turn):
        return here.at(2 * core + (part // 2 + turn) % 2, line, pair, part % 2)

    stays = [
        jnp.logical_and(2 * ((turn + part) % 2) + core == part, part // 2 == core)
        for turn in range(2)
    ]
    greet_all(here, target, source, stays)

    def deal(src, dst, turn):
        return copies.send(
            lambda: (src((turn + part) % 2), dst(turn), target(turn)), stays[turn]
        )

    dealt = [deal(lambda m: hidden.at[m, 0], lambda t: rows_buf.at[t], turn) for turn in range(2)]
    dealt_ints = [deal(lambda m: ints.at[m], lambda t: ints_out.at[t], turn) for turn in range(2)]
    dealt_bias = [deal(lambda m: bias.at[m], lambda t: bias_buf.at[t], turn) for turn in range(2)]

    early = [
        (w_key, lambda shard: wkv_buf.at[shard, :, pl.ds(0, width)]),
        (w_value, lambda shard: wkv_buf.at[shard, :, pl.ds(width, width)]),
        (vectors, lambda shard: vectors_buf.at[shard]),
        (w_query, lambda shard: wq_buf.at[shard]),
    ]
    late = [
        (w_up, held_up, lambda shard: up_out.at[shard]),
        (w_down, held_down, lambda shard: down_out.at[shard]),
        (w_out, held_out, lambda shard: out_out.at[shard]),
    ]
    across = [
        copies.send(lambda src=src, place=place: (src, place(me), here.pair_peer(1)))
        for src, place in early
    ]
    ready = [copies.load(lambda src=src, place=place: (src, place(me))) for src, place in early]
    arrive = [
        copies.send(lambda src=src, place=place: (src, place(me), here.core_peer))
        for src, place in early
    ]

    def half_cut(src, which):
        half = src.shape[0] // 2
        return pl.ds(pl.multiple_of(which * half, 16), half)

    halves = [
        copies.send(
            lambda src=src, place=place: (
                src.at[half_cut(src, side)],
                place(me).at[half_cut(src, side)],
                here.pair_peer(1),
            )
        )
        for src, _, place in late[:2]
    ]
    out_across = copies.send(lambda: (w_out, out_out.at[me], here.pair_peer(1)))
    staged = [copies.load(lambda src=src, held=held: (src, held)) for src, held, _ in late]
    ends = [
        copies.send(lambda src=src, place=place: (src, place(me), here.core_peer))
        for src, _, place in late
    ]
    placed = []

    crossed = []
    from_core = {}
    for turn in range(2):
        dealt[turn].wait_recv()
        for flip in range(1, lines):
            crossed.append(
                copies.send(
                    lambda turn=turn, flip=flip: (
                        rows_buf.at[turn],
                        rows_buf.at[flip * 2 + turn],
                        here.line_peer(flip),
                    )
                )
            )
        from_core[turn] = copies.send(
            lambda turn=turn: (rows_buf.at[turn], rows_buf.at[lines * 2 + turn], here.core_peer)
        )
    for turn in range(2):
        dealt_ints[turn].wait_recv()
    pos_ready = copies.load(lambda: (ints_out, pos))
    for copy, (src, held, place) in zip(staged, late):
        copy.wait()
        placed.append(copies.load(lambda held=held, place=place: (held, place(me))))
    theirs = (pair ^ 1) * 2 + core
    for copy, (src, place) in zip(across, early):
        copy.wait_recv()
        arrive.append(
            copies.send(lambda place=place: (place(theirs), place(theirs), here.core_peer))
        )
    for n, copy in enumerate(crossed):
        copy.wait_recv()
        from_core[2 + n] = copies.send(
            lambda n=n: (rows_buf.at[2 + n], rows_buf.at[lines * 2 + 2 + n], here.core_peer)
        )
    gradients = [
        deal(lambda m: out_grad.at[m, 0], lambda t: grads_out.at[t], turn) for turn in range(2)
    ]
    for copy in ready + arrive:
        copy.wait() if copy in ready else copy.wait_recv()
    keep = [
        copies.load(lambda: (wq_buf, query_out)),
        copies.load(lambda: (wkv_buf, kv_weight_out)),
    ]
    relayed = []

    def relay(n):
        halves[n].wait_recv()
        src, _, place = late[n]
        relayed.append(
            copies.send(
                lambda: (
                    place(theirs).at[half_cut(src, side)],
                    place(theirs).at[half_cut(src, side)],
                    here.line_peer(1),
                )
            )
        )
        ends.append(
            copies.send(
                lambda: (
                    place(theirs).at[half_cut(src, side)],
                    place(theirs).at[half_cut(src, side)],
                    here.core_peer,
                )
            )
        )

    def relay_last(n):
        relayed[n].wait_recv()
        src, _, place = late[n]
        ends.append(
            copies.send(
                lambda: (
                    place(theirs).at[half_cut(src, 1 - side)],
                    place(theirs).at[half_cut(src, 1 - side)],
                    here.core_peer,
                )
            )
        )

    def relay_out():
        out_across.wait_recv()
        ends.append(
            copies.send(lambda: (out_out.at[theirs], out_out.at[theirs], here.core_peer))
        )

    vectors_total = vectors_buf[0]
    for w in range(1, w_size):
        vectors_total = vectors_total + vectors_buf[w]
    vectors_out[...] = vectors_total
    kv_bias = jnp.concatenate(
        [jnp.zeros((1, width), f32), vectors_out[pl.ds(1, 1), :]], axis=1
    )
    query_bias = vectors_out[pl.ds(0, 1), :]

    weight = wq_buf[...].reshape(width, width)
    for turn in range(2):
        rows = pl.ds(turn * tok, tok)
        q_buf[rows, :] = (
            (dot_nn(rows_buf[turn], weight) + query_bias) * score_scale
        ).astype(bf16)

    def keys_and_values(step):
        for n in range(lines * 2, chunks):

            @pl.when(step == n)
            def _(n=n):
                from_core[n - lines * 2].wait_recv()

        both = dot_nn(rows_buf[step], wkv_buf[...].reshape(width, 2 * width))
        both = both + kv_bias
        kv_buf[pl.ds(step * chunk_blocks, chunk_blocks)] = both.astype(bf16).reshape(
            chunk_blocks, BLOCK, 2 * width
        )

        return step

    lax.fori_loop(0, chunks, lambda step, carry: (keys_and_values(step), carry)[1], 0)
    keep += [
        copies.load(lambda: (q_buf, queries_out)),
        copies.load(lambda: (kv_buf, kv_out)),
        copies.load(lambda: (rows_buf, rows_out)),
        copies.load(lambda: (rows_buf.at[pl.ds(0, 2)], own_out)),
    ]
    relay(0)
    pos_ready.wait()
    for turn in range(2):
        dealt_bias[turn].wait_recv()
    head_of_lane = lax.broadcasted_iota(jnp.int32, (BLOCK, LANES), 1) // HEAD_DIM

    def put(i, slot):
        return pltpu.make_async_copy(probs_buf.at[slot], probs_out.at[i], probs_sem.at[slot])

    def attend_block(i, carry):
        turn, row, slot = i // chunk_blocks, i % chunk_blocks, i % 2
        for j in range(CANDS):
            cat[j * BLOCK : (j + 1) * BLOCK, :] = kv_buf[pos[turn, 0, row * CANDS + j]]

        @pl.when(i >= 2)
        def _():
            put(i - 2, slot).wait()

        mine = pl.ds(pl.multiple_of(i * BLOCK, BLOCK), BLOCK)
        masked = bias_buf[turn, row]
        for g in range(groups):
            lanes = slice(g * LANES, (g + 1) * LANES)
            v_lanes = slice(width + g * LANES, width + (g + 1) * LANES)
            q_all = spread_heads(q_buf[mine, lanes], head_of_lane)
            scores = dot_nt(q_all, cat[:, lanes]) + masked
            row_max = jnp.max(scores, axis=-1, keepdims=True)
            shifted = jnp.exp(scores - row_max)
            row_total = jnp.sum(shifted, axis=-1, keepdims=True)
            shares = (shifted * (1.0 / row_total)).astype(bf16)
            probs_buf[slot, g] = shares
            mixed = dot_nn(shares, cat[:, v_lanes])
            ctx_buf[mine, lanes] = pick_heads(mixed, head_of_lane).astype(bf16)
        put(i, slot).start()

        @pl.when(i == blocks - 3)
        def _():
            relay(1)

        return carry

    lax.fori_loop(0, blocks, attend_block, 0)
    keep.append(copies.load(lambda: (ctx_buf, context_out)))
    for n in range(2):
        relay_last(n)
        if n == 0:
            relay_out()
    for copy in gradients + ends:
        copy.wait_recv()
    for copy in placed + keep:
        copy.wait()
    for n in range(2):
        put(blocks - 2 + n, n).wait()
    copies.finish()


def front_all(ctx_size, w_size, hidden, out_grad, ints, bias, vectors, weights):
    w_query, w_key, w_value, w_out, w_up, w_down = weights
    lines = ctx_size // 4
    tok, width = hidden.shape[2], hidden.shape[3]
    rows = w_query.shape[0]
    chunks = lines * 4
    blocks = 2 * tok // BLOCK
    keys = CANDS * BLOCK
    groups = width // LANES
    probs_shape = (groups, GROUP * BLOCK, keys)
    key_blocks = chunks * tok // BLOCK
    shapes = [
        ((chunks, tok, width), bf16),
        ((2, tok, width), bf16),
        (ints.shape, ints.dtype),
        (vectors.shape, f32),
        ((w_size, rows, width), bf16),
        ((w_size, rows, 2 * width), bf16),
        ((w_size, rows, width), bf16),
        ((w_size,) + w_up.shape, bf16),
        ((w_size,) + w_down.shape, bf16),
        ((2 * tok, width), bf16),
        ((key_blocks, BLOCK, 2 * width), bf16),
        ((2 * tok, width), bf16),
        ((blocks,) + probs_shape, bf16),
        ((2, tok, width), bf16),
    ]
    any_space = pl.BlockSpec(memory_space=pl.ANY)
    out_specs = [any_space] * len(shapes)
    out_specs[3] = pl.BlockSpec(memory_space=pltpu.VMEM)
    return pl.pallas_call(
        functools.partial(front_kernel, ctx_size, w_size),
        in_specs=[any_space] * 11,
        out_specs=out_specs,
        out_shape=[jax.ShapeDtypeStruct(shape, dtype) for shape, dtype in shapes],
        scratch_shapes=[
            pltpu.VMEM(w_up.shape, bf16),
            pltpu.VMEM(w_down.shape, bf16),
            pltpu.VMEM(w_out.shape, bf16),
            pltpu.VMEM((chunks, tok, width), bf16),
            pltpu.VMEM((w_size, rows, width), bf16),
            pltpu.VMEM((w_size, rows, 2 * width), bf16),
            pltpu.VMEM((w_size,) + vectors.shape, f32),
            pltpu.VMEM(bias.shape, f32),
            pltpu.VMEM((2 * tok, width), bf16),
            pltpu.VMEM((2 * tok, width), bf16),
            pltpu.VMEM((key_blocks, BLOCK, 2 * width), bf16),
            pltpu.VMEM((keys, 2 * width), bf16),
            pltpu.VMEM((2,) + probs_shape, bf16),
            pltpu.SMEM(ints.shape, ints.dtype),
            pltpu.SemaphoreType.DMA((2,)),
            (
                pltpu.SemaphoreType.DMA((24,)),
                pltpu.SemaphoreType.DMA((64,)),
                pltpu.SemaphoreType.DMA((64,)),
            ),
        ],
        compiler_params=pltpu.CompilerParams(
            collective_id=0, has_side_effects=True, vmem_limit_bytes=56 << 20
        ),
        name="front_all",
    )(hidden, out_grad, ints, bias, vectors, w_query, w_key, w_value, w_out, w_up, w_down)


def make_local(ctx_size, w_size):
    def local(
        hidden,
        out_grad,
        doc_lengths,
        rand_pick,
        w_query,
        w_key,
        w_value,
        w_out,
        w_up,
        w_down,
        b_query,
        b_value,
        b_out,
        b_up,
        b_down,
        ln1_gain,
        ln1_shift,
        ln2_gain,
        ln2_shift,
    ):
        wires = Wires(ctx_size, w_size)
        tok, width = hidden.shape[2], hidden.shape[3]
        ff = w_up.shape[1]
        tok_blocks = tok // BLOCK
        lines, pairs = wires.lines, wires.pairs
        micro = wires.part // 2

        vectors = [b_query, b_value, b_out, b_up, b_down, ln1_gain, ln1_shift, ln2_gain, ln2_shift]
        vector_sizes = [vector.shape[0] for vector in vectors]
        merged = lines == 2 and pairs == 2
        in_chunk = jnp.arange(tok_blocks, dtype=jnp.int32)
        if merged:
            ints, bias = prepare(ctx_size, w_size, doc_lengths, rand_pick)
            flat = jnp.zeros((8 * b_query.shape[0],), f32)
            narrow = [vector for vector in vectors if vector is not b_up]
            for n, vector in enumerate(narrow):
                size = vector.shape[0]
                flat = flat + jnp.pad(vector.astype(f32), (n * size, (7 - n) * size))
            table = lax.dynamic_update_slice(
                jnp.zeros((16, width), f32),
                flat.reshape(8, -1),
                (jnp.int32(0), wires.w * b_query.shape[0]),
            )
            table = lax.dynamic_update_slice(
                table, b_up.astype(f32)[None], (8 + wires.w, jnp.int32(0))
            )
            (
                all_rows,
                grads_dealt,
                ints_dealt,
                vector_table,
                full_query,
                full_kv,
                full_out,
                full_up,
                full_down,
                queries,
                kv,
                context,
                probs,
                own_rows,
            ) = front_all(
                ctx_size,
                w_size,
                hidden,
                out_grad,
                ints,
                bias,
                table,
                (w_query, w_key, w_value, w_out, w_up, w_down),
            )
            bias_out, bias_down, gain_one, shift_one, gain_two, shift_two = [
                vector_table[n] for n in range(2, 8)
            ]
            bias_up = vector_table[8:12].reshape(-1)
        else:
            small_ints = jnp.concatenate(
                [rand_pick.reshape(MICRO, -1), doc_lengths.reshape(MICRO, -1)], axis=1
            )
            int_count = small_ints.shape[1]
            small_ints = jnp.pad(small_ints, ((0, 0), (0, 1024 - int_count))).reshape(MICRO, 8, 128)
            vector_row = vector_sizes[0]
            (
                all_rows,
                grads_dealt,
                ints_dealt,
                vector_table,
                full_query,
                full_kv,
                full_out,
                full_up,
                full_down,
            ) = gather_all(
                ctx_size,
                w_size,
                hidden,
                out_grad,
                small_ints,
                jnp.concatenate(
                    [vector.astype(f32).reshape(-1, vector_row) for vector in vectors], axis=0
                ),
                (w_query, w_key, w_value, w_out, w_up, w_down),
            )
            ints_dealt = ints_dealt.reshape(MICRO, -1)
            spread = []
            at = 0
            for size in vector_sizes:
                count = size // vector_row
                spread.append(vector_table[:, at : at + count].reshape(-1))
                at += count
            (
                bias_query,
                bias_value,
                bias_out,
                bias_up,
                bias_down,
                gain_one,
                shift_one,
                gain_two,
                shift_two,
            ) = spread

            picks = jnp.stack(
                [ints_dealt[turn, : tok_blocks * 3].reshape(tok_blocks, 3) for turn in range(2)]
            ).reshape(-1, 3)
            lengths = ints_dealt[0, tok_blocks * 3 : int_count]
            chunk_ids = [
                (2 * wires.core + (micro + turn) % 2) * lines + wires.line for turn in range(2)
            ]
            my_blocks = jnp.concatenate([chunk * tok_blocks + in_chunk for chunk in chunk_ids])
            safe_blocks, allowed = candidates(my_blocks, lengths, picks)
            chunk = safe_blocks // tok_blocks
            chunk_part, chunk_line = chunk // lines, chunk % lines
            place = (
                ((chunk_part // 2) ^ wires.core) * lines + (chunk_line ^ wires.line)
            ) * 2 + (chunk_part + micro) % 2
            pos = (place * tok_blocks + safe_blocks % tok_blocks).reshape(-1).astype(jnp.int32)
            bias = jnp.repeat(jnp.where(allowed, 0.0, masked_score).astype(f32), BLOCK, axis=1)[:, None]

            queries = ((dot_nn(all_rows.reshape(-1, width)[: 2 * tok], full_query.reshape(-1, width)) + bias_query) * score_scale).astype(bf16)
            kv_bias = jnp.concatenate([jnp.zeros_like(bias_value), bias_value])
            kv = (dot_nn(all_rows.reshape(-1, width), full_kv.reshape(-1, 2 * width)) + kv_bias).astype(bf16)
            context, probs = attend(pos, queries, bias, kv)
        all_rows = all_rows.reshape(-1, width)
        if not merged:
            own_rows = all_rows[: 2 * tok]
        own_rows = own_rows.reshape(-1, width)
        grads_dealt = grads_dealt.reshape(-1, width)
        full_query, full_kv, full_out, full_up, full_down = [
            full.reshape(-1, full.shape[2]) for full in (full_query, full_kv, full_out, full_up, full_down)
        ]
        rows_f32 = own_rows.astype(f32)

        attn_out = dot_nn(context, full_out) + bias_out
        normed, ln1_back = jax.vjp(layer_norm, rows_f32 + attn_out, gain_one, shift_one)
        normed_low = normed.astype(bf16)
        up_pre = dot_nn(normed_low, full_up) + bias_up
        gelu_out, gelu_back = jax.vjp(lambda v: jax.nn.gelu(v, approximate=True), up_pre)
        activated = gelu_out.astype(bf16)
        branch = dot_nn(activated, full_down) + bias_down
        final, ln2_back = jax.vjp(layer_norm, normed + branch, gain_two, shift_two)
        final = final.astype(bf16)

        def term_of(rows_a, rows_b, scale=None):
            term = dot_tn(rows_a, rows_b)
            if scale is not None:
                term = term * scale
            return term.astype(bf16).reshape(pairs, 2, -1, rows_b.shape[1])

        d_mid, grad_gain_two, grad_shift_two = ln2_back(grads_dealt.astype(f32))
        d_branch = d_mid.astype(bf16)
        term_down = term_of(activated, d_branch)
        d_act = dot_nt(d_branch, full_down)
        d_up = gelu_back(d_act)[0].astype(bf16)
        term_up = term_of(normed_low, d_up)
        d_normed = dot_nt(d_up, full_up) + d_mid
        d_sum, grad_gain_one, grad_shift_one = ln1_back(d_normed)
        d_attn = d_sum.astype(bf16)
        term_out = term_of(context, d_attn)
        d_context = dot_nt(d_attn, full_out).astype(bf16)

        def table_of(vectors):
            return jnp.concatenate([vector.reshape(w_size, -1) for vector in vectors], axis=1)

        def column_sums(rows_a):
            return jnp.sum(rows_a.astype(f32), axis=0)

        sums = (
            column_sums(d_attn),
            column_sums(d_up),
            column_sums(d_branch),
            grad_gain_one,
            grad_shift_one,
            grad_gain_two,
            grad_shift_two,
        )
        shard = width // w_size
        if merged:
            table = table_of(sums)
            table = jnp.pad(table, ((0, 8 - w_size), (0, 0)))
            term_down = term_down.reshape(pairs, 2, -1, shard, width)
            by_block = (-1, BLOCK, width)
            up, down, out_query, key_value, block_out, grad_hidden, table = back_all(
                ctx_size,
                w_size,
                (ints_dealt, table),
                (
                    queries,
                    d_context,
                    d_sum.reshape(by_block),
                    probs,
                    kv,
                    all_rows.reshape(by_block),
                    full_kv.reshape(-1, BLOCK, 2 * width),
                    full_query,
                    final.reshape(2, -1, BLOCK, width),
                    term_up,
                    term_down,
                    term_out,
                ),
                (width, tok, all_rows.shape[0], table.shape),
            )
            row = lax.dynamic_slice(table, (wires.w, jnp.int32(0)), (1, table.shape[1]))[0]
            both = lax.dynamic_slice(
                table, (jnp.int32(w_size), wires.w * shard), (2, shard)
            )
            small = [both[0], both[1]]
            at = 0
            for size in vector_sizes[2:]:
                small.append(row[at : at + size])
                at += size

            return (
                block_out.reshape(2, 1, tok, width),
                grad_hidden.reshape(2, 1, tok, width).astype(f32),
                out_query[1].astype(f32),
                key_value[0].astype(f32),
                key_value[1].astype(f32),
                out_query[0].astype(f32),
                up.astype(f32),
                down.astype(f32),
                *small,
            )

        d_query, d_kv = attend_back(pos, queries, d_context, probs, kv)

        through = dot_nt(d_kv, full_kv).astype(bf16)
        near = d_sum + score_scale * dot_nt(d_query, full_query)
        term_kv = term_of(all_rows, d_kv)
        term_query = term_of(own_rows, d_query, score_scale)

        sums = (score_scale * column_sums(d_query), column_sums(d_kv[:, width:])) + sums
        table = table_of(sums)[:, None]
        term_down = term_down.reshape(pairs, 2, -1, shard, width)
        summed, block_out, grad_hidden, table = finish_all(
            ctx_size,
            w_size,
            (term_up, term_down, term_query, term_kv, term_out),
            ("wide", "tall", "wide", "wide", "wide"),
            through.reshape(-1, tok, width),
            near.reshape(-1, tok, width),
            final.reshape(-1, tok, width),
            table,
        )
        row = lax.dynamic_slice(
            table, (wires.w, jnp.int32(0), jnp.int32(0)), (1, 1, table.shape[2])
        )[0, 0]
        small = []
        at = 0
        for size in vector_sizes:
            small.append(row[at : at + size])
            at += size

        parts = lines // 2
        at = 0

        def wide(columns):
            nonlocal at
            count = columns * parts // width
            pieces = summed[at : at + count].astype(f32)
            at += count
            return jnp.concatenate([pieces[c] for c in range(count)], axis=1)

        grad_up = wide(ff)
        count = ff * parts // width
        grad_down = summed[at : at + count].astype(f32).reshape(-1, parts, shard, width // parts)
        grad_down = jnp.swapaxes(grad_down, 1, 2).reshape(-1, width)
        at += count
        grad_query, grad_key, grad_value, grad_out = [wide(width) for _ in range(4)]
        return (
            block_out[:, None],
            grad_hidden.astype(f32)[:, None],
            grad_query,
            grad_key,
            grad_value,
            grad_out,
            grad_up,
            grad_down,
            *small,
        )

    return local


def solution(mesh):
    tokens = P(None, "wshard", "ctx", None)
    in_specs = (
        tokens,
        tokens,
        P(None, "wshard", None),
        tokens,
        *[P("wshard", None)] * 6,
        *[P("wshard")] * 9,
    )
    out_specs = (tokens, tokens, *[P("wshard", None)] * 6, *[P("wshard")] * 9)
    return jax.shard_map(
        make_local(mesh.shape["ctx"], mesh.shape["wshard"]),
        mesh=mesh,
        in_specs=in_specs,
        out_specs=out_specs,
        check_vma=False,
    )
```

```python
import functools
import heapq
import math

import jax
import jax.numpy as jnp
from jax import lax
from jax.experimental import pallas as pl
from jax.experimental.pallas import tpu as pltpu
from jax.sharding import PartitionSpec as P

HEADS = 12
HEAD_DIM = 64
BLOCK = 64
MICRO = 2
GROUP = 4
LANES = GROUP * HEAD_DIM
CANDS = 8

masked_score = -1e30
norm_eps = 1e-12
score_scale = 1.0 / math.sqrt(HEAD_DIM)
bf16 = jnp.bfloat16
f32 = jnp.float32
MESH = pl.DeviceIdType.MESH


def layer_norm(values, ln_gain, ln_shift):
    center = values - jnp.mean(values, axis=-1, keepdims=True)
    spread = jnp.mean(center * center, axis=-1, keepdims=True)
    return center * lax.rsqrt(spread + norm_eps) * ln_gain + ln_shift


def candidates(blocks, lengths, chosen_raw):
    doc_ends = jnp.cumsum(lengths)
    doc_starts = doc_ends - lengths
    owner_doc = jnp.sum((blocks[:, None] >= doc_ends[None, :]).astype(jnp.int32), axis=1)
    doc_ids = jnp.arange(lengths.shape[0], dtype=jnp.int32)
    member = (owner_doc[:, None] == doc_ids[None, :]).astype(jnp.int32)
    doc_first = jnp.sum(member * doc_starts[None, :], axis=1)
    length = jnp.sum(member * lengths[None, :], axis=1)
    randoms = doc_first[:, None] + chosen_raw % length[:, None]
    columns = [blocks, blocks - 1, blocks + 1, doc_first, doc_first + 1]
    for column in range(chosen_raw.shape[1]):
        columns.append(randoms[:, column])
    chosen = jnp.stack(columns, axis=1)
    inside = (chosen >= doc_first[:, None]) & (chosen < (doc_first + length)[:, None])
    is_fresh = [jnp.ones(blocks.shape, dtype=jnp.bool_)]
    for column in range(1, chosen.shape[1]):
        is_fresh.append(jnp.all(chosen[:, :column] != chosen[:, column : column + 1], axis=1))
    allowed = inside & jnp.stack(is_fresh, axis=1)
    safe_blocks = jnp.where(allowed, chosen, blocks[:, None])
    return (safe_blocks, allowed)


def dot_nt(a, b):
    return lax.dot_general(a, b, (((1,), (1,)), ((), ())), preferred_element_type=f32)


def dot_nn(a, b):
    return lax.dot_general(a, b, (((1,), (0,)), ((), ())), preferred_element_type=f32)


def dot_tn(a, b):
    return lax.dot_general(a, b, (((0,), (0,)), ((), ())), preferred_element_type=f32)


def spread_heads(rows, head_of_lane):
    zero = jnp.zeros_like(rows)
    return jnp.concatenate([jnp.where(head_of_lane == h, rows, zero) for h in range(GROUP)], axis=0)


def pick_heads(rows, head_of_lane):
    total = jnp.zeros((BLOCK, LANES), f32)
    for h in range(GROUP):
        total = jnp.where(head_of_lane == h, rows[h * BLOCK : (h + 1) * BLOCK], total)
    return total


def attend_kernel(groups, width, pos_ref, q_ref, bias_ref, kv_ref, ctx_ref, probs_ref, cat):
    i = pl.program_id(0)
    for j in range(CANDS):
        start = pl.multiple_of(pos_ref[i * CANDS + j] * BLOCK, BLOCK)
        cat[j * BLOCK : (j + 1) * BLOCK, :] = kv_ref[pl.ds(start, BLOCK), :]
    head_of_lane = lax.broadcasted_iota(jnp.int32, (BLOCK, LANES), 1) // HEAD_DIM
    bias = bias_ref[0]
    for g in range(groups):
        lanes = slice(g * LANES, (g + 1) * LANES)
        v_lanes = slice(width + g * LANES, width + (g + 1) * LANES)
        q_all = spread_heads(q_ref[:, lanes], head_of_lane)
        scores = dot_nt(q_all, cat[:, lanes]) + bias
        row_max = jnp.max(scores, axis=-1, keepdims=True)
        shifted = jnp.exp(scores - row_max)
        row_total = jnp.sum(shifted, axis=-1, keepdims=True)
        probs = (shifted * (1.0 / row_total)).astype(bf16)
        probs_ref[0, g] = probs
        mixed = dot_nn(probs, cat[:, v_lanes])
        ctx_ref[:, lanes] = pick_heads(mixed, head_of_lane).astype(bf16)


def attend(pos, queries, bias, kv):
    rows, width = queries.shape
    blocks = rows // BLOCK
    groups = width // LANES
    keys = CANDS * BLOCK
    return pl.pallas_call(
        functools.partial(attend_kernel, groups, width),
        grid_spec=pltpu.PrefetchScalarGridSpec(
            num_scalar_prefetch=1,
            grid=(blocks,),
            in_specs=[
                pl.BlockSpec((BLOCK, width), lambda i, p: (i, 0)),
                pl.BlockSpec((1, 1, keys), lambda i, p: (i, 0, 0)),
                pl.BlockSpec(kv.shape, lambda i, p: (0, 0), pipeline_mode=pl.Buffered(1)),
            ],
            out_specs=[
                pl.BlockSpec((BLOCK, width), lambda i, p: (i, 0)),
                pl.BlockSpec((1, groups, GROUP * BLOCK, keys), lambda i, p: (i, 0, 0, 0)),
            ],
            scratch_shapes=[pltpu.VMEM((keys, 2 * width), bf16)],
        ),
        out_shape=[
            jax.ShapeDtypeStruct((rows, width), bf16),
            jax.ShapeDtypeStruct((blocks, groups, GROUP * BLOCK, keys), bf16),
        ],
        compiler_params=pltpu.CompilerParams(vmem_limit_bytes=48 << 20),
        cost_estimate=pl.CostEstimate(
            flops=blocks * groups * 4 * GROUP * BLOCK * keys * LANES,
            bytes_accessed=kv.size * 2 + rows * width * 4 + blocks * groups * GROUP * BLOCK * keys * 2,
            transcendentals=blocks * groups * GROUP * BLOCK * keys,
        ),
        name="attend",
    )(pos, queries, bias, kv)


def attend_back_kernel(
    groups, width, pos_ref, q_ref, dctx_ref, probs_ref, kv_ref, dq_ref, dkv_ref, cat, acc
):
    i = pl.program_id(0)

    @pl.when(i == 0)
    def _():
        acc[...] = jnp.zeros_like(acc)

    for j in range(CANDS):
        start = pl.multiple_of(pos_ref[i * CANDS + j] * BLOCK, BLOCK)
        cat[j * BLOCK : (j + 1) * BLOCK, :] = kv_ref[pl.ds(start, BLOCK), :]
    head_of_lane = lax.broadcasted_iota(jnp.int32, (BLOCK, LANES), 1) // HEAD_DIM
    for g in range(groups):
        lanes = slice(g * LANES, (g + 1) * LANES)
        v_lanes = slice(width + g * LANES, width + (g + 1) * LANES)
        q_all = spread_heads(q_ref[:, lanes], head_of_lane)
        d_all = spread_heads(dctx_ref[:, lanes], head_of_lane)
        probs_low = probs_ref[0, g]
        probs = probs_low.astype(f32)
        d_probs = dot_nt(d_all, cat[:, v_lanes])
        row_inner = jnp.sum(probs * d_probs, axis=-1, keepdims=True)
        d_scores = (probs * (d_probs - row_inner)).astype(bf16)
        dq_ref[:, lanes] = pick_heads(dot_nn(d_scores, cat[:, lanes]), head_of_lane).astype(bf16)
        d_key = dot_tn(d_scores, q_all)
        d_value = dot_tn(probs_low, d_all)
        for j in range(CANDS):
            start = pl.multiple_of(pos_ref[i * CANDS + j] * BLOCK, BLOCK)
            part = slice(j * BLOCK, (j + 1) * BLOCK)
            acc[pl.ds(start, BLOCK), lanes] += d_key[part]
            acc[pl.ds(start, BLOCK), v_lanes] += d_value[part]

    @pl.when(i == pl.num_programs(0) - 1)
    def _():
        dkv_ref[...] = acc[...].astype(bf16)


def attend_back(pos, queries, d_context, probs, kv):
    rows, width = queries.shape
    blocks = rows // BLOCK
    groups = width // LANES
    keys = CANDS * BLOCK
    return pl.pallas_call(
        functools.partial(attend_back_kernel, groups, width),
        grid_spec=pltpu.PrefetchScalarGridSpec(
            num_scalar_prefetch=1,
            grid=(blocks,),
            in_specs=[
                pl.BlockSpec((BLOCK, width), lambda i, p: (i, 0)),
                pl.BlockSpec((BLOCK, width), lambda i, p: (i, 0)),
                pl.BlockSpec((1, groups, GROUP * BLOCK, keys), lambda i, p: (i, 0, 0, 0)),
                pl.BlockSpec(kv.shape, lambda i, p: (0, 0), pipeline_mode=pl.Buffered(1)),
            ],
            out_specs=[
                pl.BlockSpec((BLOCK, width), lambda i, p: (i, 0)),
                pl.BlockSpec(kv.shape, lambda i, p: (0, 0), pipeline_mode=pl.Buffered(1)),
            ],
            scratch_shapes=[pltpu.VMEM((keys, 2 * width), bf16), pltpu.VMEM(kv.shape, f32)],
        ),
        out_shape=[
            jax.ShapeDtypeStruct((rows, width), bf16),
            jax.ShapeDtypeStruct(kv.shape, bf16),
        ],
        compiler_params=pltpu.CompilerParams(vmem_limit_bytes=60 << 20),
        cost_estimate=pl.CostEstimate(
            flops=blocks * groups * 8 * GROUP * BLOCK * keys * LANES,
            bytes_accessed=kv.size * 4 + rows * width * 6 + blocks * groups * GROUP * BLOCK * keys * 2,
            transcendentals=0,
        ),
        name="attend_back",
    )(pos, queries, d_context, probs, kv)


class Wires:
    def __init__(self, ctx_size, w_size):
        self.ctx_size, self.w_size = ctx_size, w_size
        self.lines = ctx_size // 4
        self.pairs = w_size // 2
        self.ctx = lax.axis_index("ctx")
        self.w = lax.axis_index("wshard")
        self.part = self.ctx // self.lines
        self.line = self.ctx % self.lines
        self.pair = self.w // 2
        self.core = self.w % 2

    def at(self, part, line, pair, core):
        return (part * self.lines + line, pair * 2 + core)

    @property
    def core_peer(self):
        return self.at(self.part, self.line, self.pair, 1 - self.core)

    def pair_peer(self, flip):
        return self.at(self.part, self.line, self.pair ^ flip, self.core)

    def line_peer(self, flip):
        return self.at(self.part, self.line ^ flip, self.pair, self.core)

    def part_peer(self, flip):
        return self.at(self.part ^ flip, self.line, self.pair, self.core)

    def move(self, value, to):
        perm = []
        for ctx in range(self.ctx_size):
            for w in range(self.w_size):
                part, line, pair, core = to(ctx // self.lines, ctx % self.lines, w // 2, w % 2)
                target = (part * self.lines + line) * self.w_size + pair * 2 + core
                perm.append((ctx * self.w_size + w, target))
        return lax.ppermute(value, ("ctx", "wshard"), perm)

    def to_core(self, value):
        return self.move(value, lambda part, line, pair, core: (part, line, pair, 1 - core))

    def to_pair(self, value, flip):
        return self.move(value, lambda part, line, pair, core: (part, line, pair ^ flip, core))

    def to_line(self, value, flip):
        return self.move(value, lambda part, line, pair, core: (part, line ^ flip, pair, core))

    def to_part(self, value, flip):
        return self.move(value, lambda part, line, pair, core: (part ^ flip, line, pair, core))

    def deal(self, value, turn):
        return self.move(
            value,
            lambda part, line, pair, core: (2 * ((turn + part) % 2) + core, line, pair, part // 2),
        )

    def deal_back(self, value, turn):
        return self.move(
            value,
            lambda part, line, pair, core: (2 * core + (part // 2 + turn) % 2, line, pair, part % 2),
        )


def bits(count):
    flips = []
    flip = 1
    while flip < count:
        flips.append(flip)
        flip *= 2
    return flips


def gather_kernel(wires_of, refs, outs, own_shards, local_sem, send_sem, recv_sem):
    hidden, out_grad, ints, vectors, w_query, w_key, w_value, w_out, w_up, w_down = refs
    rows_out, grads_out, ints_out, vectors_out, query_out, kv_out, out_out, up_out, down_out = outs
    here = wires_of()
    lines, pairs = here.lines, here.pairs
    part, line, pair, core = here.part, here.line, here.pair, here.core
    width = w_query.shape[1]
    used = [0]
    sent = []
    local = []
    placed = []

    def at(part, line, pair, core):
        return (part * lines + line, pair * 2 + core)

    core_peer = at(part, line, pair, 1 - core)

    def line_peer(flip):
        return at(part, line ^ flip, pair, core)

    def pair_peer(flip):
        return at(part, line, pair ^ flip, core)

    def deal_target(turn):
        return at(2 * ((turn + part) % 2) + core, line, pair, part // 2)

    def deal_source(turn):
        return at(2 * core + (part // 2 + turn) % 2, line, pair, part % 2)

    stays = [
        jnp.logical_and(
            2 * ((turn + part) % 2) + core == part, part // 2 == core
        )
        for turn in range(2)
    ]

    barrier = pltpu.get_barrier_semaphore()

    def greet(device):
        pl.semaphore_signal(barrier, inc=1, device_id=device, device_id_type=MESH)

    peers = [core_peer]
    peers += [line_peer(flip) for flip in range(1, lines)]
    peers += [pair_peer(flip) for flip in range(1, pairs)]
    for device in peers:
        greet(device)
    for turn in range(2):

        @pl.when(jnp.logical_not(stays[turn]))
        def _(turn=turn):
            greet(deal_target(turn))
            greet(deal_source(turn))

    staying = sum(stay.astype(jnp.int32) for stay in stays)
    pl.semaphore_wait(barrier, len(peers) + 4 - 2 * staying)

    def send(src, dst, device, stay=None):
        n = used[0]
        used[0] += 1
        copy = pltpu.make_async_remote_copy(
            src_ref=src,
            dst_ref=dst,
            send_sem=send_sem.at[n],
            recv_sem=recv_sem.at[n],
            device_id=device,
            device_id_type=MESH,
        )
        if stay is None:
            copy.start()
        else:

            @pl.when(stay)
            def _():
                pltpu.make_async_copy(src, dst, recv_sem.at[n]).start()

            @pl.when(jnp.logical_not(stay))
            def _():
                copy.start()

        sent.append((copy, stay))
        return copy

    def stage(src, held):
        copy = pltpu.make_async_copy(src, held, local_sem.at[len(local)])
        copy.start()
        local.append(copy)

    def place_held(held, dst):
        local[len(placed)].wait()
        copy = pltpu.make_async_copy(held, dst, local_sem.at[len(local) + len(placed)])
        copy.start()
        placed.append(copy)

    me = pair * 2 + core

    dealt = [
        send(
            hidden.at[(turn + part) % 2, 0],
            rows_out.at[turn],
            deal_target(turn),
            stays[turn],
        )
        for turn in range(2)
    ]

    matrices = [
        (w_up, lambda shard: up_out.at[shard], True),
        (w_down, lambda shard: down_out.at[shard], True),
        (w_query, lambda shard: query_out.at[shard], False),
        (w_key, lambda shard: kv_out.at[shard, :, :width], False),
        (w_value, lambda shard: kv_out.at[shard, :, width:], False),
        (w_out, lambda shard: out_out.at[shard], False),
        (vectors, lambda shard: vectors_out.at[shard], False),
    ]
    side = line % 2
    for (src, _, _), held in zip(matrices, own_shards):
        stage(src, held)

    def half_cuts(src):
        half = src.shape[0] // 2
        first = pl.ds(pl.multiple_of(side * half, 8), half)
        return first, pl.ds(pl.multiple_of((1 - side) * half, 8), half)

    halves = [
        (
            flip,
            src,
            place,
            send(src.at[half_cuts(src)[0]], place(me).at[half_cuts(src)[0]], pair_peer(flip)),
        )
        for src, place, split in matrices
        if split
        for flip in range(1, pairs)
    ]
    late = [
        send(ints.at[(turn + part) % 2], ints_out.at[turn], deal_target(turn), stays[turn])
        for turn in range(2)
    ]
    for src, place, _ in matrices:
        late.append(send(src, place(me), core_peer))

    crossed = []
    for turn in range(2):
        dealt[turn].wait_recv()
        for flip in range(1, lines):
            crossed.append(
                (
                    flip * 2 + turn,
                    send(rows_out.at[turn], rows_out.at[flip * 2 + turn], line_peer(flip)),
                )
            )
        late.append(send(rows_out.at[turn], rows_out.at[lines * 2 + turn], core_peer))
    for (src, place, _), held in zip(matrices, own_shards):
        place_held(held, place(me))

    relayed = []
    whole = [
        (src, place, flip)
        for src, place, split in matrices
        if not split
        for flip in range(1, pairs)
    ]
    direct = []
    for step, (flip, src, place, copy) in enumerate(halves):
        copy.wait_recv()
        first, second = half_cuts(src)
        shard = (pair ^ flip) * 2 + core
        got = place(shard).at[first]
        relayed.append((place(shard).at[second], send(got, got, line_peer(1))))
        late.append(send(got, got, core_peer))
        share = -(-len(whole) // len(halves))
        for src, place, flip in whole[step * share : (step + 1) * share]:
            direct.append((flip, place, send(src, place(me), pair_peer(flip))))
    late += [
        send(
            out_grad.at[(turn + part) % 2, 0],
            grads_out.at[turn],
            deal_target(turn),
            stays[turn],
        )
        for turn in range(2)
    ]
    for index, copy in crossed:
        copy.wait_recv()
        late.append(send(rows_out.at[index], rows_out.at[lines * 2 + index], core_peer))
    for flip, place, copy in direct:
        copy.wait_recv()
        shard = (pair ^ flip) * 2 + core
        late.append(send(place(shard), place(shard), core_peer))
    for got, copy in relayed:
        copy.wait_recv()
        late.append(send(got, got, core_peer))
    for copy in late:
        copy.wait_recv()
    for copy in placed:
        copy.wait()
    for copy, stay in sent:
        if stay is None:
            copy.wait_send()
        else:

            @pl.when(jnp.logical_not(stay))
            def _(copy=copy):
                copy.wait_send()


def gather_all(ctx_size, w_size, hidden, out_grad, ints, vectors, weights):
    w_query, w_key, w_value, w_out, w_up, w_down = weights
    lines, pairs = ctx_size // 4, w_size // 2
    tok, width = hidden.shape[2], hidden.shape[3]
    rows = w_query.shape[0]
    shapes = [
        ((lines * 4, tok, width), bf16),
        ((2, tok, width), bf16),
        (ints.shape, ints.dtype),
        ((w_size,) + vectors.shape, f32),
        ((w_size, rows, width), bf16),
        ((w_size, rows, 2 * width), bf16),
        ((w_size, rows, width), bf16),
        ((w_size,) + w_up.shape, bf16),
        ((w_size,) + w_down.shape, bf16),
    ]
    sems = 16 + 8 * lines + 20 * pairs

    def body(*refs):
        gather_kernel(
            lambda: Wires(ctx_size, w_size), refs[:10], refs[10:19], refs[19:26], *refs[26:]
        )

    return pl.pallas_call(
        body,
        in_specs=[pl.BlockSpec(memory_space=pl.ANY)] * 10,
        out_specs=[pl.BlockSpec(memory_space=pl.ANY)] * len(shapes),
        out_shape=[jax.ShapeDtypeStruct(shape, dtype) for shape, dtype in shapes],
        scratch_shapes=[
            *[
                pltpu.VMEM(shard.shape, shard.dtype)
                for shard in (w_up, w_down, w_query, w_key, w_value, w_out, vectors)
            ],
            pltpu.SemaphoreType.DMA((14,)),
            pltpu.SemaphoreType.DMA((sems,)),
            pltpu.SemaphoreType.DMA((sems,)),
        ],
        compiler_params=pltpu.CompilerParams(collective_id=0, has_side_effects=True),
        name="gather_all",
    )(hidden, out_grad, ints, vectors, w_query, w_key, w_value, w_out, w_up, w_down)


class Sent:
    def __init__(self, make, stay=None):
        self.make, self.stay = make, stay

    def wait(self):
        self.make().wait()

    def wait_recv(self):
        self.make().wait_recv()


class Copies:
    def __init__(self, local_sem, send_sem, recv_sem):
        self.local_sem, self.send_sem, self.recv_sem = local_sem, send_sem, recv_sem
        self.locals, self.sent = 0, []

    def load(self, pair):
        n = self.locals
        self.locals += 1
        copy = Sent(lambda: pltpu.make_async_copy(*pair(), self.local_sem.at[n]))
        copy.make().start()
        return copy

    def send(self, triple, stay=None):
        n = len(self.sent)

        def make():
            src, dst, device = triple()
            return pltpu.make_async_remote_copy(
                src_ref=src,
                dst_ref=dst,
                send_sem=self.send_sem.at[n],
                recv_sem=self.recv_sem.at[n],
                device_id=device,
                device_id_type=MESH,
            )

        if stay is None:
            make().start()
        else:

            @pl.when(stay)
            def _():
                src, dst, _ = triple()
                pltpu.make_async_copy(src, dst, self.recv_sem.at[n]).start()

            @pl.when(jnp.logical_not(stay))
            def _():
                make().start()

        copy = Sent(make, stay)
        self.sent.append(copy)
        return copy

    def finish(self):
        for copy in self.sent:
            if copy.stay is None:
                copy.make().wait_send()
            else:

                @pl.when(jnp.logical_not(copy.stay))
                def _(copy=copy):
                    copy.make().wait_send()


def add_blocks(dst, *srcs):
    if len(dst.shape) == 3:

        def each(i, carry):
            total = srcs[0][i].astype(f32)
            for src in srcs[1:]:
                total = total + src[i].astype(f32)
            dst[i] = total.astype(dst.dtype)
            return carry

        lax.fori_loop(0, dst.shape[0], each, 0)
        return
    rows = dst.shape[0]
    step = 48 if rows % 48 == 0 else 32

    def body(i, carry):
        cut = pl.ds(pl.multiple_of(i * step, step), step)
        total = srcs[0][cut, :].astype(f32)
        for src in srcs[1:]:
            total = total + src[cut, :].astype(f32)
        dst[cut, :] = total.astype(dst.dtype)
        return carry

    lax.fori_loop(0, rows // step, body, 0)


class Events:
    def __init__(self):
        self.items = []

    def add(self, time, action):
        self.items.append((time, len(self.items), action))

    def take(self, until):
        due = sorted([item for item in self.items if item[0] <= until], key=lambda item: item[:2])
        self.items = [item for item in self.items if item[0] > until]
        return [action for _, _, action in due]

    def run(self, until=math.inf):
        for action in self.take(until):
            action()


class Plan:
    def __init__(self, events):
        self.events, self.heap, self.free, self.count = events, [], {}, 0

    def at(self, time, action):
        heapq.heappush(self.heap, (time, self.count, action))
        self.count += 1

    def do(self, time, action):
        self.events.add(time, action)

    def send(self, link, time, length, then):
        def start(now):
            begin = max(now, self.free.get(link, 0.0))
            self.free[link] = begin + length
            self.at(begin + length + 2.0, then)

        self.at(time, start)

    def run(self):
        while self.heap:
            time, _, action = heapq.heappop(self.heap)
            action(time)


def group_scratch(lines, pairs, rows, columns, lines_first=False):
    block = (rows, columns)
    return [
        pltpu.VMEM((2 * lines, pairs) + block, bf16),
        pltpu.VMEM((2 * lines, pairs) + block, bf16),
        pltpu.VMEM((2 * lines, max(pairs - 1, 1)) + block, bf16),
        pltpu.VMEM((2 * lines,) + block, bf16),
        pltpu.VMEM((2, pairs if lines_first else lines - 1) + block, bf16),
        pltpu.VMEM((2,) + block, bf16),
        pltpu.VMEM((2,) + block, bf16),
        pltpu.VMEM((2,) + block, bf16),
    ]


GROUP_SCRATCH = 8
BACK_GROUPS = 6
LINES_FIRST = (True, False, True, True, False, False)
ROWS_DELAY = (10.0, 20.0)


def reduce_group(here, copies, plan, chunks, scratch, place, unit, core_times, lines_first=False):
    from_core, own, from_pairs, paired, from_lines, lined, from_parts, parted = scratch
    lines, pairs = here.lines, here.pairs
    line, pair, core, part = here.line, here.pair, here.core, here.part
    low_part = part % 2
    state = {}

    def to_core(i, view):
        state["core", i] = copies.send(lambda: (view(), from_core.at[i], here.core_peer))

    def begin(i):
        to_core(i, lambda: chunks[i](1 - core))
        state["own", i] = copies.load(lambda: (chunks[i](core), own.at[i]))

    def over_core(i):
        if ("own", i) in state:
            state["own", i].wait()
        state["core", i].wait_recv()
        for p in range(pairs):
            add_blocks(own.at[i, p], own.at[i, p], from_core.at[i, p])
        if lines_first:
            return
        state["pair", i] = [
            copies.send(
                lambda flip=flip: (
                    own.at[i, pair ^ flip],
                    from_pairs.at[i, flip - 1],
                    here.pair_peer(flip),
                )
            )
            for flip in range(1, pairs)
        ]

    def over_pairs(i):
        for copy in state["pair", i]:
            copy.wait_recv()
        add_blocks(
            paired.at[i], own.at[i, pair], *[from_pairs.at[i, flip - 1] for flip in range(1, pairs)]
        )

    def to_lines(h):
        state["line", h] = [
            copies.send(
                lambda flip=flip: (
                    paired.at[h * lines + (line ^ flip)],
                    from_lines.at[h, flip - 1],
                    here.line_peer(flip),
                )
            )
            for flip in range(1, lines)
        ]

    def over_lines(h):
        for copy in state["line", h]:
            copy.wait_recv()
        add_blocks(
            lined.at[h],
            paired.at[h * lines + line],
            *[from_lines.at[h, flip - 1] for flip in range(1, lines)],
        )

    def both_to_lines(h):
        state["line", h] = copies.send(
            lambda: (own.at[h * lines + (line ^ 1)], from_lines.at[h], here.line_peer(1))
        )

    def both_over_lines(h):
        state["line", h].wait_recv()
        for p in range(pairs):
            add_blocks(
                paired.at[h * pairs + p], own.at[h * lines + line, p], from_lines.at[h, p]
            )
        state["pair", h] = copies.send(
            lambda: (
                paired.at[h * pairs + (pair ^ 1)],
                from_pairs.at[h, 0],
                here.pair_peer(1),
            )
        )

    def last_over_pairs(h):
        state["pair", h].wait_recv()
        add_blocks(lined.at[h], paired.at[h * pairs + pair], from_pairs.at[h, 0])

    def to_part_one():
        state["one"] = copies.send(
            lambda: (lined.at[1 - low_part], from_parts.at[0], here.part_peer(1))
        )

    def over_part_one():
        state["one"].wait_recv()
        add_blocks(parted.at[0], lined.at[low_part], from_parts.at[0])
        state["two"] = copies.send(lambda: (parted.at[0], from_parts.at[1], here.part_peer(2)))

    def mine():
        return place(low_part, line)

    def other():
        return place(1 - low_part, line)

    def over_part_two():
        state["two"].wait_recv()
        add_blocks(parted.at[1], parted.at[0], from_parts.at[1])
        state["back"] = copies.send(lambda: (parted.at[1], mine(), here.part_peer(1)))
        state["place"] = copies.load(lambda: (parted.at[1], mine()))
        state["spread"] = [
            copies.send(lambda flip=flip: (parted.at[1], mine(), here.line_peer(flip)))
            for flip in range(1, lines)
        ]

    def spread_other():
        state["back"].wait_recv()
        state["spread"] += [
            copies.send(lambda flip=flip: (other(), other(), here.line_peer(flip)))
            for flip in range(1, lines)
        ]

    def end():
        state["place"].wait()
        for copy in state["spread"]:
            copy.wait_recv()

    lined_h = []

    def core_done(i, now):
        plan.do(now, functools.partial(over_core, i))
        if lines_first:
            if i % lines == lines - 1:
                h = i // lines
                plan.do(now + 0.01, functools.partial(both_to_lines, h))
                plan.send("y", now + 0.7, pairs * unit, functools.partial(both_lined, h))
            return
        plan.send("x", now + 0.7, (pairs - 1) * unit, functools.partial(pairs_done, i))

    def pairs_done(i, now):
        plan.do(now, functools.partial(over_pairs, i))
        if i % lines == lines - 1:
            h = i // lines
            plan.do(now + 0.01, functools.partial(to_lines, h))
            plan.send("y", now + 0.3, (lines - 1) * unit, functools.partial(lines_done, h))

    def both_lined(h, now):
        plan.do(now, functools.partial(both_over_lines, h))
        plan.send("x", now + 0.7, unit, functools.partial(last_paired, h))

    def last_paired(h, now):
        plan.do(now, functools.partial(last_over_pairs, h))
        all_lined(h, now)

    def lines_done(h, now):
        plan.do(now, functools.partial(over_lines, h))
        all_lined(h, now)

    def all_lined(h, now):
        lined_h.append(h)
        if len(lined_h) == 2:
            plan.do(now + 0.01, to_part_one)
            plan.send("z", now + 0.3, unit, one_done)

    def one_done(now):
        plan.do(now, over_part_one)
        plan.send("z", now + 0.3, 2 * unit, two_done)

    def two_done(now):
        plan.do(now, over_part_two)
        plan.send("z", now + 0.3, unit, back_done)
        plan.send("y", now + 0.3, (lines - 1) * unit, lambda now: None)

    def back_done(now):
        plan.do(now, spread_other)
        plan.send("y", now + 0.1, (lines - 1) * unit, lambda now: None)

    for i in range(2 * lines):
        if chunks[i] is not None:
            plan.do(core_times[i - 2] + 0.01 if i >= 2 else -100.0, functools.partial(begin, i))
        plan.at(core_times[i], functools.partial(core_done, i))
    plan.do(10000.0, end)
    return to_core


def chunk_views(refs, kinds, width):
    views = []
    for ref, kind in zip(refs, kinds):
        if kind == "wide":
            for c in range(ref.shape[3] // width):
                views.append(
                    lambda core, ref=ref, cut=slice(c * width, (c + 1) * width): ref.at[
                        :, core, :, cut
                    ]
                )
        else:
            for b in range(ref.shape[2]):
                for c in range(ref.shape[4] // width):
                    views.append(
                        lambda core, ref=ref, b=b, cut=slice(c * width, (c + 1) * width): ref.at[
                            :, core, b, :, cut
                        ]
                    )
    return views


def finish_kernel(ctx_size, w_size, kinds, tables, *refs):
    here = Wires(ctx_size, w_size)
    lines, pairs = here.lines, here.pairs
    part, line, pair, core = here.part, here.line, here.pair, here.core
    terms = refs[: len(kinds)]
    through, near, final, table = refs[len(kinds) : len(kinds) + 4]
    at = len(kinds) + 4
    out, final_out, grad_out, table_out = refs[at : at + 4]
    at += 4
    groups = (len(refs) - at - 8) // GROUP_SCRATCH
    scratches = [
        refs[at + g * GROUP_SCRATCH : at + (g + 1) * GROUP_SCRATCH] for g in range(groups)
    ]
    at += groups * GROUP_SCRATCH
    g_core, g_own, g_line, g_near, g_sum, table_in, table_sum = refs[at : at + 7]
    copies = Copies(*refs[at + 7])
    micro = part // 2

    def back_target(turn):
        return here.at(2 * core + (micro + turn) % 2, line, pair, part % 2)

    def back_source(turn):
        return here.at(2 * ((turn + part) % 2) + core, line, pair, part // 2)

    stays = [
        jnp.logical_and(2 * core + (micro + turn) % 2 == part, part % 2 == core)
        for turn in range(2)
    ]
    barrier = pltpu.get_barrier_semaphore()

    def greet(device):
        pl.semaphore_signal(barrier, inc=1, device_id=device, device_id_type=MESH)

    peers = [here.core_peer, here.part_peer(1), here.part_peer(2)]
    peers += [here.line_peer(flip) for flip in range(1, lines)]
    peers += [here.pair_peer(flip) for flip in range(1, pairs)]
    for device in peers:
        greet(device)
    for turn in range(2):

        @pl.when(jnp.logical_not(stays[turn]))
        def _(turn=turn):
            greet(back_target(turn))
            greet(back_source(turn))

    staying = sum(stay.astype(jnp.int32) for stay in stays)
    pl.semaphore_wait(barrier, len(peers) + 4 - 2 * staying)

    events = Events()
    state = {}
    count = 2 * lines

    def begin_rows():
        state["core"] = [
            copies.send(lambda j=j: (through.at[count + j], g_core.at[j], here.core_peer))
            for j in range(count)
        ]
        state["own"] = [
            copies.load(lambda j=j: (through.at[j], g_own.at[j])) for j in range(count)
        ]
        state["near"] = copies.load(lambda: (near, g_near))
        state["out"] = [
            copies.send(
                lambda turn=turn: (final.at[turn], final_out.at[micro], back_target(turn)),
                stays[turn],
            )
            for turn in range(2)
        ]

    def rows_over_core():
        for j in reversed(range(count)):
            state["own"][j].wait()
            state["core"][j].wait_recv()
            add_blocks(g_own.at[j], g_own.at[j], g_core.at[j])
            if j >= 2:
                state["line", j] = copies.send(
                    lambda j=j: (g_own.at[j], g_line.at[j - 2], here.line_peer(j // 2))
                )

    def rows_over_lines():
        state["near"].wait()
        state["back"] = []
        for turn in range(2):
            others = []
            for flip in range(1, lines):
                state["line", 2 * flip + turn].wait_recv()
                others.append(g_line.at[2 * flip + turn - 2])
            add_blocks(g_sum.at[turn], g_near.at[turn], g_own.at[turn], *others)
            state["back"].append(
                copies.send(
                    lambda turn=turn: (g_sum.at[turn], grad_out.at[micro], back_target(turn)),
                    stays[turn],
                )
            )

    def end_rows():
        for copy in state["out"] + state["back"]:
            copy.wait_recv()

    steps = [here.core_peer]
    steps += [here.pair_peer(flip) for flip in bits(pairs)]
    steps += [here.line_peer(flip) for flip in bits(lines)]
    steps += [here.part_peer(flip) for flip in bits(4)]

    def table_send(n):
        src = table if n == 0 else table_sum.at[n - 1]
        state["table", n] = copies.send(lambda: (src, table_in.at[n], steps[n]))

    def table_step(n):
        state["table", n].wait_recv()
        before = table[...] if n == 0 else table_sum[n - 1]
        total = before + table_in[n]
        if n + 1 < len(steps):
            table_sum[n] = total
            table_send(n + 1)
        else:
            table_out[...] = total

    plan = Plan(events)
    events.add(-1001.0, begin_rows)
    events.add(-1000.5, lambda: table_send(0))
    events.add(0.5, rows_over_core)
    events.add(17.0, rows_over_lines)
    events.add(9000.0, end_rows)
    for n in range(len(steps)):
        events.add(2.5 + n * 6.0, functools.partial(table_step, n))
    views = chunk_views(terms, kinds, out.shape[2])
    size = 2 * lines
    for g in range(groups):
        reduce_group(
            here,
            copies,
            plan,
            views[g * size : (g + 1) * size],
            scratches[g],
            lambda h, line, g=g: out.at[g * size + h * lines + line],
            6.0,
            [2.0 + 1.5 * (g * size + i) for i in range(size)],
        )
    plan.run()
    events.run()
    copies.finish()


def finish_all(ctx_size, w_size, terms, kinds, through, near, final, table):
    lines, pairs = ctx_size // 4, w_size // 2
    count = 2 * lines
    tok, width = through.shape[1:]
    rows = width // w_size
    columns = width // (lines // 2)
    chunks = sum(term.size for term in terms) // (w_size * rows * columns)
    groups = chunks // (2 * lines)
    table_steps = 1 + len(bits(pairs)) + len(bits(lines)) + len(bits(4))
    block = (tok, width)
    any_space = pl.BlockSpec(memory_space=pl.ANY)
    in_vmem = pl.BlockSpec(memory_space=pltpu.VMEM)
    sems = 40 + 10 * lines + groups * 2 * lines * (6 + pairs)
    scratch = []
    for _ in range(groups):
        scratch += group_scratch(lines, pairs, rows, columns)
    scratch += [
        pltpu.VMEM((count,) + block, bf16),
        pltpu.VMEM((count,) + block, bf16),
        pltpu.VMEM((max(count - 2, 1),) + block, bf16),
        pltpu.VMEM((2,) + block, f32),
        pltpu.VMEM((2,) + block, bf16),
        pltpu.VMEM((table_steps,) + table.shape, f32),
        pltpu.VMEM((table_steps,) + table.shape, f32),
        (
            pltpu.SemaphoreType.DMA((sems,)),
            pltpu.SemaphoreType.DMA((sems,)),
            pltpu.SemaphoreType.DMA((sems,)),
        ),
    ]
    return pl.pallas_call(
        functools.partial(finish_kernel, ctx_size, w_size, kinds, table_steps),
        in_specs=[any_space] * (len(terms) + 3) + [in_vmem],
        out_specs=[any_space, any_space, any_space, in_vmem],
        out_shape=[
            jax.ShapeDtypeStruct((chunks, rows, columns), bf16),
            jax.ShapeDtypeStruct((2,) + block, bf16),
            jax.ShapeDtypeStruct((2,) + block, bf16),
            jax.ShapeDtypeStruct(table.shape, f32),
        ],
        scratch_shapes=scratch,
        compiler_params=pltpu.CompilerParams(
            collective_id=1, has_side_effects=True, vmem_limit_bytes=60 << 20
        ),
        name="finish_all",
    )(*terms, through, near, final, table)


def greet_all(here, back_target, back_source, stays):
    lines, pairs = here.lines, here.pairs
    barrier = pltpu.get_barrier_semaphore()

    def greet(device):
        pl.semaphore_signal(barrier, inc=1, device_id=device, device_id_type=MESH)

    peers = [here.core_peer, here.part_peer(1), here.part_peer(2)]
    peers += [here.line_peer(flip) for flip in range(1, lines)]
    peers += [here.pair_peer(flip) for flip in range(1, pairs)]
    for device in peers:
        greet(device)
    for turn in range(2):

        @pl.when(jnp.logical_not(stays[turn]))
        def _(turn=turn):
            greet(back_target(turn))
            greet(back_source(turn))

    staying = sum(stay.astype(jnp.int32) for stay in stays)
    pl.semaphore_wait(barrier, len(peers) + 4 - 2 * staying)


def back_kernel(ctx_size, w_size, *refs):
    here = Wires(ctx_size, w_size)
    lines, pairs = here.lines, here.pairs
    part, line, pair, core = here.part, here.line, here.pair, here.core
    micro = part // 2
    (
        named,
        table,
        queries,
        d_context,
        d_sum,
        probs,
        kv,
        rows_all,
        full_kv,
        full_query,
        final,
        term_up,
        term_down,
        term_out,
    ) = refs[:14]
    up_out, down_out, oq_out, kv_out, final_out, grad_out, table_out = refs[14:21]
    scratches = [
        refs[21 + g * GROUP_SCRATCH : 21 + (g + 1) * GROUP_SCRATCH] for g in range(BACK_GROUPS)
    ]
    (
        kv_buf,
        slots,
        cat,
        probs_buf,
        q_buf,
        dctx_buf,
        rows_buf,
        wq_buf,
        q_other,
        kv_other,
        g_near,
        g_core,
        g_line,
        g_sum,
        acc,
        value_sums,
        table_in,
        table_sum,
        probs_sem,
        sems,
    ) = refs[21 + BACK_GROUPS * GROUP_SCRATCH :]
    copies = Copies(*sems)
    own_tokens, width = q_buf.shape
    key_blocks = kv_buf.shape[0]
    tokens = key_blocks * BLOCK
    blocks = own_tokens // BLOCK
    piece = blocks // 2
    groups = width // LANES
    keys = CANDS * BLOCK
    shard = width // w_size
    half = width // 2

    def back_target(turn):
        return here.at(2 * core + (micro + turn) % 2, line, pair, part % 2)

    def back_source(turn):
        return here.at(2 * ((turn + part) % 2) + core, line, pair, part // 2)

    stays = [
        jnp.logical_and(2 * core + (micro + turn) % 2 == part, part % 2 == core)
        for turn in range(2)
    ]

    def fetch(i, slot):
        return pltpu.make_async_copy(probs.at[i], probs_buf.at[slot], probs_sem.at[slot])

    greet_all(here, back_target, back_source, stays)

    events = Events()
    state = {}
    count = 2 * lines

    w_kv = slots.at[pl.ds(0, width // BLOCK)]
    rows_from = 16
    all_rows = slots.at[pl.ds(rows_from, key_blocks), :, pl.ds(0, width)]
    through_from = rows_from + key_blocks

    def through_other(j):
        return slots.at[pl.ds(through_from + j * piece, piece), :, pl.ds(0, width)]

    def through_own(j):
        return slots.at[pl.ds(through_from + j * piece, piece), :, pl.ds(width, width)]

    def send_out():
        state["out"] = [
            copies.send(
                lambda turn=turn: (final.at[turn], final_out.at[micro], back_target(turn)),
                stays[turn],
            )
            for turn in range(2)
        ]

    def rows_over_core(turn):
        for j in reversed(range(turn, count, 2)):
            state["through", j].wait_recv()
            add_blocks(through_own(j), through_own(j), g_core.at[j])
            if j >= 2:
                state["line", j] = copies.send(
                    lambda j=j: (through_own(j), g_line.at[j - 2], here.line_peer(j // 2))
                )

    def rows_over_lines(turn):
        others = []
        for flip in range(1, lines):
            state["line", 2 * flip + turn].wait_recv()
            others.append(g_line.at[2 * flip + turn - 2])
        add_blocks(
            g_sum.at[turn], g_near.at[pl.ds(turn * piece, piece)], through_own(turn), *others
        )
        state["back", turn] = copies.send(
            lambda: (g_sum.at[turn], grad_out.at[micro], back_target(turn)), stays[turn]
        )

    def end_rows():
        for copy in state["out"] + [state["back", turn] for turn in range(2)]:
            copy.wait_recv()

    steps = [lambda: here.core_peer]
    steps += [lambda flip=flip: here.pair_peer(flip) for flip in bits(pairs)]
    steps += [lambda flip=flip: here.line_peer(flip) for flip in bits(lines)]
    steps += [lambda flip=flip: here.part_peer(flip) for flip in bits(4)]

    def table_send(n):
        state["table", n] = copies.send(lambda: (table_sum.at[n], table_in.at[n], steps[n]()))

    def table_step(n):
        state["table", n].wait_recv()
        total = table_sum[n] + table_in[n]
        if n + 1 < len(steps):
            table_sum[n + 1] = total
            table_send(n + 1)
        else:
            table_out[...] = total

    attend_at, attend_step = 9.0, 2.6
    gather_at = attend_at + blocks * attend_step + 3.0
    gather_step = 1.4
    through_at = gather_at + 8 * gather_step + 1.0
    through_step = 1.3
    terms_at = through_at + 8 * through_step
    terms_step = 2.6
    terms_end = terms_at + 4 * terms_step
    plan = Plan(events)
    plan.send("z", 0.0, 18.0, lambda now: None)

    views = chunk_views((term_up, term_down), ("wide", "tall"), half)
    size = 2 * lines
    ffn_groups = BACK_GROUPS - 2

    def half_columns(number):
        return pl.ds(pl.multiple_of(number * half, 128), half)

    def up_place(g):
        return lambda h, line: up_out.at[:, half_columns(g * size + h * lines + line)]

    def down_place(g):
        return lambda h, line: down_out.at[
            pl.ds(pl.multiple_of((2 * g + h) * shard, 16), shard), half_columns(line)
        ]

    places = [up_place(g) for g in range(ffn_groups // 2)]
    places += [down_place(g) for g in range(ffn_groups // 2)]
    for g in range(ffn_groups):
        order = [g * size + i for i in range(size)]
        reduce_group(
            here,
            copies,
            plan,
            views[g * size : (g + 1) * size],
            scratches[g],
            places[g],
            3.0,
            [max(2.5 + 0.7 * n, 3.0 * n - 9.0) for n in order],
            LINES_FIRST[g],
        )
    out_views = [
        lambda side, cut=slice(c * half, (c + 1) * half): term_out.at[:, side, :, cut]
        for c in range(2)
    ]
    q_own = scratches[ffn_groups][1]
    q_to_core = reduce_group(
        here,
        copies,
        plan,
        out_views + [None, None],
        scratches[ffn_groups],
        lambda h, line: oq_out.at[h, :, half_columns(line)],
        3.0,
        [gather_at + 2.0 + 1.5 * i for i in range(4)],
        LINES_FIRST[ffn_groups],
    )
    kv_own = scratches[ffn_groups + 1][1]
    kv_to_core = reduce_group(
        here,
        copies,
        plan,
        [None] * 4,
        scratches[ffn_groups + 1],
        lambda h, line: kv_out.at[h, :, half_columns(line)],
        3.0,
        [terms_at + (i + 1) * terms_step + 1.5 for i in range(4)],
        LINES_FIRST[ffn_groups + 1],
    )
    plan.do(-200.0, send_out)
    rows_at = through_at + 2 * count * through_step + 0.5

    def rows_done(turn, now):
        plan.do(now, functools.partial(rows_over_lines, turn))
        plan.send("z", now + 0.7, 9.0, lambda now: None)

    for turn in range(2):
        rows_time = rows_at + ROWS_DELAY[turn]
        plan.do(rows_time, functools.partial(rows_over_core, turn))
        plan.send("y", rows_time + 0.7, 9.0, functools.partial(rows_done, turn))
    plan.do(9000.0, end_rows)
    for n in range(len(steps)):
        plan.do(through_at + 3.0 + n * 5.0, functools.partial(table_step, n))
    plan.run()

    def stepped(number, at, each, body):
        def loop(step, carry):
            body(step)
            for n in range(number):
                due = events.take(at + (n + 1) * each)
                if due:

                    @pl.when(step == n)
                    def _(due=due):
                        for action in due:
                            action()

            return carry

        lax.fori_loop(0, number, loop, 0)

    events.run(0.0)
    first = [
        copies.load(lambda: (kv, kv_buf)),
        copies.load(lambda: (queries, q_buf)),
        copies.load(lambda: (d_context, dctx_buf)),
    ]
    later = [
        copies.load(lambda: (rows_all.at[pl.ds(0, blocks)], rows_buf)),
        copies.load(lambda: (full_query, wq_buf)),
        copies.load(lambda: (d_sum, g_near)),
    ]

    fetch(0, 0).start()
    events.run(attend_at)
    for copy in first:
        copy.wait()
    slots[blocks * CANDS] = jnp.zeros((BLOCK, 2 * width), bf16)

    head_of_lane = lax.broadcasted_iota(jnp.int32, (BLOCK, LANES), 1) // HEAD_DIM

    def attend_block(i):
        slot = i % 2
        fetch(i, slot).wait()

        @pl.when(i + 1 < blocks)
        def _():
            fetch(i + 1, 1 - slot).start()

        for j in range(CANDS):
            place = named[i // piece, 0, (i % piece) * CANDS + j]
            cat[j * BLOCK : (j + 1) * BLOCK, :] = kv_buf[place]
        mine = pl.ds(pl.multiple_of(i * BLOCK, BLOCK), BLOCK)
        rows = pl.ds(i * CANDS, CANDS)
        by_slot = (CANDS, BLOCK, LANES)
        for g in range(groups):
            lanes = slice(g * LANES, (g + 1) * LANES)
            v_lanes = slice(width + g * LANES, width + (g + 1) * LANES)
            q_all = spread_heads(q_buf[mine, lanes], head_of_lane)
            d_all = spread_heads(dctx_buf[mine, lanes], head_of_lane)
            probs_low = probs_buf[slot, g]
            shares = probs_low.astype(f32)
            d_probs = dot_nt(d_all, cat[:, v_lanes])
            row_inner = jnp.sum(shares * d_probs, axis=-1, keepdims=True)
            d_scores = (shares * (d_probs - row_inner)).astype(bf16)
            slots[rows, :, lanes] = dot_tn(d_scores, q_all).astype(bf16).reshape(by_slot)
            slots[rows, :, v_lanes] = dot_tn(probs_low, d_all).astype(bf16).reshape(by_slot)
            q_buf[mine, lanes] = pick_heads(dot_nn(d_scores, cat[:, lanes]), head_of_lane).astype(
                bf16
            )

    stepped(blocks, attend_at, attend_step, attend_block)

    for copy in later:
        copy.wait()
    for c in range(2):
        columns = slice(c * half, (c + 1) * half)
        own_rows = rows_buf[...].reshape(own_tokens, width)
        acc[...] = dot_tn(own_rows, q_buf[:, columns]) * score_scale
        for p in range(pairs):
            for side, place in ((core, q_own.at[2 + c, p]), (1 - core, q_other.at[c, p])):
                start = pl.multiple_of((2 * p + side) * shard, shard)
                place[...] = acc[pl.ds(start, shard), :].astype(bf16)
        q_to_core(2 + c, lambda c=c: q_other.at[c])

    def near_step(step, carry):
        cut = pl.ds(pl.multiple_of(step * BLOCK * 2, BLOCK * 2), BLOCK * 2)
        near = dot_nt(q_buf[cut, :], wq_buf[...]) * score_scale
        g_near[pl.ds(step * 2, 2)] += near.reshape(2, BLOCK, width)
        return carry

    lax.fori_loop(0, own_tokens // (BLOCK * 2), near_step, 0)
    value_sums[...] = jnp.zeros_like(value_sums)

    sub = value_sums.shape[0]

    def gather_some(step):
        def one(n, carry):
            block = step * (key_blocks // 8) + n

            users = [named[i // piece, 1, block * piece + i % piece] for i in range(blocks)]
            for r in range(BLOCK // sub):
                cut = slice(r * sub, (r + 1) * sub)
                total = jnp.zeros((sub, 2 * width), f32)
                for i in range(blocks):
                    total = total + slots[users[i], cut, :].astype(f32)
                kv_buf[block, cut, :] = total.astype(bf16)
                value_sums[...] += total[:, width:]
            return carry

        lax.fori_loop(0, key_blocks // 8, one, 0)

    stepped(8, gather_at, gather_step, gather_some)
    weights = copies.load(lambda: (full_kv, w_kv))
    every = copies.load(lambda: (rows_all, all_rows))
    table_sum[0] = table[...]
    table_sum[0, pl.ds(w_size, 1), pl.ds(0, width)] = score_scale * jnp.sum(
        q_buf[...].astype(f32), axis=0, keepdims=True
    )
    table_sum[0, pl.ds(w_size + 1, 1), pl.ds(0, width)] = jnp.sum(
        value_sums[...], axis=0, keepdims=True
    )
    table_send(0)
    weights.wait()

    def through_tile(j, left, step):
        given = kv_buf[pl.ds(j * piece, piece)].reshape(piece * BLOCK, 2 * width)
        weight = slots[pl.ds(0, width // BLOCK)].reshape(width, 2 * width)
        tile = dot_nt(given, weight).astype(bf16).reshape(piece, BLOCK, width)
        slots[pl.ds(through_from + step * piece, piece), :, pl.ds(left, width)] = tile

    def other_tile(step):
        through_tile(count + step, 0, step)
        for n in range(count):

            @pl.when(step == n)
            def _(n=n):
                state["through", n] = copies.send(
                    lambda: (through_other(n), g_core.at[n], here.core_peer)
                )

    def own_tile(step):
        through_tile(step, width, step)

    stepped(count, through_at, through_step, other_tile)
    stepped(count, through_at + count * through_step, through_step, own_tile)
    every.wait()

    def kv_terms(c):
        columns = pl.ds(pl.multiple_of(c * half, 128), half)
        acc[...] = jnp.zeros_like(acc)

        def deep(t, carry):
            rows = slots[pl.ds(rows_from + t * blocks, blocks), :, 0:width]
            given = kv_buf[pl.ds(t * blocks, blocks), :, columns]
            acc[...] += dot_tn(
                rows.reshape(own_tokens, width), given.reshape(own_tokens, half)
            )
            return carry

        lax.fori_loop(0, tokens // own_tokens, deep, 0)
        for p in range(pairs):
            for side, place in ((core, kv_own.at[c, p]), (1 - core, kv_other.at[c, p])):
                start = pl.multiple_of((2 * p + side) * shard, shard)
                place[...] = acc[pl.ds(start, shard), :].astype(bf16)
        for n in range(4):

            @pl.when(c == n)
            def _(n=n):
                kv_to_core(n, lambda: kv_other.at[n])

    stepped(4, terms_at, terms_step, kv_terms)
    events.run()
    copies.finish()


def back_all(ctx_size, w_size, small, large, shapes):
    width, tok, tokens, table_shape = shapes
    lines, pairs = ctx_size // 4, w_size // 2
    rows = width // w_size
    own_tokens = 2 * tok
    blocks = own_tokens // BLOCK
    keys = CANDS * BLOCK
    half = width // 2
    table_steps = 1 + len(bits(pairs)) + len(bits(lines)) + len(bits(4))
    any_space = pl.BlockSpec(memory_space=pl.ANY)
    in_vmem = pl.BlockSpec(memory_space=pltpu.VMEM)
    in_smem = pl.BlockSpec(memory_space=pltpu.SMEM)
    scratch = []
    for lines_first in LINES_FIRST:
        scratch += group_scratch(lines, pairs, rows, half, lines_first)
    piece = (tok // BLOCK, BLOCK, width)
    scratch += [
        pltpu.VMEM((tokens // BLOCK, BLOCK, 2 * width), bf16),
        pltpu.VMEM((blocks * CANDS + 1, BLOCK, 2 * width), bf16),
        pltpu.VMEM((keys, 2 * width), bf16),
        pltpu.VMEM((2, width // LANES, GROUP * BLOCK, keys), bf16),
        pltpu.VMEM((own_tokens, width), bf16),
        pltpu.VMEM((own_tokens, width), bf16),
        pltpu.VMEM((blocks, BLOCK, width), bf16),
        pltpu.VMEM((width, width), bf16),
        pltpu.VMEM((2, pairs, rows, half), bf16),
        pltpu.VMEM((4, pairs, rows, half), bf16),
        pltpu.VMEM((blocks, BLOCK, width), f32),
        pltpu.VMEM((2 * lines,) + piece, bf16),
        pltpu.VMEM((2 * lines - 2,) + piece, bf16),
        pltpu.VMEM((2,) + piece, bf16),
        pltpu.VMEM((width, half), f32),
        pltpu.VMEM((16, width), f32),
        pltpu.VMEM((table_steps,) + table_shape, f32),
        pltpu.VMEM((table_steps,) + table_shape, f32),
        pltpu.SemaphoreType.DMA((2,)),
        (
            pltpu.SemaphoreType.DMA((60,)),
            pltpu.SemaphoreType.DMA((160,)),
            pltpu.SemaphoreType.DMA((160,)),
        ),
    ]
    return pl.pallas_call(
        functools.partial(back_kernel, ctx_size, w_size),
        in_specs=[in_smem, in_vmem] + [any_space] * len(large),
        out_specs=[any_space] * 6 + [in_vmem],
        out_shape=[
            jax.ShapeDtypeStruct((rows, 4 * width), bf16),
            jax.ShapeDtypeStruct((4 * rows, width), bf16),
            jax.ShapeDtypeStruct((2, rows, width), bf16),
            jax.ShapeDtypeStruct((2, rows, width), bf16),
            jax.ShapeDtypeStruct((2,) + piece, bf16),
            jax.ShapeDtypeStruct((2,) + piece, bf16),
            jax.ShapeDtypeStruct(table_shape, f32),
        ],
        scratch_shapes=scratch,
        compiler_params=pltpu.CompilerParams(
            collective_id=1, has_side_effects=True, vmem_limit_bytes=67043328
        ),
        name="back_all",
    )(*small, *large)


def prepare_kernel(ctx_size, w_size, lengths, picks, ints, bias):
    here = Wires(ctx_size, w_size)
    lines = here.lines
    micros, _, chunk_blocks, randoms = picks.shape
    slots = 2 * chunk_blocks * CANDS
    head = lax.broadcasted_iota(jnp.int32, (1, CANDS * BLOCK), 1) // BLOCK
    key_blocks = ctx_size * chunk_blocks
    one, nothing = jnp.int32(1), jnp.int32(0)

    for m in range(micros):

        def clear(n, carry):
            ints[m, 1, n] = jnp.int32(slots)
            return carry

        lax.fori_loop(0, key_blocks * chunk_blocks, clear, 0)
        turn = lax.rem(m + here.part, 2)
        for b in range(chunk_blocks):
            block = here.ctx * chunk_blocks + b
            begin, first, length = nothing, nothing, one
            for d in range(lengths.shape[2]):
                size = lengths[m, 0, d]
                end = begin + size
                inside = jnp.logical_and(block >= begin, block < end)
                first = jnp.where(inside, begin, first)
                length = jnp.where(inside, size, length)
                begin = end
            chosen = [block, block - 1, block + 1, first, first + 1]
            for r in range(randoms):
                chosen.append(first + lax.rem(picks[m, 0, b, r], length))
            row = jnp.zeros(head.shape, f32)
            for j, candidate in enumerate(chosen):
                allowed = jnp.logical_and(candidate >= first, candidate < first + length)
                for earlier in chosen[:j]:
                    allowed = jnp.logical_and(allowed, candidate != earlier)
                safe = jnp.where(allowed, candidate, block)
                chunk = lax.div(safe, chunk_blocks)
                chunk_part, chunk_line = lax.div(chunk, lines), lax.rem(chunk, lines)
                low, high = lax.rem(chunk_part, 2), lax.div(chunk_part, 2)
                place = (high ^ lax.div(here.part, 2)) * lines + (chunk_line ^ here.line)
                place = (place * 2 + lax.rem(low + m, 2)) * chunk_blocks
                place = place + lax.rem(safe, chunk_blocks)
                ints[m, 0, b * CANDS + j] = place

                @pl.when(allowed)
                def _(place=place, b=b, j=j):
                    ints[m, 1, place * chunk_blocks + b] = (turn * chunk_blocks + b) * CANDS + j

                score = jnp.where(allowed, 0.0, masked_score).astype(f32)
                row = jnp.where(head == j, score, row)
            bias[m, b] = row


def prepare(ctx_size, w_size, lengths, picks):
    micros, _, chunk_blocks, _ = picks.shape
    return pl.pallas_call(
        functools.partial(prepare_kernel, ctx_size, w_size),
        in_specs=[pl.BlockSpec(memory_space=pltpu.SMEM)] * 2,
        out_specs=[pl.BlockSpec(memory_space=pltpu.SMEM), pl.BlockSpec(memory_space=pltpu.VMEM)],
        out_shape=[
            jax.ShapeDtypeStruct((micros, 8, 128), jnp.int32),
            jax.ShapeDtypeStruct((micros, chunk_blocks, 1, CANDS * BLOCK), f32),
        ],
        name="prepare",
    )(lengths, picks)


def front_kernel(ctx_size, w_size, *refs):
    here = Wires(ctx_size, w_size)
    lines, pairs = here.lines, here.pairs
    part, line, pair, core = here.part, here.line, here.pair, here.core
    (
        hidden,
        out_grad,
        ints,
        bias,
        vectors,
        w_query,
        w_key,
        w_value,
        w_out,
        w_up,
        w_down,
    ) = refs[:11]
    (
        rows_out,
        grads_out,
        ints_out,
        vectors_out,
        query_out,
        kv_weight_out,
        out_out,
        up_out,
        down_out,
        queries_out,
        kv_out,
        context_out,
        probs_out,
        own_out,
    ) = refs[11:25]
    (
        held_up,
        held_down,
        held_out,
        rows_buf,
        wq_buf,
        wkv_buf,
        vectors_buf,
        bias_buf,
        q_buf,
        ctx_buf,
        kv_buf,
        cat,
        probs_buf,
        pos,
        probs_sem,
        sems,
    ) = refs[25:]
    copies = Copies(*sems)
    width = w_query.shape[1]
    tok = rows_buf.shape[1]
    chunk_blocks = tok // BLOCK
    blocks = 2 * chunk_blocks
    groups = width // LANES
    chunks = rows_buf.shape[0]
    me = pair * 2 + core
    side = line % 2

    def target(turn):
        return here.at(2 * ((turn + part) % 2) + core, line, pair, part // 2)

    def source(turn):
        return here.at(2 * core + (part // 2 + turn) % 2, line, pair, part % 2)

    stays = [
        jnp.logical_and(2 * ((turn + part) % 2) + core == part, part // 2 == core)
        for turn in range(2)
    ]
    greet_all(here, target, source, stays)

    def deal(src, dst, turn):
        return copies.send(
            lambda: (src((turn + part) % 2), dst(turn), target(turn)), stays[turn]
        )

    dealt = [deal(lambda m: hidden.at[m, 0], lambda t: rows_buf.at[t], turn) for turn in range(2)]
    dealt_ints = [deal(lambda m: ints.at[m], lambda t: ints_out.at[t], turn) for turn in range(2)]
    dealt_bias = [deal(lambda m: bias.at[m], lambda t: bias_buf.at[t], turn) for turn in range(2)]

    early = [
        (w_key, lambda shard: wkv_buf.at[shard, :, pl.ds(0, width)]),
        (w_value, lambda shard: wkv_buf.at[shard, :, pl.ds(width, width)]),
        (vectors, lambda shard: vectors_buf.at[shard]),
        (w_query, lambda shard: wq_buf.at[shard]),
    ]
    late = [
        (w_up, held_up, lambda shard: up_out.at[shard]),
        (w_down, held_down, lambda shard: down_out.at[shard]),
        (w_out, held_out, lambda shard: out_out.at[shard]),
    ]
    across = [
        copies.send(lambda src=src, place=place: (src, place(me), here.pair_peer(1)))
        for src, place in early
    ]
    ready = [copies.load(lambda src=src, place=place: (src, place(me))) for src, place in early]
    arrive = [
        copies.send(lambda src=src, place=place: (src, place(me), here.core_peer))
        for src, place in early
    ]

    def half_cut(src, which):
        half = src.shape[0] // 2
        return pl.ds(pl.multiple_of(which * half, 16), half)

    halves = [
        copies.send(
            lambda src=src, place=place: (
                src.at[half_cut(src, side)],
                place(me).at[half_cut(src, side)],
                here.pair_peer(1),
            )
        )
        for src, _, place in late[:2]
    ]
    out_across = copies.send(lambda: (w_out, out_out.at[me], here.pair_peer(1)))
    staged = [copies.load(lambda src=src, held=held: (src, held)) for src, held, _ in late]
    ends = [
        copies.send(lambda src=src, place=place: (src, place(me), here.core_peer))
        for src, _, place in late
    ]
    placed = []

    crossed = []
    from_core = {}
    for turn in range(2):
        dealt[turn].wait_recv()
        for flip in range(1, lines):
            crossed.append(
                copies.send(
                    lambda turn=turn, flip=flip: (
                        rows_buf.at[turn],
                        rows_buf.at[flip * 2 + turn],
                        here.line_peer(flip),
                    )
                )
            )
        from_core[turn] = copies.send(
            lambda turn=turn: (rows_buf.at[turn], rows_buf.at[lines * 2 + turn], here.core_peer)
        )
    for turn in range(2):
        dealt_ints[turn].wait_recv()
    pos_ready = copies.load(lambda: (ints_out, pos))
    for copy, (src, held, place) in zip(staged, late):
        copy.wait()
        placed.append(copies.load(lambda held=held, place=place: (held, place(me))))
    theirs = (pair ^ 1) * 2 + core
    for copy, (src, place) in zip(across, early):
        copy.wait_recv()
        arrive.append(
            copies.send(lambda place=place: (place(theirs), place(theirs), here.core_peer))
        )
    for n, copy in enumerate(crossed):
        copy.wait_recv()
        from_core[2 + n] = copies.send(
            lambda n=n: (rows_buf.at[2 + n], rows_buf.at[lines * 2 + 2 + n], here.core_peer)
        )
    gradients = [
        deal(lambda m: out_grad.at[m, 0], lambda t: grads_out.at[t], turn) for turn in range(2)
    ]
    for copy in ready + arrive:
        copy.wait() if copy in ready else copy.wait_recv()
    keep = [
        copies.load(lambda: (wq_buf, query_out)),
        copies.load(lambda: (wkv_buf, kv_weight_out)),
    ]
    relayed = []

    def relay(n):
        halves[n].wait_recv()
        src, _, place = late[n]
        relayed.append(
            copies.send(
                lambda: (
                    place(theirs).at[half_cut(src, side)],
                    place(theirs).at[half_cut(src, side)],
                    here.line_peer(1),
                )
            )
        )
        ends.append(
            copies.send(
                lambda: (
                    place(theirs).at[half_cut(src, side)],
                    place(theirs).at[half_cut(src, side)],
                    here.core_peer,
                )
            )
        )

    def relay_last(n):
        relayed[n].wait_recv()
        src, _, place = late[n]
        ends.append(
            copies.send(
                lambda: (
                    place(theirs).at[half_cut(src, 1 - side)],
                    place(theirs).at[half_cut(src, 1 - side)],
                    here.core_peer,
                )
            )
        )

    def relay_out():
        out_across.wait_recv()
        ends.append(
            copies.send(lambda: (out_out.at[theirs], out_out.at[theirs], here.core_peer))
        )

    vectors_total = vectors_buf[0]
    for w in range(1, w_size):
        vectors_total = vectors_total + vectors_buf[w]
    vectors_out[...] = vectors_total
    kv_bias = jnp.concatenate(
        [jnp.zeros((1, width), f32), vectors_out[pl.ds(1, 1), :]], axis=1
    )
    query_bias = vectors_out[pl.ds(0, 1), :]

    weight = wq_buf[...].reshape(width, width)
    for turn in range(2):
        rows = pl.ds(turn * tok, tok)
        q_buf[rows, :] = (
            (dot_nn(rows_buf[turn], weight) + query_bias) * score_scale
        ).astype(bf16)

    def keys_and_values(step):
        for n in range(lines * 2, chunks):

            @pl.when(step == n)
            def _(n=n):
                from_core[n - lines * 2].wait_recv()

        both = dot_nn(rows_buf[step], wkv_buf[...].reshape(width, 2 * width))
        both = both + kv_bias
        kv_buf[pl.ds(step * chunk_blocks, chunk_blocks)] = both.astype(bf16).reshape(
            chunk_blocks, BLOCK, 2 * width
        )

        return step

    lax.fori_loop(0, chunks, lambda step, carry: (keys_and_values(step), carry)[1], 0)
    keep += [
        copies.load(lambda: (q_buf, queries_out)),
        copies.load(lambda: (kv_buf, kv_out)),
        copies.load(lambda: (rows_buf, rows_out)),
        copies.load(lambda: (rows_buf.at[pl.ds(0, 2)], own_out)),
    ]
    relay(0)
    pos_ready.wait()
    for turn in range(2):
        dealt_bias[turn].wait_recv()
    head_of_lane = lax.broadcasted_iota(jnp.int32, (BLOCK, LANES), 1) // HEAD_DIM

    def put(i, slot):
        return pltpu.make_async_copy(probs_buf.at[slot], probs_out.at[i], probs_sem.at[slot])

    def attend_block(i, carry):
        turn, row, slot = i // chunk_blocks, i % chunk_blocks, i % 2
        for j in range(CANDS):
            cat[j * BLOCK : (j + 1) * BLOCK, :] = kv_buf[pos[turn, 0, row * CANDS + j]]

        @pl.when(i >= 2)
        def _():
            put(i - 2, slot).wait()

        mine = pl.ds(pl.multiple_of(i * BLOCK, BLOCK), BLOCK)
        masked = bias_buf[turn, row]
        for g in range(groups):
            lanes = slice(g * LANES, (g + 1) * LANES)
            v_lanes = slice(width + g * LANES, width + (g + 1) * LANES)
            q_all = spread_heads(q_buf[mine, lanes], head_of_lane)
            scores = dot_nt(q_all, cat[:, lanes]) + masked
            row_max = jnp.max(scores, axis=-1, keepdims=True)
            shifted = jnp.exp(scores - row_max)
            row_total = jnp.sum(shifted, axis=-1, keepdims=True)
            shares = (shifted * (1.0 / row_total)).astype(bf16)
            probs_buf[slot, g] = shares
            mixed = dot_nn(shares, cat[:, v_lanes])
            ctx_buf[mine, lanes] = pick_heads(mixed, head_of_lane).astype(bf16)
        put(i, slot).start()

        @pl.when(i == blocks - 3)
        def _():
            relay(1)

        return carry

    lax.fori_loop(0, blocks, attend_block, 0)
    keep.append(copies.load(lambda: (ctx_buf, context_out)))
    for n in range(2):
        relay_last(n)
        if n == 0:
            relay_out()
    for copy in gradients + ends:
        copy.wait_recv()
    for copy in placed + keep:
        copy.wait()
    for n in range(2):
        put(blocks - 2 + n, n).wait()
    copies.finish()


def front_all(ctx_size, w_size, hidden, out_grad, ints, bias, vectors, weights):
    w_query, w_key, w_value, w_out, w_up, w_down = weights
    lines = ctx_size // 4
    tok, width = hidden.shape[2], hidden.shape[3]
    rows = w_query.shape[0]
    chunks = lines * 4
    blocks = 2 * tok // BLOCK
    keys = CANDS * BLOCK
    groups = width // LANES
    probs_shape = (groups, GROUP * BLOCK, keys)
    key_blocks = chunks * tok // BLOCK
    shapes = [
        ((chunks, tok, width), bf16),
        ((2, tok, width), bf16),
        (ints.shape, ints.dtype),
        (vectors.shape, f32),
        ((w_size, rows, width), bf16),
        ((w_size, rows, 2 * width), bf16),
        ((w_size, rows, width), bf16),
        ((w_size,) + w_up.shape, bf16),
        ((w_size,) + w_down.shape, bf16),
        ((2 * tok, width), bf16),
        ((key_blocks, BLOCK, 2 * width), bf16),
        ((2 * tok, width), bf16),
        ((blocks,) + probs_shape, bf16),
        ((2, tok, width), bf16),
    ]
    any_space = pl.BlockSpec(memory_space=pl.ANY)
    out_specs = [any_space] * len(shapes)
    out_specs[3] = pl.BlockSpec(memory_space=pltpu.VMEM)
    return pl.pallas_call(
        functools.partial(front_kernel, ctx_size, w_size),
        in_specs=[any_space] * 11,
        out_specs=out_specs,
        out_shape=[jax.ShapeDtypeStruct(shape, dtype) for shape, dtype in shapes],
        scratch_shapes=[
            pltpu.VMEM(w_up.shape, bf16),
            pltpu.VMEM(w_down.shape, bf16),
            pltpu.VMEM(w_out.shape, bf16),
            pltpu.VMEM((chunks, tok, width), bf16),
            pltpu.VMEM((w_size, rows, width), bf16),
            pltpu.VMEM((w_size, rows, 2 * width), bf16),
            pltpu.VMEM((w_size,) + vectors.shape, f32),
            pltpu.VMEM(bias.shape, f32),
            pltpu.VMEM((2 * tok, width), bf16),
            pltpu.VMEM((2 * tok, width), bf16),
            pltpu.VMEM((key_blocks, BLOCK, 2 * width), bf16),
            pltpu.VMEM((keys, 2 * width), bf16),
            pltpu.VMEM((2,) + probs_shape, bf16),
            pltpu.SMEM(ints.shape, ints.dtype),
            pltpu.SemaphoreType.DMA((2,)),
            (
                pltpu.SemaphoreType.DMA((24,)),
                pltpu.SemaphoreType.DMA((64,)),
                pltpu.SemaphoreType.DMA((64,)),
            ),
        ],
        compiler_params=pltpu.CompilerParams(
            collective_id=0, has_side_effects=True, vmem_limit_bytes=56 << 20
        ),
        name="front_all",
    )(hidden, out_grad, ints, bias, vectors, w_query, w_key, w_value, w_out, w_up, w_down)


def make_local(ctx_size, w_size):
    def local(
        hidden,
        out_grad,
        doc_lengths,
        rand_pick,
        w_query,
        w_key,
        w_value,
        w_out,
        w_up,
        w_down,
        b_query,
        b_value,
        b_out,
        b_up,
        b_down,
        ln1_gain,
        ln1_shift,
        ln2_gain,
        ln2_shift,
    ):
        wires = Wires(ctx_size, w_size)
        tok, width = hidden.shape[2], hidden.shape[3]
        ff = w_up.shape[1]
        tok_blocks = tok // BLOCK
        lines, pairs = wires.lines, wires.pairs
        micro = wires.part // 2

        vectors = [b_query, b_value, b_out, b_up, b_down, ln1_gain, ln1_shift, ln2_gain, ln2_shift]
        vector_sizes = [vector.shape[0] for vector in vectors]
        merged = lines == 2 and pairs == 2
        in_chunk = jnp.arange(tok_blocks, dtype=jnp.int32)
        if merged:
            ints, bias = prepare(ctx_size, w_size, doc_lengths, rand_pick)
            flat = jnp.zeros((8 * b_query.shape[0],), f32)
            narrow = [vector for vector in vectors if vector is not b_up]
            for n, vector in enumerate(narrow):
                size = vector.shape[0]
                flat = flat + jnp.pad(vector.astype(f32), (n * size, (7 - n) * size))
            table = lax.dynamic_update_slice(
                jnp.zeros((16, width), f32),
                flat.reshape(8, -1),
                (jnp.int32(0), wires.w * b_query.shape[0]),
            )
            table = lax.dynamic_update_slice(
                table, b_up.astype(f32)[None], (8 + wires.w, jnp.int32(0))
            )
            (
                all_rows,
                grads_dealt,
                ints_dealt,
                vector_table,
                full_query,
                full_kv,
                full_out,
                full_up,
                full_down,
                queries,
                kv,
                context,
                probs,
                own_rows,
            ) = front_all(
                ctx_size,
                w_size,
                hidden,
                out_grad,
                ints,
                bias,
                table,
                (w_query, w_key, w_value, w_out, w_up, w_down),
            )
            bias_out, bias_down, gain_one, shift_one, gain_two, shift_two = [
                vector_table[n] for n in range(2, 8)
            ]
            bias_up = vector_table[8:12].reshape(-1)
        else:
            small_ints = jnp.concatenate(
                [rand_pick.reshape(MICRO, -1), doc_lengths.reshape(MICRO, -1)], axis=1
            )
            int_count = small_ints.shape[1]
            small_ints = jnp.pad(small_ints, ((0, 0), (0, 1024 - int_count))).reshape(MICRO, 8, 128)
            vector_row = vector_sizes[0]
            (
                all_rows,
                grads_dealt,
                ints_dealt,
                vector_table,
                full_query,
                full_kv,
                full_out,
                full_up,
                full_down,
            ) = gather_all(
                ctx_size,
                w_size,
                hidden,
                out_grad,
                small_ints,
                jnp.concatenate(
                    [vector.astype(f32).reshape(-1, vector_row) for vector in vectors], axis=0
                ),
                (w_query, w_key, w_value, w_out, w_up, w_down),
            )
            ints_dealt = ints_dealt.reshape(MICRO, -1)
            spread = []
            at = 0
            for size in vector_sizes:
                count = size // vector_row
                spread.append(vector_table[:, at : at + count].reshape(-1))
                at += count
            (
                bias_query,
                bias_value,
                bias_out,
                bias_up,
                bias_down,
                gain_one,
                shift_one,
                gain_two,
                shift_two,
            ) = spread

            picks = jnp.stack(
                [ints_dealt[turn, : tok_blocks * 3].reshape(tok_blocks, 3) for turn in range(2)]
            ).reshape(-1, 3)
            lengths = ints_dealt[0, tok_blocks * 3 : int_count]
            chunk_ids = [
                (2 * wires.core + (micro + turn) % 2) * lines + wires.line for turn in range(2)
            ]
            my_blocks = jnp.concatenate([chunk * tok_blocks + in_chunk for chunk in chunk_ids])
            safe_blocks, allowed = candidates(my_blocks, lengths, picks)
            chunk = safe_blocks // tok_blocks
            chunk_part, chunk_line = chunk // lines, chunk % lines
            place = (
                ((chunk_part // 2) ^ wires.core) * lines + (chunk_line ^ wires.line)
            ) * 2 + (chunk_part + micro) % 2
            pos = (place * tok_blocks + safe_blocks % tok_blocks).reshape(-1).astype(jnp.int32)
            bias = jnp.repeat(jnp.where(allowed, 0.0, masked_score).astype(f32), BLOCK, axis=1)[:, None]

            queries = ((dot_nn(all_rows.reshape(-1, width)[: 2 * tok], full_query.reshape(-1, width)) + bias_query) * score_scale).astype(bf16)
            kv_bias = jnp.concatenate([jnp.zeros_like(bias_value), bias_value])
            kv = (dot_nn(all_rows.reshape(-1, width), full_kv.reshape(-1, 2 * width)) + kv_bias).astype(bf16)
            context, probs = attend(pos, queries, bias, kv)
        all_rows = all_rows.reshape(-1, width)
        if not merged:
            own_rows = all_rows[: 2 * tok]
        own_rows = own_rows.reshape(-1, width)
        grads_dealt = grads_dealt.reshape(-1, width)
        full_query, full_kv, full_out, full_up, full_down = [
            full.reshape(-1, full.shape[2]) for full in (full_query, full_kv, full_out, full_up, full_down)
        ]
        rows_f32 = own_rows.astype(f32)

        attn_out = dot_nn(context, full_out) + bias_out
        normed, ln1_back = jax.vjp(layer_norm, rows_f32 + attn_out, gain_one, shift_one)
        normed_low = normed.astype(bf16)
        up_pre = dot_nn(normed_low, full_up) + bias_up
        gelu_out, gelu_back = jax.vjp(lambda v: jax.nn.gelu(v, approximate=True), up_pre)
        activated = gelu_out.astype(bf16)
        branch = dot_nn(activated, full_down) + bias_down
        final, ln2_back = jax.vjp(layer_norm, normed + branch, gain_two, shift_two)
        final = final.astype(bf16)

        def term_of(rows_a, rows_b, scale=None):
            term = dot_tn(rows_a, rows_b)
            if scale is not None:
                term = term * scale
            return term.astype(bf16).reshape(pairs, 2, -1, rows_b.shape[1])

        d_mid, grad_gain_two, grad_shift_two = ln2_back(grads_dealt.astype(f32))
        d_branch = d_mid.astype(bf16)
        term_down = term_of(activated, d_branch)
        d_act = dot_nt(d_branch, full_down)
        d_up = gelu_back(d_act)[0].astype(bf16)
        term_up = term_of(normed_low, d_up)
        d_normed = dot_nt(d_up, full_up) + d_mid
        d_sum, grad_gain_one, grad_shift_one = ln1_back(d_normed)
        d_attn = d_sum.astype(bf16)
        term_out = term_of(context, d_attn)
        d_context = dot_nt(d_attn, full_out).astype(bf16)

        def table_of(vectors):
            return jnp.concatenate([vector.reshape(w_size, -1) for vector in vectors], axis=1)

        def column_sums(rows_a):
            return jnp.sum(rows_a.astype(f32), axis=0)

        sums = (
            column_sums(d_attn),
            column_sums(d_up),
            column_sums(d_branch),
            grad_gain_one,
            grad_shift_one,
            grad_gain_two,
            grad_shift_two,
        )
        shard = width // w_size
        if merged:
            table = table_of(sums)
            table = jnp.pad(table, ((0, 8 - w_size), (0, 0)))
            term_down = term_down.reshape(pairs, 2, -1, shard, width)
            by_block = (-1, BLOCK, width)
            up, down, out_query, key_value, block_out, grad_hidden, table = back_all(
                ctx_size,
                w_size,
                (ints_dealt, table),
                (
                    queries,
                    d_context,
                    d_sum.reshape(by_block),
                    probs,
                    kv,
                    all_rows.reshape(by_block),
                    full_kv.reshape(-1, BLOCK, 2 * width),
                    full_query,
                    final.reshape(2, -1, BLOCK, width),
                    term_up,
                    term_down,
                    term_out,
                ),
                (width, tok, all_rows.shape[0], table.shape),
            )
            row = lax.dynamic_slice(table, (wires.w, jnp.int32(0)), (1, table.shape[1]))[0]
            both = lax.dynamic_slice(
                table, (jnp.int32(w_size), wires.w * shard), (2, shard)
            )
            small = [both[0], both[1]]
            at = 0
            for size in vector_sizes[2:]:
                small.append(row[at : at + size])
                at += size

            return (
                block_out.reshape(2, 1, tok, width),
                grad_hidden.reshape(2, 1, tok, width).astype(f32),
                out_query[1].astype(f32),
                key_value[0].astype(f32),
                key_value[1].astype(f32),
                out_query[0].astype(f32),
                up.astype(f32),
                down.astype(f32),
                *small,
            )

        d_query, d_kv = attend_back(pos, queries, d_context, probs, kv)

        through = dot_nt(d_kv, full_kv).astype(bf16)
        near = d_sum + score_scale * dot_nt(d_query, full_query)
        term_kv = term_of(all_rows, d_kv)
        term_query = term_of(own_rows, d_query, score_scale)

        sums = (score_scale * column_sums(d_query), column_sums(d_kv[:, width:])) + sums
        table = table_of(sums)[:, None]
        term_down = term_down.reshape(pairs, 2, -1, shard, width)
        summed, block_out, grad_hidden, table = finish_all(
            ctx_size,
            w_size,
            (term_up, term_down, term_query, term_kv, term_out),
            ("wide", "tall", "wide", "wide", "wide"),
            through.reshape(-1, tok, width),
            near.reshape(-1, tok, width),
            final.reshape(-1, tok, width),
            table,
        )
        row = lax.dynamic_slice(
            table, (wires.w, jnp.int32(0), jnp.int32(0)), (1, 1, table.shape[2])
        )[0, 0]
        small = []
        at = 0
        for size in vector_sizes:
            small.append(row[at : at + size])
            at += size

        parts = lines // 2
        at = 0

        def wide(columns):
            nonlocal at
            count = columns * parts // width
            pieces = summed[at : at + count].astype(f32)
            at += count
            return jnp.concatenate([pieces[c] for c in range(count)], axis=1)

        grad_up = wide(ff)
        count = ff * parts // width
        grad_down = summed[at : at + count].astype(f32).reshape(-1, parts, shard, width // parts)
        grad_down = jnp.swapaxes(grad_down, 1, 2).reshape(-1, width)
        at += count
        grad_query, grad_key, grad_value, grad_out = [wide(width) for _ in range(4)]
        return (
            block_out[:, None],
            grad_hidden.astype(f32)[:, None],
            grad_query,
            grad_key,
            grad_value,
            grad_out,
            grad_up,
            grad_down,
            *small,
        )

    return local


def solution(mesh):
    tokens = P(None, "wshard", "ctx", None)
    in_specs = (
        tokens,
        tokens,
        P(None, "wshard", None),
        tokens,
        *[P("wshard", None)] * 6,
        *[P("wshard")] * 9,
    )
    out_specs = (tokens, tokens, *[P("wshard", None)] * 6, *[P("wshard")] * 9)
    return jax.shard_map(
        make_local(mesh.shape["ctx"], mesh.shape["wshard"]),
        mesh=mesh,
        in_specs=in_specs,
        out_specs=out_specs,
        check_vma=False,
    )
```

```python
import functools
import heapq
import math

import jax
import jax.numpy as jnp
from jax import lax
from jax.experimental import pallas as pl
from jax.experimental.pallas import tpu as pltpu
from jax.sharding import PartitionSpec as P

HEADS = 12
HEAD_DIM = 64
BLOCK = 64
MICRO = 2
GROUP = 4
LANES = GROUP * HEAD_DIM
CANDS = 8

masked_score = -1e30
norm_eps = 1e-12
score_scale = 1.0 / math.sqrt(HEAD_DIM)
bf16 = jnp.bfloat16
f32 = jnp.float32
MESH = pl.DeviceIdType.MESH


def layer_norm(values, ln_gain, ln_shift):
    center = values - jnp.mean(values, axis=-1, keepdims=True)
    spread = jnp.mean(center * center, axis=-1, keepdims=True)
    return center * lax.rsqrt(spread + norm_eps) * ln_gain + ln_shift


def candidates(blocks, lengths, chosen_raw):
    doc_ends = jnp.cumsum(lengths)
    doc_starts = doc_ends - lengths
    owner_doc = jnp.sum((blocks[:, None] >= doc_ends[None, :]).astype(jnp.int32), axis=1)
    doc_ids = jnp.arange(lengths.shape[0], dtype=jnp.int32)
    member = (owner_doc[:, None] == doc_ids[None, :]).astype(jnp.int32)
    doc_first = jnp.sum(member * doc_starts[None, :], axis=1)
    length = jnp.sum(member * lengths[None, :], axis=1)
    randoms = doc_first[:, None] + chosen_raw % length[:, None]
    columns = [blocks, blocks - 1, blocks + 1, doc_first, doc_first + 1]
    for column in range(chosen_raw.shape[1]):
        columns.append(randoms[:, column])
    chosen = jnp.stack(columns, axis=1)
    inside = (chosen >= doc_first[:, None]) & (chosen < (doc_first + length)[:, None])
    is_fresh = [jnp.ones(blocks.shape, dtype=jnp.bool_)]
    for column in range(1, chosen.shape[1]):
        is_fresh.append(jnp.all(chosen[:, :column] != chosen[:, column : column + 1], axis=1))
    allowed = inside & jnp.stack(is_fresh, axis=1)
    safe_blocks = jnp.where(allowed, chosen, blocks[:, None])
    return (safe_blocks, allowed)


def dot_nt(a, b):
    return lax.dot_general(a, b, (((1,), (1,)), ((), ())), preferred_element_type=f32)


def dot_nn(a, b):
    return lax.dot_general(a, b, (((1,), (0,)), ((), ())), preferred_element_type=f32)


def dot_tn(a, b):
    return lax.dot_general(a, b, (((0,), (0,)), ((), ())), preferred_element_type=f32)


def spread_heads(rows, head_of_lane):
    zero = jnp.zeros_like(rows)
    return jnp.concatenate([jnp.where(head_of_lane == h, rows, zero) for h in range(GROUP)], axis=0)


def pick_heads(rows, head_of_lane):
    total = jnp.zeros((BLOCK, LANES), f32)
    for h in range(GROUP):
        total = jnp.where(head_of_lane == h, rows[h * BLOCK : (h + 1) * BLOCK], total)
    return total


def attend_kernel(groups, width, pos_ref, q_ref, bias_ref, kv_ref, ctx_ref, probs_ref, cat):
    i = pl.program_id(0)
    for j in range(CANDS):
        start = pl.multiple_of(pos_ref[i * CANDS + j] * BLOCK, BLOCK)
        cat[j * BLOCK : (j + 1) * BLOCK, :] = kv_ref[pl.ds(start, BLOCK), :]
    head_of_lane = lax.broadcasted_iota(jnp.int32, (BLOCK, LANES), 1) // HEAD_DIM
    bias = bias_ref[0]
    for g in range(groups):
        lanes = slice(g * LANES, (g + 1) * LANES)
        v_lanes = slice(width + g * LANES, width + (g + 1) * LANES)
        q_all = spread_heads(q_ref[:, lanes], head_of_lane)
        scores = dot_nt(q_all, cat[:, lanes]) + bias
        row_max = jnp.max(scores, axis=-1, keepdims=True)
        shifted = jnp.exp(scores - row_max)
        row_total = jnp.sum(shifted, axis=-1, keepdims=True)
        probs = (shifted * (1.0 / row_total)).astype(bf16)
        probs_ref[0, g] = probs
        mixed = dot_nn(probs, cat[:, v_lanes])
        ctx_ref[:, lanes] = pick_heads(mixed, head_of_lane).astype(bf16)


def attend(pos, queries, bias, kv):
    rows, width = queries.shape
    blocks = rows // BLOCK
    groups = width // LANES
    keys = CANDS * BLOCK
    return pl.pallas_call(
        functools.partial(attend_kernel, groups, width),
        grid_spec=pltpu.PrefetchScalarGridSpec(
            num_scalar_prefetch=1,
            grid=(blocks,),
            in_specs=[
                pl.BlockSpec((BLOCK, width), lambda i, p: (i, 0)),
                pl.BlockSpec((1, 1, keys), lambda i, p: (i, 0, 0)),
                pl.BlockSpec(kv.shape, lambda i, p: (0, 0), pipeline_mode=pl.Buffered(1)),
            ],
            out_specs=[
                pl.BlockSpec((BLOCK, width), lambda i, p: (i, 0)),
                pl.BlockSpec((1, groups, GROUP * BLOCK, keys), lambda i, p: (i, 0, 0, 0)),
            ],
            scratch_shapes=[pltpu.VMEM((keys, 2 * width), bf16)],
        ),
        out_shape=[
            jax.ShapeDtypeStruct((rows, width), bf16),
            jax.ShapeDtypeStruct((blocks, groups, GROUP * BLOCK, keys), bf16),
        ],
        compiler_params=pltpu.CompilerParams(vmem_limit_bytes=48 << 20),
        cost_estimate=pl.CostEstimate(
            flops=blocks * groups * 4 * GROUP * BLOCK * keys * LANES,
            bytes_accessed=kv.size * 2 + rows * width * 4 + blocks * groups * GROUP * BLOCK * keys * 2,
            transcendentals=blocks * groups * GROUP * BLOCK * keys,
        ),
        name="attend",
    )(pos, queries, bias, kv)


def attend_back_kernel(
    groups, width, pos_ref, q_ref, dctx_ref, probs_ref, kv_ref, dq_ref, dkv_ref, cat, acc
):
    i = pl.program_id(0)

    @pl.when(i == 0)
    def _():
        acc[...] = jnp.zeros_like(acc)

    for j in range(CANDS):
        start = pl.multiple_of(pos_ref[i * CANDS + j] * BLOCK, BLOCK)
        cat[j * BLOCK : (j + 1) * BLOCK, :] = kv_ref[pl.ds(start, BLOCK), :]
    head_of_lane = lax.broadcasted_iota(jnp.int32, (BLOCK, LANES), 1) // HEAD_DIM
    for g in range(groups):
        lanes = slice(g * LANES, (g + 1) * LANES)
        v_lanes = slice(width + g * LANES, width + (g + 1) * LANES)
        q_all = spread_heads(q_ref[:, lanes], head_of_lane)
        d_all = spread_heads(dctx_ref[:, lanes], head_of_lane)
        probs_low = probs_ref[0, g]
        probs = probs_low.astype(f32)
        d_probs = dot_nt(d_all, cat[:, v_lanes])
        row_inner = jnp.sum(probs * d_probs, axis=-1, keepdims=True)
        d_scores = (probs * (d_probs - row_inner)).astype(bf16)
        dq_ref[:, lanes] = pick_heads(dot_nn(d_scores, cat[:, lanes]), head_of_lane).astype(bf16)
        d_key = dot_tn(d_scores, q_all)
        d_value = dot_tn(probs_low, d_all)
        for j in range(CANDS):
            start = pl.multiple_of(pos_ref[i * CANDS + j] * BLOCK, BLOCK)
            part = slice(j * BLOCK, (j + 1) * BLOCK)
            acc[pl.ds(start, BLOCK), lanes] += d_key[part]
            acc[pl.ds(start, BLOCK), v_lanes] += d_value[part]

    @pl.when(i == pl.num_programs(0) - 1)
    def _():
        dkv_ref[...] = acc[...].astype(bf16)


def attend_back(pos, queries, d_context, probs, kv):
    rows, width = queries.shape
    blocks = rows // BLOCK
    groups = width // LANES
    keys = CANDS * BLOCK
    return pl.pallas_call(
        functools.partial(attend_back_kernel, groups, width),
        grid_spec=pltpu.PrefetchScalarGridSpec(
            num_scalar_prefetch=1,
            grid=(blocks,),
            in_specs=[
                pl.BlockSpec((BLOCK, width), lambda i, p: (i, 0)),
                pl.BlockSpec((BLOCK, width), lambda i, p: (i, 0)),
                pl.BlockSpec((1, groups, GROUP * BLOCK, keys), lambda i, p: (i, 0, 0, 0)),
                pl.BlockSpec(kv.shape, lambda i, p: (0, 0), pipeline_mode=pl.Buffered(1)),
            ],
            out_specs=[
                pl.BlockSpec((BLOCK, width), lambda i, p: (i, 0)),
                pl.BlockSpec(kv.shape, lambda i, p: (0, 0), pipeline_mode=pl.Buffered(1)),
            ],
            scratch_shapes=[pltpu.VMEM((keys, 2 * width), bf16), pltpu.VMEM(kv.shape, f32)],
        ),
        out_shape=[
            jax.ShapeDtypeStruct((rows, width), bf16),
            jax.ShapeDtypeStruct(kv.shape, bf16),
        ],
        compiler_params=pltpu.CompilerParams(vmem_limit_bytes=60 << 20),
        cost_estimate=pl.CostEstimate(
            flops=blocks * groups * 8 * GROUP * BLOCK * keys * LANES,
            bytes_accessed=kv.size * 4 + rows * width * 6 + blocks * groups * GROUP * BLOCK * keys * 2,
            transcendentals=0,
        ),
        name="attend_back",
    )(pos, queries, d_context, probs, kv)


class Wires:
    def __init__(self, ctx_size, w_size):
        self.ctx_size, self.w_size = ctx_size, w_size
        self.lines = ctx_size // 4
        self.pairs = w_size // 2
        self.ctx = lax.axis_index("ctx")
        self.w = lax.axis_index("wshard")
        self.part = self.ctx // self.lines
        self.line = self.ctx % self.lines
        self.pair = self.w // 2
        self.core = self.w % 2

    def at(self, part, line, pair, core):
        return (part * self.lines + line, pair * 2 + core)

    @property
    def core_peer(self):
        return self.at(self.part, self.line, self.pair, 1 - self.core)

    def pair_peer(self, flip):
        return self.at(self.part, self.line, self.pair ^ flip, self.core)

    def line_peer(self, flip):
        return self.at(self.part, self.line ^ flip, self.pair, self.core)

    def part_peer(self, flip):
        return self.at(self.part ^ flip, self.line, self.pair, self.core)

    def move(self, value, to):
        perm = []
        for ctx in range(self.ctx_size):
            for w in range(self.w_size):
                part, line, pair, core = to(ctx // self.lines, ctx % self.lines, w // 2, w % 2)
                target = (part * self.lines + line) * self.w_size + pair * 2 + core
                perm.append((ctx * self.w_size + w, target))
        return lax.ppermute(value, ("ctx", "wshard"), perm)

    def to_core(self, value):
        return self.move(value, lambda part, line, pair, core: (part, line, pair, 1 - core))

    def to_pair(self, value, flip):
        return self.move(value, lambda part, line, pair, core: (part, line, pair ^ flip, core))

    def to_line(self, value, flip):
        return self.move(value, lambda part, line, pair, core: (part, line ^ flip, pair, core))

    def to_part(self, value, flip):
        return self.move(value, lambda part, line, pair, core: (part ^ flip, line, pair, core))

    def deal(self, value, turn):
        return self.move(
            value,
            lambda part, line, pair, core: (2 * ((turn + part) % 2) + core, line, pair, part // 2),
        )

    def deal_back(self, value, turn):
        return self.move(
            value,
            lambda part, line, pair, core: (2 * core + (part // 2 + turn) % 2, line, pair, part % 2),
        )


def bits(count):
    flips = []
    flip = 1
    while flip < count:
        flips.append(flip)
        flip *= 2
    return flips


def gather_kernel(wires_of, refs, outs, own_shards, local_sem, send_sem, recv_sem):
    hidden, out_grad, ints, vectors, w_query, w_key, w_value, w_out, w_up, w_down = refs
    rows_out, grads_out, ints_out, vectors_out, query_out, kv_out, out_out, up_out, down_out = outs
    here = wires_of()
    lines, pairs = here.lines, here.pairs
    part, line, pair, core = here.part, here.line, here.pair, here.core
    width = w_query.shape[1]
    used = [0]
    sent = []
    local = []
    placed = []

    def at(part, line, pair, core):
        return (part * lines + line, pair * 2 + core)

    core_peer = at(part, line, pair, 1 - core)

    def line_peer(flip):
        return at(part, line ^ flip, pair, core)

    def pair_peer(flip):
        return at(part, line, pair ^ flip, core)

    def deal_target(turn):
        return at(2 * ((turn + part) % 2) + core, line, pair, part // 2)

    def deal_source(turn):
        return at(2 * core + (part // 2 + turn) % 2, line, pair, part % 2)

    stays = [
        jnp.logical_and(
            2 * ((turn + part) % 2) + core == part, part // 2 == core
        )
        for turn in range(2)
    ]

    barrier = pltpu.get_barrier_semaphore()

    def greet(device):
        pl.semaphore_signal(barrier, inc=1, device_id=device, device_id_type=MESH)

    peers = [core_peer]
    peers += [line_peer(flip) for flip in range(1, lines)]
    peers += [pair_peer(flip) for flip in range(1, pairs)]
    for device in peers:
        greet(device)
    for turn in range(2):

        @pl.when(jnp.logical_not(stays[turn]))
        def _(turn=turn):
            greet(deal_target(turn))
            greet(deal_source(turn))

    staying = sum(stay.astype(jnp.int32) for stay in stays)
    pl.semaphore_wait(barrier, len(peers) + 4 - 2 * staying)

    def send(src, dst, device, stay=None):
        n = used[0]
        used[0] += 1
        copy = pltpu.make_async_remote_copy(
            src_ref=src,
            dst_ref=dst,
            send_sem=send_sem.at[n],
            recv_sem=recv_sem.at[n],
            device_id=device,
            device_id_type=MESH,
        )
        if stay is None:
            copy.start()
        else:

            @pl.when(stay)
            def _():
                pltpu.make_async_copy(src, dst, recv_sem.at[n]).start()

            @pl.when(jnp.logical_not(stay))
            def _():
                copy.start()

        sent.append((copy, stay))
        return copy

    def stage(src, held):
        copy = pltpu.make_async_copy(src, held, local_sem.at[len(local)])
        copy.start()
        local.append(copy)

    def place_held(held, dst):
        local[len(placed)].wait()
        copy = pltpu.make_async_copy(held, dst, local_sem.at[len(local) + len(placed)])
        copy.start()
        placed.append(copy)

    me = pair * 2 + core

    dealt = [
        send(
            hidden.at[(turn + part) % 2, 0],
            rows_out.at[turn],
            deal_target(turn),
            stays[turn],
        )
        for turn in range(2)
    ]

    matrices = [
        (w_up, lambda shard: up_out.at[shard], True),
        (w_down, lambda shard: down_out.at[shard], True),
        (w_query, lambda shard: query_out.at[shard], False),
        (w_key, lambda shard: kv_out.at[shard, :, :width], False),
        (w_value, lambda shard: kv_out.at[shard, :, width:], False),
        (w_out, lambda shard: out_out.at[shard], False),
        (vectors, lambda shard: vectors_out.at[shard], False),
    ]
    side = line % 2
    for (src, _, _), held in zip(matrices, own_shards):
        stage(src, held)

    def half_cuts(src):
        half = src.shape[0] // 2
        first = pl.ds(pl.multiple_of(side * half, 8), half)
        return first, pl.ds(pl.multiple_of((1 - side) * half, 8), half)

    halves = [
        (
            flip,
            src,
            place,
            send(src.at[half_cuts(src)[0]], place(me).at[half_cuts(src)[0]], pair_peer(flip)),
        )
        for src, place, split in matrices
        if split
        for flip in range(1, pairs)
    ]
    late = [
        send(ints.at[(turn + part) % 2], ints_out.at[turn], deal_target(turn), stays[turn])
        for turn in range(2)
    ]
    for src, place, _ in matrices:
        late.append(send(src, place(me), core_peer))

    crossed = []
    for turn in range(2):
        dealt[turn].wait_recv()
        for flip in range(1, lines):
            crossed.append(
                (
                    flip * 2 + turn,
                    send(rows_out.at[turn], rows_out.at[flip * 2 + turn], line_peer(flip)),
                )
            )
        late.append(send(rows_out.at[turn], rows_out.at[lines * 2 + turn], core_peer))
    for (src, place, _), held in zip(matrices, own_shards):
        place_held(held, place(me))

    relayed = []
    whole = [
        (src, place, flip)
        for src, place, split in matrices
        if not split
        for flip in range(1, pairs)
    ]
    direct = []
    for step, (flip, src, place, copy) in enumerate(halves):
        copy.wait_recv()
        first, second = half_cuts(src)
        shard = (pair ^ flip) * 2 + core
        got = place(shard).at[first]
        relayed.append((place(shard).at[second], send(got, got, line_peer(1))))
        late.append(send(got, got, core_peer))
        share = -(-len(whole) // len(halves))
        for src, place, flip in whole[step * share : (step + 1) * share]:
            direct.append((flip, place, send(src, place(me), pair_peer(flip))))
    late += [
        send(
            out_grad.at[(turn + part) % 2, 0],
            grads_out.at[turn],
            deal_target(turn),
            stays[turn],
        )
        for turn in range(2)
    ]
    for index, copy in crossed:
        copy.wait_recv()
        late.append(send(rows_out.at[index], rows_out.at[lines * 2 + index], core_peer))
    for flip, place, copy in direct:
        copy.wait_recv()
        shard = (pair ^ flip) * 2 + core
        late.append(send(place(shard), place(shard), core_peer))
    for got, copy in relayed:
        copy.wait_recv()
        late.append(send(got, got, core_peer))
    for copy in late:
        copy.wait_recv()
    for copy in placed:
        copy.wait()
    for copy, stay in sent:
        if stay is None:
            copy.wait_send()
        else:

            @pl.when(jnp.logical_not(stay))
            def _(copy=copy):
                copy.wait_send()


def gather_all(ctx_size, w_size, hidden, out_grad, ints, vectors, weights):
    w_query, w_key, w_value, w_out, w_up, w_down = weights
    lines, pairs = ctx_size // 4, w_size // 2
    tok, width = hidden.shape[2], hidden.shape[3]
    rows = w_query.shape[0]
    shapes = [
        ((lines * 4, tok, width), bf16),
        ((2, tok, width), bf16),
        (ints.shape, ints.dtype),
        ((w_size,) + vectors.shape, f32),
        ((w_size, rows, width), bf16),
        ((w_size, rows, 2 * width), bf16),
        ((w_size, rows, width), bf16),
        ((w_size,) + w_up.shape, bf16),
        ((w_size,) + w_down.shape, bf16),
    ]
    sems = 16 + 8 * lines + 20 * pairs

    def body(*refs):
        gather_kernel(
            lambda: Wires(ctx_size, w_size), refs[:10], refs[10:19], refs[19:26], *refs[26:]
        )

    return pl.pallas_call(
        body,
        in_specs=[pl.BlockSpec(memory_space=pl.ANY)] * 10,
        out_specs=[pl.BlockSpec(memory_space=pl.ANY)] * len(shapes),
        out_shape=[jax.ShapeDtypeStruct(shape, dtype) for shape, dtype in shapes],
        scratch_shapes=[
            *[
                pltpu.VMEM(shard.shape, shard.dtype)
                for shard in (w_up, w_down, w_query, w_key, w_value, w_out, vectors)
            ],
            pltpu.SemaphoreType.DMA((14,)),
            pltpu.SemaphoreType.DMA((sems,)),
            pltpu.SemaphoreType.DMA((sems,)),
        ],
        compiler_params=pltpu.CompilerParams(collective_id=0, has_side_effects=True),
        name="gather_all",
    )(hidden, out_grad, ints, vectors, w_query, w_key, w_value, w_out, w_up, w_down)


class Sent:
    def __init__(self, make, stay=None):
        self.make, self.stay = make, stay

    def wait(self):
        self.make().wait()

    def wait_recv(self):
        self.make().wait_recv()


class Copies:
    def __init__(self, local_sem, send_sem, recv_sem):
        self.local_sem, self.send_sem, self.recv_sem = local_sem, send_sem, recv_sem
        self.locals, self.sent = 0, []

    def load(self, pair):
        n = self.locals
        self.locals += 1
        copy = Sent(lambda: pltpu.make_async_copy(*pair(), self.local_sem.at[n]))
        copy.make().start()
        return copy

    def send(self, triple, stay=None):
        n = len(self.sent)

        def make():
            src, dst, device = triple()
            return pltpu.make_async_remote_copy(
                src_ref=src,
                dst_ref=dst,
                send_sem=self.send_sem.at[n],
                recv_sem=self.recv_sem.at[n],
                device_id=device,
                device_id_type=MESH,
            )

        if stay is None:
            make().start()
        else:

            @pl.when(stay)
            def _():
                src, dst, _ = triple()
                pltpu.make_async_copy(src, dst, self.recv_sem.at[n]).start()

            @pl.when(jnp.logical_not(stay))
            def _():
                make().start()

        copy = Sent(make, stay)
        self.sent.append(copy)
        return copy

    def finish(self):
        for copy in self.sent:
            if copy.stay is None:
                copy.make().wait_send()
            else:

                @pl.when(jnp.logical_not(copy.stay))
                def _(copy=copy):
                    copy.make().wait_send()


def add_blocks(dst, *srcs):
    if len(dst.shape) == 3:

        def each(i, carry):
            total = srcs[0][i].astype(f32)
            for src in srcs[1:]:
                total = total + src[i].astype(f32)
            dst[i] = total.astype(dst.dtype)
            return carry

        lax.fori_loop(0, dst.shape[0], each, 0)
        return
    rows = dst.shape[0]
    step = 48 if rows % 48 == 0 else 32

    def body(i, carry):
        cut = pl.ds(pl.multiple_of(i * step, step), step)
        total = srcs[0][cut, :].astype(f32)
        for src in srcs[1:]:
            total = total + src[cut, :].astype(f32)
        dst[cut, :] = total.astype(dst.dtype)
        return carry

    lax.fori_loop(0, rows // step, body, 0)


class Events:
    def __init__(self):
        self.items = []

    def add(self, time, action):
        self.items.append((time, len(self.items), action))

    def take(self, until):
        due = sorted([item for item in self.items if item[0] <= until], key=lambda item: item[:2])
        self.items = [item for item in self.items if item[0] > until]
        return [action for _, _, action in due]

    def run(self, until=math.inf):
        for action in self.take(until):
            action()


class Plan:
    def __init__(self, events):
        self.events, self.heap, self.free, self.count = events, [], {}, 0

    def at(self, time, action):
        heapq.heappush(self.heap, (time, self.count, action))
        self.count += 1

    def do(self, time, action):
        self.events.add(time, action)

    def send(self, link, time, length, then):
        def start(now):
            begin = max(now, self.free.get(link, 0.0))
            self.free[link] = begin + length
            self.at(begin + length + 2.0, then)

        self.at(time, start)

    def run(self):
        while self.heap:
            time, _, action = heapq.heappop(self.heap)
            action(time)


def group_scratch(lines, pairs, rows, columns, lines_first=False):
    block = (rows, columns)
    return [
        pltpu.VMEM((2 * lines, pairs) + block, bf16),
        pltpu.VMEM((2 * lines, pairs) + block, bf16),
        pltpu.VMEM((2 * lines, max(pairs - 1, 1)) + block, bf16),
        pltpu.VMEM((2 * lines,) + block, bf16),
        pltpu.VMEM((2, pairs if lines_first else lines - 1) + block, bf16),
        pltpu.VMEM((2,) + block, bf16),
        pltpu.VMEM((2,) + block, bf16),
        pltpu.VMEM((2,) + block, bf16),
    ]


GROUP_SCRATCH = 8
BACK_GROUPS = 6
LINES_FIRST = (True, False, True, True, False, False)
ROWS_DELAY = (10.0, 20.0)


def reduce_group(here, copies, plan, chunks, scratch, place, unit, core_times, lines_first=False):
    from_core, own, from_pairs, paired, from_lines, lined, from_parts, parted = scratch
    lines, pairs = here.lines, here.pairs
    line, pair, core, part = here.line, here.pair, here.core, here.part
    low_part = part % 2
    state = {}

    def to_core(i, view):
        state["core", i] = copies.send(lambda: (view(), from_core.at[i], here.core_peer))

    def begin(i):
        to_core(i, lambda: chunks[i](1 - core))
        state["own", i] = copies.load(lambda: (chunks[i](core), own.at[i]))

    def over_core(i):
        if ("own", i) in state:
            state["own", i].wait()
        state["core", i].wait_recv()
        for p in range(pairs):
            add_blocks(own.at[i, p], own.at[i, p], from_core.at[i, p])
        if lines_first:
            return
        state["pair", i] = [
            copies.send(
                lambda flip=flip: (
                    own.at[i, pair ^ flip],
                    from_pairs.at[i, flip - 1],
                    here.pair_peer(flip),
                )
            )
            for flip in range(1, pairs)
        ]

    def over_pairs(i):
        for copy in state["pair", i]:
            copy.wait_recv()
        add_blocks(
            paired.at[i], own.at[i, pair], *[from_pairs.at[i, flip - 1] for flip in range(1, pairs)]
        )

    def to_lines(h):
        state["line", h] = [
            copies.send(
                lambda flip=flip: (
                    paired.at[h * lines + (line ^ flip)],
                    from_lines.at[h, flip - 1],
                    here.line_peer(flip),
                )
            )
            for flip in range(1, lines)
        ]

    def over_lines(h):
        for copy in state["line", h]:
            copy.wait_recv()
        add_blocks(
            lined.at[h],
            paired.at[h * lines + line],
            *[from_lines.at[h, flip - 1] for flip in range(1, lines)],
        )

    def both_to_lines(h):
        state["line", h] = copies.send(
            lambda: (own.at[h * lines + (line ^ 1)], from_lines.at[h], here.line_peer(1))
        )

    def both_over_lines(h):
        state["line", h].wait_recv()
        for p in range(pairs):
            add_blocks(
                paired.at[h * pairs + p], own.at[h * lines + line, p], from_lines.at[h, p]
            )
        state["pair", h] = copies.send(
            lambda: (
                paired.at[h * pairs + (pair ^ 1)],
                from_pairs.at[h, 0],
                here.pair_peer(1),
            )
        )

    def last_over_pairs(h):
        state["pair", h].wait_recv()
        add_blocks(lined.at[h], paired.at[h * pairs + pair], from_pairs.at[h, 0])

    def to_part_one():
        state["one"] = copies.send(
            lambda: (lined.at[1 - low_part], from_parts.at[0], here.part_peer(1))
        )

    def over_part_one():
        state["one"].wait_recv()
        add_blocks(parted.at[0], lined.at[low_part], from_parts.at[0])
        state["two"] = copies.send(lambda: (parted.at[0], from_parts.at[1], here.part_peer(2)))

    def mine():
        return place(low_part, line)

    def other():
        return place(1 - low_part, line)

    def over_part_two():
        state["two"].wait_recv()
        add_blocks(parted.at[1], parted.at[0], from_parts.at[1])
        state["back"] = copies.send(lambda: (parted.at[1], mine(), here.part_peer(1)))
        state["place"] = copies.load(lambda: (parted.at[1], mine()))
        state["spread"] = [
            copies.send(lambda flip=flip: (parted.at[1], mine(), here.line_peer(flip)))
            for flip in range(1, lines)
        ]

    def spread_other():
        state["back"].wait_recv()
        state["spread"] += [
            copies.send(lambda flip=flip: (other(), other(), here.line_peer(flip)))
            for flip in range(1, lines)
        ]

    def end():
        state["place"].wait()
        for copy in state["spread"]:
            copy.wait_recv()

    lined_h = []

    def core_done(i, now):
        plan.do(now, functools.partial(over_core, i))
        if lines_first:
            if i % lines == lines - 1:
                h = i // lines
                plan.do(now + 0.01, functools.partial(both_to_lines, h))
                plan.send("y", now + 0.7, pairs * unit, functools.partial(both_lined, h))
            return
        plan.send("x", now + 0.7, (pairs - 1) * unit, functools.partial(pairs_done, i))

    def pairs_done(i, now):
        plan.do(now, functools.partial(over_pairs, i))
        if i % lines == lines - 1:
            h = i // lines
            plan.do(now + 0.01, functools.partial(to_lines, h))
            plan.send("y", now + 0.3, (lines - 1) * unit, functools.partial(lines_done, h))

    def both_lined(h, now):
        plan.do(now, functools.partial(both_over_lines, h))
        plan.send("x", now + 0.7, unit, functools.partial(last_paired, h))

    def last_paired(h, now):
        plan.do(now, functools.partial(last_over_pairs, h))
        all_lined(h, now)

    def lines_done(h, now):
        plan.do(now, functools.partial(over_lines, h))
        all_lined(h, now)

    def all_lined(h, now):
        lined_h.append(h)
        if len(lined_h) == 2:
            plan.do(now + 0.01, to_part_one)
            plan.send("z", now + 0.3, unit, one_done)

    def one_done(now):
        plan.do(now, over_part_one)
        plan.send("z", now + 0.3, 2 * unit, two_done)

    def two_done(now):
        plan.do(now, over_part_two)
        plan.send("z", now + 0.3, unit, back_done)
        plan.send("y", now + 0.3, (lines - 1) * unit, lambda now: None)

    def back_done(now):
        plan.do(now, spread_other)
        plan.send("y", now + 0.1, (lines - 1) * unit, lambda now: None)

    for i in range(2 * lines):
        if chunks[i] is not None:
            plan.do(core_times[i - 2] + 0.01 if i >= 2 else -100.0, functools.partial(begin, i))
        plan.at(core_times[i], functools.partial(core_done, i))
    plan.do(10000.0, end)
    return to_core


def chunk_views(refs, kinds, width):
    views = []
    for ref, kind in zip(refs, kinds):
        if kind == "wide":
            for c in range(ref.shape[3] // width):
                views.append(
                    lambda core, ref=ref, cut=slice(c * width, (c + 1) * width): ref.at[
                        :, core, :, cut
                    ]
                )
        else:
            for b in range(ref.shape[2]):
                for c in range(ref.shape[4] // width):
                    views.append(
                        lambda core, ref=ref, b=b, cut=slice(c * width, (c + 1) * width): ref.at[
                            :, core, b, :, cut
                        ]
                    )
    return views


def finish_kernel(ctx_size, w_size, kinds, tables, *refs):
    here = Wires(ctx_size, w_size)
    lines, pairs = here.lines, here.pairs
    part, line, pair, core = here.part, here.line, here.pair, here.core
    terms = refs[: len(kinds)]
    through, near, final, table = refs[len(kinds) : len(kinds) + 4]
    at = len(kinds) + 4
    out, final_out, grad_out, table_out = refs[at : at + 4]
    at += 4
    groups = (len(refs) - at - 8) // GROUP_SCRATCH
    scratches = [
        refs[at + g * GROUP_SCRATCH : at + (g + 1) * GROUP_SCRATCH] for g in range(groups)
    ]
    at += groups * GROUP_SCRATCH
    g_core, g_own, g_line, g_near, g_sum, table_in, table_sum = refs[at : at + 7]
    copies = Copies(*refs[at + 7])
    micro = part // 2

    def back_target(turn):
        return here.at(2 * core + (micro + turn) % 2, line, pair, part % 2)

    def back_source(turn):
        return here.at(2 * ((turn + part) % 2) + core, line, pair, part // 2)

    stays = [
        jnp.logical_and(2 * core + (micro + turn) % 2 == part, part % 2 == core)
        for turn in range(2)
    ]
    barrier = pltpu.get_barrier_semaphore()

    def greet(device):
        pl.semaphore_signal(barrier, inc=1, device_id=device, device_id_type=MESH)

    peers = [here.core_peer, here.part_peer(1), here.part_peer(2)]
    peers += [here.line_peer(flip) for flip in range(1, lines)]
    peers += [here.pair_peer(flip) for flip in range(1, pairs)]
    for device in peers:
        greet(device)
    for turn in range(2):

        @pl.when(jnp.logical_not(stays[turn]))
        def _(turn=turn):
            greet(back_target(turn))
            greet(back_source(turn))

    staying = sum(stay.astype(jnp.int32) for stay in stays)
    pl.semaphore_wait(barrier, len(peers) + 4 - 2 * staying)

    events = Events()
    state = {}
    count = 2 * lines

    def begin_rows():
        state["core"] = [
            copies.send(lambda j=j: (through.at[count + j], g_core.at[j], here.core_peer))
            for j in range(count)
        ]
        state["own"] = [
            copies.load(lambda j=j: (through.at[j], g_own.at[j])) for j in range(count)
        ]
        state["near"] = copies.load(lambda: (near, g_near))
        state["out"] = [
            copies.send(
                lambda turn=turn: (final.at[turn], final_out.at[micro], back_target(turn)),
                stays[turn],
            )
            for turn in range(2)
        ]

    def rows_over_core():
        for j in reversed(range(count)):
            state["own"][j].wait()
            state["core"][j].wait_recv()
            add_blocks(g_own.at[j], g_own.at[j], g_core.at[j])
            if j >= 2:
                state["line", j] = copies.send(
                    lambda j=j: (g_own.at[j], g_line.at[j - 2], here.line_peer(j // 2))
                )

    def rows_over_lines():
        state["near"].wait()
        state["back"] = []
        for turn in range(2):
            others = []
            for flip in range(1, lines):
                state["line", 2 * flip + turn].wait_recv()
                others.append(g_line.at[2 * flip + turn - 2])
            add_blocks(g_sum.at[turn], g_near.at[turn], g_own.at[turn], *others)
            state["back"].append(
                copies.send(
                    lambda turn=turn: (g_sum.at[turn], grad_out.at[micro], back_target(turn)),
                    stays[turn],
                )
            )

    def end_rows():
        for copy in state["out"] + state["back"]:
            copy.wait_recv()

    steps = [here.core_peer]
    steps += [here.pair_peer(flip) for flip in bits(pairs)]
    steps += [here.line_peer(flip) for flip in bits(lines)]
    steps += [here.part_peer(flip) for flip in bits(4)]

    def table_send(n):
        src = table if n == 0 else table_sum.at[n - 1]
        state["table", n] = copies.send(lambda: (src, table_in.at[n], steps[n]))

    def table_step(n):
        state["table", n].wait_recv()
        before = table[...] if n == 0 else table_sum[n - 1]
        total = before + table_in[n]
        if n + 1 < len(steps):
            table_sum[n] = total
            table_send(n + 1)
        else:
            table_out[...] = total

    plan = Plan(events)
    events.add(-1001.0, begin_rows)
    events.add(-1000.5, lambda: table_send(0))
    events.add(0.5, rows_over_core)
    events.add(17.0, rows_over_lines)
    events.add(9000.0, end_rows)
    for n in range(len(steps)):
        events.add(2.5 + n * 6.0, functools.partial(table_step, n))
    views = chunk_views(terms, kinds, out.shape[2])
    size = 2 * lines
    for g in range(groups):
        reduce_group(
            here,
            copies,
            plan,
            views[g * size : (g + 1) * size],
            scratches[g],
            lambda h, line, g=g: out.at[g * size + h * lines + line],
            6.0,
            [2.0 + 1.5 * (g * size + i) for i in range(size)],
        )
    plan.run()
    events.run()
    copies.finish()


def finish_all(ctx_size, w_size, terms, kinds, through, near, final, table):
    lines, pairs = ctx_size // 4, w_size // 2
    count = 2 * lines
    tok, width = through.shape[1:]
    rows = width // w_size
    columns = width // (lines // 2)
    chunks = sum(term.size for term in terms) // (w_size * rows * columns)
    groups = chunks // (2 * lines)
    table_steps = 1 + len(bits(pairs)) + len(bits(lines)) + len(bits(4))
    block = (tok, width)
    any_space = pl.BlockSpec(memory_space=pl.ANY)
    in_vmem = pl.BlockSpec(memory_space=pltpu.VMEM)
    sems = 40 + 10 * lines + groups * 2 * lines * (6 + pairs)
    scratch = []
    for _ in range(groups):
        scratch += group_scratch(lines, pairs, rows, columns)
    scratch += [
        pltpu.VMEM((count,) + block, bf16),
        pltpu.VMEM((count,) + block, bf16),
        pltpu.VMEM((max(count - 2, 1),) + block, bf16),
        pltpu.VMEM((2,) + block, f32),
        pltpu.VMEM((2,) + block, bf16),
        pltpu.VMEM((table_steps,) + table.shape, f32),
        pltpu.VMEM((table_steps,) + table.shape, f32),
        (
            pltpu.SemaphoreType.DMA((sems,)),
            pltpu.SemaphoreType.DMA((sems,)),
            pltpu.SemaphoreType.DMA((sems,)),
        ),
    ]
    return pl.pallas_call(
        functools.partial(finish_kernel, ctx_size, w_size, kinds, table_steps),
        in_specs=[any_space] * (len(terms) + 3) + [in_vmem],
        out_specs=[any_space, any_space, any_space, in_vmem],
        out_shape=[
            jax.ShapeDtypeStruct((chunks, rows, columns), bf16),
            jax.ShapeDtypeStruct((2,) + block, bf16),
            jax.ShapeDtypeStruct((2,) + block, bf16),
            jax.ShapeDtypeStruct(table.shape, f32),
        ],
        scratch_shapes=scratch,
        compiler_params=pltpu.CompilerParams(
            collective_id=1, has_side_effects=True, vmem_limit_bytes=60 << 20
        ),
        name="finish_all",
    )(*terms, through, near, final, table)


def greet_all(here, back_target, back_source, stays):
    lines, pairs = here.lines, here.pairs
    barrier = pltpu.get_barrier_semaphore()

    def greet(device):
        pl.semaphore_signal(barrier, inc=1, device_id=device, device_id_type=MESH)

    peers = [here.core_peer, here.part_peer(1), here.part_peer(2)]
    peers += [here.line_peer(flip) for flip in range(1, lines)]
    peers += [here.pair_peer(flip) for flip in range(1, pairs)]
    for device in peers:
        greet(device)
    for turn in range(2):

        @pl.when(jnp.logical_not(stays[turn]))
        def _(turn=turn):
            greet(back_target(turn))
            greet(back_source(turn))

    staying = sum(stay.astype(jnp.int32) for stay in stays)
    pl.semaphore_wait(barrier, len(peers) + 4 - 2 * staying)


def back_kernel(ctx_size, w_size, *refs):
    here = Wires(ctx_size, w_size)
    lines, pairs = here.lines, here.pairs
    part, line, pair, core = here.part, here.line, here.pair, here.core
    micro = part // 2
    (
        named,
        table,
        queries,
        d_context,
        d_sum,
        probs,
        kv,
        rows_all,
        full_kv,
        full_query,
        final,
        term_up,
        term_down,
        term_out,
    ) = refs[:14]
    up_out, down_out, oq_out, kv_out, final_out, grad_out, table_out = refs[14:21]
    scratches = [
        refs[21 + g * GROUP_SCRATCH : 21 + (g + 1) * GROUP_SCRATCH] for g in range(BACK_GROUPS)
    ]
    (
        kv_buf,
        slots,
        cat,
        probs_buf,
        q_buf,
        dctx_buf,
        rows_buf,
        wq_buf,
        q_other,
        kv_other,
        g_near,
        g_core,
        g_line,
        g_sum,
        acc,
        value_sums,
        table_in,
        table_sum,
        probs_sem,
        sems,
    ) = refs[21 + BACK_GROUPS * GROUP_SCRATCH :]
    copies = Copies(*sems)
    own_tokens, width = q_buf.shape
    key_blocks = kv_buf.shape[0]
    tokens = key_blocks * BLOCK
    blocks = own_tokens // BLOCK
    piece = blocks // 2
    groups = width // LANES
    keys = CANDS * BLOCK
    shard = width // w_size
    half = width // 2

    def back_target(turn):
        return here.at(2 * core + (micro + turn) % 2, line, pair, part % 2)

    def back_source(turn):
        return here.at(2 * ((turn + part) % 2) + core, line, pair, part // 2)

    stays = [
        jnp.logical_and(2 * core + (micro + turn) % 2 == part, part % 2 == core)
        for turn in range(2)
    ]

    def fetch(i, slot):
        return pltpu.make_async_copy(probs.at[i], probs_buf.at[slot], probs_sem.at[slot])

    greet_all(here, back_target, back_source, stays)

    events = Events()
    state = {}
    count = 2 * lines

    w_kv = slots.at[pl.ds(0, width // BLOCK)]
    rows_from = 16
    all_rows = slots.at[pl.ds(rows_from, key_blocks), :, pl.ds(0, width)]
    through_from = rows_from + key_blocks

    def through_other(j):
        return slots.at[pl.ds(through_from + j * piece, piece), :, pl.ds(0, width)]

    def through_own(j):
        return slots.at[pl.ds(through_from + j * piece, piece), :, pl.ds(width, width)]

    def send_out():
        state["out"] = [
            copies.send(
                lambda turn=turn: (final.at[turn], final_out.at[micro], back_target(turn)),
                stays[turn],
            )
            for turn in range(2)
        ]

    def rows_over_core(turn):
        for j in reversed(range(turn, count, 2)):
            state["through", j].wait_recv()
            add_blocks(through_own(j), through_own(j), g_core.at[j])
            if j >= 2:
                state["line", j] = copies.send(
                    lambda j=j: (through_own(j), g_line.at[j - 2], here.line_peer(j // 2))
                )

    def rows_over_lines(turn):
        others = []
        for flip in range(1, lines):
            state["line", 2 * flip + turn].wait_recv()
            others.append(g_line.at[2 * flip + turn - 2])
        add_blocks(
            g_sum.at[turn], g_near.at[pl.ds(turn * piece, piece)], through_own(turn), *others
        )
        state["back", turn] = copies.send(
            lambda: (g_sum.at[turn], grad_out.at[micro], back_target(turn)), stays[turn]
        )

    def end_rows():
        for copy in state["out"] + [state["back", turn] for turn in range(2)]:
            copy.wait_recv()

    steps = [lambda: here.core_peer]
    steps += [lambda flip=flip: here.pair_peer(flip) for flip in bits(pairs)]
    steps += [lambda flip=flip: here.line_peer(flip) for flip in bits(lines)]
    steps += [lambda flip=flip: here.part_peer(flip) for flip in bits(4)]

    def table_send(n):
        state["table", n] = copies.send(lambda: (table_sum.at[n], table_in.at[n], steps[n]()))

    def table_step(n):
        state["table", n].wait_recv()
        total = table_sum[n] + table_in[n]
        if n + 1 < len(steps):
            table_sum[n + 1] = total
            table_send(n + 1)
        else:
            table_out[...] = total

    attend_at, attend_step = 9.0, 2.6
    gather_at = attend_at + blocks * attend_step + 3.0
    gather_step = 1.4
    through_at = gather_at + 8 * gather_step + 1.0
    through_step = 1.3
    terms_at = through_at + 8 * through_step
    terms_step = 2.6
    terms_end = terms_at + 4 * terms_step
    plan = Plan(events)
    plan.send("z", 0.0, 18.0, lambda now: None)

    views = chunk_views((term_up, term_down), ("wide", "tall"), half)
    size = 2 * lines
    ffn_groups = BACK_GROUPS - 2

    def half_columns(number):
        return pl.ds(pl.multiple_of(number * half, 128), half)

    def up_place(g):
        return lambda h, line: up_out.at[:, half_columns(g * size + h * lines + line)]

    def down_place(g):
        return lambda h, line: down_out.at[
            pl.ds(pl.multiple_of((2 * g + h) * shard, 16), shard), half_columns(line)
        ]

    places = [up_place(g) for g in range(ffn_groups // 2)]
    places += [down_place(g) for g in range(ffn_groups // 2)]
    for g in range(ffn_groups):
        order = [g * size + i for i in range(size)]
        reduce_group(
            here,
            copies,
            plan,
            views[g * size : (g + 1) * size],
            scratches[g],
            places[g],
            3.0,
            [max(2.5 + 0.7 * n, 3.0 * n - 12.0) for n in order],
            LINES_FIRST[g],
        )
    out_views = [
        lambda side, cut=slice(c * half, (c + 1) * half): term_out.at[:, side, :, cut]
        for c in range(2)
    ]
    q_own = scratches[ffn_groups][1]
    q_to_core = reduce_group(
        here,
        copies,
        plan,
        out_views + [None, None],
        scratches[ffn_groups],
        lambda h, line: oq_out.at[h, :, half_columns(line)],
        3.0,
        [gather_at + 2.0 + 1.5 * i for i in range(4)],
        LINES_FIRST[ffn_groups],
    )
    kv_own = scratches[ffn_groups + 1][1]
    kv_to_core = reduce_group(
        here,
        copies,
        plan,
        [None] * 4,
        scratches[ffn_groups + 1],
        lambda h, line: kv_out.at[h, :, half_columns(line)],
        3.0,
        [terms_at + (i + 1) * terms_step + 1.5 for i in range(4)],
        LINES_FIRST[ffn_groups + 1],
    )
    plan.do(-200.0, send_out)
    rows_at = through_at + 2 * count * through_step + 0.5

    def rows_done(turn, now):
        plan.do(now, functools.partial(rows_over_lines, turn))
        plan.send("z", now + 0.7, 9.0, lambda now: None)

    for turn in range(2):
        rows_time = rows_at + ROWS_DELAY[turn]
        plan.do(rows_time, functools.partial(rows_over_core, turn))
        plan.send("y", rows_time + 0.7, 9.0, functools.partial(rows_done, turn))
    plan.do(9000.0, end_rows)
    for n in range(len(steps)):
        plan.do(through_at + 3.0 + n * 5.0, functools.partial(table_step, n))
    plan.run()

    def stepped(number, at, each, body):
        def loop(step, carry):
            body(step)
            for n in range(number):
                due = events.take(at + (n + 1) * each)
                if due:

                    @pl.when(step == n)
                    def _(due=due):
                        for action in due:
                            action()

            return carry

        lax.fori_loop(0, number, loop, 0)

    events.run(0.0)
    first = [
        copies.load(lambda: (kv, kv_buf)),
        copies.load(lambda: (queries, q_buf)),
        copies.load(lambda: (d_context, dctx_buf)),
    ]
    later = [
        copies.load(lambda: (rows_all.at[pl.ds(0, blocks)], rows_buf)),
        copies.load(lambda: (full_query, wq_buf)),
        copies.load(lambda: (d_sum, g_near)),
    ]

    fetch(0, 0).start()
    events.run(attend_at)
    for copy in first:
        copy.wait()
    slots[blocks * CANDS] = jnp.zeros((BLOCK, 2 * width), bf16)

    head_of_lane = lax.broadcasted_iota(jnp.int32, (BLOCK, LANES), 1) // HEAD_DIM

    def attend_block(i):
        slot = i % 2
        fetch(i, slot).wait()

        @pl.when(i + 1 < blocks)
        def _():
            fetch(i + 1, 1 - slot).start()

        for j in range(CANDS):
            place = named[i // piece, 0, (i % piece) * CANDS + j]
            cat[j * BLOCK : (j + 1) * BLOCK, :] = kv_buf[place]
        mine = pl.ds(pl.multiple_of(i * BLOCK, BLOCK), BLOCK)
        rows = pl.ds(i * CANDS, CANDS)
        by_slot = (CANDS, BLOCK, LANES)
        for g in range(groups):
            lanes = slice(g * LANES, (g + 1) * LANES)
            v_lanes = slice(width + g * LANES, width + (g + 1) * LANES)
            q_all = spread_heads(q_buf[mine, lanes], head_of_lane)
            d_all = spread_heads(dctx_buf[mine, lanes], head_of_lane)
            probs_low = probs_buf[slot, g]
            shares = probs_low.astype(f32)
            d_probs = dot_nt(d_all, cat[:, v_lanes])
            row_inner = jnp.sum(shares * d_probs, axis=-1, keepdims=True)
            d_scores = (shares * (d_probs - row_inner)).astype(bf16)
            slots[rows, :, lanes] = dot_tn(d_scores, q_all).astype(bf16).reshape(by_slot)
            slots[rows, :, v_lanes] = dot_tn(probs_low, d_all).astype(bf16).reshape(by_slot)
            q_buf[mine, lanes] = pick_heads(dot_nn(d_scores, cat[:, lanes]), head_of_lane).astype(
                bf16
            )

    stepped(blocks, attend_at, attend_step, attend_block)

    for copy in later:
        copy.wait()
    for c in range(2):
        columns = slice(c * half, (c + 1) * half)
        own_rows = rows_buf[...].reshape(own_tokens, width)
        acc[...] = dot_tn(own_rows, q_buf[:, columns]) * score_scale
        for p in range(pairs):
            for side, place in ((core, q_own.at[2 + c, p]), (1 - core, q_other.at[c, p])):
                start = pl.multiple_of((2 * p + side) * shard, shard)
                place[...] = acc[pl.ds(start, shard), :].astype(bf16)
        q_to_core(2 + c, lambda c=c: q_other.at[c])

    def near_step(step, carry):
        cut = pl.ds(pl.multiple_of(step * BLOCK * 2, BLOCK * 2), BLOCK * 2)
        near = dot_nt(q_buf[cut, :], wq_buf[...]) * score_scale
        g_near[pl.ds(step * 2, 2)] += near.reshape(2, BLOCK, width)
        return carry

    lax.fori_loop(0, own_tokens // (BLOCK * 2), near_step, 0)
    value_sums[...] = jnp.zeros_like(value_sums)

    sub = value_sums.shape[0]

    def gather_some(step):
        def one(n, carry):
            block = step * (key_blocks // 8) + n

            users = [named[i // piece, 1, block * piece + i % piece] for i in range(blocks)]
            for r in range(BLOCK // sub):
                cut = slice(r * sub, (r + 1) * sub)
                total = jnp.zeros((sub, 2 * width), f32)
                for i in range(blocks):
                    total = total + slots[users[i], cut, :].astype(f32)
                kv_buf[block, cut, :] = total.astype(bf16)
                value_sums[...] += total[:, width:]
            return carry

        lax.fori_loop(0, key_blocks // 8, one, 0)

    stepped(8, gather_at, gather_step, gather_some)
    weights = copies.load(lambda: (full_kv, w_kv))
    every = copies.load(lambda: (rows_all, all_rows))
    table_sum[0] = table[...]
    table_sum[0, pl.ds(w_size, 1), pl.ds(0, width)] = score_scale * jnp.sum(
        q_buf[...].astype(f32), axis=0, keepdims=True
    )
    table_sum[0, pl.ds(w_size + 1, 1), pl.ds(0, width)] = jnp.sum(
        value_sums[...], axis=0, keepdims=True
    )
    table_send(0)
    weights.wait()

    def through_tile(j, left, step):
        given = kv_buf[pl.ds(j * piece, piece)].reshape(piece * BLOCK, 2 * width)
        weight = slots[pl.ds(0, width // BLOCK)].reshape(width, 2 * width)
        tile = dot_nt(given, weight).astype(bf16).reshape(piece, BLOCK, width)
        slots[pl.ds(through_from + step * piece, piece), :, pl.ds(left, width)] = tile

    def other_tile(step):
        through_tile(count + step, 0, step)
        for n in range(count):

            @pl.when(step == n)
            def _(n=n):
                state["through", n] = copies.send(
                    lambda: (through_other(n), g_core.at[n], here.core_peer)
                )

    def own_tile(step):
        through_tile(step, width, step)

    stepped(count, through_at, through_step, other_tile)
    stepped(count, through_at + count * through_step, through_step, own_tile)
    every.wait()

    def kv_terms(c):
        columns = pl.ds(pl.multiple_of(c * half, 128), half)
        acc[...] = jnp.zeros_like(acc)

        def deep(t, carry):
            rows = slots[pl.ds(rows_from + t * blocks, blocks), :, 0:width]
            given = kv_buf[pl.ds(t * blocks, blocks), :, columns]
            acc[...] += dot_tn(
                rows.reshape(own_tokens, width), given.reshape(own_tokens, half)
            )
            return carry

        lax.fori_loop(0, tokens // own_tokens, deep, 0)
        for p in range(pairs):
            for side, place in ((core, kv_own.at[c, p]), (1 - core, kv_other.at[c, p])):
                start = pl.multiple_of((2 * p + side) * shard, shard)
                place[...] = acc[pl.ds(start, shard), :].astype(bf16)
        for n in range(4):

            @pl.when(c == n)
            def _(n=n):
                kv_to_core(n, lambda: kv_other.at[n])

    stepped(4, terms_at, terms_step, kv_terms)
    events.run()
    copies.finish()


def back_all(ctx_size, w_size, small, large, shapes):
    width, tok, tokens, table_shape = shapes
    lines, pairs = ctx_size // 4, w_size // 2
    rows = width // w_size
    own_tokens = 2 * tok
    blocks = own_tokens // BLOCK
    keys = CANDS * BLOCK
    half = width // 2
    table_steps = 1 + len(bits(pairs)) + len(bits(lines)) + len(bits(4))
    any_space = pl.BlockSpec(memory_space=pl.ANY)
    in_vmem = pl.BlockSpec(memory_space=pltpu.VMEM)
    in_smem = pl.BlockSpec(memory_space=pltpu.SMEM)
    scratch = []
    for lines_first in LINES_FIRST:
        scratch += group_scratch(lines, pairs, rows, half, lines_first)
    piece = (tok // BLOCK, BLOCK, width)
    scratch += [
        pltpu.VMEM((tokens // BLOCK, BLOCK, 2 * width), bf16),
        pltpu.VMEM((blocks * CANDS + 1, BLOCK, 2 * width), bf16),
        pltpu.VMEM((keys, 2 * width), bf16),
        pltpu.VMEM((2, width // LANES, GROUP * BLOCK, keys), bf16),
        pltpu.VMEM((own_tokens, width), bf16),
        pltpu.VMEM((own_tokens, width), bf16),
        pltpu.VMEM((blocks, BLOCK, width), bf16),
        pltpu.VMEM((width, width), bf16),
        pltpu.VMEM((2, pairs, rows, half), bf16),
        pltpu.VMEM((4, pairs, rows, half), bf16),
        pltpu.VMEM((blocks, BLOCK, width), f32),
        pltpu.VMEM((2 * lines,) + piece, bf16),
        pltpu.VMEM((2 * lines - 2,) + piece, bf16),
        pltpu.VMEM((2,) + piece, bf16),
        pltpu.VMEM((width, half), f32),
        pltpu.VMEM((16, width), f32),
        pltpu.VMEM((table_steps,) + table_shape, f32),
        pltpu.VMEM((table_steps,) + table_shape, f32),
        pltpu.SemaphoreType.DMA((2,)),
        (
            pltpu.SemaphoreType.DMA((60,)),
            pltpu.SemaphoreType.DMA((160,)),
            pltpu.SemaphoreType.DMA((160,)),
        ),
    ]
    return pl.pallas_call(
        functools.partial(back_kernel, ctx_size, w_size),
        in_specs=[in_smem, in_vmem] + [any_space] * len(large),
        out_specs=[any_space] * 6 + [in_vmem],
        out_shape=[
            jax.ShapeDtypeStruct((rows, 4 * width), bf16),
            jax.ShapeDtypeStruct((4 * rows, width), bf16),
            jax.ShapeDtypeStruct((2, rows, width), bf16),
            jax.ShapeDtypeStruct((2, rows, width), bf16),
            jax.ShapeDtypeStruct((2,) + piece, bf16),
            jax.ShapeDtypeStruct((2,) + piece, bf16),
            jax.ShapeDtypeStruct(table_shape, f32),
        ],
        scratch_shapes=scratch,
        compiler_params=pltpu.CompilerParams(
            collective_id=1, has_side_effects=True, vmem_limit_bytes=67043328
        ),
        name="back_all",
    )(*small, *large)


def prepare_kernel(ctx_size, w_size, lengths, picks, ints, bias):
    here = Wires(ctx_size, w_size)
    lines = here.lines
    micros, _, chunk_blocks, randoms = picks.shape
    slots = 2 * chunk_blocks * CANDS
    head = lax.broadcasted_iota(jnp.int32, (1, CANDS * BLOCK), 1) // BLOCK
    key_blocks = ctx_size * chunk_blocks
    one, nothing = jnp.int32(1), jnp.int32(0)

    for m in range(micros):

        def clear(n, carry):
            for k in range(32):
                ints[m, 1, n * 32 + k] = jnp.int32(slots)
            return carry

        lax.fori_loop(0, key_blocks * chunk_blocks // 32, clear, 0)
        turn = lax.rem(m + here.part, 2)
        for b in range(chunk_blocks):
            block = here.ctx * chunk_blocks + b
            begin, first, length = nothing, nothing, one
            for d in range(lengths.shape[2]):
                size = lengths[m, 0, d]
                end = begin + size
                inside = jnp.logical_and(block >= begin, block < end)
                first = jnp.where(inside, begin, first)
                length = jnp.where(inside, size, length)
                begin = end
            chosen = [block, block - 1, block + 1, first, first + 1]
            for r in range(randoms):
                chosen.append(first + lax.rem(picks[m, 0, b, r], length))
            row = jnp.zeros(head.shape, f32)
            for j, candidate in enumerate(chosen):
                allowed = jnp.logical_and(candidate >= first, candidate < first + length)
                for earlier in chosen[:j]:
                    allowed = jnp.logical_and(allowed, candidate != earlier)
                safe = jnp.where(allowed, candidate, block)
                chunk = lax.div(safe, chunk_blocks)
                chunk_part, chunk_line = lax.div(chunk, lines), lax.rem(chunk, lines)
                low, high = lax.rem(chunk_part, 2), lax.div(chunk_part, 2)
                place = (high ^ lax.div(here.part, 2)) * lines + (chunk_line ^ here.line)
                place = (place * 2 + lax.rem(low + m, 2)) * chunk_blocks
                place = place + lax.rem(safe, chunk_blocks)
                ints[m, 0, b * CANDS + j] = place

                @pl.when(allowed)
                def _(place=place, b=b, j=j):
                    ints[m, 1, place * chunk_blocks + b] = (turn * chunk_blocks + b) * CANDS + j

                score = jnp.where(allowed, 0.0, masked_score).astype(f32)
                row = jnp.where(head == j, score, row)
            bias[m, b] = row


def prepare(ctx_size, w_size, lengths, picks):
    micros, _, chunk_blocks, _ = picks.shape
    return pl.pallas_call(
        functools.partial(prepare_kernel, ctx_size, w_size),
        in_specs=[pl.BlockSpec(memory_space=pltpu.SMEM)] * 2,
        out_specs=[pl.BlockSpec(memory_space=pltpu.SMEM), pl.BlockSpec(memory_space=pltpu.VMEM)],
        out_shape=[
            jax.ShapeDtypeStruct((micros, 8, 128), jnp.int32),
            jax.ShapeDtypeStruct((micros, chunk_blocks, 1, CANDS * BLOCK), f32),
        ],
        name="prepare",
    )(lengths, picks)


def front_kernel(ctx_size, w_size, *refs):
    here = Wires(ctx_size, w_size)
    lines, pairs = here.lines, here.pairs
    part, line, pair, core = here.part, here.line, here.pair, here.core
    (
        hidden,
        out_grad,
        ints,
        bias,
        vectors,
        w_query,
        w_key,
        w_value,
        w_out,
        w_up,
        w_down,
    ) = refs[:11]
    (
        rows_out,
        grads_out,
        ints_out,
        vectors_out,
        query_out,
        kv_weight_out,
        out_out,
        up_out,
        down_out,
        queries_out,
        kv_out,
        context_out,
        probs_out,
        own_out,
    ) = refs[11:25]
    (
        held_up,
        held_down,
        held_out,
        rows_buf,
        wq_buf,
        wkv_buf,
        vectors_buf,
        bias_buf,
        q_buf,
        ctx_buf,
        kv_buf,
        cat,
        probs_buf,
        pos,
        probs_sem,
        sems,
    ) = refs[25:]
    copies = Copies(*sems)
    width = w_query.shape[1]
    tok = rows_buf.shape[1]
    chunk_blocks = tok // BLOCK
    blocks = 2 * chunk_blocks
    groups = width // LANES
    chunks = rows_buf.shape[0]
    me = pair * 2 + core
    side = line % 2

    def target(turn):
        return here.at(2 * ((turn + part) % 2) + core, line, pair, part // 2)

    def source(turn):
        return here.at(2 * core + (part // 2 + turn) % 2, line, pair, part % 2)

    stays = [
        jnp.logical_and(2 * ((turn + part) % 2) + core == part, part // 2 == core)
        for turn in range(2)
    ]
    greet_all(here, target, source, stays)

    def deal(src, dst, turn):
        return copies.send(
            lambda: (src((turn + part) % 2), dst(turn), target(turn)), stays[turn]
        )

    dealt = [deal(lambda m: hidden.at[m, 0], lambda t: rows_buf.at[t], turn) for turn in range(2)]
    dealt_ints = [deal(lambda m: ints.at[m], lambda t: ints_out.at[t], turn) for turn in range(2)]
    dealt_bias = [deal(lambda m: bias.at[m], lambda t: bias_buf.at[t], turn) for turn in range(2)]

    early = [
        (w_key, lambda shard: wkv_buf.at[shard, :, pl.ds(0, width)]),
        (w_value, lambda shard: wkv_buf.at[shard, :, pl.ds(width, width)]),
        (vectors, lambda shard: vectors_buf.at[shard]),
        (w_query, lambda shard: wq_buf.at[shard]),
    ]
    late = [
        (w_up, held_up, lambda shard: up_out.at[shard]),
        (w_down, held_down, lambda shard: down_out.at[shard]),
        (w_out, held_out, lambda shard: out_out.at[shard]),
    ]
    across = [
        copies.send(lambda src=src, place=place: (src, place(me), here.pair_peer(1)))
        for src, place in early
    ]
    ready = [copies.load(lambda src=src, place=place: (src, place(me))) for src, place in early]
    arrive = [
        copies.send(lambda src=src, place=place: (src, place(me), here.core_peer))
        for src, place in early
    ]

    def half_cut(src, which):
        half = src.shape[0] // 2
        return pl.ds(pl.multiple_of(which * half, 16), half)

    halves = [
        copies.send(
            lambda src=src, place=place: (
                src.at[half_cut(src, side)],
                place(me).at[half_cut(src, side)],
                here.pair_peer(1),
            )
        )
        for src, _, place in late[:2]
    ]
    out_across = copies.send(lambda: (w_out, out_out.at[me], here.pair_peer(1)))
    staged = [copies.load(lambda src=src, held=held: (src, held)) for src, held, _ in late]
    ends = [
        copies.send(lambda src=src, place=place: (src, place(me), here.core_peer))
        for src, _, place in late
    ]
    placed = []

    crossed = []
    from_core = {}
    for turn in range(2):
        dealt[turn].wait_recv()
        for flip in range(1, lines):
            crossed.append(
                copies.send(
                    lambda turn=turn, flip=flip: (
                        rows_buf.at[turn],
                        rows_buf.at[flip * 2 + turn],
                        here.line_peer(flip),
                    )
                )
            )
        from_core[turn] = copies.send(
            lambda turn=turn: (rows_buf.at[turn], rows_buf.at[lines * 2 + turn], here.core_peer)
        )
    for turn in range(2):
        dealt_ints[turn].wait_recv()
    pos_ready = copies.load(lambda: (ints_out, pos))
    for copy, (src, held, place) in zip(staged, late):
        copy.wait()
        placed.append(copies.load(lambda held=held, place=place: (held, place(me))))
    theirs = (pair ^ 1) * 2 + core
    for copy, (src, place) in zip(across, early):
        copy.wait_recv()
        arrive.append(
            copies.send(lambda place=place: (place(theirs), place(theirs), here.core_peer))
        )
    for n, copy in enumerate(crossed):
        copy.wait_recv()
        from_core[2 + n] = copies.send(
            lambda n=n: (rows_buf.at[2 + n], rows_buf.at[lines * 2 + 2 + n], here.core_peer)
        )
    gradients = [
        deal(lambda m: out_grad.at[m, 0], lambda t: grads_out.at[t], turn) for turn in range(2)
    ]
    for copy in ready + arrive:
        copy.wait() if copy in ready else copy.wait_recv()
    keep = [
        copies.load(lambda: (wq_buf, query_out)),
        copies.load(lambda: (wkv_buf, kv_weight_out)),
    ]
    relayed = []

    def relay(n):
        halves[n].wait_recv()
        src, _, place = late[n]
        relayed.append(
            copies.send(
                lambda: (
                    place(theirs).at[half_cut(src, side)],
                    place(theirs).at[half_cut(src, side)],
                    here.line_peer(1),
                )
            )
        )
        ends.append(
            copies.send(
                lambda: (
                    place(theirs).at[half_cut(src, side)],
                    place(theirs).at[half_cut(src, side)],
                    here.core_peer,
                )
            )
        )

    def relay_last(n):
        relayed[n].wait_recv()
        src, _, place = late[n]
        ends.append(
            copies.send(
                lambda: (
                    place(theirs).at[half_cut(src, 1 - side)],
                    place(theirs).at[half_cut(src, 1 - side)],
                    here.core_peer,
                )
            )
        )

    def relay_out():
        out_across.wait_recv()
        ends.append(
            copies.send(lambda: (out_out.at[theirs], out_out.at[theirs], here.core_peer))
        )

    vectors_total = vectors_buf[0]
    for w in range(1, w_size):
        vectors_total = vectors_total + vectors_buf[w]
    vectors_out[...] = vectors_total
    kv_bias = jnp.concatenate(
        [jnp.zeros((1, width), f32), vectors_out[pl.ds(1, 1), :]], axis=1
    )
    query_bias = vectors_out[pl.ds(0, 1), :]

    weight = wq_buf[...].reshape(width, width)
    for turn in range(2):
        rows = pl.ds(turn * tok, tok)
        q_buf[rows, :] = (
            (dot_nn(rows_buf[turn], weight) + query_bias) * score_scale
        ).astype(bf16)

    def keys_and_values(step):
        for n in range(lines * 2, chunks):

            @pl.when(step == n)
            def _(n=n):
                from_core[n - lines * 2].wait_recv()

        both = dot_nn(rows_buf[step], wkv_buf[...].reshape(width, 2 * width))
        both = both + kv_bias
        kv_buf[pl.ds(step * chunk_blocks, chunk_blocks)] = both.astype(bf16).reshape(
            chunk_blocks, BLOCK, 2 * width
        )

        return step

    lax.fori_loop(0, chunks, lambda step, carry: (keys_and_values(step), carry)[1], 0)
    keep += [
        copies.load(lambda: (q_buf, queries_out)),
        copies.load(lambda: (kv_buf, kv_out)),
        copies.load(lambda: (rows_buf, rows_out)),
        copies.load(lambda: (rows_buf.at[pl.ds(0, 2)], own_out)),
    ]
    relay(0)
    pos_ready.wait()
    for turn in range(2):
        dealt_bias[turn].wait_recv()
    head_of_lane = lax.broadcasted_iota(jnp.int32, (BLOCK, LANES), 1) // HEAD_DIM

    def put(i, slot):
        return pltpu.make_async_copy(probs_buf.at[slot], probs_out.at[i], probs_sem.at[slot])

    def attend_block(i, carry):
        turn, row, slot = i // chunk_blocks, i % chunk_blocks, i % 2
        for j in range(CANDS):
            cat[j * BLOCK : (j + 1) * BLOCK, :] = kv_buf[pos[turn, 0, row * CANDS + j]]

        @pl.when(i >= 2)
        def _():
            put(i - 2, slot).wait()

        mine = pl.ds(pl.multiple_of(i * BLOCK, BLOCK), BLOCK)
        masked = bias_buf[turn, row]
        for g in range(groups):
            lanes = slice(g * LANES, (g + 1) * LANES)
            v_lanes = slice(width + g * LANES, width + (g + 1) * LANES)
            q_all = spread_heads(q_buf[mine, lanes], head_of_lane)
            scores = dot_nt(q_all, cat[:, lanes]) + masked
            row_max = jnp.max(scores, axis=-1, keepdims=True)
            shifted = jnp.exp(scores - row_max)
            row_total = jnp.sum(shifted, axis=-1, keepdims=True)
            shares = (shifted * (1.0 / row_total)).astype(bf16)
            probs_buf[slot, g] = shares
            mixed = dot_nn(shares, cat[:, v_lanes])
            ctx_buf[mine, lanes] = pick_heads(mixed, head_of_lane).astype(bf16)
        put(i, slot).start()

        @pl.when(i == blocks - 3)
        def _():
            relay(1)

        return carry

    lax.fori_loop(0, blocks, attend_block, 0)
    keep.append(copies.load(lambda: (ctx_buf, context_out)))
    for n in range(2):
        relay_last(n)
        if n == 0:
            relay_out()
    for copy in gradients + ends:
        copy.wait_recv()
    for copy in placed + keep:
        copy.wait()
    for n in range(2):
        put(blocks - 2 + n, n).wait()
    copies.finish()


def front_all(ctx_size, w_size, hidden, out_grad, ints, bias, vectors, weights):
    w_query, w_key, w_value, w_out, w_up, w_down = weights
    lines = ctx_size // 4
    tok, width = hidden.shape[2], hidden.shape[3]
    rows = w_query.shape[0]
    chunks = lines * 4
    blocks = 2 * tok // BLOCK
    keys = CANDS * BLOCK
    groups = width // LANES
    probs_shape = (groups, GROUP * BLOCK, keys)
    key_blocks = chunks * tok // BLOCK
    shapes = [
        ((chunks, tok, width), bf16),
        ((2, tok, width), bf16),
        (ints.shape, ints.dtype),
        (vectors.shape, f32),
        ((w_size, rows, width), bf16),
        ((w_size, rows, 2 * width), bf16),
        ((w_size, rows, width), bf16),
        ((w_size,) + w_up.shape, bf16),
        ((w_size,) + w_down.shape, bf16),
        ((2 * tok, width), bf16),
        ((key_blocks, BLOCK, 2 * width), bf16),
        ((2 * tok, width), bf16),
        ((blocks,) + probs_shape, bf16),
        ((2, tok, width), bf16),
    ]
    any_space = pl.BlockSpec(memory_space=pl.ANY)
    out_specs = [any_space] * len(shapes)
    out_specs[3] = pl.BlockSpec(memory_space=pltpu.VMEM)
    return pl.pallas_call(
        functools.partial(front_kernel, ctx_size, w_size),
        in_specs=[any_space] * 11,
        out_specs=out_specs,
        out_shape=[jax.ShapeDtypeStruct(shape, dtype) for shape, dtype in shapes],
        scratch_shapes=[
            pltpu.VMEM(w_up.shape, bf16),
            pltpu.VMEM(w_down.shape, bf16),
            pltpu.VMEM(w_out.shape, bf16),
            pltpu.VMEM((chunks, tok, width), bf16),
            pltpu.VMEM((w_size, rows, width), bf16),
            pltpu.VMEM((w_size, rows, 2 * width), bf16),
            pltpu.VMEM((w_size,) + vectors.shape, f32),
            pltpu.VMEM(bias.shape, f32),
            pltpu.VMEM((2 * tok, width), bf16),
            pltpu.VMEM((2 * tok, width), bf16),
            pltpu.VMEM((key_blocks, BLOCK, 2 * width), bf16),
            pltpu.VMEM((keys, 2 * width), bf16),
            pltpu.VMEM((2,) + probs_shape, bf16),
            pltpu.SMEM(ints.shape, ints.dtype),
            pltpu.SemaphoreType.DMA((2,)),
            (
                pltpu.SemaphoreType.DMA((24,)),
                pltpu.SemaphoreType.DMA((64,)),
                pltpu.SemaphoreType.DMA((64,)),
            ),
        ],
        compiler_params=pltpu.CompilerParams(
            collective_id=0, has_side_effects=True, vmem_limit_bytes=56 << 20
        ),
        name="front_all",
    )(hidden, out_grad, ints, bias, vectors, w_query, w_key, w_value, w_out, w_up, w_down)


def make_local(ctx_size, w_size):
    def local(
        hidden,
        out_grad,
        doc_lengths,
        rand_pick,
        w_query,
        w_key,
        w_value,
        w_out,
        w_up,
        w_down,
        b_query,
        b_value,
        b_out,
        b_up,
        b_down,
        ln1_gain,
        ln1_shift,
        ln2_gain,
        ln2_shift,
    ):
        wires = Wires(ctx_size, w_size)
        tok, width = hidden.shape[2], hidden.shape[3]
        ff = w_up.shape[1]
        tok_blocks = tok // BLOCK
        lines, pairs = wires.lines, wires.pairs
        micro = wires.part // 2

        vectors = [b_query, b_value, b_out, b_up, b_down, ln1_gain, ln1_shift, ln2_gain, ln2_shift]
        vector_sizes = [vector.shape[0] for vector in vectors]
        merged = lines == 2 and pairs == 2
        in_chunk = jnp.arange(tok_blocks, dtype=jnp.int32)
        if merged:
            ints, bias = prepare(ctx_size, w_size, doc_lengths, rand_pick)
            flat = jnp.zeros((8 * b_query.shape[0],), f32)
            narrow = [vector for vector in vectors if vector is not b_up]
            for n, vector in enumerate(narrow):
                size = vector.shape[0]
                flat = flat + jnp.pad(vector.astype(f32), (n * size, (7 - n) * size))
            table = lax.dynamic_update_slice(
                jnp.zeros((16, width), f32),
                flat.reshape(8, -1),
                (jnp.int32(0), wires.w * b_query.shape[0]),
            )
            table = lax.dynamic_update_slice(
                table, b_up.astype(f32)[None], (8 + wires.w, jnp.int32(0))
            )
            (
                all_rows,
                grads_dealt,
                ints_dealt,
                vector_table,
                full_query,
                full_kv,
                full_out,
                full_up,
                full_down,
                queries,
                kv,
                context,
                probs,
                own_rows,
            ) = front_all(
                ctx_size,
                w_size,
                hidden,
                out_grad,
                ints,
                bias,
                table,
                (w_query, w_key, w_value, w_out, w_up, w_down),
            )
            bias_out, bias_down, gain_one, shift_one, gain_two, shift_two = [
                vector_table[n] for n in range(2, 8)
            ]
            bias_up = vector_table[8:12].reshape(-1)
        else:
            small_ints = jnp.concatenate(
                [rand_pick.reshape(MICRO, -1), doc_lengths.reshape(MICRO, -1)], axis=1
            )
            int_count = small_ints.shape[1]
            small_ints = jnp.pad(small_ints, ((0, 0), (0, 1024 - int_count))).reshape(MICRO, 8, 128)
            vector_row = vector_sizes[0]
            (
                all_rows,
                grads_dealt,
                ints_dealt,
                vector_table,
                full_query,
                full_kv,
                full_out,
                full_up,
                full_down,
            ) = gather_all(
                ctx_size,
                w_size,
                hidden,
                out_grad,
                small_ints,
                jnp.concatenate(
                    [vector.astype(f32).reshape(-1, vector_row) for vector in vectors], axis=0
                ),
                (w_query, w_key, w_value, w_out, w_up, w_down),
            )
            ints_dealt = ints_dealt.reshape(MICRO, -1)
            spread = []
            at = 0
            for size in vector_sizes:
                count = size // vector_row
                spread.append(vector_table[:, at : at + count].reshape(-1))
                at += count
            (
                bias_query,
                bias_value,
                bias_out,
                bias_up,
                bias_down,
                gain_one,
                shift_one,
                gain_two,
                shift_two,
            ) = spread

            picks = jnp.stack(
                [ints_dealt[turn, : tok_blocks * 3].reshape(tok_blocks, 3) for turn in range(2)]
            ).reshape(-1, 3)
            lengths = ints_dealt[0, tok_blocks * 3 : int_count]
            chunk_ids = [
                (2 * wires.core + (micro + turn) % 2) * lines + wires.line for turn in range(2)
            ]
            my_blocks = jnp.concatenate([chunk * tok_blocks + in_chunk for chunk in chunk_ids])
            safe_blocks, allowed = candidates(my_blocks, lengths, picks)
            chunk = safe_blocks // tok_blocks
            chunk_part, chunk_line = chunk // lines, chunk % lines
            place = (
                ((chunk_part // 2) ^ wires.core) * lines + (chunk_line ^ wires.line)
            ) * 2 + (chunk_part + micro) % 2
            pos = (place * tok_blocks + safe_blocks % tok_blocks).reshape(-1).astype(jnp.int32)
            bias = jnp.repeat(jnp.where(allowed, 0.0, masked_score).astype(f32), BLOCK, axis=1)[:, None]

            queries = ((dot_nn(all_rows.reshape(-1, width)[: 2 * tok], full_query.reshape(-1, width)) + bias_query) * score_scale).astype(bf16)
            kv_bias = jnp.concatenate([jnp.zeros_like(bias_value), bias_value])
            kv = (dot_nn(all_rows.reshape(-1, width), full_kv.reshape(-1, 2 * width)) + kv_bias).astype(bf16)
            context, probs = attend(pos, queries, bias, kv)
        all_rows = all_rows.reshape(-1, width)
        if not merged:
            own_rows = all_rows[: 2 * tok]
        own_rows = own_rows.reshape(-1, width)
        grads_dealt = grads_dealt.reshape(-1, width)
        full_query, full_kv, full_out, full_up, full_down = [
            full.reshape(-1, full.shape[2]) for full in (full_query, full_kv, full_out, full_up, full_down)
        ]
        rows_f32 = own_rows.astype(f32)

        attn_out = dot_nn(context, full_out) + bias_out
        normed, ln1_back = jax.vjp(layer_norm, rows_f32 + attn_out, gain_one, shift_one)
        normed_low = normed.astype(bf16)
        up_pre = dot_nn(normed_low, full_up) + bias_up
        gelu_out, gelu_back = jax.vjp(lambda v: jax.nn.gelu(v, approximate=True), up_pre)
        activated = gelu_out.astype(bf16)
        branch = dot_nn(activated, full_down) + bias_down
        final, ln2_back = jax.vjp(layer_norm, normed + branch, gain_two, shift_two)
        final = final.astype(bf16)

        def term_of(rows_a, rows_b, scale=None):
            term = dot_tn(rows_a, rows_b)
            if scale is not None:
                term = term * scale
            return term.astype(bf16).reshape(pairs, 2, -1, rows_b.shape[1])

        d_mid, grad_gain_two, grad_shift_two = ln2_back(grads_dealt.astype(f32))
        d_branch = d_mid.astype(bf16)
        term_down = term_of(activated, d_branch)
        d_act = dot_nt(d_branch, full_down)
        d_up = gelu_back(d_act)[0].astype(bf16)
        term_up = term_of(normed_low, d_up)
        d_normed = dot_nt(d_up, full_up) + d_mid
        d_sum, grad_gain_one, grad_shift_one = ln1_back(d_normed)
        d_attn = d_sum.astype(bf16)
        term_out = term_of(context, d_attn)
        d_context = dot_nt(d_attn, full_out).astype(bf16)

        def table_of(vectors):
            return jnp.concatenate([vector.reshape(w_size, -1) for vector in vectors], axis=1)

        def column_sums(rows_a):
            return jnp.sum(rows_a.astype(f32), axis=0)

        sums = (
            column_sums(d_attn),
            column_sums(d_up),
            column_sums(d_branch),
            grad_gain_one,
            grad_shift_one,
            grad_gain_two,
            grad_shift_two,
        )
        shard = width // w_size
        if merged:
            table = table_of(sums)
            table = jnp.pad(table, ((0, 8 - w_size), (0, 0)))
            term_down = term_down.reshape(pairs, 2, -1, shard, width)
            by_block = (-1, BLOCK, width)
            up, down, out_query, key_value, block_out, grad_hidden, table = back_all(
                ctx_size,
                w_size,
                (ints_dealt, table),
                (
                    queries,
                    d_context,
                    d_sum.reshape(by_block),
                    probs,
                    kv,
                    all_rows.reshape(by_block),
                    full_kv.reshape(-1, BLOCK, 2 * width),
                    full_query,
                    final.reshape(2, -1, BLOCK, width),
                    term_up,
                    term_down,
                    term_out,
                ),
                (width, tok, all_rows.shape[0], table.shape),
            )
            row = lax.dynamic_slice(table, (wires.w, jnp.int32(0)), (1, table.shape[1]))[0]
            both = lax.dynamic_slice(
                table, (jnp.int32(w_size), wires.w * shard), (2, shard)
            )
            small = [both[0], both[1]]
            at = 0
            for size in vector_sizes[2:]:
                small.append(row[at : at + size])
                at += size

            return (
                block_out.reshape(2, 1, tok, width),
                grad_hidden.reshape(2, 1, tok, width).astype(f32),
                out_query[1].astype(f32),
                key_value[0].astype(f32),
                key_value[1].astype(f32),
                out_query[0].astype(f32),
                up.astype(f32),
                down.astype(f32),
                *small,
            )

        d_query, d_kv = attend_back(pos, queries, d_context, probs, kv)

        through = dot_nt(d_kv, full_kv).astype(bf16)
        near = d_sum + score_scale * dot_nt(d_query, full_query)
        term_kv = term_of(all_rows, d_kv)
        term_query = term_of(own_rows, d_query, score_scale)

        sums = (score_scale * column_sums(d_query), column_sums(d_kv[:, width:])) + sums
        table = table_of(sums)[:, None]
        term_down = term_down.reshape(pairs, 2, -1, shard, width)
        summed, block_out, grad_hidden, table = finish_all(
            ctx_size,
            w_size,
            (term_up, term_down, term_query, term_kv, term_out),
            ("wide", "tall", "wide", "wide", "wide"),
            through.reshape(-1, tok, width),
            near.reshape(-1, tok, width),
            final.reshape(-1, tok, width),
            table,
        )
        row = lax.dynamic_slice(
            table, (wires.w, jnp.int32(0), jnp.int32(0)), (1, 1, table.shape[2])
        )[0, 0]
        small = []
        at = 0
        for size in vector_sizes:
            small.append(row[at : at + size])
            at += size

        parts = lines // 2
        at = 0

        def wide(columns):
            nonlocal at
            count = columns * parts // width
            pieces = summed[at : at + count].astype(f32)
            at += count
            return jnp.concatenate([pieces[c] for c in range(count)], axis=1)

        grad_up = wide(ff)
        count = ff * parts // width
        grad_down = summed[at : at + count].astype(f32).reshape(-1, parts, shard, width // parts)
        grad_down = jnp.swapaxes(grad_down, 1, 2).reshape(-1, width)
        at += count
        grad_query, grad_key, grad_value, grad_out = [wide(width) for _ in range(4)]
        return (
            block_out[:, None],
            grad_hidden.astype(f32)[:, None],
            grad_query,
            grad_key,
            grad_value,
            grad_out,
            grad_up,
            grad_down,
            *small,
        )

    return local


def solution(mesh):
    tokens = P(None, "wshard", "ctx", None)
    in_specs = (
        tokens,
        tokens,
        P(None, "wshard", None),
        tokens,
        *[P("wshard", None)] * 6,
        *[P("wshard")] * 9,
    )
    out_specs = (tokens, tokens, *[P("wshard", None)] * 6, *[P("wshard")] * 9)
    return jax.shard_map(
        make_local(mesh.shape["ctx"], mesh.shape["wshard"]),
        mesh=mesh,
        in_specs=in_specs,
        out_specs=out_specs,
        check_vma=False,
    )
```

```python
import functools
import heapq
import math

import jax
import jax.numpy as jnp
from jax import lax
from jax.experimental import pallas as pl
from jax.experimental.pallas import tpu as pltpu
from jax.sharding import PartitionSpec as P

HEADS = 12
HEAD_DIM = 64
BLOCK = 64
MICRO = 2
GROUP = 4
LANES = GROUP * HEAD_DIM
CANDS = 8

masked_score = -1e30
norm_eps = 1e-12
score_scale = 1.0 / math.sqrt(HEAD_DIM)
bf16 = jnp.bfloat16
f32 = jnp.float32
MESH = pl.DeviceIdType.MESH


def layer_norm(values, ln_gain, ln_shift):
    center = values - jnp.mean(values, axis=-1, keepdims=True)
    spread = jnp.mean(center * center, axis=-1, keepdims=True)
    return center * lax.rsqrt(spread + norm_eps) * ln_gain + ln_shift


def candidates(blocks, lengths, chosen_raw):
    doc_ends = jnp.cumsum(lengths)
    doc_starts = doc_ends - lengths
    owner_doc = jnp.sum((blocks[:, None] >= doc_ends[None, :]).astype(jnp.int32), axis=1)
    doc_ids = jnp.arange(lengths.shape[0], dtype=jnp.int32)
    member = (owner_doc[:, None] == doc_ids[None, :]).astype(jnp.int32)
    doc_first = jnp.sum(member * doc_starts[None, :], axis=1)
    length = jnp.sum(member * lengths[None, :], axis=1)
    randoms = doc_first[:, None] + chosen_raw % length[:, None]
    columns = [blocks, blocks - 1, blocks + 1, doc_first, doc_first + 1]
    for column in range(chosen_raw.shape[1]):
        columns.append(randoms[:, column])
    chosen = jnp.stack(columns, axis=1)
    inside = (chosen >= doc_first[:, None]) & (chosen < (doc_first + length)[:, None])
    is_fresh = [jnp.ones(blocks.shape, dtype=jnp.bool_)]
    for column in range(1, chosen.shape[1]):
        is_fresh.append(jnp.all(chosen[:, :column] != chosen[:, column : column + 1], axis=1))
    allowed = inside & jnp.stack(is_fresh, axis=1)
    safe_blocks = jnp.where(allowed, chosen, blocks[:, None])
    return (safe_blocks, allowed)


def dot_nt(a, b):
    return lax.dot_general(a, b, (((1,), (1,)), ((), ())), preferred_element_type=f32)


def dot_nn(a, b):
    return lax.dot_general(a, b, (((1,), (0,)), ((), ())), preferred_element_type=f32)


def dot_tn(a, b):
    return lax.dot_general(a, b, (((0,), (0,)), ((), ())), preferred_element_type=f32)


def spread_heads(rows, head_of_lane):
    zero = jnp.zeros_like(rows)
    return jnp.concatenate([jnp.where(head_of_lane == h, rows, zero) for h in range(GROUP)], axis=0)


def pick_heads(rows, head_of_lane):
    total = jnp.zeros((BLOCK, LANES), f32)
    for h in range(GROUP):
        total = jnp.where(head_of_lane == h, rows[h * BLOCK : (h + 1) * BLOCK], total)
    return total


def attend_kernel(groups, width, pos_ref, q_ref, bias_ref, kv_ref, ctx_ref, probs_ref, cat):
    i = pl.program_id(0)
    for j in range(CANDS):
        start = pl.multiple_of(pos_ref[i * CANDS + j] * BLOCK, BLOCK)
        cat[j * BLOCK : (j + 1) * BLOCK, :] = kv_ref[pl.ds(start, BLOCK), :]
    head_of_lane = lax.broadcasted_iota(jnp.int32, (BLOCK, LANES), 1) // HEAD_DIM
    bias = bias_ref[0]
    for g in range(groups):
        lanes = slice(g * LANES, (g + 1) * LANES)
        v_lanes = slice(width + g * LANES, width + (g + 1) * LANES)
        q_all = spread_heads(q_ref[:, lanes], head_of_lane)
        scores = dot_nt(q_all, cat[:, lanes]) + bias
        row_max = jnp.max(scores, axis=-1, keepdims=True)
        shifted = jnp.exp(scores - row_max)
        row_total = jnp.sum(shifted, axis=-1, keepdims=True)
        probs = (shifted * (1.0 / row_total)).astype(bf16)
        probs_ref[0, g] = probs
        mixed = dot_nn(probs, cat[:, v_lanes])
        ctx_ref[:, lanes] = pick_heads(mixed, head_of_lane).astype(bf16)


def attend(pos, queries, bias, kv):
    rows, width = queries.shape
    blocks = rows // BLOCK
    groups = width // LANES
    keys = CANDS * BLOCK
    return pl.pallas_call(
        functools.partial(attend_kernel, groups, width),
        grid_spec=pltpu.PrefetchScalarGridSpec(
            num_scalar_prefetch=1,
            grid=(blocks,),
            in_specs=[
                pl.BlockSpec((BLOCK, width), lambda i, p: (i, 0)),
                pl.BlockSpec((1, 1, keys), lambda i, p: (i, 0, 0)),
                pl.BlockSpec(kv.shape, lambda i, p: (0, 0), pipeline_mode=pl.Buffered(1)),
            ],
            out_specs=[
                pl.BlockSpec((BLOCK, width), lambda i, p: (i, 0)),
                pl.BlockSpec((1, groups, GROUP * BLOCK, keys), lambda i, p: (i, 0, 0, 0)),
            ],
            scratch_shapes=[pltpu.VMEM((keys, 2 * width), bf16)],
        ),
        out_shape=[
            jax.ShapeDtypeStruct((rows, width), bf16),
            jax.ShapeDtypeStruct((blocks, groups, GROUP * BLOCK, keys), bf16),
        ],
        compiler_params=pltpu.CompilerParams(vmem_limit_bytes=48 << 20),
        cost_estimate=pl.CostEstimate(
            flops=blocks * groups * 4 * GROUP * BLOCK * keys * LANES,
            bytes_accessed=kv.size * 2 + rows * width * 4 + blocks * groups * GROUP * BLOCK * keys * 2,
            transcendentals=blocks * groups * GROUP * BLOCK * keys,
        ),
        name="attend",
    )(pos, queries, bias, kv)


def attend_back_kernel(
    groups, width, pos_ref, q_ref, dctx_ref, probs_ref, kv_ref, dq_ref, dkv_ref, cat, acc
):
    i = pl.program_id(0)

    @pl.when(i == 0)
    def _():
        acc[...] = jnp.zeros_like(acc)

    for j in range(CANDS):
        start = pl.multiple_of(pos_ref[i * CANDS + j] * BLOCK, BLOCK)
        cat[j * BLOCK : (j + 1) * BLOCK, :] = kv_ref[pl.ds(start, BLOCK), :]
    head_of_lane = lax.broadcasted_iota(jnp.int32, (BLOCK, LANES), 1) // HEAD_DIM
    for g in range(groups):
        lanes = slice(g * LANES, (g + 1) * LANES)
        v_lanes = slice(width + g * LANES, width + (g + 1) * LANES)
        q_all = spread_heads(q_ref[:, lanes], head_of_lane)
        d_all = spread_heads(dctx_ref[:, lanes], head_of_lane)
        probs_low = probs_ref[0, g]
        probs = probs_low.astype(f32)
        d_probs = dot_nt(d_all, cat[:, v_lanes])
        row_inner = jnp.sum(probs * d_probs, axis=-1, keepdims=True)
        d_scores = (probs * (d_probs - row_inner)).astype(bf16)
        dq_ref[:, lanes] = pick_heads(dot_nn(d_scores, cat[:, lanes]), head_of_lane).astype(bf16)
        d_key = dot_tn(d_scores, q_all)
        d_value = dot_tn(probs_low, d_all)
        for j in range(CANDS):
            start = pl.multiple_of(pos_ref[i * CANDS + j] * BLOCK, BLOCK)
            part = slice(j * BLOCK, (j + 1) * BLOCK)
            acc[pl.ds(start, BLOCK), lanes] += d_key[part]
            acc[pl.ds(start, BLOCK), v_lanes] += d_value[part]

    @pl.when(i == pl.num_programs(0) - 1)
    def _():
        dkv_ref[...] = acc[...].astype(bf16)


def attend_back(pos, queries, d_context, probs, kv):
    rows, width = queries.shape
    blocks = rows // BLOCK
    groups = width // LANES
    keys = CANDS * BLOCK
    return pl.pallas_call(
        functools.partial(attend_back_kernel, groups, width),
        grid_spec=pltpu.PrefetchScalarGridSpec(
            num_scalar_prefetch=1,
            grid=(blocks,),
            in_specs=[
                pl.BlockSpec((BLOCK, width), lambda i, p: (i, 0)),
                pl.BlockSpec((BLOCK, width), lambda i, p: (i, 0)),
                pl.BlockSpec((1, groups, GROUP * BLOCK, keys), lambda i, p: (i, 0, 0, 0)),
                pl.BlockSpec(kv.shape, lambda i, p: (0, 0), pipeline_mode=pl.Buffered(1)),
            ],
            out_specs=[
                pl.BlockSpec((BLOCK, width), lambda i, p: (i, 0)),
                pl.BlockSpec(kv.shape, lambda i, p: (0, 0), pipeline_mode=pl.Buffered(1)),
            ],
            scratch_shapes=[pltpu.VMEM((keys, 2 * width), bf16), pltpu.VMEM(kv.shape, f32)],
        ),
        out_shape=[
            jax.ShapeDtypeStruct((rows, width), bf16),
            jax.ShapeDtypeStruct(kv.shape, bf16),
        ],
        compiler_params=pltpu.CompilerParams(vmem_limit_bytes=60 << 20),
        cost_estimate=pl.CostEstimate(
            flops=blocks * groups * 8 * GROUP * BLOCK * keys * LANES,
            bytes_accessed=kv.size * 4 + rows * width * 6 + blocks * groups * GROUP * BLOCK * keys * 2,
            transcendentals=0,
        ),
        name="attend_back",
    )(pos, queries, d_context, probs, kv)


class Wires:
    def __init__(self, ctx_size, w_size):
        self.ctx_size, self.w_size = ctx_size, w_size
        self.lines = ctx_size // 4
        self.pairs = w_size // 2
        self.ctx = lax.axis_index("ctx")
        self.w = lax.axis_index("wshard")
        self.part = self.ctx // self.lines
        self.line = self.ctx % self.lines
        self.pair = self.w // 2
        self.core = self.w % 2

    def at(self, part, line, pair, core):
        return (part * self.lines + line, pair * 2 + core)

    @property
    def core_peer(self):
        return self.at(self.part, self.line, self.pair, 1 - self.core)

    def pair_peer(self, flip):
        return self.at(self.part, self.line, self.pair ^ flip, self.core)

    def line_peer(self, flip):
        return self.at(self.part, self.line ^ flip, self.pair, self.core)

    def part_peer(self, flip):
        return self.at(self.part ^ flip, self.line, self.pair, self.core)

    def move(self, value, to):
        perm = []
        for ctx in range(self.ctx_size):
            for w in range(self.w_size):
                part, line, pair, core = to(ctx // self.lines, ctx % self.lines, w // 2, w % 2)
                target = (part * self.lines + line) * self.w_size + pair * 2 + core
                perm.append((ctx * self.w_size + w, target))
        return lax.ppermute(value, ("ctx", "wshard"), perm)

    def to_core(self, value):
        return self.move(value, lambda part, line, pair, core: (part, line, pair, 1 - core))

    def to_pair(self, value, flip):
        return self.move(value, lambda part, line, pair, core: (part, line, pair ^ flip, core))

    def to_line(self, value, flip):
        return self.move(value, lambda part, line, pair, core: (part, line ^ flip, pair, core))

    def to_part(self, value, flip):
        return self.move(value, lambda part, line, pair, core: (part ^ flip, line, pair, core))

    def deal(self, value, turn):
        return self.move(
            value,
            lambda part, line, pair, core: (2 * ((turn + part) % 2) + core, line, pair, part // 2),
        )

    def deal_back(self, value, turn):
        return self.move(
            value,
            lambda part, line, pair, core: (2 * core + (part // 2 + turn) % 2, line, pair, part % 2),
        )


def bits(count):
    flips = []
    flip = 1
    while flip < count:
        flips.append(flip)
        flip *= 2
    return flips


def gather_kernel(wires_of, refs, outs, own_shards, local_sem, send_sem, recv_sem):
    hidden, out_grad, ints, vectors, w_query, w_key, w_value, w_out, w_up, w_down = refs
    rows_out, grads_out, ints_out, vectors_out, query_out, kv_out, out_out, up_out, down_out = outs
    here = wires_of()
    lines, pairs = here.lines, here.pairs
    part, line, pair, core = here.part, here.line, here.pair, here.core
    width = w_query.shape[1]
    used = [0]
    sent = []
    local = []
    placed = []

    def at(part, line, pair, core):
        return (part * lines + line, pair * 2 + core)

    core_peer = at(part, line, pair, 1 - core)

    def line_peer(flip):
        return at(part, line ^ flip, pair, core)

    def pair_peer(flip):
        return at(part, line, pair ^ flip, core)

    def deal_target(turn):
        return at(2 * ((turn + part) % 2) + core, line, pair, part // 2)

    def deal_source(turn):
        return at(2 * core + (part // 2 + turn) % 2, line, pair, part % 2)

    stays = [
        jnp.logical_and(
            2 * ((turn + part) % 2) + core == part, part // 2 == core
        )
        for turn in range(2)
    ]

    barrier = pltpu.get_barrier_semaphore()

    def greet(device):
        pl.semaphore_signal(barrier, inc=1, device_id=device, device_id_type=MESH)

    peers = [core_peer]
    peers += [line_peer(flip) for flip in range(1, lines)]
    peers += [pair_peer(flip) for flip in range(1, pairs)]
    for device in peers:
        greet(device)
    for turn in range(2):

        @pl.when(jnp.logical_not(stays[turn]))
        def _(turn=turn):
            greet(deal_target(turn))
            greet(deal_source(turn))

    staying = sum(stay.astype(jnp.int32) for stay in stays)
    pl.semaphore_wait(barrier, len(peers) + 4 - 2 * staying)

    def send(src, dst, device, stay=None):
        n = used[0]
        used[0] += 1
        copy = pltpu.make_async_remote_copy(
            src_ref=src,
            dst_ref=dst,
            send_sem=send_sem.at[n],
            recv_sem=recv_sem.at[n],
            device_id=device,
            device_id_type=MESH,
        )
        if stay is None:
            copy.start()
        else:

            @pl.when(stay)
            def _():
                pltpu.make_async_copy(src, dst, recv_sem.at[n]).start()

            @pl.when(jnp.logical_not(stay))
            def _():
                copy.start()

        sent.append((copy, stay))
        return copy

    def stage(src, held):
        copy = pltpu.make_async_copy(src, held, local_sem.at[len(local)])
        copy.start()
        local.append(copy)

    def place_held(held, dst):
        local[len(placed)].wait()
        copy = pltpu.make_async_copy(held, dst, local_sem.at[len(local) + len(placed)])
        copy.start()
        placed.append(copy)

    me = pair * 2 + core

    dealt = [
        send(
            hidden.at[(turn + part) % 2, 0],
            rows_out.at[turn],
            deal_target(turn),
            stays[turn],
        )
        for turn in range(2)
    ]

    matrices = [
        (w_up, lambda shard: up_out.at[shard], True),
        (w_down, lambda shard: down_out.at[shard], True),
        (w_query, lambda shard: query_out.at[shard], False),
        (w_key, lambda shard: kv_out.at[shard, :, :width], False),
        (w_value, lambda shard: kv_out.at[shard, :, width:], False),
        (w_out, lambda shard: out_out.at[shard], False),
        (vectors, lambda shard: vectors_out.at[shard], False),
    ]
    side = line % 2
    for (src, _, _), held in zip(matrices, own_shards):
        stage(src, held)

    def half_cuts(src):
        half = src.shape[0] // 2
        first = pl.ds(pl.multiple_of(side * half, 8), half)
        return first, pl.ds(pl.multiple_of((1 - side) * half, 8), half)

    halves = [
        (
            flip,
            src,
            place,
            send(src.at[half_cuts(src)[0]], place(me).at[half_cuts(src)[0]], pair_peer(flip)),
        )
        for src, place, split in matrices
        if split
        for flip in range(1, pairs)
    ]
    late = [
        send(ints.at[(turn + part) % 2], ints_out.at[turn], deal_target(turn), stays[turn])
        for turn in range(2)
    ]
    for src, place, _ in matrices:
        late.append(send(src, place(me), core_peer))

    crossed = []
    for turn in range(2):
        dealt[turn].wait_recv()
        for flip in range(1, lines):
            crossed.append(
                (
                    flip * 2 + turn,
                    send(rows_out.at[turn], rows_out.at[flip * 2 + turn], line_peer(flip)),
                )
            )
        late.append(send(rows_out.at[turn], rows_out.at[lines * 2 + turn], core_peer))
    for (src, place, _), held in zip(matrices, own_shards):
        place_held(held, place(me))

    relayed = []
    whole = [
        (src, place, flip)
        for src, place, split in matrices
        if not split
        for flip in range(1, pairs)
    ]
    direct = []
    for step, (flip, src, place, copy) in enumerate(halves):
        copy.wait_recv()
        first, second = half_cuts(src)
        shard = (pair ^ flip) * 2 + core
        got = place(shard).at[first]
        relayed.append((place(shard).at[second], send(got, got, line_peer(1))))
        late.append(send(got, got, core_peer))
        share = -(-len(whole) // len(halves))
        for src, place, flip in whole[step * share : (step + 1) * share]:
            direct.append((flip, place, send(src, place(me), pair_peer(flip))))
    late += [
        send(
            out_grad.at[(turn + part) % 2, 0],
            grads_out.at[turn],
            deal_target(turn),
            stays[turn],
        )
        for turn in range(2)
    ]
    for index, copy in crossed:
        copy.wait_recv()
        late.append(send(rows_out.at[index], rows_out.at[lines * 2 + index], core_peer))
    for flip, place, copy in direct:
        copy.wait_recv()
        shard = (pair ^ flip) * 2 + core
        late.append(send(place(shard), place(shard), core_peer))
    for got, copy in relayed:
        copy.wait_recv()
        late.append(send(got, got, core_peer))
    for copy in late:
        copy.wait_recv()
    for copy in placed:
        copy.wait()
    for copy, stay in sent:
        if stay is None:
            copy.wait_send()
        else:

            @pl.when(jnp.logical_not(stay))
            def _(copy=copy):
                copy.wait_send()


def gather_all(ctx_size, w_size, hidden, out_grad, ints, vectors, weights):
    w_query, w_key, w_value, w_out, w_up, w_down = weights
    lines, pairs = ctx_size // 4, w_size // 2
    tok, width = hidden.shape[2], hidden.shape[3]
    rows = w_query.shape[0]
    shapes = [
        ((lines * 4, tok, width), bf16),
        ((2, tok, width), bf16),
        (ints.shape, ints.dtype),
        ((w_size,) + vectors.shape, f32),
        ((w_size, rows, width), bf16),
        ((w_size, rows, 2 * width), bf16),
        ((w_size, rows, width), bf16),
        ((w_size,) + w_up.shape, bf16),
        ((w_size,) + w_down.shape, bf16),
    ]
    sems = 16 + 8 * lines + 20 * pairs

    def body(*refs):
        gather_kernel(
            lambda: Wires(ctx_size, w_size), refs[:10], refs[10:19], refs[19:26], *refs[26:]
        )

    return pl.pallas_call(
        body,
        in_specs=[pl.BlockSpec(memory_space=pl.ANY)] * 10,
        out_specs=[pl.BlockSpec(memory_space=pl.ANY)] * len(shapes),
        out_shape=[jax.ShapeDtypeStruct(shape, dtype) for shape, dtype in shapes],
        scratch_shapes=[
            *[
                pltpu.VMEM(shard.shape, shard.dtype)
                for shard in (w_up, w_down, w_query, w_key, w_value, w_out, vectors)
            ],
            pltpu.SemaphoreType.DMA((14,)),
            pltpu.SemaphoreType.DMA((sems,)),
            pltpu.SemaphoreType.DMA((sems,)),
        ],
        compiler_params=pltpu.CompilerParams(collective_id=0, has_side_effects=True),
        name="gather_all",
    )(hidden, out_grad, ints, vectors, w_query, w_key, w_value, w_out, w_up, w_down)


class Sent:
    def __init__(self, make, stay=None):
        self.make, self.stay = make, stay

    def wait(self):
        self.make().wait()

    def wait_recv(self):
        self.make().wait_recv()


class Copies:
    def __init__(self, local_sem, send_sem, recv_sem):
        self.local_sem, self.send_sem, self.recv_sem = local_sem, send_sem, recv_sem
        self.locals, self.sent = 0, []

    def load(self, pair):
        n = self.locals
        self.locals += 1
        copy = Sent(lambda: pltpu.make_async_copy(*pair(), self.local_sem.at[n]))
        copy.make().start()
        return copy

    def send(self, triple, stay=None):
        n = len(self.sent)

        def make():
            src, dst, device = triple()
            return pltpu.make_async_remote_copy(
                src_ref=src,
                dst_ref=dst,
                send_sem=self.send_sem.at[n],
                recv_sem=self.recv_sem.at[n],
                device_id=device,
                device_id_type=MESH,
            )

        if stay is None:
            make().start()
        else:

            @pl.when(stay)
            def _():
                src, dst, _ = triple()
                pltpu.make_async_copy(src, dst, self.recv_sem.at[n]).start()

            @pl.when(jnp.logical_not(stay))
            def _():
                make().start()

        copy = Sent(make, stay)
        self.sent.append(copy)
        return copy

    def finish(self):
        for copy in self.sent:
            if copy.stay is None:
                copy.make().wait_send()
            else:

                @pl.when(jnp.logical_not(copy.stay))
                def _(copy=copy):
                    copy.make().wait_send()


def add_blocks(dst, *srcs):
    if len(dst.shape) == 3:

        def each(i, carry):
            total = srcs[0][i].astype(f32)
            for src in srcs[1:]:
                total = total + src[i].astype(f32)
            dst[i] = total.astype(dst.dtype)
            return carry

        lax.fori_loop(0, dst.shape[0], each, 0)
        return
    rows = dst.shape[0]
    step = 48 if rows % 48 == 0 else 32

    def body(i, carry):
        cut = pl.ds(pl.multiple_of(i * step, step), step)
        total = srcs[0][cut, :].astype(f32)
        for src in srcs[1:]:
            total = total + src[cut, :].astype(f32)
        dst[cut, :] = total.astype(dst.dtype)
        return carry

    lax.fori_loop(0, rows // step, body, 0)


class Events:
    def __init__(self):
        self.items = []

    def add(self, time, action):
        self.items.append((time, len(self.items), action))

    def take(self, until):
        due = sorted([item for item in self.items if item[0] <= until], key=lambda item: item[:2])
        self.items = [item for item in self.items if item[0] > until]
        return [action for _, _, action in due]

    def run(self, until=math.inf):
        for action in self.take(until):
            action()


class Plan:
    def __init__(self, events):
        self.events, self.heap, self.free, self.count = events, [], {}, 0

    def at(self, time, action):
        heapq.heappush(self.heap, (time, self.count, action))
        self.count += 1

    def do(self, time, action):
        self.events.add(time, action)

    def send(self, link, time, length, then):
        def start(now):
            begin = max(now, self.free.get(link, 0.0))
            self.free[link] = begin + length
            self.at(begin + length + 2.0, then)

        self.at(time, start)

    def run(self):
        while self.heap:
            time, _, action = heapq.heappop(self.heap)
            action(time)


def group_scratch(lines, pairs, rows, columns, lines_first=False):
    block = (rows, columns)
    return [
        pltpu.VMEM((2 * lines, pairs) + block, bf16),
        pltpu.VMEM((2 * lines, pairs) + block, bf16),
        pltpu.VMEM((2 * lines, max(pairs - 1, 1)) + block, bf16),
        pltpu.VMEM((2 * lines,) + block, bf16),
        pltpu.VMEM((2, pairs if lines_first else lines - 1) + block, bf16),
        pltpu.VMEM((2,) + block, bf16),
        pltpu.VMEM((2,) + block, bf16),
        pltpu.VMEM((2,) + block, bf16),
    ]


GROUP_SCRATCH = 8
BACK_GROUPS = 6
LINES_FIRST = (True, False, True, True, False, False)
ROWS_DELAY = (10.0, 20.0)


def reduce_group(here, copies, plan, chunks, scratch, place, unit, core_times, lines_first=False):
    from_core, own, from_pairs, paired, from_lines, lined, from_parts, parted = scratch
    lines, pairs = here.lines, here.pairs
    line, pair, core, part = here.line, here.pair, here.core, here.part
    low_part = part % 2
    state = {}

    def to_core(i, view):
        state["core", i] = copies.send(lambda: (view(), from_core.at[i], here.core_peer))

    def begin(i):
        to_core(i, lambda: chunks[i](1 - core))
        state["own", i] = copies.load(lambda: (chunks[i](core), own.at[i]))

    def over_core(i):
        if ("own", i) in state:
            state["own", i].wait()
        state["core", i].wait_recv()
        for p in range(pairs):
            add_blocks(own.at[i, p], own.at[i, p], from_core.at[i, p])
        if lines_first:
            return
        state["pair", i] = [
            copies.send(
                lambda flip=flip: (
                    own.at[i, pair ^ flip],
                    from_pairs.at[i, flip - 1],
                    here.pair_peer(flip),
                )
            )
            for flip in range(1, pairs)
        ]

    def over_pairs(i):
        for copy in state["pair", i]:
            copy.wait_recv()
        add_blocks(
            paired.at[i], own.at[i, pair], *[from_pairs.at[i, flip - 1] for flip in range(1, pairs)]
        )

    def to_lines(h):
        state["line", h] = [
            copies.send(
                lambda flip=flip: (
                    paired.at[h * lines + (line ^ flip)],
                    from_lines.at[h, flip - 1],
                    here.line_peer(flip),
                )
            )
            for flip in range(1, lines)
        ]

    def over_lines(h):
        for copy in state["line", h]:
            copy.wait_recv()
        add_blocks(
            lined.at[h],
            paired.at[h * lines + line],
            *[from_lines.at[h, flip - 1] for flip in range(1, lines)],
        )

    def both_to_lines(h):
        state["line", h] = copies.send(
            lambda: (own.at[h * lines + (line ^ 1)], from_lines.at[h], here.line_peer(1))
        )

    def both_over_lines(h):
        state["line", h].wait_recv()
        for p in range(pairs):
            add_blocks(
                paired.at[h * pairs + p], own.at[h * lines + line, p], from_lines.at[h, p]
            )
        state["pair", h] = copies.send(
            lambda: (
                paired.at[h * pairs + (pair ^ 1)],
                from_pairs.at[h, 0],
                here.pair_peer(1),
            )
        )

    def last_over_pairs(h):
        state["pair", h].wait_recv()
        add_blocks(lined.at[h], paired.at[h * pairs + pair], from_pairs.at[h, 0])

    def to_part_one():
        state["one"] = copies.send(
            lambda: (lined.at[1 - low_part], from_parts.at[0], here.part_peer(1))
        )

    def over_part_one():
        state["one"].wait_recv()
        add_blocks(parted.at[0], lined.at[low_part], from_parts.at[0])
        state["two"] = copies.send(lambda: (parted.at[0], from_parts.at[1], here.part_peer(2)))

    def mine():
        return place(low_part, line)

    def other():
        return place(1 - low_part, line)

    def over_part_two():
        state["two"].wait_recv()
        add_blocks(parted.at[1], parted.at[0], from_parts.at[1])
        state["back"] = copies.send(lambda: (parted.at[1], mine(), here.part_peer(1)))
        state["place"] = copies.load(lambda: (parted.at[1], mine()))
        state["spread"] = [
            copies.send(lambda flip=flip: (parted.at[1], mine(), here.line_peer(flip)))
            for flip in range(1, lines)
        ]

    def spread_other():
        state["back"].wait_recv()
        state["spread"] += [
            copies.send(lambda flip=flip: (other(), other(), here.line_peer(flip)))
            for flip in range(1, lines)
        ]

    def end():
        state["place"].wait()
        for copy in state["spread"]:
            copy.wait_recv()

    lined_h = []

    def core_done(i, now):
        plan.do(now, functools.partial(over_core, i))
        if lines_first:
            if i % lines == lines - 1:
                h = i // lines
                plan.do(now + 0.01, functools.partial(both_to_lines, h))
                plan.send("y", now + 0.7, pairs * unit, functools.partial(both_lined, h))
            return
        plan.send("x", now + 0.7, (pairs - 1) * unit, functools.partial(pairs_done, i))

    def pairs_done(i, now):
        plan.do(now, functools.partial(over_pairs, i))
        if i % lines == lines - 1:
            h = i // lines
            plan.do(now + 0.01, functools.partial(to_lines, h))
            plan.send("y", now + 0.3, (lines - 1) * unit, functools.partial(lines_done, h))

    def both_lined(h, now):
        plan.do(now, functools.partial(both_over_lines, h))
        plan.send("x", now + 0.7, unit, functools.partial(last_paired, h))

    def last_paired(h, now):
        plan.do(now, functools.partial(last_over_pairs, h))
        all_lined(h, now)

    def lines_done(h, now):
        plan.do(now, functools.partial(over_lines, h))
        all_lined(h, now)

    def all_lined(h, now):
        lined_h.append(h)
        if len(lined_h) == 2:
            plan.do(now + 0.01, to_part_one)
            plan.send("z", now + 0.3, unit, one_done)

    def one_done(now):
        plan.do(now, over_part_one)
        plan.send("z", now + 0.3, 2 * unit, two_done)

    def two_done(now):
        plan.do(now, over_part_two)
        plan.send("z", now + 0.3, unit, back_done)
        plan.send("y", now + 0.3, (lines - 1) * unit, lambda now: None)

    def back_done(now):
        plan.do(now, spread_other)
        plan.send("y", now + 0.1, (lines - 1) * unit, lambda now: None)

    for i in range(2 * lines):
        if chunks[i] is not None:
            plan.do(core_times[i - 2] + 0.01 if i >= 2 else -100.0, functools.partial(begin, i))
        plan.at(core_times[i], functools.partial(core_done, i))
    plan.do(10000.0, end)
    return to_core


def chunk_views(refs, kinds, width):
    views = []
    for ref, kind in zip(refs, kinds):
        if kind == "wide":
            for c in range(ref.shape[3] // width):
                views.append(
                    lambda core, ref=ref, cut=slice(c * width, (c + 1) * width): ref.at[
                        :, core, :, cut
                    ]
                )
        else:
            for b in range(ref.shape[2]):
                for c in range(ref.shape[4] // width):
                    views.append(
                        lambda core, ref=ref, b=b, cut=slice(c * width, (c + 1) * width): ref.at[
                            :, core, b, :, cut
                        ]
                    )
    return views


def finish_kernel(ctx_size, w_size, kinds, tables, *refs):
    here = Wires(ctx_size, w_size)
    lines, pairs = here.lines, here.pairs
    part, line, pair, core = here.part, here.line, here.pair, here.core
    terms = refs[: len(kinds)]
    through, near, final, table = refs[len(kinds) : len(kinds) + 4]
    at = len(kinds) + 4
    out, final_out, grad_out, table_out = refs[at : at + 4]
    at += 4
    groups = (len(refs) - at - 8) // GROUP_SCRATCH
    scratches = [
        refs[at + g * GROUP_SCRATCH : at + (g + 1) * GROUP_SCRATCH] for g in range(groups)
    ]
    at += groups * GROUP_SCRATCH
    g_core, g_own, g_line, g_near, g_sum, table_in, table_sum = refs[at : at + 7]
    copies = Copies(*refs[at + 7])
    micro = part // 2

    def back_target(turn):
        return here.at(2 * core + (micro + turn) % 2, line, pair, part % 2)

    def back_source(turn):
        return here.at(2 * ((turn + part) % 2) + core, line, pair, part // 2)

    stays = [
        jnp.logical_and(2 * core + (micro + turn) % 2 == part, part % 2 == core)
        for turn in range(2)
    ]
    barrier = pltpu.get_barrier_semaphore()

    def greet(device):
        pl.semaphore_signal(barrier, inc=1, device_id=device, device_id_type=MESH)

    peers = [here.core_peer, here.part_peer(1), here.part_peer(2)]
    peers += [here.line_peer(flip) for flip in range(1, lines)]
    peers += [here.pair_peer(flip) for flip in range(1, pairs)]
    for device in peers:
        greet(device)
    for turn in range(2):

        @pl.when(jnp.logical_not(stays[turn]))
        def _(turn=turn):
            greet(back_target(turn))
            greet(back_source(turn))

    staying = sum(stay.astype(jnp.int32) for stay in stays)
    pl.semaphore_wait(barrier, len(peers) + 4 - 2 * staying)

    events = Events()
    state = {}
    count = 2 * lines

    def begin_rows():
        state["core"] = [
            copies.send(lambda j=j: (through.at[count + j], g_core.at[j], here.core_peer))
            for j in range(count)
        ]
        state["own"] = [
            copies.load(lambda j=j: (through.at[j], g_own.at[j])) for j in range(count)
        ]
        state["near"] = copies.load(lambda: (near, g_near))
        state["out"] = [
            copies.send(
                lambda turn=turn: (final.at[turn], final_out.at[micro], back_target(turn)),
                stays[turn],
            )
            for turn in range(2)
        ]

    def rows_over_core():
        for j in reversed(range(count)):
            state["own"][j].wait()
            state["core"][j].wait_recv()
            add_blocks(g_own.at[j], g_own.at[j], g_core.at[j])
            if j >= 2:
                state["line", j] = copies.send(
                    lambda j=j: (g_own.at[j], g_line.at[j - 2], here.line_peer(j // 2))
                )

    def rows_over_lines():
        state["near"].wait()
        state["back"] = []
        for turn in range(2):
            others = []
            for flip in range(1, lines):
                state["line", 2 * flip + turn].wait_recv()
                others.append(g_line.at[2 * flip + turn - 2])
            add_blocks(g_sum.at[turn], g_near.at[turn], g_own.at[turn], *others)
            state["back"].append(
                copies.send(
                    lambda turn=turn: (g_sum.at[turn], grad_out.at[micro], back_target(turn)),
                    stays[turn],
                )
            )

    def end_rows():
        for copy in state["out"] + state["back"]:
            copy.wait_recv()

    steps = [here.core_peer]
    steps += [here.pair_peer(flip) for flip in bits(pairs)]
    steps += [here.line_peer(flip) for flip in bits(lines)]
    steps += [here.part_peer(flip) for flip in bits(4)]

    def table_send(n):
        src = table if n == 0 else table_sum.at[n - 1]
        state["table", n] = copies.send(lambda: (src, table_in.at[n], steps[n]))

    def table_step(n):
        state["table", n].wait_recv()
        before = table[...] if n == 0 else table_sum[n - 1]
        total = before + table_in[n]
        if n + 1 < len(steps):
            table_sum[n] = total
            table_send(n + 1)
        else:
            table_out[...] = total

    plan = Plan(events)
    events.add(-1001.0, begin_rows)
    events.add(-1000.5, lambda: table_send(0))
    events.add(0.5, rows_over_core)
    events.add(17.0, rows_over_lines)
    events.add(9000.0, end_rows)
    for n in range(len(steps)):
        events.add(2.5 + n * 6.0, functools.partial(table_step, n))
    views = chunk_views(terms, kinds, out.shape[2])
    size = 2 * lines
    for g in range(groups):
        reduce_group(
            here,
            copies,
            plan,
            views[g * size : (g + 1) * size],
            scratches[g],
            lambda h, line, g=g: out.at[g * size + h * lines + line],
            6.0,
            [2.0 + 1.5 * (g * size + i) for i in range(size)],
        )
    plan.run()
    events.run()
    copies.finish()


def finish_all(ctx_size, w_size, terms, kinds, through, near, final, table):
    lines, pairs = ctx_size // 4, w_size // 2
    count = 2 * lines
    tok, width = through.shape[1:]
    rows = width // w_size
    columns = width // (lines // 2)
    chunks = sum(term.size for term in terms) // (w_size * rows * columns)
    groups = chunks // (2 * lines)
    table_steps = 1 + len(bits(pairs)) + len(bits(lines)) + len(bits(4))
    block = (tok, width)
    any_space = pl.BlockSpec(memory_space=pl.ANY)
    in_vmem = pl.BlockSpec(memory_space=pltpu.VMEM)
    sems = 40 + 10 * lines + groups * 2 * lines * (6 + pairs)
    scratch = []
    for _ in range(groups):
        scratch += group_scratch(lines, pairs, rows, columns)
    scratch += [
        pltpu.VMEM((count,) + block, bf16),
        pltpu.VMEM((count,) + block, bf16),
        pltpu.VMEM((max(count - 2, 1),) + block, bf16),
        pltpu.VMEM((2,) + block, f32),
        pltpu.VMEM((2,) + block, bf16),
        pltpu.VMEM((table_steps,) + table.shape, f32),
        pltpu.VMEM((table_steps,) + table.shape, f32),
        (
            pltpu.SemaphoreType.DMA((sems,)),
            pltpu.SemaphoreType.DMA((sems,)),
            pltpu.SemaphoreType.DMA((sems,)),
        ),
    ]
    return pl.pallas_call(
        functools.partial(finish_kernel, ctx_size, w_size, kinds, table_steps),
        in_specs=[any_space] * (len(terms) + 3) + [in_vmem],
        out_specs=[any_space, any_space, any_space, in_vmem],
        out_shape=[
            jax.ShapeDtypeStruct((chunks, rows, columns), bf16),
            jax.ShapeDtypeStruct((2,) + block, bf16),
            jax.ShapeDtypeStruct((2,) + block, bf16),
            jax.ShapeDtypeStruct(table.shape, f32),
        ],
        scratch_shapes=scratch,
        compiler_params=pltpu.CompilerParams(
            collective_id=1, has_side_effects=True, vmem_limit_bytes=60 << 20
        ),
        name="finish_all",
    )(*terms, through, near, final, table)


def greet_all(here, back_target, back_source, stays):
    lines, pairs = here.lines, here.pairs
    barrier = pltpu.get_barrier_semaphore()

    def greet(device):
        pl.semaphore_signal(barrier, inc=1, device_id=device, device_id_type=MESH)

    peers = [here.core_peer, here.part_peer(1), here.part_peer(2)]
    peers += [here.line_peer(flip) for flip in range(1, lines)]
    peers += [here.pair_peer(flip) for flip in range(1, pairs)]
    for device in peers:
        greet(device)
    for turn in range(2):

        @pl.when(jnp.logical_not(stays[turn]))
        def _(turn=turn):
            greet(back_target(turn))
            greet(back_source(turn))

    staying = sum(stay.astype(jnp.int32) for stay in stays)
    pl.semaphore_wait(barrier, len(peers) + 4 - 2 * staying)


def back_kernel(ctx_size, w_size, *refs):
    here = Wires(ctx_size, w_size)
    lines, pairs = here.lines, here.pairs
    part, line, pair, core = here.part, here.line, here.pair, here.core
    micro = part // 2
    (
        named,
        table,
        queries,
        d_context,
        d_sum,
        probs,
        kv,
        rows_all,
        full_kv,
        full_query,
        final,
        term_up,
        term_down,
        term_out,
    ) = refs[:14]
    up_out, down_out, oq_out, kv_out, final_out, grad_out, table_out = refs[14:21]
    scratches = [
        refs[21 + g * GROUP_SCRATCH : 21 + (g + 1) * GROUP_SCRATCH] for g in range(BACK_GROUPS)
    ]
    (
        kv_buf,
        slots,
        cat,
        probs_buf,
        q_buf,
        dctx_buf,
        rows_buf,
        wq_buf,
        q_other,
        kv_other,
        g_near,
        g_core,
        g_line,
        g_sum,
        acc,
        value_sums,
        table_in,
        table_sum,
        probs_sem,
        sems,
    ) = refs[21 + BACK_GROUPS * GROUP_SCRATCH :]
    copies = Copies(*sems)
    own_tokens, width = q_buf.shape
    key_blocks = kv_buf.shape[0]
    tokens = key_blocks * BLOCK
    blocks = own_tokens // BLOCK
    piece = blocks // 2
    groups = width // LANES
    keys = CANDS * BLOCK
    shard = width // w_size
    half = width // 2

    def back_target(turn):
        return here.at(2 * core + (micro + turn) % 2, line, pair, part % 2)

    def back_source(turn):
        return here.at(2 * ((turn + part) % 2) + core, line, pair, part // 2)

    stays = [
        jnp.logical_and(2 * core + (micro + turn) % 2 == part, part % 2 == core)
        for turn in range(2)
    ]

    def fetch(i, slot):
        return pltpu.make_async_copy(probs.at[i], probs_buf.at[slot], probs_sem.at[slot])

    greet_all(here, back_target, back_source, stays)

    events = Events()
    state = {}
    count = 2 * lines

    w_kv = slots.at[pl.ds(0, width // BLOCK)]
    rows_from = 16
    all_rows = slots.at[pl.ds(rows_from, key_blocks), :, pl.ds(0, width)]
    through_from = rows_from + key_blocks

    def through_other(j):
        return slots.at[pl.ds(through_from + j * piece, piece), :, pl.ds(0, width)]

    def through_own(j):
        return slots.at[pl.ds(through_from + j * piece, piece), :, pl.ds(width, width)]

    def send_out():
        state["out"] = [
            copies.send(
                lambda turn=turn: (final.at[turn], final_out.at[micro], back_target(turn)),
                stays[turn],
            )
            for turn in range(2)
        ]

    def rows_over_core(turn):
        for j in reversed(range(turn, count, 2)):
            state["through", j].wait_recv()
            add_blocks(through_own(j), through_own(j), g_core.at[j])
            if j >= 2:
                state["line", j] = copies.send(
                    lambda j=j: (through_own(j), g_line.at[j - 2], here.line_peer(j // 2))
                )

    def rows_over_lines(turn):
        others = []
        for flip in range(1, lines):
            state["line", 2 * flip + turn].wait_recv()
            others.append(g_line.at[2 * flip + turn - 2])
        add_blocks(
            g_sum.at[turn], g_near.at[pl.ds(turn * piece, piece)], through_own(turn), *others
        )
        state["back", turn] = copies.send(
            lambda: (g_sum.at[turn], grad_out.at[micro], back_target(turn)), stays[turn]
        )

    def end_rows():
        for copy in state["out"] + [state["back", turn] for turn in range(2)]:
            copy.wait_recv()

    steps = [lambda: here.core_peer]
    steps += [lambda flip=flip: here.pair_peer(flip) for flip in bits(pairs)]
    steps += [lambda flip=flip: here.line_peer(flip) for flip in bits(lines)]
    steps += [lambda flip=flip: here.part_peer(flip) for flip in bits(4)]

    def table_send(n):
        state["table", n] = copies.send(lambda: (table_sum.at[n], table_in.at[n], steps[n]()))

    def table_step(n):
        state["table", n].wait_recv()
        total = table_sum[n] + table_in[n]
        if n + 1 < len(steps):
            table_sum[n + 1] = total
            table_send(n + 1)
        else:
            table_out[...] = total

    attend_at, attend_step = 9.0, 2.6
    gather_at = attend_at + blocks * attend_step + 3.0
    gather_step = 1.4
    through_at = gather_at + 8 * gather_step + 1.0
    through_step = 1.3
    terms_at = through_at + 8 * through_step
    terms_step = 2.6
    terms_end = terms_at + 4 * terms_step
    plan = Plan(events)
    plan.send("z", 0.0, 18.0, lambda now: None)

    views = chunk_views((term_up, term_down), ("wide", "tall"), half)
    size = 2 * lines
    ffn_groups = BACK_GROUPS - 2

    def half_columns(number):
        return pl.ds(pl.multiple_of(number * half, 128), half)

    def up_place(g):
        return lambda h, line: up_out.at[:, half_columns(g * size + h * lines + line)]

    def down_place(g):
        return lambda h, line: down_out.at[
            pl.ds(pl.multiple_of((2 * g + h) * shard, 16), shard), half_columns(line)
        ]

    places = [up_place(g) for g in range(ffn_groups // 2)]
    places += [down_place(g) for g in range(ffn_groups // 2)]
    for g in range(ffn_groups):
        order = [g * size + i for i in range(size)]
        reduce_group(
            here,
            copies,
            plan,
            views[g * size : (g + 1) * size],
            scratches[g],
            places[g],
            3.0,
            [max(2.5 + 0.7 * n, 3.0 * n - 12.0) for n in order],
            LINES_FIRST[g],
        )
    out_views = [
        lambda side, cut=slice(c * half, (c + 1) * half): term_out.at[:, side, :, cut]
        for c in range(2)
    ]
    q_own = scratches[ffn_groups][1]
    q_to_core = reduce_group(
        here,
        copies,
        plan,
        out_views + [None, None],
        scratches[ffn_groups],
        lambda h, line: oq_out.at[h, :, half_columns(line)],
        3.0,
        [gather_at + 2.0 + 1.5 * i for i in range(4)],
        LINES_FIRST[ffn_groups],
    )
    kv_own = scratches[ffn_groups + 1][1]
    kv_to_core = reduce_group(
        here,
        copies,
        plan,
        [None] * 4,
        scratches[ffn_groups + 1],
        lambda h, line: kv_out.at[h, :, half_columns(line)],
        3.0,
        [terms_at + (i + 1) * terms_step + 1.5 for i in range(4)],
        LINES_FIRST[ffn_groups + 1],
    )
    plan.do(-200.0, send_out)
    rows_at = through_at + 2 * count * through_step + 0.5

    def rows_done(turn, now):
        plan.do(now, functools.partial(rows_over_lines, turn))
        plan.send("z", now + 0.7, 9.0, lambda now: None)

    for turn in range(2):
        rows_time = rows_at + ROWS_DELAY[turn]
        plan.do(rows_time, functools.partial(rows_over_core, turn))
        plan.send("y", rows_time + 0.7, 9.0, functools.partial(rows_done, turn))
    plan.do(9000.0, end_rows)
    for n in range(len(steps)):
        plan.do(through_at + 3.0 + n * 5.0, functools.partial(table_step, n))
    plan.run()

    def stepped(number, at, each, body):
        def loop(step, carry):
            body(step)
            for n in range(number):
                due = events.take(at + (n + 1) * each)
                if due:

                    @pl.when(step == n)
                    def _(due=due):
                        for action in due:
                            action()

            return carry

        lax.fori_loop(0, number, loop, 0)

    events.run(0.0)
    first = [
        copies.load(lambda: (kv, kv_buf)),
        copies.load(lambda: (queries, q_buf)),
        copies.load(lambda: (d_context, dctx_buf)),
    ]
    later = [
        copies.load(lambda: (rows_all.at[pl.ds(0, blocks)], rows_buf)),
        copies.load(lambda: (full_query, wq_buf)),
        copies.load(lambda: (d_sum, g_near)),
    ]

    fetch(0, 0).start()
    events.run(attend_at)
    for copy in first:
        copy.wait()
    slots[blocks * CANDS] = jnp.zeros((BLOCK, 2 * width), bf16)

    head_of_lane = lax.broadcasted_iota(jnp.int32, (BLOCK, LANES), 1) // HEAD_DIM

    def attend_block(i):
        slot = i % 2
        fetch(i, slot).wait()

        @pl.when(i + 1 < blocks)
        def _():
            fetch(i + 1, 1 - slot).start()

        for j in range(CANDS):
            place = named[i // piece, 0, (i % piece) * CANDS + j]
            cat[j * BLOCK : (j + 1) * BLOCK, :] = kv_buf[place]
        mine = pl.ds(pl.multiple_of(i * BLOCK, BLOCK), BLOCK)
        rows = pl.ds(i * CANDS, CANDS)
        by_slot = (CANDS, BLOCK, LANES)
        for g in range(groups):
            lanes = slice(g * LANES, (g + 1) * LANES)
            v_lanes = slice(width + g * LANES, width + (g + 1) * LANES)
            q_all = spread_heads(q_buf[mine, lanes], head_of_lane)
            d_all = spread_heads(dctx_buf[mine, lanes], head_of_lane)
            probs_low = probs_buf[slot, g]
            shares = probs_low.astype(f32)
            d_probs = dot_nt(d_all, cat[:, v_lanes])
            row_inner = jnp.sum(shares * d_probs, axis=-1, keepdims=True)
            d_scores = (shares * (d_probs - row_inner)).astype(bf16)
            slots[rows, :, lanes] = dot_tn(d_scores, q_all).astype(bf16).reshape(by_slot)
            slots[rows, :, v_lanes] = dot_tn(probs_low, d_all).astype(bf16).reshape(by_slot)
            q_buf[mine, lanes] = pick_heads(dot_nn(d_scores, cat[:, lanes]), head_of_lane).astype(
                bf16
            )

    stepped(blocks, attend_at, attend_step, attend_block)

    for copy in later:
        copy.wait()
    for c in range(2):
        columns = slice(c * half, (c + 1) * half)
        own_rows = rows_buf[...].reshape(own_tokens, width)
        acc[...] = dot_tn(own_rows, q_buf[:, columns]) * score_scale
        for p in range(pairs):
            for side, place in ((core, q_own.at[2 + c, p]), (1 - core, q_other.at[c, p])):
                start = pl.multiple_of((2 * p + side) * shard, shard)
                place[...] = acc[pl.ds(start, shard), :].astype(bf16)
        q_to_core(2 + c, lambda c=c: q_other.at[c])

    def near_step(step, carry):
        cut = pl.ds(pl.multiple_of(step * BLOCK * 2, BLOCK * 2), BLOCK * 2)
        near = dot_nt(q_buf[cut, :], wq_buf[...]) * score_scale
        g_near[pl.ds(step * 2, 2)] += near.reshape(2, BLOCK, width)
        return carry

    lax.fori_loop(0, own_tokens // (BLOCK * 2), near_step, 0)
    value_sums[...] = jnp.zeros_like(value_sums)

    sub = value_sums.shape[0]

    def gather_some(step):
        def one(n, carry):
            block = step * (key_blocks // 8) + n

            users = [named[i // piece, 1, block * piece + i % piece] for i in range(blocks)]
            for r in range(BLOCK // sub):
                cut = slice(r * sub, (r + 1) * sub)
                total = jnp.zeros((sub, 2 * width), f32)
                for i in range(blocks):
                    total = total + slots[users[i], cut, :].astype(f32)
                kv_buf[block, cut, :] = total.astype(bf16)
                value_sums[...] += total[:, width:]
            return carry

        lax.fori_loop(0, key_blocks // 8, one, 0)

    stepped(8, gather_at, gather_step, gather_some)
    weights = copies.load(lambda: (full_kv, w_kv))
    every = copies.load(lambda: (rows_all, all_rows))
    table_sum[0] = jnp.zeros(table_sum.shape[1:], f32)
    table_sum[0, pl.ds(0, w_size), :] = table[...]
    table_sum[0, pl.ds(w_size, 1), pl.ds(0, width)] = score_scale * jnp.sum(
        q_buf[...].astype(f32), axis=0, keepdims=True
    )
    table_sum[0, pl.ds(w_size + 1, 1), pl.ds(0, width)] = jnp.sum(
        value_sums[...], axis=0, keepdims=True
    )
    table_send(0)
    weights.wait()

    def through_tile(j, left, step):
        given = kv_buf[pl.ds(j * piece, piece)].reshape(piece * BLOCK, 2 * width)
        weight = slots[pl.ds(0, width // BLOCK)].reshape(width, 2 * width)
        tile = dot_nt(given, weight).astype(bf16).reshape(piece, BLOCK, width)
        slots[pl.ds(through_from + step * piece, piece), :, pl.ds(left, width)] = tile

    def other_tile(step):
        through_tile(count + step, 0, step)
        for n in range(count):

            @pl.when(step == n)
            def _(n=n):
                state["through", n] = copies.send(
                    lambda: (through_other(n), g_core.at[n], here.core_peer)
                )

    def own_tile(step):
        through_tile(step, width, step)

    stepped(count, through_at, through_step, other_tile)
    stepped(count, through_at + count * through_step, through_step, own_tile)
    every.wait()

    def kv_terms(c):
        columns = pl.ds(pl.multiple_of(c * half, 128), half)
        acc[...] = jnp.zeros_like(acc)

        def deep(t, carry):
            rows = slots[pl.ds(rows_from + t * blocks, blocks), :, 0:width]
            given = kv_buf[pl.ds(t * blocks, blocks), :, columns]
            acc[...] += dot_tn(
                rows.reshape(own_tokens, width), given.reshape(own_tokens, half)
            )
            return carry

        lax.fori_loop(0, tokens // own_tokens, deep, 0)
        for p in range(pairs):
            for side, place in ((core, kv_own.at[c, p]), (1 - core, kv_other.at[c, p])):
                start = pl.multiple_of((2 * p + side) * shard, shard)
                place[...] = acc[pl.ds(start, shard), :].astype(bf16)
        for n in range(4):

            @pl.when(c == n)
            def _(n=n):
                kv_to_core(n, lambda: kv_other.at[n])

    stepped(4, terms_at, terms_step, kv_terms)
    events.run()
    copies.finish()


def back_all(ctx_size, w_size, small, large, shapes):
    width, tok, tokens, table_shape = shapes
    lines, pairs = ctx_size // 4, w_size // 2
    rows = width // w_size
    own_tokens = 2 * tok
    blocks = own_tokens // BLOCK
    keys = CANDS * BLOCK
    half = width // 2
    table_steps = 1 + len(bits(pairs)) + len(bits(lines)) + len(bits(4))
    any_space = pl.BlockSpec(memory_space=pl.ANY)
    in_vmem = pl.BlockSpec(memory_space=pltpu.VMEM)
    in_smem = pl.BlockSpec(memory_space=pltpu.SMEM)
    scratch = []
    for lines_first in LINES_FIRST:
        scratch += group_scratch(lines, pairs, rows, half, lines_first)
    piece = (tok // BLOCK, BLOCK, width)
    scratch += [
        pltpu.VMEM((tokens // BLOCK, BLOCK, 2 * width), bf16),
        pltpu.VMEM((blocks * CANDS + 1, BLOCK, 2 * width), bf16),
        pltpu.VMEM((keys, 2 * width), bf16),
        pltpu.VMEM((2, width // LANES, GROUP * BLOCK, keys), bf16),
        pltpu.VMEM((own_tokens, width), bf16),
        pltpu.VMEM((own_tokens, width), bf16),
        pltpu.VMEM((blocks, BLOCK, width), bf16),
        pltpu.VMEM((width, width), bf16),
        pltpu.VMEM((2, pairs, rows, half), bf16),
        pltpu.VMEM((4, pairs, rows, half), bf16),
        pltpu.VMEM((blocks, BLOCK, width), f32),
        pltpu.VMEM((2 * lines,) + piece, bf16),
        pltpu.VMEM((2 * lines - 2,) + piece, bf16),
        pltpu.VMEM((2,) + piece, bf16),
        pltpu.VMEM((width, half), f32),
        pltpu.VMEM((16, width), f32),
        pltpu.VMEM((table_steps,) + table_shape, f32),
        pltpu.VMEM((table_steps,) + table_shape, f32),
        pltpu.SemaphoreType.DMA((2,)),
        (
            pltpu.SemaphoreType.DMA((60,)),
            pltpu.SemaphoreType.DMA((160,)),
            pltpu.SemaphoreType.DMA((160,)),
        ),
    ]
    return pl.pallas_call(
        functools.partial(back_kernel, ctx_size, w_size),
        in_specs=[in_smem, in_vmem] + [any_space] * len(large),
        out_specs=[any_space] * 6 + [in_vmem],
        out_shape=[
            jax.ShapeDtypeStruct((rows, 4 * width), bf16),
            jax.ShapeDtypeStruct((4 * rows, width), bf16),
            jax.ShapeDtypeStruct((2, rows, width), bf16),
            jax.ShapeDtypeStruct((2, rows, width), bf16),
            jax.ShapeDtypeStruct((2,) + piece, bf16),
            jax.ShapeDtypeStruct((2,) + piece, bf16),
            jax.ShapeDtypeStruct(table_shape, f32),
        ],
        scratch_shapes=scratch,
        compiler_params=pltpu.CompilerParams(
            collective_id=1, has_side_effects=True, vmem_limit_bytes=67043328
        ),
        name="back_all",
    )(*small, *large)


def prepare_kernel(ctx_size, w_size, lengths, picks, ints, bias):
    here = Wires(ctx_size, w_size)
    lines = here.lines
    micros, _, chunk_blocks, randoms = picks.shape
    slots = 2 * chunk_blocks * CANDS
    head = lax.broadcasted_iota(jnp.int32, (1, CANDS * BLOCK), 1) // BLOCK
    key_blocks = ctx_size * chunk_blocks
    one, nothing = jnp.int32(1), jnp.int32(0)

    for m in range(micros):

        def clear(n, carry):
            for k in range(32):
                ints[m, 1, n * 32 + k] = jnp.int32(slots)
            return carry

        lax.fori_loop(0, key_blocks * chunk_blocks // 32, clear, 0)
        turn = lax.rem(m + here.part, 2)
        for b in range(chunk_blocks):
            block = here.ctx * chunk_blocks + b
            begin, first, length = nothing, nothing, one
            for d in range(lengths.shape[2]):
                size = lengths[m, 0, d]
                end = begin + size
                inside = jnp.logical_and(block >= begin, block < end)
                first = jnp.where(inside, begin, first)
                length = jnp.where(inside, size, length)
                begin = end
            chosen = [block, block - 1, block + 1, first, first + 1]
            for r in range(randoms):
                chosen.append(first + lax.rem(picks[m, 0, b, r], length))
            row = jnp.zeros(head.shape, f32)
            for j, candidate in enumerate(chosen):
                allowed = jnp.logical_and(candidate >= first, candidate < first + length)
                for earlier in chosen[:j]:
                    allowed = jnp.logical_and(allowed, candidate != earlier)
                safe = jnp.where(allowed, candidate, block)
                chunk = lax.div(safe, chunk_blocks)
                chunk_part, chunk_line = lax.div(chunk, lines), lax.rem(chunk, lines)
                low, high = lax.rem(chunk_part, 2), lax.div(chunk_part, 2)
                place = (high ^ lax.div(here.part, 2)) * lines + (chunk_line ^ here.line)
                place = (place * 2 + lax.rem(low + m, 2)) * chunk_blocks
                place = place + lax.rem(safe, chunk_blocks)
                ints[m, 0, b * CANDS + j] = place

                @pl.when(allowed)
                def _(place=place, b=b, j=j):
                    ints[m, 1, place * chunk_blocks + b] = (turn * chunk_blocks + b) * CANDS + j

                score = jnp.where(allowed, 0.0, masked_score).astype(f32)
                row = jnp.where(head == j, score, row)
            bias[m, b] = row


def prepare(ctx_size, w_size, lengths, picks):
    micros, _, chunk_blocks, _ = picks.shape
    return pl.pallas_call(
        functools.partial(prepare_kernel, ctx_size, w_size),
        in_specs=[pl.BlockSpec(memory_space=pltpu.SMEM)] * 2,
        out_specs=[pl.BlockSpec(memory_space=pltpu.SMEM), pl.BlockSpec(memory_space=pltpu.VMEM)],
        out_shape=[
            jax.ShapeDtypeStruct((micros, 8, 128), jnp.int32),
            jax.ShapeDtypeStruct((micros, chunk_blocks, 1, CANDS * BLOCK), f32),
        ],
        name="prepare",
    )(lengths, picks)


def front_kernel(ctx_size, w_size, *refs):
    here = Wires(ctx_size, w_size)
    lines, pairs = here.lines, here.pairs
    part, line, pair, core = here.part, here.line, here.pair, here.core
    (
        hidden,
        out_grad,
        ints,
        bias,
        vectors,
        w_query,
        w_key,
        w_value,
        w_out,
        w_up,
        w_down,
    ) = refs[:11]
    (
        rows_out,
        grads_out,
        ints_out,
        vectors_out,
        query_out,
        kv_weight_out,
        out_out,
        up_out,
        down_out,
        queries_out,
        kv_out,
        context_out,
        probs_out,
        own_out,
    ) = refs[11:25]
    (
        held_up,
        held_down,
        held_out,
        rows_buf,
        wq_buf,
        wkv_buf,
        vectors_buf,
        bias_buf,
        q_buf,
        ctx_buf,
        kv_buf,
        cat,
        probs_buf,
        pos,
        probs_sem,
        sems,
    ) = refs[25:]
    copies = Copies(*sems)
    width = w_query.shape[1]
    tok = rows_buf.shape[1]
    chunk_blocks = tok // BLOCK
    blocks = 2 * chunk_blocks
    groups = width // LANES
    chunks = rows_buf.shape[0]
    me = pair * 2 + core
    side = line % 2

    def target(turn):
        return here.at(2 * ((turn + part) % 2) + core, line, pair, part // 2)

    def source(turn):
        return here.at(2 * core + (part // 2 + turn) % 2, line, pair, part % 2)

    stays = [
        jnp.logical_and(2 * ((turn + part) % 2) + core == part, part // 2 == core)
        for turn in range(2)
    ]
    greet_all(here, target, source, stays)

    def deal(src, dst, turn):
        return copies.send(
            lambda: (src((turn + part) % 2), dst(turn), target(turn)), stays[turn]
        )

    dealt = [deal(lambda m: hidden.at[m, 0], lambda t: rows_buf.at[t], turn) for turn in range(2)]
    dealt_ints = [deal(lambda m: ints.at[m], lambda t: ints_out.at[t], turn) for turn in range(2)]
    dealt_bias = [deal(lambda m: bias.at[m], lambda t: bias_buf.at[t], turn) for turn in range(2)]

    early = [
        (w_key, lambda shard: wkv_buf.at[shard, :, pl.ds(0, width)]),
        (w_value, lambda shard: wkv_buf.at[shard, :, pl.ds(width, width)]),
        (vectors, lambda shard: vectors_buf.at[shard]),
        (w_query, lambda shard: wq_buf.at[shard]),
    ]
    late = [
        (w_up, held_up, lambda shard: up_out.at[shard]),
        (w_down, held_down, lambda shard: down_out.at[shard]),
        (w_out, held_out, lambda shard: out_out.at[shard]),
    ]
    across = [
        copies.send(lambda src=src, place=place: (src, place(me), here.pair_peer(1)))
        for src, place in early
    ]
    ready = [copies.load(lambda src=src, place=place: (src, place(me))) for src, place in early]
    arrive = [
        copies.send(lambda src=src, place=place: (src, place(me), here.core_peer))
        for src, place in early
    ]

    def half_cut(src, which):
        half = src.shape[0] // 2
        return pl.ds(pl.multiple_of(which * half, 16), half)

    halves = [
        copies.send(
            lambda src=src, place=place: (
                src.at[half_cut(src, side)],
                place(me).at[half_cut(src, side)],
                here.pair_peer(1),
            )
        )
        for src, _, place in late[:2]
    ]
    out_across = copies.send(lambda: (w_out, out_out.at[me], here.pair_peer(1)))
    staged = [copies.load(lambda src=src, held=held: (src, held)) for src, held, _ in late]
    ends = [
        copies.send(lambda src=src, place=place: (src, place(me), here.core_peer))
        for src, _, place in late
    ]
    placed = []

    crossed = []
    from_core = {}
    for turn in range(2):
        dealt[turn].wait_recv()
        for flip in range(1, lines):
            crossed.append(
                copies.send(
                    lambda turn=turn, flip=flip: (
                        rows_buf.at[turn],
                        rows_buf.at[flip * 2 + turn],
                        here.line_peer(flip),
                    )
                )
            )
        from_core[turn] = copies.send(
            lambda turn=turn: (rows_buf.at[turn], rows_buf.at[lines * 2 + turn], here.core_peer)
        )
    for turn in range(2):
        dealt_ints[turn].wait_recv()
    pos_ready = copies.load(lambda: (ints_out, pos))
    for copy, (src, held, place) in zip(staged, late):
        copy.wait()
        placed.append(copies.load(lambda held=held, place=place: (held, place(me))))
    theirs = (pair ^ 1) * 2 + core
    for copy, (src, place) in zip(across, early):
        copy.wait_recv()
        arrive.append(
            copies.send(lambda place=place: (place(theirs), place(theirs), here.core_peer))
        )
    for n, copy in enumerate(crossed):
        copy.wait_recv()
        from_core[2 + n] = copies.send(
            lambda n=n: (rows_buf.at[2 + n], rows_buf.at[lines * 2 + 2 + n], here.core_peer)
        )
    gradients = [
        deal(lambda m: out_grad.at[m, 0], lambda t: grads_out.at[t], turn) for turn in range(2)
    ]
    for copy in ready + arrive:
        copy.wait() if copy in ready else copy.wait_recv()
    keep = [
        copies.load(lambda: (wq_buf, query_out)),
        copies.load(lambda: (wkv_buf, kv_weight_out)),
    ]
    relayed = []

    def relay(n):
        halves[n].wait_recv()
        src, _, place = late[n]
        relayed.append(
            copies.send(
                lambda: (
                    place(theirs).at[half_cut(src, side)],
                    place(theirs).at[half_cut(src, side)],
                    here.line_peer(1),
                )
            )
        )
        ends.append(
            copies.send(
                lambda: (
                    place(theirs).at[half_cut(src, side)],
                    place(theirs).at[half_cut(src, side)],
                    here.core_peer,
                )
            )
        )

    def relay_last(n):
        relayed[n].wait_recv()
        src, _, place = late[n]
        ends.append(
            copies.send(
                lambda: (
                    place(theirs).at[half_cut(src, 1 - side)],
                    place(theirs).at[half_cut(src, 1 - side)],
                    here.core_peer,
                )
            )
        )

    def relay_out():
        out_across.wait_recv()
        ends.append(
            copies.send(lambda: (out_out.at[theirs], out_out.at[theirs], here.core_peer))
        )

    vectors_total = vectors_buf[0]
    for w in range(1, w_size):
        vectors_total = vectors_total + vectors_buf[w]
    vectors_out[...] = vectors_total
    kv_bias = jnp.concatenate(
        [jnp.zeros((1, width), f32), vectors_out[pl.ds(1, 1), :]], axis=1
    )
    query_bias = vectors_out[pl.ds(0, 1), :]

    weight = wq_buf[...].reshape(width, width)
    for turn in range(2):
        rows = pl.ds(turn * tok, tok)
        q_buf[rows, :] = (
            (dot_nn(rows_buf[turn], weight) + query_bias) * score_scale
        ).astype(bf16)

    def keys_and_values(step):
        for n in range(lines * 2, chunks):

            @pl.when(step == n)
            def _(n=n):
                from_core[n - lines * 2].wait_recv()

        both = dot_nn(rows_buf[step], wkv_buf[...].reshape(width, 2 * width))
        both = both + kv_bias
        kv_buf[pl.ds(step * chunk_blocks, chunk_blocks)] = both.astype(bf16).reshape(
            chunk_blocks, BLOCK, 2 * width
        )

        return step

    lax.fori_loop(0, chunks, lambda step, carry: (keys_and_values(step), carry)[1], 0)
    keep += [
        copies.load(lambda: (q_buf, queries_out)),
        copies.load(lambda: (kv_buf, kv_out)),
        copies.load(lambda: (rows_buf, rows_out)),
        copies.load(lambda: (rows_buf.at[pl.ds(0, 2)], own_out)),
    ]
    relay(0)
    pos_ready.wait()
    for turn in range(2):
        dealt_bias[turn].wait_recv()
    head_of_lane = lax.broadcasted_iota(jnp.int32, (BLOCK, LANES), 1) // HEAD_DIM

    def put(i, slot):
        return pltpu.make_async_copy(probs_buf.at[slot], probs_out.at[i], probs_sem.at[slot])

    def attend_block(i, carry):
        turn, row, slot = i // chunk_blocks, i % chunk_blocks, i % 2
        for j in range(CANDS):
            cat[j * BLOCK : (j + 1) * BLOCK, :] = kv_buf[pos[turn, 0, row * CANDS + j]]

        @pl.when(i >= 2)
        def _():
            put(i - 2, slot).wait()

        mine = pl.ds(pl.multiple_of(i * BLOCK, BLOCK), BLOCK)
        masked = bias_buf[turn, row]
        for g in range(groups):
            lanes = slice(g * LANES, (g + 1) * LANES)
            v_lanes = slice(width + g * LANES, width + (g + 1) * LANES)
            q_all = spread_heads(q_buf[mine, lanes], head_of_lane)
            scores = dot_nt(q_all, cat[:, lanes]) + masked
            row_max = jnp.max(scores, axis=-1, keepdims=True)
            shifted = jnp.exp(scores - row_max)
            row_total = jnp.sum(shifted, axis=-1, keepdims=True)
            shares = (shifted * (1.0 / row_total)).astype(bf16)
            probs_buf[slot, g] = shares
            mixed = dot_nn(shares, cat[:, v_lanes])
            ctx_buf[mine, lanes] = pick_heads(mixed, head_of_lane).astype(bf16)
        put(i, slot).start()

        @pl.when(i == blocks - 3)
        def _():
            relay(1)

        return carry

    lax.fori_loop(0, blocks, attend_block, 0)
    keep.append(copies.load(lambda: (ctx_buf, context_out)))
    for n in range(2):
        relay_last(n)
        if n == 0:
            relay_out()
    for copy in gradients + ends:
        copy.wait_recv()
    for copy in placed + keep:
        copy.wait()
    for n in range(2):
        put(blocks - 2 + n, n).wait()
    copies.finish()


def front_all(ctx_size, w_size, hidden, out_grad, ints, bias, vectors, weights):
    w_query, w_key, w_value, w_out, w_up, w_down = weights
    lines = ctx_size // 4
    tok, width = hidden.shape[2], hidden.shape[3]
    rows = w_query.shape[0]
    chunks = lines * 4
    blocks = 2 * tok // BLOCK
    keys = CANDS * BLOCK
    groups = width // LANES
    probs_shape = (groups, GROUP * BLOCK, keys)
    key_blocks = chunks * tok // BLOCK
    shapes = [
        ((chunks, tok, width), bf16),
        ((2, tok, width), bf16),
        (ints.shape, ints.dtype),
        (vectors.shape, f32),
        ((w_size, rows, width), bf16),
        ((w_size, rows, 2 * width), bf16),
        ((w_size, rows, width), bf16),
        ((w_size,) + w_up.shape, bf16),
        ((w_size,) + w_down.shape, bf16),
        ((2 * tok, width), bf16),
        ((key_blocks, BLOCK, 2 * width), bf16),
        ((2 * tok, width), bf16),
        ((blocks,) + probs_shape, bf16),
        ((2, tok, width), bf16),
    ]
    any_space = pl.BlockSpec(memory_space=pl.ANY)
    out_specs = [any_space] * len(shapes)
    out_specs[3] = pl.BlockSpec(memory_space=pltpu.VMEM)
    return pl.pallas_call(
        functools.partial(front_kernel, ctx_size, w_size),
        in_specs=[any_space] * 11,
        out_specs=out_specs,
        out_shape=[jax.ShapeDtypeStruct(shape, dtype) for shape, dtype in shapes],
        scratch_shapes=[
            pltpu.VMEM(w_up.shape, bf16),
            pltpu.VMEM(w_down.shape, bf16),
            pltpu.VMEM(w_out.shape, bf16),
            pltpu.VMEM((chunks, tok, width), bf16),
            pltpu.VMEM((w_size, rows, width), bf16),
            pltpu.VMEM((w_size, rows, 2 * width), bf16),
            pltpu.VMEM((w_size,) + vectors.shape, f32),
            pltpu.VMEM(bias.shape, f32),
            pltpu.VMEM((2 * tok, width), bf16),
            pltpu.VMEM((2 * tok, width), bf16),
            pltpu.VMEM((key_blocks, BLOCK, 2 * width), bf16),
            pltpu.VMEM((keys, 2 * width), bf16),
            pltpu.VMEM((2,) + probs_shape, bf16),
            pltpu.SMEM(ints.shape, ints.dtype),
            pltpu.SemaphoreType.DMA((2,)),
            (
                pltpu.SemaphoreType.DMA((24,)),
                pltpu.SemaphoreType.DMA((64,)),
                pltpu.SemaphoreType.DMA((64,)),
            ),
        ],
        compiler_params=pltpu.CompilerParams(
            collective_id=0, has_side_effects=True, vmem_limit_bytes=56 << 20
        ),
        name="front_all",
    )(hidden, out_grad, ints, bias, vectors, w_query, w_key, w_value, w_out, w_up, w_down)


def make_local(ctx_size, w_size):
    def local(
        hidden,
        out_grad,
        doc_lengths,
        rand_pick,
        w_query,
        w_key,
        w_value,
        w_out,
        w_up,
        w_down,
        b_query,
        b_value,
        b_out,
        b_up,
        b_down,
        ln1_gain,
        ln1_shift,
        ln2_gain,
        ln2_shift,
    ):
        wires = Wires(ctx_size, w_size)
        tok, width = hidden.shape[2], hidden.shape[3]
        ff = w_up.shape[1]
        tok_blocks = tok // BLOCK
        lines, pairs = wires.lines, wires.pairs
        micro = wires.part // 2

        vectors = [b_query, b_value, b_out, b_up, b_down, ln1_gain, ln1_shift, ln2_gain, ln2_shift]
        vector_sizes = [vector.shape[0] for vector in vectors]
        merged = lines == 2 and pairs == 2
        in_chunk = jnp.arange(tok_blocks, dtype=jnp.int32)
        if merged:
            ints, bias = prepare(ctx_size, w_size, doc_lengths, rand_pick)
            flat = jnp.zeros((8 * b_query.shape[0],), f32)
            narrow = [vector for vector in vectors if vector is not b_up]
            for n, vector in enumerate(narrow):
                size = vector.shape[0]
                flat = flat + jnp.pad(vector.astype(f32), (n * size, (7 - n) * size))
            table = lax.dynamic_update_slice(
                jnp.zeros((16, width), f32),
                flat.reshape(8, -1),
                (jnp.int32(0), wires.w * b_query.shape[0]),
            )
            table = lax.dynamic_update_slice(
                table, b_up.astype(f32)[None], (8 + wires.w, jnp.int32(0))
            )
            (
                all_rows,
                grads_dealt,
                ints_dealt,
                vector_table,
                full_query,
                full_kv,
                full_out,
                full_up,
                full_down,
                queries,
                kv,
                context,
                probs,
                own_rows,
            ) = front_all(
                ctx_size,
                w_size,
                hidden,
                out_grad,
                ints,
                bias,
                table,
                (w_query, w_key, w_value, w_out, w_up, w_down),
            )
            bias_out, bias_down, gain_one, shift_one, gain_two, shift_two = [
                vector_table[n] for n in range(2, 8)
            ]
            bias_up = vector_table[8:12].reshape(-1)
        else:
            small_ints = jnp.concatenate(
                [rand_pick.reshape(MICRO, -1), doc_lengths.reshape(MICRO, -1)], axis=1
            )
            int_count = small_ints.shape[1]
            small_ints = jnp.pad(small_ints, ((0, 0), (0, 1024 - int_count))).reshape(MICRO, 8, 128)
            vector_row = vector_sizes[0]
            (
                all_rows,
                grads_dealt,
                ints_dealt,
                vector_table,
                full_query,
                full_kv,
                full_out,
                full_up,
                full_down,
            ) = gather_all(
                ctx_size,
                w_size,
                hidden,
                out_grad,
                small_ints,
                jnp.concatenate(
                    [vector.astype(f32).reshape(-1, vector_row) for vector in vectors], axis=0
                ),
                (w_query, w_key, w_value, w_out, w_up, w_down),
            )
            ints_dealt = ints_dealt.reshape(MICRO, -1)
            spread = []
            at = 0
            for size in vector_sizes:
                count = size // vector_row
                spread.append(vector_table[:, at : at + count].reshape(-1))
                at += count
            (
                bias_query,
                bias_value,
                bias_out,
                bias_up,
                bias_down,
                gain_one,
                shift_one,
                gain_two,
                shift_two,
            ) = spread

            picks = jnp.stack(
                [ints_dealt[turn, : tok_blocks * 3].reshape(tok_blocks, 3) for turn in range(2)]
            ).reshape(-1, 3)
            lengths = ints_dealt[0, tok_blocks * 3 : int_count]
            chunk_ids = [
                (2 * wires.core + (micro + turn) % 2) * lines + wires.line for turn in range(2)
            ]
            my_blocks = jnp.concatenate([chunk * tok_blocks + in_chunk for chunk in chunk_ids])
            safe_blocks, allowed = candidates(my_blocks, lengths, picks)
            chunk = safe_blocks // tok_blocks
            chunk_part, chunk_line = chunk // lines, chunk % lines
            place = (
                ((chunk_part // 2) ^ wires.core) * lines + (chunk_line ^ wires.line)
            ) * 2 + (chunk_part + micro) % 2
            pos = (place * tok_blocks + safe_blocks % tok_blocks).reshape(-1).astype(jnp.int32)
            bias = jnp.repeat(jnp.where(allowed, 0.0, masked_score).astype(f32), BLOCK, axis=1)[:, None]

            queries = ((dot_nn(all_rows.reshape(-1, width)[: 2 * tok], full_query.reshape(-1, width)) + bias_query) * score_scale).astype(bf16)
            kv_bias = jnp.concatenate([jnp.zeros_like(bias_value), bias_value])
            kv = (dot_nn(all_rows.reshape(-1, width), full_kv.reshape(-1, 2 * width)) + kv_bias).astype(bf16)
            context, probs = attend(pos, queries, bias, kv)
        all_rows = all_rows.reshape(-1, width)
        if not merged:
            own_rows = all_rows[: 2 * tok]
        own_rows = own_rows.reshape(-1, width)
        grads_dealt = grads_dealt.reshape(-1, width)
        full_query, full_kv, full_out, full_up, full_down = [
            full.reshape(-1, full.shape[2]) for full in (full_query, full_kv, full_out, full_up, full_down)
        ]
        rows_f32 = own_rows.astype(f32)

        attn_out = dot_nn(context, full_out) + bias_out
        normed, ln1_back = jax.vjp(layer_norm, rows_f32 + attn_out, gain_one, shift_one)
        normed_low = normed.astype(bf16)
        up_pre = dot_nn(normed_low, full_up) + bias_up
        gelu_out, gelu_back = jax.vjp(lambda v: jax.nn.gelu(v, approximate=True), up_pre)
        activated = gelu_out.astype(bf16)
        branch = dot_nn(activated, full_down) + bias_down
        final, ln2_back = jax.vjp(layer_norm, normed + branch, gain_two, shift_two)
        final = final.astype(bf16)

        def term_of(rows_a, rows_b, scale=None):
            term = dot_tn(rows_a, rows_b)
            if scale is not None:
                term = term * scale
            return term.astype(bf16).reshape(pairs, 2, -1, rows_b.shape[1])

        d_mid, grad_gain_two, grad_shift_two = ln2_back(grads_dealt.astype(f32))
        d_branch = d_mid.astype(bf16)
        term_down = term_of(activated, d_branch)
        d_act = dot_nt(d_branch, full_down)
        d_up = gelu_back(d_act)[0].astype(bf16)
        term_up = term_of(normed_low, d_up)
        d_normed = dot_nt(d_up, full_up) + d_mid
        d_sum, grad_gain_one, grad_shift_one = ln1_back(d_normed)
        d_attn = d_sum.astype(bf16)
        term_out = term_of(context, d_attn)
        d_context = dot_nt(d_attn, full_out).astype(bf16)

        def table_of(vectors):
            return jnp.concatenate([vector.reshape(w_size, -1) for vector in vectors], axis=1)

        def column_sums(rows_a):
            return jnp.sum(rows_a.astype(f32), axis=0)

        sums = (
            column_sums(d_attn),
            column_sums(d_up),
            column_sums(d_branch),
            grad_gain_one,
            grad_shift_one,
            grad_gain_two,
            grad_shift_two,
        )
        shard = width // w_size
        if merged:
            table = table_of(sums)
            term_down = term_down.reshape(pairs, 2, -1, shard, width)
            by_block = (-1, BLOCK, width)
            up, down, out_query, key_value, block_out, grad_hidden, table = back_all(
                ctx_size,
                w_size,
                (ints_dealt, table),
                (
                    queries,
                    d_context,
                    d_sum.reshape(by_block),
                    probs,
                    kv,
                    all_rows.reshape(by_block),
                    full_kv.reshape(-1, BLOCK, 2 * width),
                    full_query,
                    final.reshape(2, -1, BLOCK, width),
                    term_up,
                    term_down,
                    term_out,
                ),
                (width, tok, all_rows.shape[0], (8, table.shape[1])),
            )
            row = lax.dynamic_slice(table, (wires.w, jnp.int32(0)), (1, table.shape[1]))[0]
            both = lax.dynamic_slice(
                table, (jnp.int32(w_size), wires.w * shard), (2, shard)
            )
            small = [both[0], both[1]]
            at = 0
            for size in vector_sizes[2:]:
                small.append(row[at : at + size])
                at += size

            return (
                block_out.reshape(2, 1, tok, width),
                grad_hidden.reshape(2, 1, tok, width).astype(f32),
                out_query[1].astype(f32),
                key_value[0].astype(f32),
                key_value[1].astype(f32),
                out_query[0].astype(f32),
                up.astype(f32),
                down.astype(f32),
                *small,
            )

        d_query, d_kv = attend_back(pos, queries, d_context, probs, kv)

        through = dot_nt(d_kv, full_kv).astype(bf16)
        near = d_sum + score_scale * dot_nt(d_query, full_query)
        term_kv = term_of(all_rows, d_kv)
        term_query = term_of(own_rows, d_query, score_scale)

        sums = (score_scale * column_sums(d_query), column_sums(d_kv[:, width:])) + sums
        table = table_of(sums)[:, None]
        term_down = term_down.reshape(pairs, 2, -1, shard, width)
        summed, block_out, grad_hidden, table = finish_all(
            ctx_size,
            w_size,
            (term_up, term_down, term_query, term_kv, term_out),
            ("wide", "tall", "wide", "wide", "wide"),
            through.reshape(-1, tok, width),
            near.reshape(-1, tok, width),
            final.reshape(-1, tok, width),
            table,
        )
        row = lax.dynamic_slice(
            table, (wires.w, jnp.int32(0), jnp.int32(0)), (1, 1, table.shape[2])
        )[0, 0]
        small = []
        at = 0
        for size in vector_sizes:
            small.append(row[at : at + size])
            at += size

        parts = lines // 2
        at = 0

        def wide(columns):
            nonlocal at
            count = columns * parts // width
            pieces = summed[at : at + count].astype(f32)
            at += count
            return jnp.concatenate([pieces[c] for c in range(count)], axis=1)

        grad_up = wide(ff)
        count = ff * parts // width
        grad_down = summed[at : at + count].astype(f32).reshape(-1, parts, shard, width // parts)
        grad_down = jnp.swapaxes(grad_down, 1, 2).reshape(-1, width)
        at += count
        grad_query, grad_key, grad_value, grad_out = [wide(width) for _ in range(4)]
        return (
            block_out[:, None],
            grad_hidden.astype(f32)[:, None],
            grad_query,
            grad_key,
            grad_value,
            grad_out,
            grad_up,
            grad_down,
            *small,
        )

    return local


def solution(mesh):
    tokens = P(None, "wshard", "ctx", None)
    in_specs = (
        tokens,
        tokens,
        P(None, "wshard", None),
        tokens,
        *[P("wshard", None)] * 6,
        *[P("wshard")] * 9,
    )
    out_specs = (tokens, tokens, *[P("wshard", None)] * 6, *[P("wshard")] * 9)
    return jax.shard_map(
        make_local(mesh.shape["ctx"], mesh.shape["wshard"]),
        mesh=mesh,
        in_specs=in_specs,
        out_specs=out_specs,
        check_vma=False,
    )
```
